768 devices in a mesh: dp: 12 (over x, z_hi), tensor: 64 (over y, z_lo, core).
Axes of the slice: x: 4, y: 8, z: 12 (z_hi: 3, z_lo: 4; z = z_hi * 4 + z_lo), core: 2. Of those that a mesh axis runs over, the one named last changes fastest.
Arguments:
- queries: bfloat16 [4608, 8192], P('dp', 'tensor'), may hold values from -180 to 180
- keys: bfloat16 [4608, 1024], P('dp'), may hold values from -4.5 to 4.5
- values: bfloat16 [4608, 1024], P('dp'), may hold values from -6 to 6
- grad_out: bfloat16 [4608, 8192], P('dp', 'tensor'), may hold values from -3 to 3
- weight: float32 [8256, 8192], P('dp', 'tensor'), as said below
- first_code: bfloat16 [8256, 8192], P('dp', 'tensor'), may hold values from -1 to 1, as said below
- first_rows: float32 [8256], P('dp'), may hold values from 0.2 to 5
- first_cols: float32 [8192], P('tensor'), may hold values from 0.2 to 5
- second_code: bfloat16 [8256, 8192], P('dp', 'tensor'), may hold values from 0 to 1, as said below
- second_rows: float32 [8256], P('dp'), may hold values from 0.5 to 20
- second_cols: float32 [8192], P('tensor'), may hold values from 0.5 to 20
Outputs:
- grad_queries: bfloat16 [4608, 8192], P('dp', 'tensor')
- new_weight: float32 [8256, 8192], P('dp', 'tensor')
- next_first_code: bfloat16 [8256, 8192], P('dp', 'tensor')
- next_first_rows: float32 [8256], P('dp')
- next_first_cols: float32 [8192], P('tensor')
- next_second_code: bfloat16 [8256, 8192], P('dp', 'tensor')
- next_second_rows: float32 [8256], P('dp')
- next_second_cols: float32 [8192], P('tensor')
The draws below stay inside these ranges and needn't reach their ends.
Inputs may be any that keep to these rules, and one draw needn't show every extreme that they name: `weight`: rows 8192 onward are zero. `first_code`: rows 8192 onward are zero. `second_code`: rows 8192 onward are zero; all other entries are 0.05 or more.
All inputs are finite; a program needn't handle non-finite values.
Results may differ from the reference program's by a relative error of at most 0.023.
Values may be sent and summed in bfloat16 or wider, within the bound.
A program may use at most 64 MiB of HBM per device.

```python
import math
import jax
import jax.numpy as jnp
from jax import lax

D = 8192
H = 64
KVH = 8
HD = 128
SEQ = 384
TOK = 4608
CPAD = 8256


def paired_draw(key):
    count = TOK // SEQ
    queries = jnp.clip(jax.random.normal(jax.random.fold_in(key, 101), (count, SEQ, H * HD), jnp.float32), -4.5, 4.5)
    keys = jnp.clip(jax.random.normal(jax.random.fold_in(key, 102), (count, SEQ, KVH * HD), jnp.float32), -4.5, 4.5)
    return (queries.reshape(TOK, H * HD), keys.reshape(TOK, KVH * HD))


def draw_queries(key, part):
    return paired_draw(key)[0].astype(jnp.bfloat16)


def draw_keys(key, part):
    return paired_draw(key)[1].astype(jnp.bfloat16)


def real_rows():
    return jnp.arange(CPAD)[:, None] < D


def draw_weight(key, part):
    filled = jax.random.normal(key, (CPAD, H * HD), jnp.float32) * (H * HD) ** (-0.5)
    return jnp.where(real_rows(), filled, 0.0)


def draw_first_code(key, part):
    filled = jax.random.uniform(key, (CPAD, H * HD), jnp.float32, -1.0, 1.0)
    return jnp.where(real_rows(), filled, 0.0).astype(jnp.bfloat16)


def draw_second_code(key, part):
    filled = jax.random.uniform(key, (CPAD, H * HD), jnp.float32, 0.05, 1.0)
    return jnp.where(real_rows(), filled, 0.0).astype(jnp.bfloat16)


def levels(rng, dims, shards, smallest, largest):
    def one(position, parts):
        draws = jax.random.uniform(jax.random.fold_in(jax.random.fold_in(rng, 6), position), (parts,), jnp.float32, smallest / len(shards), largest / len(shards))
        return jnp.repeat(jnp.exp(draws), dims[position] // parts).reshape((-1,) + (1,) * (len(dims) - position - 1))

    loudness = one(*shards[0])
    for cut in shards[1:]:
        loudness = loudness * one(*cut)
    return loudness


def scatter_about(key, dims, spread, most, split=(), dtype=jnp.bfloat16):
    level = levels(key, dims, split, -0.22, 0.18) if split else 1.0
    array = jax.random.normal(key, dims, jnp.float32) * spread * level
    return jnp.minimum(jnp.maximum(array, -most), most).astype(dtype)


def setup_inputs(seed: int = 0) -> dict:
    streams_of = jax.random.split(jax.random.key(seed), 12)
    return {
        "queries": draw_queries(jax.random.fold_in(streams_of[11], 71), 0),
        "keys": draw_keys(jax.random.fold_in(streams_of[11], 71), 0),
        "values": scatter_about(streams_of[2], (TOK, KVH * HD), 1.0, 6.0, ((0, 12),)),
        "grad_out": scatter_about(streams_of[3], (TOK, D), 0.5, 3.0, ((0, 12), (1, 64))),
        "weight": draw_weight(jax.random.fold_in(streams_of[11], 71), 0),
        "first_code": draw_first_code(jax.random.fold_in(streams_of[11], 71), 0),
        "first_rows": jnp.clip(jnp.exp(math.log(5.0) - 3.218876 * jax.random.uniform(streams_of[6], (CPAD,), jnp.float32) ** levels(streams_of[6], (CPAD,), ((0, 12),), -0.2, 0.2)), 0.2, 5.0),
        "first_cols": jnp.clip(jnp.exp(math.log(5.0) - 3.218876 * jax.random.uniform(streams_of[7], (H * HD,), jnp.float32) ** levels(streams_of[7], (H * HD,), ((0, 64),), -0.2, 0.2)), 0.2, 5.0),
        "second_code": draw_second_code(jax.random.fold_in(streams_of[11], 71), 0),
        "second_rows": jnp.clip(jnp.exp(math.log(20.0) - 3.6888795 * jax.random.uniform(streams_of[9], (CPAD,), jnp.float32) ** levels(streams_of[9], (CPAD,), ((0, 12),), -0.2, 0.2)), 0.5, 20.0),
        "second_cols": jnp.clip(jnp.exp(math.log(20.0) - 3.6888795 * jax.random.uniform(streams_of[10], (H * HD,), jnp.float32) ** levels(streams_of[10], (H * HD,), ((0, 64),), -0.2, 0.2)), 0.5, 20.0),
    }


beta_first = 0.9
beta_second = 0.95
learning = 0.01
decay_rate = 0.1
adam_eps = 1e-08
code_eps = 1e-06
correct_first = 1.0 - 0.9 ** 10
correct_second = 1.0 - 0.95 ** 10

def reference(queries, keys, values, grad_out, weight, first_code, first_rows, first_cols, second_code, second_rows, second_cols):
    count = queries.shape[0] // SEQ
    group = H // KVH
    factor = HD ** (-0.5)
    weight_half = weight.astype(jnp.bfloat16)
    grad_att = jnp.dot(grad_out, weight_half[:D], preferred_element_type=jnp.float32)
    grad_half = grad_att.astype(jnp.bfloat16)
    future = jnp.arange(SEQ)[None, :] > jnp.arange(SEQ)[:, None]

    def per_sequence(inputs):
        query_block, key_block, value_block, grad_block = inputs
        query_heads = query_block.reshape(SEQ, H, HD).astype(jnp.float32)
        key_heads = jnp.repeat(key_block.reshape(SEQ, KVH, HD), group, axis=1).astype(jnp.float32)
        value_heads = jnp.repeat(value_block.reshape(SEQ, KVH, HD), group, axis=1).astype(jnp.float32)
        scores = jnp.einsum('qhd,khd->hqk', query_heads, key_heads) * factor
        scores = jnp.where(future[None], -1e+30, scores)
        highest = lax.optimization_barrier(jnp.max(scores, axis=-1, keepdims=True))
        exponent = jnp.exp(scores - highest)
        probabilities = exponent / lax.optimization_barrier(jnp.sum(exponent, axis=-1, keepdims=True))
        weights_half = probabilities.astype(jnp.bfloat16)
        attended = jnp.einsum('hqk,khd->qhd', weights_half.astype(jnp.float32), value_heads).astype(jnp.bfloat16)
        grad_heads = grad_block.reshape(SEQ, H, HD).astype(jnp.float32)
        grad_probs = jnp.einsum('qhd,khd->hqk', grad_heads, value_heads)
        row_dot = lax.optimization_barrier(jnp.sum(grad_heads * attended.astype(jnp.float32), axis=-1))
        grad_scores = (probabilities * (grad_probs - row_dot.T[:, :, None])).astype(jnp.bfloat16)
        grad_query = (jnp.einsum('hqk,khd->qhd', grad_scores.astype(jnp.float32), key_heads) * factor).astype(jnp.bfloat16)
        return (grad_query.reshape(SEQ, H * HD), attended.reshape(SEQ, H * HD))
    grad_queries, attended = lax.map(per_sequence, (queries.reshape(count, SEQ, H * HD), keys.reshape(count, SEQ, KVH * HD), values.reshape(count, SEQ, KVH * HD), grad_half.reshape(count, SEQ, H * HD)))

    def accumulate(total, inputs):
        grad_block, att_block = inputs
        term = jnp.dot(grad_block.T, att_block, preferred_element_type=jnp.float32)
        return (total + lax.optimization_barrier(term.astype(jnp.bfloat16)).astype(jnp.float32), 0)
    weight_grad, unused = lax.scan(accumulate, jnp.zeros((D, H * HD), jnp.float32), (grad_out.reshape(count, SEQ, D), attended))
    weight_grad = jnp.pad(weight_grad, ((0, CPAD - D), (0, 0)))
    first = first_code.astype(jnp.float32) * jnp.minimum(first_rows[:, None], first_cols[None, :])
    second = second_code.astype(jnp.float32) * jnp.minimum(second_rows[:, None], second_cols[None, :])
    first_new = beta_first * first + (1.0 - beta_first) * weight_grad
    second_new = beta_second * second + (1.0 - beta_second) * weight_grad * weight_grad
    step_size = first_new / correct_first / (jnp.sqrt(second_new / correct_second) + adam_eps)
    new_weight = weight - learning * (step_size + decay_rate * weight)
    first_abs = jnp.abs(first_new)
    second_abs = jnp.abs(second_new)
    next_first_rows = lax.optimization_barrier(jnp.max(first_abs, axis=1))
    next_first_cols = lax.optimization_barrier(jnp.max(first_abs, axis=0))
    next_second_rows = lax.optimization_barrier(jnp.max(second_abs, axis=1))
    next_second_cols = lax.optimization_barrier(jnp.max(second_abs, axis=0))
    next_first_code = (first_new / (jnp.minimum(next_first_rows[:, None], next_first_cols[None, :]) + code_eps)).astype(jnp.bfloat16)
    next_second_code = (second_new / (jnp.minimum(next_second_rows[:, None], next_second_cols[None, :]) + code_eps)).astype(jnp.bfloat16)
    return (grad_queries.reshape(count * SEQ, H * HD), new_weight, next_first_code, next_first_rows, next_first_cols, next_second_code, next_second_rows, next_second_cols)
```

```python
import functools

import jax
import jax.numpy as jnp
from jax import lax
from jax.experimental import pallas as pl
from jax.experimental.pallas import tpu as pltpu
from jax.sharding import Mesh
from jax.sharding import PartitionSpec as P

NX, NZH, NY, NZL, NC = 4, 3, 8, 4, 2
AXES = ("x", "zh", "y", "zl", "core")
DP = ("x", "zh")
TENSOR = ("y", "zl", "core")
MESH = pl.DeviceIdType.MESH

HD = 128
SEQ = 384
ROWS = 688
UNIT = 16
UNITS = ROWS // UNIT
ALL_UNITS = 512
QUART = 11
QROWS = QUART * UNIT
PADROWS = 4 * QROWS
SCALE = HD ** (-0.5)

beta_first = 0.9
beta_second = 0.95
learning = 0.01
decay_rate = 0.1
adam_eps = 1e-08
code_eps = 1e-06
correct_first = 1.0 - 0.9**10
correct_second = 1.0 - 0.95**10

F32 = jnp.float32
BF16 = jnp.bfloat16
NT = (((1,), (1,)), ((), ()))


def mod(a, n):
    return lax.rem(a + n, n)


def row_chunks():
    return [(c, 128 * c, min(128, ROWS - 128 * c)) for c in range(6)]


def lane_rows(values):
    highest = jnp.max(values, axis=1, keepdims=True)
    out = []
    for c, start, size in row_chunks():
        eye = lax.broadcasted_iota(jnp.int32, (size, 128), 0) == lax.broadcasted_iota(
            jnp.int32, (size, 128), 1
        )
        out.append(
            jnp.max(jnp.where(eye, highest[start : start + size], 0.0), axis=0, keepdims=True)
        )
    out.append(jnp.zeros((2, 128), F32))
    return jnp.concatenate(out, axis=0)


def down_rows(row):
    return jnp.broadcast_to(row, (128, 128)).T


def body(
    q_hbm,
    k_hbm,
    v_hbm,
    g_hbm,
    w_hbm,
    fc_hbm,
    frow,
    fcol,
    sc_hbm,
    srow,
    scol,
    gq_out,
    nw_out,
    nfc_out,
    nfr_out,
    nfcol_out,
    nsc_out,
    nsr_out,
    nscol_out,
    q,
    kk,
    vv,
    g,
    w,
    fc,
    sc,
    gt,
    gz,
    wt,
    att,
    prob,
    acct,
    ga_stage,
    ga_in,
    dwacc,
    dw_stage,
    dw_in,
    fnew,
    snew,
    st,
    st_in,
    y_in,
    zl_in,
    mine,
    fin,
    cst,
    c_in,
    in_sem,
    r_send,
    r_recv,
    ring_send,
    ring_recv,
    d_send,
    d_recv,
    att_send,
    att_recv,
    w_send,
    w_recv,
    ga_send,
    ga_recv,
    dw_send,
    dw_recv,
    core_send,
    core_recv,
    y_send,
    y_recv,
    zl_send,
    zl_recv,
    c_send,
    c_recv,
):
    x, zh, y, zl, k = (lax.axis_index(a) for a in AXES)
    t = 8 * y + 2 * zl + k
    pair = lax.div(y, 2)

    def rcopy(src, dst, send, recv, **dev):
        return pltpu.make_async_remote_copy(
            src_ref=src, dst_ref=dst, send_sem=send, recv_sem=recv, device_id=dev, device_id_type=MESH
        )

    heads = pl.ds(pl.multiple_of(y * HD, HD), HD)
    loads = [
        pltpu.make_async_copy(src, dst, in_sem.at[i])
        for i, (src, dst) in enumerate(
            [
                (g_hbm, g),
                (q_hbm, q),
                (k_hbm.at[:, heads], kk),
                (v_hbm.at[:, heads], vv),
                (w_hbm, w),
                (fc_hbm, fc),
                (sc_hbm, sc),
            ]
        )
    ]
    for load in loads:
        load.start()

    barrier = pltpu.get_barrier_semaphore()

    def greet(i, carry):
        dy = lax.div(i, 24)
        rest = lax.rem(i, 24)
        oz = lax.div(rest, 8)
        ol = lax.div(lax.rem(rest, 8), 2)
        ok = lax.rem(rest, 2)
        ny = mod(y + dy - 1, NY)

        @pl.when(jnp.logical_not((ny == y) & (oz == zh) & (ol == zl) & (ok == k)))
        def _():
            pl.semaphore_signal(
                barrier, inc=1, device_id={"zh": oz, "y": ny, "zl": ol, "core": ok}, device_id_type=MESH
            )

        return carry

    lax.fori_loop(0, 72, greet, 0)
    for dy in range(2, 7):
        pl.semaphore_signal(barrier, inc=1, device_id={"y": mod(y + dy, NY)}, device_id_type=MESH)
    for dx in range(1, NX):
        for dz in range(NZH):
            pl.semaphore_signal(
                barrier,
                inc=1,
                device_id={"x": mod(x + dx, NX), "zh": mod(zh + dz, NZH)},
                device_id_type=MESH,
            )

    loads[0].wait()
    gt[...] = g[...].T

    my_d = 3 * pair + zh
    my_q = 2 * lax.rem(y, 2) + k
    for i in range(QUART):
        r = QUART * my_q + i

        @pl.when((r >= UNITS) | (UNITS * my_d + r >= ALL_UNITS))
        def _():
            for jj in range(NZH):
                gz[jj, pair, pl.ds(pl.multiple_of(UNIT * r, UNIT), UNIT), :] = jnp.zeros(
                    (UNIT, SEQ), BF16
                )

    for i in (1, 2, 3):
        loads[i].wait()
    for i in range(3):
        rows, cols = pl.ds(128 * i, 128), pl.ds(0, 128 * (i + 1))
        scores = (
            lax.dot_general(q[rows, :], kk[cols, :], NT, preferred_element_type=F32) * SCALE
        )
        future = lax.broadcasted_iota(jnp.int32, scores.shape, 1) > (
            lax.broadcasted_iota(jnp.int32, scores.shape, 0) + 128 * i
        )
        scores = jnp.where(future, -1e30, scores)
        exponent = jnp.exp(scores - jnp.max(scores, axis=-1, keepdims=True))
        probabilities = exponent / jnp.sum(exponent, axis=-1, keepdims=True)
        prob[rows, cols] = probabilities
        att[0, rows, :] = jnp.dot(
            probabilities.astype(BF16), vv[cols, :], preferred_element_type=F32
        ).astype(BF16)

    loads[4].wait()
    wt[x] = w[...].astype(BF16).T

    pl.semaphore_wait(barrier, 71 + 5 + 9)

    def spread(u, carry):
        unit = 8 * t + u
        d = lax.div(unit, UNITS)
        r = unit - UNITS * d
        quarter = lax.div(r, QUART)
        i = r - QUART * quarter
        zd = lax.rem(d, NZH)
        xd = lax.div(d, NZH)
        yd = 2 * xd + lax.div(quarter, 2)
        kd = lax.rem(quarter, 2)
        jj = mod(zh - zd, NZH)
        src = gt.at[pl.ds(pl.multiple_of(UNIT * u, UNIT), UNIT), :]
        place = pl.ds(pl.multiple_of(UNIT * r, UNIT), UNIT)
        home = (zd == zh) & (yd == y) & (kd == k)

        @pl.when(home)
        def _():
            gz[0, xd, place, :] = gt[pl.ds(pl.multiple_of(UNIT * u, UNIT), UNIT), :]

        for o in range(NZL):
            copy = rcopy(
                src,
                gz.at[jj, xd, place, :],
                r_send.at[u, o],
                r_recv.at[jj, i],
                zh=zd,
                y=yd,
                zl=mod(zl + o, NZL),
                core=kd,
            )
            if o == 0:
                pl.when(jnp.logical_not(home))(copy.start)
            else:
                copy.start()
        return carry

    lax.fori_loop(0, 8, spread, 0)

    sends = []
    for dz in (1, 2):
        copy = rcopy(
            att.at[0], att.at[NZH - dz], att_send.at[dz - 1], att_recv.at[NZH - dz - 1], zh=mod(zh + dz, NZH)
        )
        copy.start()
        sends.append(copy)
    for dx in (1, 3, 2):
        copy = rcopy(wt.at[x], wt.at[x], w_send.at[dx - 1], w_recv.at[NX - dx - 1], x=mod(x + dx, NX))
        copy.start()
        sends.append(copy)

    def home_ready(jj):
        def one(i, carry):
            r = QUART * my_q + i
            unit = UNITS * my_d + r
            own = lax.div(unit, 8) == t
            there = (r < UNITS) & (unit < ALL_UNITS)
            if jj == 0:
                there = there & jnp.logical_not(own)

            @pl.when(there)
            def _():
                piece = gz.at[jj, pair, pl.ds(pl.multiple_of(UNIT * r, UNIT), UNIT), :]
                rcopy(piece, piece, r_send.at[0, 0], r_recv.at[jj, i], core=k).wait_recv()

            return carry

        lax.fori_loop(0, QUART, one, 0)

    HALF = 96

    def part(jj, source, r):
        quarter = 2 * lax.rem(source, 2) + k
        start, size = 0, QROWS
        if jj == 2 and r[1] == 4:
            start, size = (0, HALF) if r[0] == 0 else (HALF, QROWS - HALF)
        return gz.at[
            jj, lax.div(source, 2), pl.ds(pl.multiple_of(QROWS * quarter + start, UNIT), size), :
        ]

    def from_source(way, hops):
        return mod(y - hops, NY) if way == 0 else mod(y + hops, NY)

    def forward(way, jj, hops):
        piece = part(jj, from_source(way, hops), (way, hops + 1))
        copy = rcopy(
            piece,
            piece,
            ring_send.at[way, jj, hops],
            ring_recv.at[way, jj, hops],
            y=mod(y + 1, NY) if way == 0 else mod(y - 1, NY),
        )
        copy.start()
        sends.append(copy)

    def arrived(way, jj, hops):
        piece = part(jj, from_source(way, hops), (way, hops))
        rcopy(
            piece, piece, ring_send.at[way, jj, hops - 1], ring_recv.at[way, jj, hops - 1], y=y
        ).wait_recv()

    def to_partner(way, jj, hops):
        piece = part(jj, from_source(way, hops), (way, hops))
        copy = rcopy(piece, piece, d_send.at[way, jj, hops], d_recv.at[way, jj, hops], core=1 - k)
        copy.start()
        sends.append(copy)

    def from_partner(way, jj, hops):
        source = from_source(way, hops)
        quarter = 2 * lax.rem(source, 2) + (1 - k)
        start, size = 0, QROWS
        if jj == 2 and hops == 4:
            start, size = (0, HALF) if way == 0 else (HALF, QROWS - HALF)
        piece = gz.at[
            jj, lax.div(source, 2), pl.ds(pl.multiple_of(QROWS * quarter + start, UNIT), size), :
        ]
        rcopy(
            piece, piece, d_send.at[way, jj, hops], d_recv.at[way, jj, hops], core=1 - k
        ).wait_recv()

    reach = {(0, 0): 4, (1, 0): 3, (0, 1): 3, (1, 1): 4, (0, 2): 4, (1, 2): 4}

    def start_ring(jj):
        home_ready(jj)
        forward(0, jj, 0)
        forward(1, jj, 0)
        to_partner(0, jj, 0)

    def pass_on(jj, hops):
        for way in (0, 1):
            if hops <= reach[way, jj]:
                arrived(way, jj, hops)
                if hops < reach[way, jj]:
                    forward(way, jj, hops)
                to_partner(way, jj, hops)

    def partner_has(jj, hops):
        for way in (0, 1):
            if hops == 0 and way == 1:
                continue
            if hops <= reach[way, jj]:
                from_partner(way, jj, hops)

    def multiply(jj, xo):
        block = gz[jj, xo, 0:ROWS, :]
        term = jnp.dot(wt[xo], block, preferred_element_type=F32)
        acct[jj] = term if jj not in started else acct[jj] + term
        started.add(jj)

    def weight_term(jj, xo):
        term = jnp.dot(gz[jj, xo, 0:ROWS, :], att[jj], preferred_element_type=F32)
        if jj == 0:
            dwacc[xo] = term
        else:
            dwacc[xo] = dwacc[xo] + term

    started = set()

    def xo_of(off):
        return mod(pair + off, NX)

    start_ring(0)
    pass_on(0, 1)
    start_ring(1)
    pass_on(0, 2)
    pass_on(1, 1)
    start_ring(2)
    for dx in (1, 2, 3):
        rcopy(wt.at[0], wt.at[mod(x + dx, NX)], w_send.at[0], w_recv.at[dx - 1], x=x).wait_recv()
    pass_on(0, 3)
    pass_on(1, 2)
    partner_has(0, 0)
    partner_has(0, 1)
    multiply(0, xo_of(0))
    weight_term(0, xo_of(0))
    pass_on(2, 1)
    pass_on(0, 4)
    partner_has(0, 2)
    partner_has(0, 3)
    multiply(0, xo_of(1))
    weight_term(0, xo_of(1))
    pass_on(1, 3)
    multiply(0, xo_of(3))
    weight_term(0, xo_of(3))
    pass_on(2, 2)
    partner_has(0, 4)
    multiply(0, xo_of(2))
    weight_term(0, xo_of(2))
    pass_on(1, 4)
    for dz in (1, 2):
        rcopy(att.at[0], att.at[dz], att_send.at[0], att_recv.at[dz - 1], zh=zh).wait_recv()
    for hops in range(5):
        partner_has(1, hops)
    for off in (0, 1, 3, 2):
        multiply(1, xo_of(off))
        weight_term(1, xo_of(off))

    def send_grad(jj):
        ga_stage[jj - 1] = acct[jj].astype(BF16)
        copy = rcopy(
            ga_stage.at[jj - 1],
            ga_in.at[NZH - jj - 1],
            ga_send.at[jj - 1],
            ga_recv.at[NZH - jj - 1],
            zh=mod(zh + jj, NZH),
        )
        copy.start()
        sends.append(copy)

    def send_term(off):
        xo = xo_of(off)

        @pl.when(xo != x)
        def _():
            dw_stage[xo] = dwacc[xo].astype(BF16)
            rcopy(
                dw_stage.at[xo],
                dw_in.at[mod(x - xo, NX) - 1],
                dw_send.at[xo],
                dw_recv.at[mod(x - xo, NX) - 1],
                x=xo,
            ).start()

    send_grad(1)
    pass_on(2, 3)
    partner_has(2, 0)
    partner_has(2, 1)
    weight_term(2, xo_of(0))
    send_term(0)
    partner_has(2, 2)
    partner_has(2, 3)
    for off in (1, 3):
        weight_term(2, xo_of(off))
        send_term(off)
    pass_on(2, 4)
    partner_has(2, 4)
    weight_term(2, xo_of(2))
    send_term(2)
    for off in (0, 1, 3, 2):
        multiply(2, xo_of(off))
    send_grad(2)

    for i in (5, 6):
        loads[i].wait()
    for dx in (1, 2, 3):
        rcopy(dw_stage.at[0], dw_in.at[dx - 1], dw_send.at[0], dw_recv.at[dx - 1], x=x).wait_recv()
    for c, start, size in row_chunks():
        rows = pl.ds(start, size)
        grad = (
            (dwacc[x, rows, :] + dw_in[0, rows, :].astype(F32))
            + dw_in[1, rows, :].astype(F32)
            + dw_in[2, rows, :].astype(F32)
        )
        tile = pl.ds(128 * c, size)
        low_first = jnp.minimum(
            down_rows(frow[0:1, 128 * c : 128 * c + 128])[:size] if size == 128
            else down_rows(jnp.concatenate([frow[0:1, tile], jnp.zeros((1, 128 - size), F32)], axis=1))[:size],
            fcol[...],
        )
        low_second = jnp.minimum(
            down_rows(srow[0:1, 128 * c : 128 * c + 128])[:size] if size == 128
            else down_rows(jnp.concatenate([srow[0:1, tile], jnp.zeros((1, 128 - size), F32)], axis=1))[:size],
            scol[...],
        )
        first = fc[rows, :].astype(F32) * low_first
        second = sc[rows, :].astype(F32) * low_second
        first_new = beta_first * first + (1.0 - beta_first) * grad
        second_new = beta_second * second + (1.0 - beta_second) * grad * grad
        step_size = first_new / correct_first / (jnp.sqrt(second_new / correct_second) + adam_eps)
        weight = w[rows, :]
        nw_out[rows, :] = weight - learning * (step_size + decay_rate * weight)
        fnew[rows, :] = first_new
        snew[rows, :] = second_new

    first_abs, second_abs = jnp.abs(fnew[...]), jnp.abs(snew[...])
    st[0] = lane_rows(first_abs)
    st[1] = lane_rows(second_abs)
    cst[0:1, :] = jnp.max(first_abs, axis=0, keepdims=True)
    cst[1:2, :] = jnp.max(second_abs, axis=0, keepdims=True)

    copy = rcopy(st.at[1 - k], st_in, core_send.at[0], core_recv.at[0], core=1 - k)
    copy.start()
    sends.append(copy)
    for rel in range(1, NX * NZH):
        dx, dz = rel // NZH, rel % NZH
        back = ((NX - dx) % NX) * NZH + (NZH - dz) % NZH
        copy = rcopy(
            cst,
            c_in.at[back - 1],
            c_send.at[rel - 1],
            c_recv.at[back - 1],
            x=mod(x + dx, NX),
            zh=mod(zh + dz, NZH),
        )
        copy.start()
        sends.append(copy)
    rcopy(st.at[0], st_in, core_send.at[0], core_recv.at[0], core=k).wait_recv()
    mine[0] = jnp.maximum(st[k], st_in[...])
    for dy in range(1, NY):
        copy = rcopy(
            mine.at[0], y_in.at[NY - dy - 1], y_send.at[dy - 1], y_recv.at[NY - dy - 1], y=mod(y + dy, NY)
        )
        copy.start()
        sends.append(copy)

    def back_rows(i):
        rows, cols = pl.ds(128 * i, 128), pl.ds(0, 128 * (i + 1))
        total = acct[0, :, rows]
        for s in range(2):
            total = total + ga_in[s, :, rows].astype(F32)
        grad_half = total.astype(BF16).T
        grad_probs = lax.dot_general(grad_half, vv[cols, :], NT, preferred_element_type=F32)
        row_dot = jnp.sum(
            grad_half.astype(F32) * att[0, rows, :].astype(F32), axis=-1, keepdims=True
        )
        grad_scores = (prob[rows, cols] * (grad_probs - row_dot)).astype(BF16)
        gq_out[rows, :] = (
            jnp.dot(grad_scores, kk[cols, :], preferred_element_type=F32) * SCALE
        ).astype(BF16)

    for s in range(2):
        rcopy(ga_stage.at[0], ga_in.at[s], ga_send.at[0], ga_recv.at[s], zh=zh).wait_recv()
    back_rows(0)
    back_rows(1)

    for dy in range(1, NY):
        rcopy(mine.at[0], y_in.at[dy - 1], y_send.at[0], y_recv.at[dy - 1], y=y).wait_recv()
    mine[1] = jnp.maximum(mine[0], jnp.max(y_in[...], axis=0))
    for dl in range(1, NZL):
        copy = rcopy(
            mine.at[1],
            zl_in.at[NZL - dl - 1],
            zl_send.at[dl - 1],
            zl_recv.at[NZL - dl - 1],
            zl=mod(zl + dl, NZL),
        )
        copy.start()
        sends.append(copy)
    back_rows(2)
    for rel in range(1, NX * NZH):
        rcopy(cst, c_in.at[rel - 1], c_send.at[0], c_recv.at[rel - 1], x=x).wait_recv()
    cols_max = jnp.maximum(cst[...], jnp.max(c_in[...], axis=0))
    nfcol_out[...] = cols_max[0:1]
    nscol_out[...] = cols_max[1:2]
    for dl in range(1, NZL):
        rcopy(mine.at[1], zl_in.at[dl - 1], zl_send.at[0], zl_recv.at[dl - 1], zl=zl).wait_recv()
    fin[k] = jnp.maximum(mine[1], jnp.max(zl_in[...], axis=0))
    copy = rcopy(fin.at[k], fin.at[k], core_send.at[1], core_recv.at[1], core=1 - k)
    copy.start()
    sends.append(copy)
    rcopy(fin.at[k], fin.at[1 - k], core_send.at[1], core_recv.at[1], core=k).wait_recv()

    for c, start, size in row_chunks():
        rows = pl.ds(start, size)
        nfr_out[0:1, start : start + size] = fin[0, c : c + 1, 0:size]
        nsr_out[0:1, start : start + size] = fin[1, c : c + 1, 0:size]
        low_first = jnp.minimum(down_rows(fin[0, c : c + 1, :])[:size], cols_max[0:1])
        low_second = jnp.minimum(down_rows(fin[1, c : c + 1, :])[:size], cols_max[1:2])
        nfc_out[rows, :] = (fnew[rows, :] / (low_first + code_eps)).astype(BF16)
        nsc_out[rows, :] = (snew[rows, :] / (low_second + code_eps)).astype(BF16)

    def drain(u, carry):
        unit = 8 * t + u
        d = lax.div(unit, UNITS)
        quarter = lax.div(unit - UNITS * d, QUART)
        home = (
            (lax.rem(d, NZH) == zh)
            & (2 * lax.div(d, NZH) + lax.div(quarter, 2) == y)
            & (lax.rem(quarter, 2) == k)
        )
        src = gt.at[pl.ds(pl.multiple_of(UNIT * u, UNIT), UNIT), :]
        for o in range(NZL):
            copy = rcopy(src, src, r_send.at[u, o], r_recv.at[0, 0], core=k)
            if o == 0:
                pl.when(jnp.logical_not(home))(copy.wait_send)
            else:
                copy.wait_send()
        return carry

    lax.fori_loop(0, 8, drain, 0)
    for copy in sends:
        copy.wait_send()
    for xo in range(NX):

        @pl.when(xo != x)
        def _():
            rcopy(dw_stage.at[xo], dw_in.at[0], dw_send.at[xo], dw_recv.at[0], x=x).wait_send()


def per_device(queries, keys, values, grad_out, weight, fc, frow, fcol, sc, srow, scol):
    shape = jax.ShapeDtypeStruct
    vmem = pl.BlockSpec(memory_space=pltpu.VMEM)
    anywhere = pl.BlockSpec(memory_space=pl.ANY)
    dma = pltpu.SemaphoreType.DMA
    outs = pl.pallas_call(
        body,
        name="whole",
        out_shape=(
            shape((SEQ, HD), BF16),
            shape((ROWS, HD), F32),
            shape((ROWS, HD), BF16),
            shape((1, ROWS), F32),
            shape((1, HD), F32),
            shape((ROWS, HD), BF16),
            shape((1, ROWS), F32),
            shape((1, HD), F32),
        ),
        in_specs=[anywhere] * 6 + [vmem, vmem, anywhere, vmem, vmem],
        out_specs=[vmem] * 8,
        scratch_shapes=[
            pltpu.VMEM((SEQ, HD), BF16),
            pltpu.VMEM((SEQ, HD), BF16),
            pltpu.VMEM((SEQ, HD), BF16),
            pltpu.VMEM((SEQ, HD), BF16),
            pltpu.VMEM((ROWS, HD), F32),
            pltpu.VMEM((ROWS, HD), BF16),
            pltpu.VMEM((ROWS, HD), BF16),
            pltpu.VMEM((HD, SEQ), BF16),
            pltpu.VMEM((NZH, NX, PADROWS, SEQ), BF16),
            pltpu.VMEM((NX, HD, ROWS), BF16),
            pltpu.VMEM((NZH, SEQ, HD), BF16),
            pltpu.VMEM((SEQ, SEQ), F32),
            pltpu.VMEM((NZH, HD, SEQ), F32),
            pltpu.VMEM((2, HD, SEQ), BF16),
            pltpu.VMEM((2, HD, SEQ), BF16),
            pltpu.VMEM((NX, ROWS, HD), F32),
            pltpu.VMEM((NX, ROWS, HD), BF16),
            pltpu.VMEM((NX - 1, ROWS, HD), BF16),
            pltpu.VMEM((ROWS, HD), F32),
            pltpu.VMEM((ROWS, HD), F32),
            pltpu.VMEM((2, 8, HD), F32),
            pltpu.VMEM((8, HD), F32),
            pltpu.VMEM((NY - 1, 8, HD), F32),
            pltpu.VMEM((NZL - 1, 8, HD), F32),
            pltpu.VMEM((2, 8, HD), F32),
            pltpu.VMEM((2, 8, HD), F32),
            pltpu.VMEM((2, HD), F32),
            pltpu.VMEM((NX * NZH - 1, 2, HD), F32),
            dma((7,)),
            dma((8, NZL)),
            dma((NZH, QUART)),
            dma((2, NZH, 4)),
            dma((2, NZH, 4)),
            dma((2, NZH, 5)),
            dma((2, NZH, 5)),
            dma((2,)),
            dma((2,)),
            dma((3,)),
            dma((3,)),
            dma((2,)),
            dma((2,)),
            dma((NX,)),
            dma((3,)),
            dma((2,)),
            dma((2,)),
            dma((NY - 1,)),
            dma((NY - 1,)),
            dma((NZL - 1,)),
            dma((NZL - 1,)),
            dma((NX * NZH - 1,)),
            dma((NX * NZH - 1,)),
        ],
        compiler_params=pltpu.CompilerParams(
            collective_id=0, has_side_effects=True, vmem_limit_bytes=48 * 1024 * 1024
        ),
    )(
        queries,
        keys,
        values,
        grad_out,
        weight,
        fc,
        frow.reshape(1, ROWS),
        fcol.reshape(1, HD),
        sc,
        srow.reshape(1, ROWS),
        scol.reshape(1, HD),
    )
    gq, nw, nfc, nfr, nfcol, nsc, nsr, nscol = outs
    return (
        gq,
        nw,
        nfc,
        nfr.reshape(ROWS),
        nfcol.reshape(HD),
        nsc,
        nsr.reshape(ROWS),
        nscol.reshape(HD),
    )


def solution(mesh):
    finer = Mesh(mesh.devices.reshape(NX, NZH, NY, NZL, NC), AXES)
    placed = (
        P(DP, TENSOR),
        P(DP, None),
        P(DP, None),
        P(DP, TENSOR),
        P(DP, TENSOR),
        P(DP, TENSOR),
        P(DP),
        P(TENSOR),
        P(DP, TENSOR),
        P(DP),
        P(TENSOR),
    )
    return jax.shard_map(
        per_device,
        mesh=finer,
        in_specs=placed,
        out_specs=(
            P(DP, TENSOR),
            P(DP, TENSOR),
            P(DP, TENSOR),
            P(DP),
            P(TENSOR),
            P(DP, TENSOR),
            P(DP),
            P(TENSOR),
        ),
        check_vma=False,
    )
```

```python
import functools

import jax
import jax.numpy as jnp
from jax import lax
from jax.experimental import pallas as pl
from jax.experimental.pallas import tpu as pltpu
from jax.sharding import Mesh
from jax.sharding import PartitionSpec as P

NX, NZH, NY, NZL, NC = 4, 3, 8, 4, 2
AXES = ("x", "zh", "y", "zl", "core")
DP = ("x", "zh")
TENSOR = ("y", "zl", "core")
MESH = pl.DeviceIdType.MESH

HD = 128
SEQ = 384
ROWS = 688
UNIT = 16
UNITS = ROWS // UNIT
ALL_UNITS = 512
QUART = 11
QROWS = QUART * UNIT
PADROWS = 4 * QROWS
HALF_ROWS = 2 * QROWS
SCALE = HD ** (-0.5)

beta_first = 0.9
beta_second = 0.95
learning = 0.01
decay_rate = 0.1
adam_eps = 1e-08
code_eps = 1e-06
correct_first = 1.0 - 0.9**10
correct_second = 1.0 - 0.95**10

F32 = jnp.float32
BF16 = jnp.bfloat16
NT = (((1,), (1,)), ((), ()))


def mod(a, n):
    return lax.rem(a + n, n)


def row_chunks():
    return [(c, 128 * c, min(128, ROWS - 128 * c)) for c in range(6)]


def lane_rows(values):
    highest = jnp.max(values, axis=1, keepdims=True)
    out = []
    for c, start, size in row_chunks():
        eye = lax.broadcasted_iota(jnp.int32, (size, 128), 0) == lax.broadcasted_iota(
            jnp.int32, (size, 128), 1
        )
        out.append(
            jnp.max(jnp.where(eye, highest[start : start + size], 0.0), axis=0, keepdims=True)
        )
    out.append(jnp.zeros((2, 128), F32))
    return jnp.concatenate(out, axis=0)


def down(vector, start, size):
    row = vector[pl.ds(start, size)].reshape(1, size)
    if size < 128:
        row = jnp.concatenate([row, jnp.zeros((1, 128 - size), F32)], axis=1)
    return down_rows(row)[:size]


def down_rows(row):
    return jnp.broadcast_to(row, (128, 128)).T


def body(
    q_hbm,
    k_hbm,
    v_hbm,
    g_hbm,
    w_hbm,
    fc_hbm,
    frow_hbm,
    fcol_hbm,
    sc_hbm,
    srow_hbm,
    scol_hbm,
    gq_out,
    nw_out,
    fnew_out,
    snew_out,
    rows_out,
    cols_out,
    q,
    kk,
    vv,
    g,
    w,
    fc,
    sc,
    frow,
    fcol,
    srow,
    scol,
    gt,
    gz,
    wt,
    att,
    prob,
    acct,
    ga_stage,
    ga_in,
    dwacc,
    dw_stage,
    dw_in,
    st,
    y_in,
    zl_in,
    mine,
    cst,
    x_in,
    zh_in,
    in_sem,
    r_send,
    r_recv,
    up_send,
    down_send,
    ring_send,
    ring_recv,
    d_send,
    d_recv,
    att_send,
    att_recv,
    w_send,
    w_recv,
    ga_send,
    ga_recv,
    dw_send,
    dw_recv,
    y_send,
    y_recv,
    zl_send,
    zl_recv,
    x_send,
    x_recv,
    zh_send,
    zh_recv,
):
    x, zh, y, zl, k = (lax.axis_index(a) for a in AXES)
    t = 8 * y + 2 * zl + k
    pair = lax.div(y, 2)

    def rcopy(src, dst, send, recv, **dev):
        return pltpu.make_async_remote_copy(
            src_ref=src, dst_ref=dst, send_sem=send, recv_sem=recv, device_id=dev, device_id_type=MESH
        )

    def slot_of(source, plane):
        return jnp.where(source == plane, 0, source + (source < plane).astype(jnp.int32))

    def other(slot):
        return slot - 1 + (slot - 1 >= zh).astype(jnp.int32)

    heads = pl.ds(pl.multiple_of(y * HD, HD), HD)
    loads = [
        pltpu.make_async_copy(src, dst, in_sem.at[i])
        for i, (src, dst) in enumerate(
            [
                (g_hbm, g),
                (q_hbm, q),
                (k_hbm.at[:, heads], kk),
                (v_hbm.at[:, heads], vv),
                (w_hbm, w),
                (fc_hbm, fc),
                (sc_hbm, sc),
                (frow_hbm, frow),
                (fcol_hbm, fcol),
                (srow_hbm, srow),
                (scol_hbm, scol),
            ]
        )
    ]
    for load in loads:
        load.start()

    barrier = pltpu.get_barrier_semaphore()

    def greet(**dev):
        pl.semaphore_signal(barrier, inc=1, device_id=dev, device_id_type=MESH)

    for dz in range(NZH):
        for dy in (0, 1, NY - 1):
            for dk in range(NC):
                if (dz, dy, dk) != (0, 0, 0):
                    greet(zh=mod(zh + dz, NZH), y=mod(y + dy, NY), core=lax.rem(k + dk, NC))
    for dl in range(1, NZL):
        greet(zl=mod(zl + dl, NZL))
        greet(zl=mod(zl + dl, NZL), core=1 - k)
    for dy in range(2, NY - 1):
        greet(y=mod(y + dy, NY))
    for dx in range(1, NX):
        greet(x=mod(x + dx, NX))
    greeted = 17 + 6 + 5 + 3

    loads[0].wait()
    gt[...] = g[...].T

    my_d = 3 * pair + zh
    my_q = 2 * lax.rem(y, 2) + k
    for i in range(QUART):
        r = QUART * my_q + i

        @pl.when((r >= UNITS) | (UNITS * my_d + r >= ALL_UNITS))
        def _():
            for jj in range(NZH):
                gz[jj, pair, pl.ds(pl.multiple_of(UNIT * r, UNIT), UNIT), :] = jnp.zeros(
                    (UNIT, SEQ), BF16
                )

    for i in (1, 2, 3):
        loads[i].wait()
    for i in range(3):
        rows, cols = pl.ds(128 * i, 128), pl.ds(0, 128 * (i + 1))
        scores = (
            lax.dot_general(q[rows, :], kk[cols, :], NT, preferred_element_type=F32) * SCALE
        )
        future = lax.broadcasted_iota(jnp.int32, scores.shape, 1) > (
            lax.broadcasted_iota(jnp.int32, scores.shape, 0) + 128 * i
        )
        scores = jnp.where(future, -1e30, scores)
        exponent = jnp.exp(scores - jnp.max(scores, axis=-1, keepdims=True))
        probabilities = exponent / jnp.sum(exponent, axis=-1, keepdims=True)
        prob[rows, cols] = probabilities
        att[0, rows, :] = jnp.dot(
            probabilities.astype(BF16), vv[cols, :], preferred_element_type=F32
        ).astype(BF16)

    loads[4].wait()
    wt[x] = w[...].astype(BF16).T

    pl.semaphore_wait(barrier, greeted)

    def unit_home(u):
        unit = 8 * t + u
        d = lax.div(unit, UNITS)
        r = unit - UNITS * d
        quarter = lax.div(r, QUART)
        zd, xd = lax.rem(d, NZH), lax.div(d, NZH)
        yd, kd = 2 * xd + lax.div(quarter, 2), lax.rem(quarter, 2)
        home = (zd == zh) & (yd == y) & (kd == k)
        return r, r - QUART * quarter, zd, xd, yd, kd, home

    def spread(u, carry):
        r, i, zd, xd, yd, kd, home = unit_home(u)
        src = gt.at[pl.ds(pl.multiple_of(UNIT * u, UNIT), UNIT), :]
        place = pl.ds(pl.multiple_of(UNIT * r, UNIT), UNIT)
        slot = slot_of(zh, zd)

        @pl.when(home)
        def _():
            gz[0, xd, place, :] = gt[pl.ds(pl.multiple_of(UNIT * u, UNIT), UNIT), :]

        @pl.when(jnp.logical_not(home))
        def _():
            rcopy(
                src, gz.at[slot, xd, place, :], r_send.at[u], r_recv.at[slot, i], zh=zd, y=yd, core=kd
            ).start()

        return carry

    lax.fori_loop(0, 8, spread, 0)

    sends = []
    def send_att():
        for slot in (1, 2):
            o = other(slot)
            there = slot_of(zh, o)
            copy = rcopy(
                att.at[0], att.at[there], att_send.at[slot - 1], att_recv.at[there - 1], zh=o
            )
            copy.start()
            sends.append(copy)

    for dx in (1, 3, 2):
        copy = rcopy(wt.at[x], wt.at[x], w_send.at[dx - 1], w_recv.at[NX - dx - 1], x=mod(x + dx, NX))
        copy.start()
        sends.append(copy)

    def chain_unit(jj, i):
        r = QUART * my_q + i
        unit = UNITS * my_d + r
        source = lax.div(unit, 8)
        from_zl = lax.rem(lax.div(source, 2), NZL)
        there = (r < UNITS) & (unit < ALL_UNITS)
        own = (source == t) & (jj == 0)
        piece = gz.at[jj, pair, pl.ds(pl.multiple_of(UNIT * r, UNIT), UNIT), :]
        up = there & (zl < NZL - 1) & (zl >= from_zl)
        down = there & (zl > 0) & (zl <= from_zl)
        up_copy = rcopy(piece, piece, up_send.at[jj, i], r_recv.at[jj, i], zl=lax.rem(zl + 1, NZL))
        down_copy = rcopy(
            piece, piece, down_send.at[jj, i], r_recv.at[jj, i], zl=lax.rem(zl + NZL - 1, NZL)
        )
        return there & jnp.logical_not(own), up, down, up_copy, down_copy

    def home_ready(jj):
        def one(i, carry):
            comes, up, down, up_copy, down_copy = chain_unit(jj, i)
            pl.when(comes)(up_copy.wait_recv)
            pl.when(up)(up_copy.start)
            pl.when(down)(down_copy.start)
            return carry

        lax.fori_loop(0, QUART, one, 0)

    HALF = 96

    def part(jj, source, r):
        quarter = 2 * lax.rem(source, 2) + k
        start, size = 0, QROWS
        if jj == 2 and r[1] == 4:
            start, size = (0, HALF) if r[0] == 0 else (HALF, QROWS - HALF)
        return gz.at[
            jj, lax.div(source, 2), pl.ds(pl.multiple_of(QROWS * quarter + start, UNIT), size), :
        ]

    def from_source(way, hops):
        return mod(y - hops, NY) if way == 0 else mod(y + hops, NY)

    def forward(way, jj, hops):
        piece = part(jj, from_source(way, hops), (way, hops + 1))
        copy = rcopy(
            piece,
            piece,
            ring_send.at[way, jj, hops],
            ring_recv.at[way, jj, hops],
            y=mod(y + 1, NY) if way == 0 else mod(y - 1, NY),
        )
        copy.start()
        sends.append(copy)

    def arrived(way, jj, hops):
        piece = part(jj, from_source(way, hops), (way, hops))
        rcopy(
            piece, piece, ring_send.at[way, jj, hops - 1], ring_recv.at[way, jj, hops - 1], y=y
        ).wait_recv()

    def to_partner(way, jj, hops):
        piece = part(jj, from_source(way, hops), (way, hops))
        copy = rcopy(piece, piece, d_send.at[way, jj, hops], d_recv.at[way, jj, hops], core=1 - k)
        copy.start()
        sends.append(copy)

    def from_partner(way, jj, hops):
        source = from_source(way, hops)
        quarter = 2 * lax.rem(source, 2) + (1 - k)
        start, size = 0, QROWS
        if jj == 2 and hops == 4:
            start, size = (0, HALF) if way == 0 else (HALF, QROWS - HALF)
        piece = gz.at[
            jj, lax.div(source, 2), pl.ds(pl.multiple_of(QROWS * quarter + start, UNIT), size), :
        ]
        rcopy(
            piece, piece, d_send.at[way, jj, hops], d_recv.at[way, jj, hops], core=1 - k
        ).wait_recv()

    reach = {(0, 0): 4, (1, 0): 3, (0, 1): 3, (1, 1): 4, (0, 2): 4, (1, 2): 4}

    def start_ring(jj):
        home_ready(jj)
        forward(0, jj, 0)
        forward(1, jj, 0)
        to_partner(0, jj, 0)

    def pass_on(jj, hops):
        for way in (0, 1):
            if hops <= reach[way, jj]:
                arrived(way, jj, hops)
                if hops < reach[way, jj]:
                    forward(way, jj, hops)
                to_partner(way, jj, hops)

    def partner_has(jj, hops):
        for way in (0, 1):
            if hops == 0 and way == 1:
                continue
            if hops <= reach[way, jj]:
                from_partner(way, jj, hops)

    def multiply(jj, xo):
        block = gz[jj, xo, 0:ROWS, :]
        term = jnp.dot(wt[xo], block, preferred_element_type=F32)
        acct[jj] = term if jj not in started else acct[jj] + term
        started.add(jj)

    def weight_term(jj, source):
        xo = lax.div(source, 2)
        rows = pl.ds(pl.multiple_of(HALF_ROWS * lax.rem(source, 2), UNIT), HALF_ROWS)
        term = jnp.dot(gz[jj, xo, rows, :], att[jj], preferred_element_type=F32)
        dwacc[xo, rows, :] = term if jj == 0 else dwacc[xo, rows, :] + term
        if jj == 2:

            @pl.when(xo != x)
            def _():
                dw_stage[xo, rows, :] = dwacc[xo, rows, :].astype(BF16)
                rel = mod(x - xo, NX) - 1
                half = lax.rem(source, 2)
                rcopy(
                    dw_stage.at[xo, rows, :],
                    dw_in.at[rel, rows, :],
                    dw_send.at[xo, half],
                    dw_recv.at[rel, half],
                    x=xo,
                ).start()

    def finish(jj, hops):
        partner_has(jj, hops)
        weight_term(jj, mod(y - hops, NY))
        if hops in (1, 2, 3):
            weight_term(jj, mod(y + hops, NY))

    started = set()

    def xo_of(off):
        return mod(pair + off, NX)

    def multiply_all(jj):
        for off in (0, 1, 3, 2):
            multiply(jj, xo_of(off))

    def send_grad(jj):
        ga_stage[jj - 1] = acct[jj].astype(BF16)
        o = other(jj)
        there = slot_of(zh, o) - 1
        copy = rcopy(
            ga_stage.at[jj - 1], ga_in.at[there], ga_send.at[jj - 1], ga_recv.at[there], zh=o
        )
        copy.start()
        sends.append(copy)

    start_ring(0)
    pass_on(0, 1)
    start_ring(1)
    send_att()
    pass_on(0, 2)
    finish(0, 0)
    pass_on(1, 1)
    finish(0, 1)
    start_ring(2)
    pass_on(0, 3)
    finish(0, 2)
    pass_on(1, 2)
    pass_on(2, 1)
    finish(0, 3)
    pass_on(0, 4)
    for dx in (1, 2, 3):
        rcopy(wt.at[0], wt.at[mod(x + dx, NX)], w_send.at[0], w_recv.at[dx - 1], x=x).wait_recv()
    pass_on(1, 3)
    finish(0, 4)
    multiply_all(0)
    pass_on(2, 2)
    for slot in (1, 2):
        rcopy(att.at[0], att.at[slot], att_send.at[0], att_recv.at[slot - 1], zh=zh).wait_recv()
    finish(1, 0)
    finish(1, 1)
    finish(1, 2)
    pass_on(1, 4)
    finish(1, 3)
    pass_on(2, 3)
    finish(1, 4)
    multiply_all(1)
    send_grad(1)
    finish(2, 0)
    finish(2, 1)
    finish(2, 2)
    finish(2, 3)
    pass_on(2, 4)
    finish(2, 4)
    multiply_all(2)
    send_grad(2)

    for load in loads[5:]:
        load.wait()
    for half in (0, 1):
        rows = pl.ds(HALF_ROWS * half, HALF_ROWS)
        for dx in (1, 2, 3):
            rcopy(
                dw_stage.at[0, rows, :],
                dw_in.at[dx - 1, rows, :],
                dw_send.at[0, half],
                dw_recv.at[dx - 1, half],
                x=x,
            ).wait_recv()
    for c, start, size in row_chunks():
        rows = pl.ds(start, size)
        grad = (
            (dwacc[x, rows, :] + dw_in[0, rows, :].astype(F32))
            + dw_in[1, rows, :].astype(F32)
            + dw_in[2, rows, :].astype(F32)
        )
        low_first = jnp.minimum(down(frow, start, size), fcol[...].reshape(1, HD))
        low_second = jnp.minimum(down(srow, start, size), scol[...].reshape(1, HD))
        first = fc[rows, :].astype(F32) * low_first
        second = sc[rows, :].astype(F32) * low_second
        first_new = beta_first * first + (1.0 - beta_first) * grad
        second_new = beta_second * second + (1.0 - beta_second) * grad * grad
        step_size = first_new / correct_first / (jnp.sqrt(second_new / correct_second) + adam_eps)
        weight = w[rows, :]
        nw_out[rows, :] = weight - learning * (step_size + decay_rate * weight)
        fnew_out[rows, :] = first_new
        snew_out[rows, :] = second_new

    first_abs, second_abs = jnp.abs(fnew_out[...]), jnp.abs(snew_out[...])
    st[0] = lane_rows(first_abs)
    st[1] = lane_rows(second_abs)
    for dy in range(1, NY):
        copy = rcopy(
            st, y_in.at[NY - dy - 1], y_send.at[dy - 1], y_recv.at[NY - dy - 1], y=mod(y + dy, NY)
        )
        copy.start()
        sends.append(copy)
    cst[0, 0:1, :] = jnp.max(first_abs, axis=0, keepdims=True)
    cst[0, 1:2, :] = jnp.max(second_abs, axis=0, keepdims=True)
    for dx in range(1, NX):
        copy = rcopy(
            cst.at[0], x_in.at[NX - dx - 1], x_send.at[dx - 1], x_recv.at[NX - dx - 1], x=mod(x + dx, NX)
        )
        copy.start()
        sends.append(copy)

    def back_rows(i):
        rows, cols = pl.ds(128 * i, 128), pl.ds(0, 128 * (i + 1))
        total = acct[0, :, rows]
        for s in range(2):
            total = total + ga_in[s, :, rows].astype(F32)
        grad_half = total.astype(BF16).T
        grad_probs = lax.dot_general(grad_half, vv[cols, :], NT, preferred_element_type=F32)
        row_dot = jnp.sum(
            grad_half.astype(F32) * att[0, rows, :].astype(F32), axis=-1, keepdims=True
        )
        grad_scores = (prob[rows, cols] * (grad_probs - row_dot)).astype(BF16)
        gq_out[rows, :] = (
            jnp.dot(grad_scores, kk[cols, :], preferred_element_type=F32) * SCALE
        ).astype(BF16)

    for s in range(2):
        rcopy(ga_stage.at[0], ga_in.at[s], ga_send.at[0], ga_recv.at[s], zh=zh).wait_recv()
    back_rows(0)
    back_rows(1)

    for dx in range(1, NX):
        rcopy(cst.at[0], x_in.at[dx - 1], x_send.at[0], x_recv.at[dx - 1], x=x).wait_recv()
    cst[1] = jnp.maximum(cst[0], jnp.max(x_in[...], axis=0))
    for slot in (1, 2):
        o = other(slot)
        there = slot_of(zh, o) - 1
        copy = rcopy(cst.at[1], zh_in.at[there], zh_send.at[slot - 1], zh_recv.at[there], zh=o)
        copy.start()
        sends.append(copy)
    for dy in range(1, NY):
        rcopy(st, y_in.at[dy - 1], y_send.at[0], y_recv.at[dy - 1], y=y).wait_recv()
    mine[...] = jnp.maximum(st[...], jnp.max(y_in[...], axis=0))
    for rel in range(1, NZL * NC):
        dl, dk = rel // NC, rel % NC
        back = NC * ((NZL - dl) % NZL) + dk - 1
        copy = rcopy(
            mine,
            zl_in.at[back],
            zl_send.at[rel - 1],
            zl_recv.at[back],
            zl=mod(zl + dl, NZL),
            core=lax.rem(k + dk, NC),
        )
        copy.start()
        sends.append(copy)
    back_rows(2)
    for slot in (1, 2):
        rcopy(cst.at[1], zh_in.at[slot - 1], zh_send.at[0], zh_recv.at[slot - 1], zh=zh).wait_recv()
    cols_out[...] = jnp.maximum(cst[1], jnp.max(zh_in[...], axis=0))
    for rel in range(1, NZL * NC):
        rcopy(mine, zl_in.at[rel - 1], zl_send.at[0], zl_recv.at[rel - 1], zl=zl).wait_recv()
    rows_out[...] = jnp.maximum(mine[...], jnp.max(zl_in[...], axis=0))

    def drain(u, carry):
        home = unit_home(u)[-1]
        src = gt.at[pl.ds(pl.multiple_of(UNIT * u, UNIT), UNIT), :]
        pl.when(jnp.logical_not(home))(rcopy(src, src, r_send.at[u], r_recv.at[0, 0], core=k).wait_send)
        return carry

    lax.fori_loop(0, 8, drain, 0)

    def drain_chain(jj):
        def one(i, carry):
            comes, up, down, up_copy, down_copy = chain_unit(jj, i)
            pl.when(up)(up_copy.wait_send)
            pl.when(down)(down_copy.wait_send)
            return carry

        lax.fori_loop(0, QUART, one, 0)

    for jj in range(NZH):
        drain_chain(jj)
    for copy in sends:
        copy.wait_send()
    for xo in range(NX):

        @pl.when(xo != x)
        def _():
            for half in (0, 1):
                rows = pl.ds(HALF_ROWS * half, HALF_ROWS)
                rcopy(
                    dw_stage.at[xo, rows, :],
                    dw_in.at[0, rows, :],
                    dw_send.at[xo, half],
                    dw_recv.at[0, half],
                    x=x,
                ).wait_send()


def codes(gq, nw, fnew, snew, rows, cols, gq_out, nw_out, nfc_out, nfr_out, nfcol_out, nsc_out, nsr_out, nscol_out):
    gq_out[...] = gq[...]
    nw_out[...] = nw[...]
    nfcol_out[...] = cols[0]
    nscol_out[...] = cols[1]
    for c, start, size in row_chunks():
        at = pl.ds(start, size)
        nfr_out[at] = rows[0, c, 0:size]
        nsr_out[at] = rows[1, c, 0:size]
        low_first = jnp.minimum(down_rows(rows[0, c : c + 1, :])[:size], cols[0:1])
        low_second = jnp.minimum(down_rows(rows[1, c : c + 1, :])[:size], cols[1:2])
        nfc_out[at, :] = (fnew[at, :] / (low_first + code_eps)).astype(BF16)
        nsc_out[at, :] = (snew[at, :] / (low_second + code_eps)).astype(BF16)


def per_device(queries, keys, values, grad_out, weight, fc, frow, fcol, sc, srow, scol):
    shape = jax.ShapeDtypeStruct
    vmem = pl.BlockSpec(memory_space=pltpu.VMEM)
    hbm = pl.BlockSpec(memory_space=pltpu.HBM)
    dma = pltpu.SemaphoreType.DMA
    gq, nw, fnew, snew, rows, cols = pl.pallas_call(
        body,
        name="whole",
        out_shape=(
            shape((SEQ, HD), BF16),
            shape((ROWS, HD), F32),
            shape((ROWS, HD), F32),
            shape((ROWS, HD), F32),
            shape((2, 8, HD), F32),
            shape((2, HD), F32),
        ),
        in_specs=[hbm] * 11,
        out_specs=[vmem] * 6,
        scratch_shapes=[
            pltpu.VMEM((SEQ, HD), BF16),
            pltpu.VMEM((SEQ, HD), BF16),
            pltpu.VMEM((SEQ, HD), BF16),
            pltpu.VMEM((SEQ, HD), BF16),
            pltpu.VMEM((ROWS, HD), F32),
            pltpu.VMEM((ROWS, HD), BF16),
            pltpu.VMEM((ROWS, HD), BF16),
            pltpu.VMEM((ROWS,), F32),
            pltpu.VMEM((HD,), F32),
            pltpu.VMEM((ROWS,), F32),
            pltpu.VMEM((HD,), F32),
            pltpu.VMEM((HD, SEQ), BF16),
            pltpu.VMEM((NZH, NX, PADROWS, SEQ), BF16),
            pltpu.VMEM((NX, HD, ROWS), BF16),
            pltpu.VMEM((NZH, SEQ, HD), BF16),
            pltpu.VMEM((SEQ, SEQ), F32),
            pltpu.VMEM((NZH, HD, SEQ), F32),
            pltpu.VMEM((2, HD, SEQ), BF16),
            pltpu.VMEM((2, HD, SEQ), BF16),
            pltpu.VMEM((NX, PADROWS, HD), F32),
            pltpu.VMEM((NX, PADROWS, HD), BF16),
            pltpu.VMEM((NX - 1, PADROWS, HD), BF16),
            pltpu.VMEM((2, 8, HD), F32),
            pltpu.VMEM((NY - 1, 2, 8, HD), F32),
            pltpu.VMEM((NZL * NC - 1, 2, 8, HD), F32),
            pltpu.VMEM((2, 8, HD), F32),
            pltpu.VMEM((2, 2, HD), F32),
            pltpu.VMEM((NX - 1, 2, HD), F32),
            pltpu.VMEM((NZH - 1, 2, HD), F32),
            dma((11,)),
            dma((8,)),
            dma((NZH, QUART)),
            dma((NZH, QUART)),
            dma((NZH, QUART)),
            dma((2, NZH, 4)),
            dma((2, NZH, 4)),
            dma((2, NZH, 5)),
            dma((2, NZH, 5)),
            dma((2,)),
            dma((2,)),
            dma((3,)),
            dma((3,)),
            dma((2,)),
            dma((2,)),
            dma((NX, 2)),
            dma((NX - 1, 2)),
            dma((NY - 1,)),
            dma((NY - 1,)),
            dma((NZL * NC - 1,)),
            dma((NZL * NC - 1,)),
            dma((NX - 1,)),
            dma((NX - 1,)),
            dma((2,)),
            dma((2,)),
        ],
        compiler_params=pltpu.CompilerParams(
            collective_id=0, has_side_effects=True, vmem_limit_bytes=48 * 1024 * 1024
        ),
    )(
        *(
            pltpu.with_memory_space_constraint(a, pltpu.HBM)
            for a in (queries, keys, values, grad_out, weight, fc, frow, fcol, sc, srow, scol)
        )
    )
    return pl.pallas_call(
        codes,
        name="codes",
        out_shape=(
            shape((SEQ, HD), BF16),
            shape((ROWS, HD), F32),
            shape((ROWS, HD), BF16),
            shape((ROWS,), F32),
            shape((HD,), F32),
            shape((ROWS, HD), BF16),
            shape((ROWS,), F32),
            shape((HD,), F32),
        ),
        compiler_params=pltpu.CompilerParams(vmem_limit_bytes=8 * 1024 * 1024),
        in_specs=[vmem] * 6,
        out_specs=[vmem] * 8,
    )(gq, nw, fnew, snew, rows, cols)


def solution(mesh):
    finer = Mesh(mesh.devices.reshape(NX, NZH, NY, NZL, NC), AXES)
    placed = (
        P(DP, TENSOR),
        P(DP, None),
        P(DP, None),
        P(DP, TENSOR),
        P(DP, TENSOR),
        P(DP, TENSOR),
        P(DP),
        P(TENSOR),
        P(DP, TENSOR),
        P(DP),
        P(TENSOR),
    )
    return jax.shard_map(
        per_device,
        mesh=finer,
        in_specs=placed,
        out_specs=(
            P(DP, TENSOR),
            P(DP, TENSOR),
            P(DP, TENSOR),
            P(DP),
            P(TENSOR),
            P(DP, TENSOR),
            P(DP),
            P(TENSOR),
        ),
        check_vma=False,
    )
```

```python
import functools

import jax
import jax.numpy as jnp
from jax import lax
from jax.experimental import pallas as pl
from jax.experimental.pallas import tpu as pltpu
from jax.sharding import Mesh
from jax.sharding import PartitionSpec as P

NX, NZH, NY, NZL, NC = 4, 3, 8, 4, 2
AXES = ("x", "zh", "y", "zl", "core")
DP = ("x", "zh")
TENSOR = ("y", "zl", "core")
MESH = pl.DeviceIdType.MESH

HD = 128
SEQ = 384
ROWS = 688
UNIT = 16
UNITS = ROWS // UNIT
ALL_UNITS = 512
QUART = 11
QROWS = QUART * UNIT
PADROWS = 4 * QROWS
HALF_ROWS = 2 * QROWS
SCALE = HD ** (-0.5)

beta_first = 0.9
beta_second = 0.95
learning = 0.01
decay_rate = 0.1
adam_eps = 1e-08
code_eps = 1e-06
correct_first = 1.0 - 0.9**10
correct_second = 1.0 - 0.95**10

F32 = jnp.float32
BF16 = jnp.bfloat16
NT = (((1,), (1,)), ((), ()))


def mod(a, n):
    return lax.rem(a + n, n)


def row_chunks():
    return [(c, 128 * c, min(128, ROWS - 128 * c)) for c in range(6)]


def lane_rows(values):
    highest = jnp.max(values, axis=1, keepdims=True)
    out = []
    for c, start, size in row_chunks():
        eye = lax.broadcasted_iota(jnp.int32, (size, 128), 0) == lax.broadcasted_iota(
            jnp.int32, (size, 128), 1
        )
        out.append(
            jnp.max(jnp.where(eye, highest[start : start + size], 0.0), axis=0, keepdims=True)
        )
    out.append(jnp.zeros((2, 128), F32))
    return jnp.concatenate(out, axis=0)


def down(vector, start, size):
    row = vector[pl.ds(start, size)].reshape(1, size)
    if size < 128:
        row = jnp.concatenate([row, jnp.zeros((1, 128 - size), F32)], axis=1)
    return down_rows(row)[:size]


def down_rows(row):
    return jnp.broadcast_to(row, (128, 128)).T


def body(
    q_hbm,
    k_hbm,
    v_hbm,
    g_hbm,
    w_hbm,
    fc_hbm,
    frow_hbm,
    fcol_hbm,
    sc_hbm,
    srow_hbm,
    scol_hbm,
    gq_out,
    nw_out,
    fnew_out,
    snew_out,
    rows_out,
    cols_out,
    q,
    kk,
    vv,
    g,
    w,
    fc,
    sc,
    frow,
    fcol,
    srow,
    scol,
    gt,
    gz,
    wt,
    att,
    prob,
    acct,
    ga_stage,
    ga_in,
    dwacc,
    dw_stage,
    dw_in,
    dwsum,
    st,
    y_in,
    zl_in,
    mine,
    cst,
    x_in,
    zh_in,
    in_sem,
    spread_send,
    up_send,
    down_send,
    relay_send,
    r_recv,
    far_recv,
    near_recv,
    ring_send,
    ring_recv,
    core_send,
    core_recv,
    att_send,
    att_recv,
    w_send,
    w_recv,
    ga_send,
    ga_recv,
    dw_send,
    dw_recv,
    y_send,
    y_recv,
    zl_send,
    zl_recv,
    x_send,
    x_recv,
    zh_send,
    zh_recv,
):
    x, zh, y, zl, k = (lax.axis_index(a) for a in AXES)
    t = 8 * y + 2 * zl + k
    pair = lax.div(y, 2)

    def rcopy(src, dst, send, recv, **dev):
        return pltpu.make_async_remote_copy(
            src_ref=src, dst_ref=dst, send_sem=send, recv_sem=recv, device_id=dev, device_id_type=MESH
        )

    def slot_of(source, plane):
        return jnp.where(source == plane, 0, source + (source < plane).astype(jnp.int32))

    def other(slot):
        return slot - 1 + (slot - 1 >= zh).astype(jnp.int32)

    heads = pl.ds(pl.multiple_of(y * HD, HD), HD)
    loads = [
        pltpu.make_async_copy(src, dst, in_sem.at[i])
        for i, (src, dst) in enumerate(
            [
                (g_hbm, g),
                (q_hbm, q),
                (k_hbm.at[:, heads], kk),
                (v_hbm.at[:, heads], vv),
                (w_hbm, w),
                (fc_hbm, fc),
                (sc_hbm, sc),
                (frow_hbm, frow),
                (fcol_hbm, fcol),
                (srow_hbm, srow),
                (scol_hbm, scol),
            ]
        )
    ]
    for load in loads:
        load.start()

    barrier = pltpu.get_barrier_semaphore()

    def greet(**dev):
        pl.semaphore_signal(barrier, inc=1, device_id=dev, device_id_type=MESH)

    across = lax.rem(zl + 2, NZL)
    for dz in (1, 2, 0):
        for dy in (0, 1, NY - 1):
            for dk in range(NC):
                there = dict(zh=mod(zh + dz, NZH), y=mod(y + dy, NY), core=lax.rem(k + dk, NC))
                greet(zl=across, **there)
                if (dz, dy, dk) != (0, 0, 0):
                    greet(**there)
    for dl in (1, 3):
        for dk in range(NC):
            greet(zl=mod(zl + dl, NZL), core=lax.rem(k + dk, NC))
    for dy in range(2, NY - 1):
        greet(y=mod(y + dy, NY))
    for dx in range(1, NX):
        greet(x=mod(x + dx, NX))
    greeted = 35 + 4 + 5 + 3

    loads[0].wait()
    gt[...] = g[...].T

    my_d = 3 * pair + zh
    my_q = 2 * lax.rem(y, 2) + k
    my_piece = 4 * pair + my_q

    def unit_of(i):
        r = QUART * my_q + i
        unit = UNITS * my_d + r
        return lax.div(unit, 8), lax.rem(unit, 8), (r < UNITS) & (unit < ALL_UNITS)

    def rows_of(i):
        return pl.ds(pl.multiple_of(UNIT * i, UNIT), UNIT)

    for i in range(QUART):

        @pl.when(jnp.logical_not(unit_of(i)[2]))
        def _():
            for jj in range(NZH):
                gz[jj, my_piece, rows_of(i), :] = jnp.zeros((UNIT, SEQ), BF16)

    pl.semaphore_wait(barrier, greeted)

    def unit_home(u):
        unit = 8 * t + u
        d = lax.div(unit, UNITS)
        r = unit - UNITS * d
        quarter = lax.div(r, QUART)
        zd, xd = lax.rem(d, NZH), lax.div(d, NZH)
        yd, kd = 2 * xd + lax.div(quarter, 2), lax.rem(quarter, 2)
        home = (zd == zh) & (yd == y) & (kd == k)
        return r - QUART * quarter, 4 * xd + quarter, zd, yd, kd, home

    def spread(u, stayed):
        i, piece, zd, yd, kd, home = unit_home(u)
        src = gt.at[rows_of(u), :]
        slot = slot_of(zh, zd)

        @pl.when(home)
        def _():
            gz[0, piece, rows_of(i), :] = gt[rows_of(u), :]

        @pl.when((zd == zh) & jnp.logical_not(home))
        def _():
            rcopy(src, gz.at[0, piece, rows_of(i), :], spread_send, r_recv.at[i], y=yd, core=kd).start()

        @pl.when(zd != zh)
        def _():
            rcopy(
                src,
                gz.at[slot, piece, rows_of(i), :],
                spread_send,
                far_recv.at[slot - 1],
                zh=zd,
                y=yd,
                zl=lax.rem(zl + 2 * lax.rem(u, 2), NZL),
                core=kd,
            ).start()

        return stayed + home.astype(jnp.int32)

    stayed = lax.fori_loop(0, 8, spread, jnp.int32(0))

    loads[4].wait()
    wt[x] = w[...].astype(BF16).T

    for dx in (1, 3, 2):
        rcopy(wt.at[x], wt.at[x], w_send, w_recv, x=mod(x + dx, NX)).start()

    for i in (1, 2, 3):
        loads[i].wait()
    for i in range(3):
        rows, cols = pl.ds(128 * i, 128), pl.ds(0, 128 * (i + 1))
        scores = (
            lax.dot_general(q[rows, :], kk[cols, :], NT, preferred_element_type=F32) * SCALE
        )
        future = lax.broadcasted_iota(jnp.int32, scores.shape, 1) > (
            lax.broadcasted_iota(jnp.int32, scores.shape, 0) + 128 * i
        )
        scores = jnp.where(future, -1e30, scores)
        exponent = jnp.exp(scores - jnp.max(scores, axis=-1, keepdims=True))
        probabilities = exponent / jnp.sum(exponent, axis=-1, keepdims=True)
        prob[rows, cols] = probabilities
        att[0, rows, :] = jnp.dot(
            probabilities.astype(BF16), vv[cols, :], preferred_element_type=F32
        ).astype(BF16)

    def send_att():
        for slot in (1, 2):
            o = other(slot)
            there = slot_of(zh, o)
            rcopy(att.at[0], att.at[there], att_send, att_recv.at[there - 1], zh=o).start()

    def wait_units(n, most, wait):
        for c in range(1, most + 1):
            pl.when(n == c)(functools.partial(wait, c))

    def chain_unit(i):
        source, u, there = unit_of(i)
        from_zl = lax.rem(lax.div(source, 2), NZL)
        piece = gz.at[0, my_piece, rows_of(i), :]
        up = there & (zl < NZL - 1) & (zl >= from_zl)
        down = there & (zl > 0) & (zl <= from_zl)
        up_copy = rcopy(piece, piece, up_send, r_recv.at[i], zl=lax.rem(zl + 1, NZL))
        down_copy = rcopy(piece, piece, down_send, r_recv.at[i], zl=lax.rem(zl + NZL - 1, NZL))
        return there & (source != t), up, down, up_copy, down_copy

    def chain(i, counts):
        comes, up, down, up_copy, down_copy = chain_unit(i)
        pl.when(comes)(up_copy.wait_recv)
        pl.when(up)(up_copy.start)
        pl.when(down)(down_copy.start)
        return counts[0] + up.astype(jnp.int32), counts[1] + down.astype(jnp.int32)

    def lands_here(i):
        source, u, there = unit_of(i)
        from_zl = lax.rem(lax.div(source, 2), NZL)
        here = lax.rem(from_zl + 2 * lax.rem(u, 2), NZL) == zl
        return there & here, there & jnp.logical_not(here)

    landing = sum(lands_here(i)[0].astype(jnp.int32) for i in range(QUART))
    coming = sum(lands_here(i)[1].astype(jnp.int32) for i in range(QUART))

    def units_came(sem, c):
        piece = gz.at[0, 0, 0 : UNIT * c, :]
        rcopy(piece, piece, spread_send, sem, zl=zl).wait_recv()

    def relay(jj):
        wait_units(landing, 6, functools.partial(units_came, far_recv.at[jj - 1]))

        def give(i, carry):
            piece = gz.at[jj, my_piece, rows_of(i), :]

            @pl.when(lands_here(i)[0])
            def _():
                for dl in (1, 3, 2):
                    rcopy(
                        piece, piece, relay_send, near_recv.at[jj - 1], zl=mod(zl + dl, NZL)
                    ).start()

            return carry

        lax.fori_loop(0, QUART, give, 0)

    HALF = 96

    def part(jj, source, core, way, hops):
        start, size = 0, QROWS
        if jj == 2 and hops == 4:
            start, size = (0, HALF) if way == 0 else (HALF, QROWS - HALF)
        return gz.at[jj, 2 * source + core, pl.ds(start, size), :]

    def from_source(way, hops):
        return mod(y - hops, NY) if way == 0 else mod(y + hops, NY)

    def forward(way, jj, hops):
        piece = part(jj, from_source(way, hops), k, way, hops + 1)
        rcopy(
            piece,
            piece,
            ring_send,
            ring_recv.at[way, jj, hops],
            y=mod(y + 1, NY) if way == 0 else mod(y - 1, NY),
        ).start()

    def arrived(way, jj, hops):
        piece = part(jj, from_source(way, hops), k, way, hops)
        rcopy(piece, piece, ring_send, ring_recv.at[way, jj, hops - 1], y=y).wait_recv()

    def to_partner(way, jj, hops):
        piece = part(jj, from_source(way, hops), k, way, hops)
        rcopy(piece, piece, core_send, core_recv.at[jj, hops], core=1 - k).start()

    def partner_has(jj, hops):
        pieces = gz.at[0, 0 : 2 if hops in (1, 2, 3) else 1]
        rcopy(pieces, pieces, core_send, core_recv.at[jj, hops], core=k).wait_recv()

    reach = {(0, 0): 4, (1, 0): 3, (0, 1): 3, (1, 1): 4, (0, 2): 4, (1, 2): 4}

    def start_ring(jj):
        if jj > 0:
            wait_units(coming, QUART, functools.partial(units_came, near_recv.at[jj - 1]))
        forward(0, jj, 0)
        forward(1, jj, 0)
        to_partner(0, jj, 0)

    def pass_on(jj, hops):
        for way in (0, 1):
            if hops <= reach[way, jj]:
                arrived(way, jj, hops)
                if hops < reach[way, jj]:
                    forward(way, jj, hops)
                to_partner(way, jj, hops)

    def multiply(jj, xo):
        block = gz[jj, pl.ds(4 * xo, 4)].reshape(PADROWS, SEQ)[:ROWS]
        term = jnp.dot(wt[xo], block, preferred_element_type=F32)
        acct[jj] = term if jj not in started else acct[jj] + term
        started.add(jj)

    def weight_term(jj, source):
        block = gz[jj, pl.ds(2 * source, 2)].reshape(HALF_ROWS, SEQ)
        term = jnp.dot(block, att[jj], preferred_element_type=F32)
        dwacc[source] = term if jj == 0 else dwacc[source] + term
        if jj == 2:
            xo, half = lax.div(source, 2), lax.rem(source, 2)

            @pl.when(xo != x)
            def _():
                dw_stage[source] = dwacc[source].astype(BF16)
                rel = mod(x - xo, NX) - 1
                rcopy(
                    dw_stage.at[source], dw_in.at[rel, half], dw_send, dw_recv.at[half], x=xo
                ).start()

    def finish(jj, hops):
        partner_has(jj, hops)
        weight_term(jj, mod(y - hops, NY))
        if hops in (1, 2, 3):
            weight_term(jj, mod(y + hops, NY))

    started = set()

    def xo_of(off):
        return mod(pair + off, NX)

    def multiply_all(jj):
        for off in (0, 1, 3, 2):
            multiply(jj, xo_of(off))

    def send_grad(jj):
        ga_stage[jj - 1] = acct[jj].astype(BF16)
        o = other(jj)
        rcopy(ga_stage.at[jj - 1], ga_in.at[slot_of(zh, o) - 1], ga_send, ga_recv, zh=o).start()

    ups, downs = lax.fori_loop(0, QUART, chain, (jnp.int32(0), jnp.int32(0)))
    start_ring(0)
    relay(1)
    relay(2)
    pass_on(0, 1)
    send_att()
    start_ring(1)
    pass_on(0, 2)
    finish(0, 0)
    pass_on(1, 1)
    finish(0, 1)
    start_ring(2)
    pass_on(0, 3)
    finish(0, 2)
    pass_on(1, 2)
    pass_on(2, 1)
    finish(0, 3)
    pass_on(0, 4)
    rcopy(wt.at[0:3], wt.at[0:3], w_send, w_recv, x=x).wait_recv()
    pass_on(1, 3)
    finish(0, 4)
    multiply_all(0)
    pass_on(2, 2)
    for slot in (1, 2):
        rcopy(att.at[0], att.at[slot], att_send, att_recv.at[slot - 1], zh=zh).wait_recv()
    finish(1, 0)
    finish(1, 1)
    finish(1, 2)
    pass_on(1, 4)
    finish(1, 3)
    pass_on(2, 3)
    finish(1, 4)
    multiply_all(1)
    send_grad(1)
    finish(2, 0)
    finish(2, 1)
    finish(2, 2)
    finish(2, 3)
    pass_on(2, 4)
    finish(2, 4)
    multiply_all(2)
    send_grad(2)

    for load in loads[5:]:
        load.wait()
    for half in (0, 1):
        piece = dw_in.at[:, half]
        rcopy(piece, piece, dw_send, dw_recv.at[half], x=x).wait_recv()
    for half in (0, 1):
        total = dwacc[2 * x + half]
        for rel in range(NX - 1):
            total = total + dw_in[rel, half].astype(F32)
        dwsum[pl.ds(HALF_ROWS * half, HALF_ROWS), :] = total
    for c, start, size in row_chunks():
        rows = pl.ds(start, size)
        grad = dwsum[rows, :]
        low_first = jnp.minimum(down(frow, start, size), fcol[...].reshape(1, HD))
        low_second = jnp.minimum(down(srow, start, size), scol[...].reshape(1, HD))
        first = fc[rows, :].astype(F32) * low_first
        second = sc[rows, :].astype(F32) * low_second
        first_new = beta_first * first + (1.0 - beta_first) * grad
        second_new = beta_second * second + (1.0 - beta_second) * grad * grad
        step_size = first_new / correct_first / (jnp.sqrt(second_new / correct_second) + adam_eps)
        weight = w[rows, :]
        nw_out[rows, :] = weight - learning * (step_size + decay_rate * weight)
        fnew_out[rows, :] = first_new
        snew_out[rows, :] = second_new

    first_abs, second_abs = jnp.abs(fnew_out[...]), jnp.abs(snew_out[...])
    st[0] = lane_rows(first_abs)
    st[1] = lane_rows(second_abs)
    for dy in range(1, NY):
        rcopy(st, y_in.at[NY - dy - 1], y_send, y_recv, y=mod(y + dy, NY)).start()
    cst[0, 0:1, :] = jnp.max(first_abs, axis=0, keepdims=True)
    cst[0, 1:2, :] = jnp.max(second_abs, axis=0, keepdims=True)
    for dx in range(1, NX):
        rcopy(cst.at[0], x_in.at[NX - dx - 1], x_send, x_recv, x=mod(x + dx, NX)).start()

    def back_rows(i):
        rows, cols = pl.ds(128 * i, 128), pl.ds(0, 128 * (i + 1))
        total = acct[0, :, rows]
        for s in range(2):
            total = total + ga_in[s, :, rows].astype(F32)
        grad_half = total.astype(BF16).T
        grad_probs = lax.dot_general(grad_half, vv[cols, :], NT, preferred_element_type=F32)
        row_dot = jnp.sum(
            grad_half.astype(F32) * att[0, rows, :].astype(F32), axis=-1, keepdims=True
        )
        grad_scores = (prob[rows, cols] * (grad_probs - row_dot)).astype(BF16)
        gq_out[rows, :] = (
            jnp.dot(grad_scores, kk[cols, :], preferred_element_type=F32) * SCALE
        ).astype(BF16)

    rcopy(ga_in, ga_in, ga_send, ga_recv, zh=zh).wait_recv()
    back_rows(0)
    back_rows(1)

    rcopy(x_in, x_in, x_send, x_recv, x=x).wait_recv()
    cst[1] = jnp.maximum(cst[0], jnp.max(x_in[...], axis=0))
    for slot in (1, 2):
        o = other(slot)
        rcopy(cst.at[1], zh_in.at[slot_of(zh, o) - 1], zh_send, zh_recv, zh=o).start()
    rcopy(y_in, y_in, y_send, y_recv, y=y).wait_recv()
    mine[...] = jnp.maximum(st[...], jnp.max(y_in[...], axis=0))
    for rel in range(1, NZL * NC):
        dl, dk = rel // NC, rel % NC
        back = NC * ((NZL - dl) % NZL) + dk - 1
        rcopy(
            mine, zl_in.at[back], zl_send, zl_recv, zl=mod(zl + dl, NZL), core=lax.rem(k + dk, NC)
        ).start()
    back_rows(2)
    rcopy(zh_in, zh_in, zh_send, zh_recv, zh=zh).wait_recv()
    cols_out[...] = jnp.maximum(cst[1], jnp.max(zh_in[...], axis=0))
    rcopy(zl_in, zl_in, zl_send, zl_recv, zl=zl).wait_recv()
    rows_out[...] = jnp.maximum(mine[...], jnp.max(zl_in[...], axis=0))

    def units_left(sem, each, c):
        pieces = gz.at[0, 0:c, 0 : UNIT * each, :]
        rcopy(pieces, pieces, sem, r_recv.at[0], zl=zl).wait_send()

    wait_units(8 - stayed, 8, functools.partial(units_left, spread_send, 1))
    wait_units(ups, QUART, functools.partial(units_left, up_send, 1))
    wait_units(downs, QUART, functools.partial(units_left, down_send, 1))
    wait_units(landing, 6, functools.partial(units_left, relay_send, 6))
    for whole, sem in (
        (gz.at[:, 0:7], ring_send),
        (gz.at[:, 0:8], core_send),
        (att.at[0:2], att_send),
        (wt.at[0:3], w_send),
        (ga_in, ga_send),
        (dw_in, dw_send),
        (y_in, y_send),
        (zl_in, zl_send),
        (x_in, x_send),
        (zh_in, zh_send),
    ):
        rcopy(whole, whole, sem, r_recv.at[0], zl=zl).wait_send()


def codes(gq, nw, fnew, snew, rows, cols, gq_out, nw_out, nfc_out, nfr_out, nfcol_out, nsc_out, nsr_out, nscol_out):
    gq_out[...] = gq[...]
    nw_out[...] = nw[...]
    nfcol_out[...] = cols[0]
    nscol_out[...] = cols[1]
    for c, start, size in row_chunks():
        at = pl.ds(start, size)
        nfr_out[at] = rows[0, c, 0:size]
        nsr_out[at] = rows[1, c, 0:size]
        low_first = jnp.minimum(down_rows(rows[0, c : c + 1, :])[:size], cols[0:1])
        low_second = jnp.minimum(down_rows(rows[1, c : c + 1, :])[:size], cols[1:2])
        nfc_out[at, :] = (fnew[at, :] / (low_first + code_eps)).astype(BF16)
        nsc_out[at, :] = (snew[at, :] / (low_second + code_eps)).astype(BF16)


def per_device(queries, keys, values, grad_out, weight, fc, frow, fcol, sc, srow, scol):
    shape = jax.ShapeDtypeStruct
    vmem = pl.BlockSpec(memory_space=pltpu.VMEM)
    hbm = pl.BlockSpec(memory_space=pltpu.HBM)
    dma = pltpu.SemaphoreType.DMA
    gq, nw, fnew, snew, rows, cols = pl.pallas_call(
        body,
        name="whole",
        out_shape=(
            shape((SEQ, HD), BF16),
            shape((ROWS, HD), F32),
            shape((ROWS, HD), F32),
            shape((ROWS, HD), F32),
            shape((2, 8, HD), F32),
            shape((2, HD), F32),
        ),
        in_specs=[hbm] * 11,
        out_specs=[vmem] * 6,
        scratch_shapes=[
            pltpu.VMEM((SEQ, HD), BF16),
            pltpu.VMEM((SEQ, HD), BF16),
            pltpu.VMEM((SEQ, HD), BF16),
            pltpu.VMEM((SEQ, HD), BF16),
            pltpu.VMEM((ROWS, HD), F32),
            pltpu.VMEM((ROWS, HD), BF16),
            pltpu.VMEM((ROWS, HD), BF16),
            pltpu.VMEM((ROWS,), F32),
            pltpu.VMEM((HD,), F32),
            pltpu.VMEM((ROWS,), F32),
            pltpu.VMEM((HD,), F32),
            pltpu.VMEM((HD, SEQ), BF16),
            pltpu.VMEM((NZH, 4 * NX, QROWS, SEQ), BF16),
            pltpu.VMEM((NX, HD, ROWS), BF16),
            pltpu.VMEM((NZH, SEQ, HD), BF16),
            pltpu.VMEM((SEQ, SEQ), F32),
            pltpu.VMEM((NZH, HD, SEQ), F32),
            pltpu.VMEM((2, HD, SEQ), BF16),
            pltpu.VMEM((2, HD, SEQ), BF16),
            pltpu.VMEM((2 * NX, HALF_ROWS, HD), F32),
            pltpu.VMEM((2 * NX, HALF_ROWS, HD), BF16),
            pltpu.VMEM((NX - 1, 2, HALF_ROWS, HD), BF16),
            pltpu.VMEM((PADROWS, HD), F32),
            pltpu.VMEM((2, 8, HD), F32),
            pltpu.VMEM((NY - 1, 2, 8, HD), F32),
            pltpu.VMEM((NZL * NC - 1, 2, 8, HD), F32),
            pltpu.VMEM((2, 8, HD), F32),
            pltpu.VMEM((2, 2, HD), F32),
            pltpu.VMEM((NX - 1, 2, HD), F32),
            pltpu.VMEM((NZH - 1, 2, HD), F32),
            dma((11,)),
            dma,
            dma,
            dma,
            dma,
            dma((QUART,)),
            dma((2,)),
            dma((2,)),
            dma,
            dma((2, NZH, 4)),
            dma,
            dma((NZH, 5)),
            dma,
            dma((2,)),
            dma,
            dma,
            dma,
            dma,
            dma,
            dma((2,)),
            dma,
            dma,
            dma,
            dma,
            dma,
            dma,
            dma,
            dma,
        ],
        compiler_params=pltpu.CompilerParams(
            collective_id=0, has_side_effects=True, vmem_limit_bytes=48 * 1024 * 1024
        ),
    )(
        *(
            pltpu.with_memory_space_constraint(a, pltpu.HBM)
            for a in (queries, keys, values, grad_out, weight, fc, frow, fcol, sc, srow, scol)
        )
    )
    return pl.pallas_call(
        codes,
        name="codes",
        out_shape=(
            shape((SEQ, HD), BF16),
            shape((ROWS, HD), F32),
            shape((ROWS, HD), BF16),
            shape((ROWS,), F32),
            shape((HD,), F32),
            shape((ROWS, HD), BF16),
            shape((ROWS,), F32),
            shape((HD,), F32),
        ),
        compiler_params=pltpu.CompilerParams(vmem_limit_bytes=8 * 1024 * 1024),
        in_specs=[vmem] * 6,
        out_specs=[vmem] * 8,
    )(gq, nw, fnew, snew, rows, cols)


def solution(mesh):
    finer = Mesh(mesh.devices.reshape(NX, NZH, NY, NZL, NC), AXES)
    placed = (
        P(DP, TENSOR),
        P(DP, None),
        P(DP, None),
        P(DP, TENSOR),
        P(DP, TENSOR),
        P(DP, TENSOR),
        P(DP),
        P(TENSOR),
        P(DP, TENSOR),
        P(DP),
        P(TENSOR),
    )
    return jax.shard_map(
        per_device,
        mesh=finer,
        in_specs=placed,
        out_specs=(
            P(DP, TENSOR),
            P(DP, TENSOR),
            P(DP, TENSOR),
            P(DP),
            P(TENSOR),
            P(DP, TENSOR),
            P(DP),
            P(TENSOR),
        ),
        check_vma=False,
    )
```

```python
import functools

import jax
import jax.numpy as jnp
from jax import lax
from jax.experimental import pallas as pl
from jax.experimental.pallas import tpu as pltpu
from jax.sharding import Mesh
from jax.sharding import PartitionSpec as P

NX, NZH, NY, NZL, NC = 4, 3, 8, 4, 2
AXES = ("x", "zh", "y", "zl", "core")
DP = ("x", "zh")
TENSOR = ("y", "zl", "core")
MESH = pl.DeviceIdType.MESH

HD = 128
SEQ = 384
ROWS = 688
UNIT = 16
UNITS = ROWS // UNIT
ALL_UNITS = 512
QUART = 11
QROWS = QUART * UNIT
PADROWS = 4 * QROWS
HALF_ROWS = 2 * QROWS
SCALE = HD ** (-0.5)

beta_first = 0.9
beta_second = 0.95
learning = 0.01
decay_rate = 0.1
adam_eps = 1e-08
code_eps = 1e-06
correct_first = 1.0 - 0.9**10
correct_second = 1.0 - 0.95**10

F32 = jnp.float32
BF16 = jnp.bfloat16
NT = (((1,), (1,)), ((), ()))


def mod(a, n):
    return lax.rem(a + n, n)


def row_chunks():
    return [(c, 128 * c, min(128, ROWS - 128 * c)) for c in range(6)]


def lane_rows(values):
    highest = jnp.max(values, axis=1, keepdims=True)
    out = []
    for c, start, size in row_chunks():
        eye = lax.broadcasted_iota(jnp.int32, (size, 128), 0) == lax.broadcasted_iota(
            jnp.int32, (size, 128), 1
        )
        out.append(
            jnp.max(jnp.where(eye, highest[start : start + size], 0.0), axis=0, keepdims=True)
        )
    out.append(jnp.zeros((2, 128), F32))
    return jnp.concatenate(out, axis=0)


def down(vector, start, size):
    row = vector[pl.ds(start, size)].reshape(1, size)
    if size < 128:
        row = jnp.concatenate([row, jnp.zeros((1, 128 - size), F32)], axis=1)
    return down_rows(row)[:size]


def down_rows(row):
    return jnp.broadcast_to(row, (128, 128)).T


def body(
    q_hbm,
    k_hbm,
    v_hbm,
    g_hbm,
    w_hbm,
    fc_hbm,
    frow_hbm,
    fcol_hbm,
    sc_hbm,
    srow_hbm,
    scol_hbm,
    gq_out,
    nw_out,
    fnew_out,
    snew_out,
    rows_out,
    cols_out,
    q,
    kk,
    vv,
    g,
    w,
    fc,
    sc,
    frow,
    fcol,
    srow,
    scol,
    gt,
    gz,
    wt,
    att,
    prob,
    acct,
    ga_stage,
    ga_in,
    dwacc,
    dw_stage,
    dw_in,
    dwsum,
    st,
    y_in,
    zl_in,
    mine,
    cst,
    x_in,
    zh_in,
    in_sem,
    spread_send,
    relay_send,
    far_recv,
    near_recv,
    ring_send,
    ring_recv,
    core_send,
    core_recv,
    att_send,
    att_recv,
    w_send,
    w_recv,
    ga_send,
    ga_recv,
    dw_send,
    dw_recv,
    y_send,
    y_recv,
    zl_send,
    zl_recv,
    x_send,
    x_recv,
    zh_send,
    zh_recv,
):
    x, zh, y, zl, k = (lax.axis_index(a) for a in AXES)
    t = 8 * y + 2 * zl + k
    pair = lax.div(y, 2)

    def rcopy(src, dst, send, recv, **dev):
        return pltpu.make_async_remote_copy(
            src_ref=src, dst_ref=dst, send_sem=send, recv_sem=recv, device_id=dev, device_id_type=MESH
        )

    def slot_of(source, plane):
        return jnp.where(source == plane, 0, source + (source < plane).astype(jnp.int32))

    def other(slot):
        return slot - 1 + (slot - 1 >= zh).astype(jnp.int32)

    heads = pl.ds(pl.multiple_of(y * HD, HD), HD)
    loads = [
        pltpu.make_async_copy(src, dst, in_sem.at[i])
        for i, (src, dst) in enumerate(
            [
                (g_hbm, g),
                (q_hbm, q),
                (k_hbm.at[:, heads], kk),
                (v_hbm.at[:, heads], vv),
                (w_hbm, w),
                (fc_hbm, fc),
                (sc_hbm, sc),
                (frow_hbm, frow),
                (fcol_hbm, fcol),
                (srow_hbm, srow),
                (scol_hbm, scol),
            ]
        )
    ]
    for load in loads:
        load.start()

    barrier = pltpu.get_barrier_semaphore()

    def greet(**dev):
        pl.semaphore_signal(barrier, inc=1, device_id=dev, device_id_type=MESH)

    across = lax.rem(zl + 2, NZL)
    for dz in (1, 2, 0):
        for dy in (0, 1, NY - 1):
            for dk in range(NC):
                there = dict(zh=mod(zh + dz, NZH), y=mod(y + dy, NY), core=lax.rem(k + dk, NC))
                greet(zl=across, **there)
                if (dz, dy, dk) != (0, 0, 0):
                    greet(**there)
    for dl in (1, 3):
        for dk in range(NC):
            greet(zl=mod(zl + dl, NZL), core=lax.rem(k + dk, NC))
    for dy in range(2, NY - 1):
        greet(y=mod(y + dy, NY))
    for dx in range(1, NX):
        greet(x=mod(x + dx, NX))
    greeted = 35 + 4 + 5 + 3

    loads[0].wait()
    gt[...] = g[...].T

    my_d = 3 * pair + zh
    my_q = 2 * lax.rem(y, 2) + k
    my_piece = 4 * pair + my_q

    def unit_of(i):
        r = QUART * my_q + i
        unit = UNITS * my_d + r
        return lax.div(unit, 8), lax.rem(unit, 8), (r < UNITS) & (unit < ALL_UNITS)

    def rows_of(i):
        return pl.ds(pl.multiple_of(UNIT * i, UNIT), UNIT)

    for i in range(QUART):

        @pl.when(jnp.logical_not(unit_of(i)[2]))
        def _():
            for jj in range(NZH):
                gz[jj, my_piece, rows_of(i), :] = jnp.zeros((UNIT, SEQ), BF16)

    pl.semaphore_wait(barrier, greeted)

    def unit_home(u):
        unit = 8 * t + u
        d = lax.div(unit, UNITS)
        r = unit - UNITS * d
        quarter = lax.div(r, QUART)
        zd, xd = lax.rem(d, NZH), lax.div(d, NZH)
        yd, kd = 2 * xd + lax.div(quarter, 2), lax.rem(quarter, 2)
        zld = lax.rem(zl + 2 * lax.rem(u, 2), NZL)
        home = (zd == zh) & (yd == y) & (kd == k) & (zld == zl)
        return r - QUART * quarter, 4 * xd + quarter, zd, yd, zld, kd, home

    def spread(wanted, u, stayed):
        i, piece, zd, yd, zld, kd, home = unit_home(u)
        slot = slot_of(zh, zd)

        @pl.when(wanted(zd) & home)
        def _():
            gz[0, piece, rows_of(i), :] = gt[rows_of(u), :]

        @pl.when(wanted(zd) & jnp.logical_not(home))
        def _():
            rcopy(
                gt.at[rows_of(u), :],
                gz.at[slot, piece, rows_of(i), :],
                spread_send,
                far_recv.at[slot],
                zh=zd,
                y=yd,
                zl=zld,
                core=kd,
            ).start()

        return stayed + home.astype(jnp.int32)

    stayed = lax.fori_loop(0, 8, functools.partial(spread, lambda zd: zd == zh), jnp.int32(0))
    lax.fori_loop(0, 8, functools.partial(spread, lambda zd: zd > zh), jnp.int32(0))

    loads[4].wait()
    wt[x] = w[...].astype(BF16).T

    for dx in (1, 3, 2):
        rcopy(wt.at[x], wt.at[x], w_send, w_recv, x=mod(x + dx, NX)).start()

    for i in (1, 2, 3):
        loads[i].wait()
    for i in range(3):
        rows, cols = pl.ds(128 * i, 128), pl.ds(0, 128 * (i + 1))
        scores = (
            lax.dot_general(q[rows, :], kk[cols, :], NT, preferred_element_type=F32) * SCALE
        )
        future = lax.broadcasted_iota(jnp.int32, scores.shape, 1) > (
            lax.broadcasted_iota(jnp.int32, scores.shape, 0) + 128 * i
        )
        scores = jnp.where(future, -1e30, scores)
        exponent = jnp.exp(scores - jnp.max(scores, axis=-1, keepdims=True))
        probabilities = exponent / jnp.sum(exponent, axis=-1, keepdims=True)
        prob[rows, cols] = probabilities
        att[0, rows, :] = jnp.dot(
            probabilities.astype(BF16), vv[cols, :], preferred_element_type=F32
        ).astype(BF16)

    def send_att():
        for slot in (1, 2):
            o = other(slot)
            there = slot_of(zh, o)
            rcopy(att.at[0], att.at[there], att_send, att_recv.at[there - 1], zh=o).start()

    def wait_units(n, most, wait):
        for c in range(1, most + 1):
            pl.when(n == c)(functools.partial(wait, c))

    def lands_here(i):
        source, u, there = unit_of(i)
        from_zl = lax.rem(lax.div(source, 2), NZL)
        here = lax.rem(from_zl + 2 * lax.rem(u, 2), NZL) == zl
        return there & here, there & jnp.logical_not(here)

    landing = sum(lands_here(i)[0].astype(jnp.int32) for i in range(QUART))
    coming = sum(lands_here(i)[1].astype(jnp.int32) for i in range(QUART))

    def units_came(sem, c):
        piece = gz.at[0, 0, 0 : UNIT * c, :]
        rcopy(piece, piece, spread_send, sem, zl=zl).wait_recv()

    def relay(jj):
        wait_units(
            landing - stayed if jj == 0 else landing, 6, functools.partial(units_came, far_recv.at[jj])
        )

        def give(i, carry):
            piece = gz.at[jj, my_piece, rows_of(i), :]

            @pl.when(lands_here(i)[0])
            def _():
                for dl in (1, 3, 2):
                    rcopy(piece, piece, relay_send, near_recv.at[jj], zl=mod(zl + dl, NZL)).start()

            return carry

        lax.fori_loop(0, QUART, give, 0)

    HALF = 96

    def part(jj, source, core, way, hops):
        start, size = 0, QROWS
        if jj == 0 and hops == 4:
            start, size = (0, HALF) if way == 0 else (HALF, QROWS - HALF)
        return gz.at[jj, 2 * source + core, pl.ds(start, size), :]

    def from_source(way, hops):
        return mod(y - hops, NY) if way == 0 else mod(y + hops, NY)

    def forward(way, jj, hops):
        piece = part(jj, from_source(way, hops), k, way, hops + 1)
        rcopy(
            piece,
            piece,
            ring_send,
            ring_recv.at[way, jj, hops],
            y=mod(y + 1, NY) if way == 0 else mod(y - 1, NY),
        ).start()

    def arrived(way, jj, hops):
        piece = part(jj, from_source(way, hops), k, way, hops)
        rcopy(piece, piece, ring_send, ring_recv.at[way, jj, hops - 1], y=y).wait_recv()

    def to_partner(way, jj, hops):
        piece = part(jj, from_source(way, hops), k, way, hops)
        rcopy(piece, piece, core_send, core_recv.at[jj, hops], core=1 - k).start()

    def partner_has(jj, hops):
        pieces = gz.at[0, 0 : 2 if hops in (1, 2, 3) else 1]
        rcopy(pieces, pieces, core_send, core_recv.at[jj, hops], core=k).wait_recv()

    reach = {(0, 0): 4, (1, 0): 4, (0, 1): 4, (1, 1): 3, (0, 2): 3, (1, 2): 4}

    def start_ring(jj):
        wait_units(coming, QUART, functools.partial(units_came, near_recv.at[jj]))
        forward(0, jj, 0)
        forward(1, jj, 0)
        to_partner(0, jj, 0)

    def pass_on(jj, hops):
        for way in (0, 1):
            if hops <= reach[way, jj]:
                arrived(way, jj, hops)
                if hops < reach[way, jj]:
                    forward(way, jj, hops)
                to_partner(way, jj, hops)

    def multiply(jj, xo):
        block = gz[jj, pl.ds(4 * xo, 4)].reshape(PADROWS, SEQ)[:ROWS]
        term = jnp.dot(wt[xo], block, preferred_element_type=F32)
        acct[jj] = term if jj not in started else acct[jj] + term
        started.add(jj)

    def weight_term(jj, source, first, last):
        block = gz[jj, pl.ds(2 * source, 2)].reshape(HALF_ROWS, SEQ)
        term = jnp.dot(block, att[jj], preferred_element_type=F32)
        dwacc[source] = term if first else dwacc[source] + term
        if last:
            xo, half = lax.div(source, 2), lax.rem(source, 2)

            @pl.when(xo != x)
            def _():
                dw_stage[source] = dwacc[source].astype(BF16)
                rel = mod(x - xo, NX) - 1
                rcopy(
                    dw_stage.at[source], dw_in.at[rel, half], dw_send, dw_recv.at[half], x=xo
                ).start()

    def finish(jj, hops):
        partner_has(jj, hops)
        done[hops] += 1
        for way in (0, 1) if hops in (1, 2, 3) else (0,):
            weight_term(jj, from_source(way, hops), done[hops] == 1, done[hops] == NZH)

    done = [0] * 5
    started = set()

    def xo_of(off):
        return mod(pair + off, NX)

    def multiply_all(jj):
        for off in (0, 1, 3, 2):
            multiply(jj, xo_of(off))

    def send_grad(jj):
        ga_stage[jj - 1] = acct[jj].astype(BF16)
        o = other(jj)
        rcopy(ga_stage.at[jj - 1], ga_in.at[slot_of(zh, o) - 1], ga_send, ga_recv, zh=o).start()

    relay(0)
    lax.fori_loop(0, 8, functools.partial(spread, lambda zd: zd < zh), jnp.int32(0))
    start_ring(0)
    relay(1)
    pass_on(0, 1)
    relay(2)
    send_att()
    start_ring(1)
    pass_on(0, 2)
    finish(0, 0)
    pass_on(1, 1)
    finish(0, 1)
    start_ring(2)
    finish(0, 2)
    pass_on(1, 2)
    pass_on(2, 1)
    rcopy(att.at[0], att.at[1], att_send, att_recv.at[0], zh=zh).wait_recv()
    finish(1, 0)
    finish(1, 1)
    pass_on(1, 3)
    finish(1, 2)
    pass_on(2, 2)
    rcopy(att.at[0], att.at[2], att_send, att_recv.at[1], zh=zh).wait_recv()
    finish(2, 0)
    finish(2, 1)
    pass_on(1, 4)
    rcopy(wt.at[0:3], wt.at[0:3], w_send, w_recv, x=x).wait_recv()
    finish(1, 3)
    pass_on(2, 3)
    finish(2, 2)
    pass_on(0, 3)
    finish(1, 4)
    multiply_all(1)
    send_grad(1)
    finish(0, 3)
    finish(2, 3)
    for off in (0, 1, 3):
        multiply(0, xo_of(off))
    pass_on(2, 4)
    finish(2, 4)
    multiply_all(2)
    send_grad(2)
    pass_on(0, 4)
    finish(0, 4)
    multiply(0, xo_of(2))

    for load in loads[5:]:
        load.wait()
    for half in (0, 1):
        piece = dw_in.at[:, half]
        rcopy(piece, piece, dw_send, dw_recv.at[half], x=x).wait_recv()
    for half in (0, 1):
        total = dwacc[2 * x + half]
        for rel in range(NX - 1):
            total = total + dw_in[rel, half].astype(F32)
        dwsum[pl.ds(HALF_ROWS * half, HALF_ROWS), :] = total
    for c, start, size in row_chunks():
        rows = pl.ds(start, size)
        grad = dwsum[rows, :]
        low_first = jnp.minimum(down(frow, start, size), fcol[...].reshape(1, HD))
        low_second = jnp.minimum(down(srow, start, size), scol[...].reshape(1, HD))
        first = fc[rows, :].astype(F32) * low_first
        second = sc[rows, :].astype(F32) * low_second
        first_new = beta_first * first + (1.0 - beta_first) * grad
        second_new = beta_second * second + (1.0 - beta_second) * grad * grad
        step_size = first_new / correct_first / (jnp.sqrt(second_new / correct_second) + adam_eps)
        weight = w[rows, :]
        nw_out[rows, :] = weight - learning * (step_size + decay_rate * weight)
        fnew_out[rows, :] = first_new
        snew_out[rows, :] = second_new

    first_abs, second_abs = jnp.abs(fnew_out[...]), jnp.abs(snew_out[...])
    st[0] = lane_rows(first_abs)
    st[1] = lane_rows(second_abs)
    for dy in range(1, NY):
        rcopy(st, y_in.at[NY - dy - 1], y_send, y_recv, y=mod(y + dy, NY)).start()
    cst[0, 0:1, :] = jnp.max(first_abs, axis=0, keepdims=True)
    cst[0, 1:2, :] = jnp.max(second_abs, axis=0, keepdims=True)
    for dx in range(1, NX):
        rcopy(cst.at[0], x_in.at[NX - dx - 1], x_send, x_recv, x=mod(x + dx, NX)).start()

    def back_rows(i):
        rows, cols = pl.ds(128 * i, 128), pl.ds(0, 128 * (i + 1))
        total = acct[0, :, rows]
        for s in range(2):
            total = total + ga_in[s, :, rows].astype(F32)
        grad_half = total.astype(BF16).T
        grad_probs = lax.dot_general(grad_half, vv[cols, :], NT, preferred_element_type=F32)
        row_dot = jnp.sum(
            grad_half.astype(F32) * att[0, rows, :].astype(F32), axis=-1, keepdims=True
        )
        grad_scores = (prob[rows, cols] * (grad_probs - row_dot)).astype(BF16)
        gq_out[rows, :] = (
            jnp.dot(grad_scores, kk[cols, :], preferred_element_type=F32) * SCALE
        ).astype(BF16)

    rcopy(x_in, x_in, x_send, x_recv, x=x).wait_recv()
    cst[1] = jnp.maximum(cst[0], jnp.max(x_in[...], axis=0))
    for slot in (1, 2):
        o = other(slot)
        rcopy(cst.at[1], zh_in.at[slot_of(zh, o) - 1], zh_send, zh_recv, zh=o).start()
    rcopy(y_in, y_in, y_send, y_recv, y=y).wait_recv()
    mine[...] = jnp.maximum(st[...], jnp.max(y_in[...], axis=0))
    for rel in range(1, NZL * NC):
        dl, dk = rel // NC, rel % NC
        back = NC * ((NZL - dl) % NZL) + dk - 1
        rcopy(
            mine, zl_in.at[back], zl_send, zl_recv, zl=mod(zl + dl, NZL), core=lax.rem(k + dk, NC)
        ).start()
    rcopy(ga_in, ga_in, ga_send, ga_recv, zh=zh).wait_recv()
    for i in range(3):
        back_rows(i)
    rcopy(zh_in, zh_in, zh_send, zh_recv, zh=zh).wait_recv()
    cols_out[...] = jnp.maximum(cst[1], jnp.max(zh_in[...], axis=0))
    rcopy(zl_in, zl_in, zl_send, zl_recv, zl=zl).wait_recv()
    rows_out[...] = jnp.maximum(mine[...], jnp.max(zl_in[...], axis=0))

    def units_left(sem, each, c):
        pieces = gz.at[0, 0:c, 0 : UNIT * each, :]
        rcopy(pieces, pieces, sem, w_recv, zl=zl).wait_send()

    wait_units(8 - stayed, 8, functools.partial(units_left, spread_send, 1))
    wait_units(landing, 6, functools.partial(units_left, relay_send, 9))
    for whole, sem in (
        (gz.at[:, 0:7], ring_send),
        (gz.at[:, 0:8], core_send),
        (att.at[0:2], att_send),
        (wt.at[0:3], w_send),
        (ga_in, ga_send),
        (dw_in, dw_send),
        (y_in, y_send),
        (zl_in, zl_send),
        (x_in, x_send),
        (zh_in, zh_send),
    ):
        rcopy(whole, whole, sem, w_recv, zl=zl).wait_send()


def codes(gq, nw, fnew, snew, rows, cols, gq_out, nw_out, nfc_out, nfr_out, nfcol_out, nsc_out, nsr_out, nscol_out):
    gq_out[...] = gq[...]
    nw_out[...] = nw[...]
    nfcol_out[...] = cols[0]
    nscol_out[...] = cols[1]
    for c, start, size in row_chunks():
        at = pl.ds(start, size)
        nfr_out[at] = rows[0, c, 0:size]
        nsr_out[at] = rows[1, c, 0:size]
        low_first = jnp.minimum(down_rows(rows[0, c : c + 1, :])[:size], cols[0:1])
        low_second = jnp.minimum(down_rows(rows[1, c : c + 1, :])[:size], cols[1:2])
        nfc_out[at, :] = (fnew[at, :] / (low_first + code_eps)).astype(BF16)
        nsc_out[at, :] = (snew[at, :] / (low_second + code_eps)).astype(BF16)


def per_device(queries, keys, values, grad_out, weight, fc, frow, fcol, sc, srow, scol):
    shape = jax.ShapeDtypeStruct
    vmem = pl.BlockSpec(memory_space=pltpu.VMEM)
    hbm = pl.BlockSpec(memory_space=pltpu.HBM)
    dma = pltpu.SemaphoreType.DMA
    gq, nw, fnew, snew, rows, cols = pl.pallas_call(
        body,
        name="whole",
        out_shape=(
            shape((SEQ, HD), BF16),
            shape((ROWS, HD), F32),
            shape((ROWS, HD), F32),
            shape((ROWS, HD), F32),
            shape((2, 8, HD), F32),
            shape((2, HD), F32),
        ),
        in_specs=[hbm] * 11,
        out_specs=[vmem] * 6,
        scratch_shapes=[
            pltpu.VMEM((SEQ, HD), BF16),
            pltpu.VMEM((SEQ, HD), BF16),
            pltpu.VMEM((SEQ, HD), BF16),
            pltpu.VMEM((SEQ, HD), BF16),
            pltpu.VMEM((ROWS, HD), F32),
            pltpu.VMEM((ROWS, HD), BF16),
            pltpu.VMEM((ROWS, HD), BF16),
            pltpu.VMEM((ROWS,), F32),
            pltpu.VMEM((HD,), F32),
            pltpu.VMEM((ROWS,), F32),
            pltpu.VMEM((HD,), F32),
            pltpu.VMEM((HD, SEQ), BF16),
            pltpu.VMEM((NZH, 4 * NX, QROWS, SEQ), BF16),
            pltpu.VMEM((NX, HD, ROWS), BF16),
            pltpu.VMEM((NZH, SEQ, HD), BF16),
            pltpu.VMEM((SEQ, SEQ), F32),
            pltpu.VMEM((NZH, HD, SEQ), F32),
            pltpu.VMEM((2, HD, SEQ), BF16),
            pltpu.VMEM((2, HD, SEQ), BF16),
            pltpu.VMEM((2 * NX, HALF_ROWS, HD), F32),
            pltpu.VMEM((2 * NX, HALF_ROWS, HD), BF16),
            pltpu.VMEM((NX - 1, 2, HALF_ROWS, HD), BF16),
            pltpu.VMEM((PADROWS, HD), F32),
            pltpu.VMEM((2, 8, HD), F32),
            pltpu.VMEM((NY - 1, 2, 8, HD), F32),
            pltpu.VMEM((NZL * NC - 1, 2, 8, HD), F32),
            pltpu.VMEM((2, 8, HD), F32),
            pltpu.VMEM((2, 2, HD), F32),
            pltpu.VMEM((NX - 1, 2, HD), F32),
            pltpu.VMEM((NZH - 1, 2, HD), F32),
            dma((11,)),
            dma,
            dma,
            dma((NZH,)),
            dma((NZH,)),
            dma,
            dma((2, NZH, 4)),
            dma,
            dma((NZH, 5)),
            dma,
            dma((2,)),
            dma,
            dma,
            dma,
            dma,
            dma,
            dma((2,)),
            dma,
            dma,
            dma,
            dma,
            dma,
            dma,
            dma,
            dma,
        ],
        compiler_params=pltpu.CompilerParams(
            collective_id=0, has_side_effects=True, vmem_limit_bytes=48 * 1024 * 1024
        ),
    )(
        *(
            pltpu.with_memory_space_constraint(a, pltpu.HBM)
            for a in (queries, keys, values, grad_out, weight, fc, frow, fcol, sc, srow, scol)
        )
    )
    return pl.pallas_call(
        codes,
        name="codes",
        out_shape=(
            shape((SEQ, HD), BF16),
            shape((ROWS, HD), F32),
            shape((ROWS, HD), BF16),
            shape((ROWS,), F32),
            shape((HD,), F32),
            shape((ROWS, HD), BF16),
            shape((ROWS,), F32),
            shape((HD,), F32),
        ),
        compiler_params=pltpu.CompilerParams(vmem_limit_bytes=8 * 1024 * 1024),
        in_specs=[vmem] * 6,
        out_specs=[vmem] * 8,
    )(gq, nw, fnew, snew, rows, cols)


def solution(mesh):
    finer = Mesh(mesh.devices.reshape(NX, NZH, NY, NZL, NC), AXES)
    placed = (
        P(DP, TENSOR),
        P(DP, None),
        P(DP, None),
        P(DP, TENSOR),
        P(DP, TENSOR),
        P(DP, TENSOR),
        P(DP),
        P(TENSOR),
        P(DP, TENSOR),
        P(DP),
        P(TENSOR),
    )
    return jax.shard_map(
        per_device,
        mesh=finer,
        in_specs=placed,
        out_specs=(
            P(DP, TENSOR),
            P(DP, TENSOR),
            P(DP, TENSOR),
            P(DP),
            P(TENSOR),
            P(DP, TENSOR),
            P(DP),
            P(TENSOR),
        ),
        check_vma=False,
    )
```

```python
import functools

import jax
import jax.numpy as jnp
from jax import lax
from jax.experimental import pallas as pl
from jax.experimental.pallas import tpu as pltpu
from jax.sharding import Mesh
from jax.sharding import PartitionSpec as P

NX, NZH, NY, NZL, NC = 4, 3, 8, 4, 2
AXES = ("x", "zh", "y", "zl", "core")
DP = ("x", "zh")
TENSOR = ("y", "zl", "core")
MESH = pl.DeviceIdType.MESH

HD = 128
SEQ = 384
ROWS = 688
UNIT = 16
UNITS = ROWS // UNIT
ALL_UNITS = 512
QUART = 11
QROWS = QUART * UNIT
PADROWS = 4 * QROWS
HALF_ROWS = 2 * QROWS
SCALE = HD ** (-0.5)

beta_first = 0.9
beta_second = 0.95
learning = 0.01
decay_rate = 0.1
adam_eps = 1e-08
code_eps = 1e-06
correct_first = 1.0 - 0.9**10
correct_second = 1.0 - 0.95**10

F32 = jnp.float32
BF16 = jnp.bfloat16
NT = (((1,), (1,)), ((), ()))


def mod(a, n):
    return lax.rem(a + n, n)


def row_chunks():
    return [(c, 128 * c, min(128, ROWS - 128 * c)) for c in range(6)]


def lane_rows(values):
    highest = jnp.max(values, axis=1, keepdims=True)
    out = []
    for c, start, size in row_chunks():
        eye = lax.broadcasted_iota(jnp.int32, (size, 128), 0) == lax.broadcasted_iota(
            jnp.int32, (size, 128), 1
        )
        out.append(
            jnp.max(jnp.where(eye, highest[start : start + size], 0.0), axis=0, keepdims=True)
        )
    out.append(jnp.zeros((2, 128), F32))
    return jnp.concatenate(out, axis=0)


def down(vector, start, size):
    row = vector[pl.ds(start, size)].reshape(1, size)
    if size < 128:
        row = jnp.concatenate([row, jnp.zeros((1, 128 - size), F32)], axis=1)
    return down_rows(row)[:size]


def down_rows(row):
    return jnp.broadcast_to(row, (128, 128)).T


def body(
    q_hbm,
    k_hbm,
    v_hbm,
    g_hbm,
    w_hbm,
    fc_hbm,
    frow_hbm,
    fcol_hbm,
    sc_hbm,
    srow_hbm,
    scol_hbm,
    gq_out,
    nw_out,
    fnew_out,
    snew_out,
    rows_out,
    cols_out,
    q,
    kk,
    vv,
    g,
    w,
    fc,
    sc,
    frow,
    fcol,
    srow,
    scol,
    gt,
    gz,
    wt,
    att,
    prob,
    own,
    gx_stage,
    gx_in,
    ga_stage,
    ga_in,
    dwacc,
    st,
    y_in,
    zl_in,
    mine,
    cst,
    x_in,
    zh_in,
    in_sem,
    spread_send,
    relay_send,
    far_recv,
    near_recv,
    ring_send,
    ring_recv,
    core_send,
    core_recv,
    att_send,
    att_recv,
    attx_send,
    attx_recv,
    gx_send,
    gx_recv,
    ga_send,
    ga_recv,
    y_send,
    y_recv,
    zl_send,
    zl_recv,
    x_send,
    x_recv,
    zh_send,
    zh_recv,
):
    x, zh, y, zl, k = (lax.axis_index(a) for a in AXES)
    t = 8 * y + 2 * zl + k
    pair = lax.div(y, 2)

    def rcopy(src, dst, send, recv, **dev):
        return pltpu.make_async_remote_copy(
            src_ref=src, dst_ref=dst, send_sem=send, recv_sem=recv, device_id=dev, device_id_type=MESH
        )

    def came(ref, recv):
        rcopy(ref, ref, core_send, recv, core=k).wait_recv()

    def slot_of(source, plane):
        return jnp.where(source == plane, 0, source + (source < plane).astype(jnp.int32))

    def other(slot):
        return slot - 1 + (slot - 1 >= zh).astype(jnp.int32)

    heads = pl.ds(pl.multiple_of(y * HD, HD), HD)
    loads = [
        pltpu.make_async_copy(src, dst, in_sem.at[i])
        for i, (src, dst) in enumerate(
            [
                (g_hbm, g),
                (q_hbm, q),
                (k_hbm.at[:, heads], kk),
                (v_hbm.at[:, heads], vv),
                (w_hbm, w),
                (fc_hbm, fc),
                (sc_hbm, sc),
                (frow_hbm, frow),
                (fcol_hbm, fcol),
                (srow_hbm, srow),
                (scol_hbm, scol),
            ]
        )
    ]
    for load in loads:
        load.start()

    home_pair = lax.rem(x + 2, NX)
    home_x = lax.rem(pair + 2, NX)
    across = lax.rem(zl + 2, NZL)

    barrier = pltpu.get_barrier_semaphore()

    def greet(**dev):
        pl.semaphore_signal(barrier, inc=1, device_id=dev, device_id_type=MESH)

    gives_over = (lax.rem(y, 2) == 0) & (y > 0) & (zl == 0) & (k == 0)
    takes_over = (x < NX - 1) & (zh == NZH - 1) & (lax.rem(y, 2) == 1) & (lax.rem(zl, 2) == 0) & (k == 1)
    for dz in (1, 2, 0):
        for half in (0, 1):
            for line in (zl, across):
                for dk in range(NC):
                    there = dict(zh=mod(zh + dz, NZH), zl=line, core=lax.rem(k + dk, NC))
                    greet(x=pair, y=2 * home_pair + half, **there)
                    greet(x=home_x, y=2 * x + half, **there)

    @pl.when(gives_over)
    def _():
        for line in (0, 2):
            greet(x=pair - 1, y=2 * home_pair + 1, zh=NZH - 1, zl=line, core=1)

    @pl.when(takes_over)
    def _():
        for z in range(NZH):
            greet(x=home_x, y=2 * x + 2, zh=z, zl=0, core=0)

    for dz in (1, 2):
        greet(zh=mod(zh + dz, NZH))
    for dx in range(1, NX):
        greet(x=mod(x + dx, NX))
    for dy in range(1, NY):
        greet(y=mod(y + dy, NY))
    for rel in range(1, NZL * NC):
        greet(zl=mod(zl + rel // NC, NZL), core=lax.rem(k + rel % NC, NC))
    greeted = 48 + 2 + 3 + 7 + 7 + 2 * gives_over.astype(jnp.int32) + 3 * takes_over.astype(jnp.int32)

    loads[0].wait()
    gt[...] = g[...].T

    my_q = 2 * lax.rem(y, 2) + k
    my_piece = 2 * y + k

    def unit_of(i):
        r = QUART * my_q + i
        unit = UNITS * (NZH * x + zh) + r
        return lax.div(unit, 8), lax.rem(unit, 8), (r < UNITS) & (unit < ALL_UNITS)

    def rows_of(i):
        return pl.ds(pl.multiple_of(UNIT * i, UNIT), UNIT)

    for i in range(QUART):

        @pl.when(jnp.logical_not(unit_of(i)[2]))
        def _():
            for jj in range(NZH):
                gz[jj, my_piece, rows_of(i), :] = jnp.zeros((UNIT, SEQ), BF16)

    pl.semaphore_wait(barrier, greeted)

    def spread(wanted, u, carry):
        unit = 8 * t + u
        d = lax.div(unit, UNITS)
        r = unit - UNITS * d
        quarter = lax.div(r, QUART)
        i = r - QUART * quarter
        zd = lax.rem(d, NZH)
        slot = slot_of(zh, zd)

        @pl.when(wanted(zd))
        def _():
            rcopy(
                gt.at[rows_of(u), :],
                gz.at[slot, 4 * home_pair + quarter, rows_of(i), :],
                spread_send,
                far_recv.at[slot],
                x=lax.div(d, NZH),
                zh=zd,
                y=2 * home_pair + lax.div(quarter, 2),
                zl=lax.rem(zl + 2 * lax.rem(u, 2), NZL),
                core=lax.rem(quarter, 2),
            ).start()

        return carry

    def spread_where(wanted):
        lax.fori_loop(0, 8, functools.partial(spread, wanted), 0)

    spread_where(lambda zd: zd == zh)
    spread_where(lambda zd: zd > zh)

    for i in (1, 2, 3):
        loads[i].wait()
    for i in range(3):
        rows, cols = pl.ds(128 * i, 128), pl.ds(0, 128 * (i + 1))
        scores = (
            lax.dot_general(q[rows, :], kk[cols, :], NT, preferred_element_type=F32) * SCALE
        )
        future = lax.broadcasted_iota(jnp.int32, scores.shape, 1) > (
            lax.broadcasted_iota(jnp.int32, scores.shape, 0) + 128 * i
        )
        scores = jnp.where(future, -1e30, scores)
        exponent = jnp.exp(scores - jnp.max(scores, axis=-1, keepdims=True))
        probabilities = exponent / jnp.sum(exponent, axis=-1, keepdims=True)
        prob[rows, cols] = probabilities
        att[0, x, rows, :] = jnp.dot(
            probabilities.astype(BF16), vv[cols, :], preferred_element_type=F32
        ).astype(BF16)

    def send_att():
        for slot in (1, 2):
            o = other(slot)
            there = slot_of(zh, o)
            rcopy(att.at[0, x], att.at[there, x], att_send, att_recv.at[there - 1], zh=o).start()

    def att_over_x(slot):
        if slot > 0:
            came(att.at[slot, x], att_recv.at[slot - 1])
        for dx in (1, 3, 2):
            rcopy(
                att.at[slot, x], att.at[slot, x], attx_send, attx_recv.at[slot], x=mod(x + dx, NX)
            ).start()

    def att_ready(slot):
        came(att.at[slot, 0:3], attx_recv.at[slot])

    def wait_units(n, most, wait):
        for c in range(1, most + 1):
            pl.when(n == c)(functools.partial(wait, c))

    def lands_here(i):
        source, u, there = unit_of(i)
        from_zl = lax.rem(lax.div(source, 2), NZL)
        here = lax.rem(from_zl + 2 * lax.rem(u, 2), NZL) == zl
        return there & here, there & jnp.logical_not(here)

    landing = sum(lands_here(i)[0].astype(jnp.int32) for i in range(QUART))
    coming = sum(lands_here(i)[1].astype(jnp.int32) for i in range(QUART))

    def units_came(recv, c):
        came(gz.at[0, 0, 0 : UNIT * c, :], recv)

    def relay(jj):
        wait_units(landing, 6, functools.partial(units_came, far_recv.at[jj]))

        def give(i, carry):
            piece = gz.at[jj, my_piece, rows_of(i), :]

            @pl.when(lands_here(i)[0])
            def _():
                for dl in (1, 3, 2):
                    rcopy(piece, piece, relay_send, near_recv.at[jj], zl=mod(zl + dl, NZL)).start()

            return carry

        lax.fori_loop(0, QUART, give, 0)

    PARTS = ((0, 96), (96, QROWS - 96))

    def reach(way, jj, part):
        return 4 if way == (part if jj == 0 else jj - 1) else 3

    def piece_of(jj, source, part):
        start, size = PARTS[part]
        return gz.at[jj, 2 * source + k, pl.ds(start, size), :]

    def from_source(way, hops):
        return mod(y - hops, NY) if way == 0 else mod(y + hops, NY)

    def forward(way, jj, hops, part):
        piece = piece_of(jj, from_source(way, hops), part)
        rcopy(
            piece,
            piece,
            ring_send,
            ring_recv.at[way, jj, hops, part],
            y=mod(y + 1, NY) if way == 0 else mod(y - 1, NY),
        ).start()

    def to_partner(way, jj, hops, part):
        piece = piece_of(jj, from_source(way, hops), part)
        rcopy(piece, piece, core_send, core_recv.at[jj, hops], core=1 - k).start()

    def start_ring(jj):
        wait_units(coming, QUART, functools.partial(units_came, near_recv.at[jj]))
        for part in (0, 1):
            for way in (0, 1):
                forward(way, jj, 0, part)
        for part in (0, 1):
            to_partner(0, jj, 0, part)

    def pass_on(jj, hops):
        for part in (0, 1):
            for way in (0, 1):
                if hops <= reach(way, jj, part):
                    came(
                        piece_of(jj, from_source(way, hops), part),
                        ring_recv.at[way, jj, hops - 1, part],
                    )
                    if hops < reach(way, jj, part):
                        forward(way, jj, hops, part)
                    to_partner(way, jj, hops, part)

    def partner_has(jj, hops):
        came(gz.at[0, 0 : 2 if hops in (1, 2, 3) else 1], core_recv.at[jj, hops])

    def weight_term(jj, source):
        block = gz[jj, pl.ds(2 * source, 2)].reshape(HALF_ROWS, SEQ)
        sequence = lax.rem(lax.div(source, 2) + 2, NX)
        term = jnp.dot(block, att[jj, sequence], preferred_element_type=F32)
        rows = pl.ds(pl.multiple_of(HALF_ROWS * lax.rem(source, 2), UNIT), HALF_ROWS)
        dwacc[rows, :] = dwacc[rows, :] + term

    def finish(jj, hops):
        for way in (0, 1) if hops in (1, 2, 3) else (0,):
            weight_term(jj, from_source(way, hops))

    def multiply(jj, off):
        p = mod(pair + off, NX)
        sequence = lax.rem(p + 2, NX)
        block = gz[jj, pl.ds(4 * p, 4)].reshape(PADROWS, SEQ)[:ROWS]
        share = jnp.dot(wt[...], block, preferred_element_type=F32)

        @pl.when(sequence == x)
        def _():
            own[jj] = share

        @pl.when(sequence != x)
        def _():
            gx_stage[jj, sequence] = share.astype(BF16)
            rel = mod(x - sequence, NX) - 1
            rcopy(
                gx_stage.at[jj, sequence], gx_in.at[jj, rel], gx_send, gx_recv.at[jj], x=sequence
            ).start()

    def over_x(jj):
        came(gx_in.at[jj], gx_recv.at[jj])
        total = own[jj]
        for rel in range(NX - 1):
            total = total + gx_in[jj, rel].astype(F32)
        if jj == 0:
            own[0] = total
        else:
            ga_stage[jj - 1] = total.astype(BF16)
            o = other(jj)
            rcopy(ga_stage.at[jj - 1], ga_in.at[slot_of(zh, o) - 1], ga_send, ga_recv, zh=o).start()

    att_over_x(0)
    relay(0)
    spread_where(lambda zd: zd < zh)

    loads[4].wait()
    wt[...] = w[...].astype(BF16).T
    dwacc[...] = jnp.zeros_like(dwacc)

    start_ring(0)
    relay(1)
    send_att()
    pass_on(0, 1)
    start_ring(1)
    relay(2)
    att_ready(0)
    partner_has(0, 0)
    finish(0, 0)
    pass_on(1, 1)
    partner_has(0, 1)
    finish(0, 1)
    start_ring(2)
    multiply(0, 0)
    pass_on(1, 2)
    att_over_x(1)
    att_over_x(2)
    pass_on(2, 1)
    for hops in (0, 1, 2):
        partner_has(1, hops)
    pass_on(1, 3)
    multiply(1, 0)
    pass_on(2, 2)
    partner_has(1, 3)
    multiply(1, 1)
    multiply(1, 3)
    pass_on(1, 4)
    pass_on(2, 3)
    partner_has(1, 4)
    multiply(1, 2)
    for hops in (0, 1, 2):
        partner_has(2, hops)
    multiply(2, 0)
    pass_on(0, 2)
    partner_has(2, 3)
    multiply(2, 1)
    multiply(2, 3)
    pass_on(2, 4)
    partner_has(2, 4)
    multiply(2, 2)
    att_ready(1)
    for hops in range(3):
        finish(1, hops)
    pass_on(0, 3)
    over_x(1)
    for hops in (3, 4):
        finish(1, hops)
    att_ready(2)
    for hops in range(5):
        finish(2, hops)
    partner_has(0, 2)
    finish(0, 2)
    partner_has(0, 3)
    finish(0, 3)
    over_x(2)
    multiply(0, 1)
    multiply(0, 3)
    pass_on(0, 4)
    partner_has(0, 4)
    finish(0, 4)
    multiply(0, 2)

    for load in loads[5:]:
        load.wait()
    for c, start, size in row_chunks():
        rows = pl.ds(start, size)
        grad = dwacc[rows, :]
        low_first = jnp.minimum(down(frow, start, size), fcol[...].reshape(1, HD))
        low_second = jnp.minimum(down(srow, start, size), scol[...].reshape(1, HD))
        first = fc[rows, :].astype(F32) * low_first
        second = sc[rows, :].astype(F32) * low_second
        first_new = beta_first * first + (1.0 - beta_first) * grad
        second_new = beta_second * second + (1.0 - beta_second) * grad * grad
        step_size = first_new / correct_first / (jnp.sqrt(second_new / correct_second) + adam_eps)
        weight = w[rows, :]
        nw_out[rows, :] = weight - learning * (step_size + decay_rate * weight)
        fnew_out[rows, :] = first_new
        snew_out[rows, :] = second_new

    first_abs, second_abs = jnp.abs(fnew_out[...]), jnp.abs(snew_out[...])
    st[0] = lane_rows(first_abs)
    st[1] = lane_rows(second_abs)
    for dy in range(1, NY):
        rcopy(st, y_in.at[NY - dy - 1], y_send, y_recv, y=mod(y + dy, NY)).start()
    cst[0, 0:1, :] = jnp.max(first_abs, axis=0, keepdims=True)
    cst[0, 1:2, :] = jnp.max(second_abs, axis=0, keepdims=True)
    for dx in range(1, NX):
        rcopy(cst.at[0], x_in.at[NX - dx - 1], x_send, x_recv, x=mod(x + dx, NX)).start()

    def back_rows(i):
        rows, cols = pl.ds(128 * i, 128), pl.ds(0, 128 * (i + 1))
        total = own[0, :, rows]
        for s in range(2):
            total = total + ga_in[s, :, rows].astype(F32)
        grad_half = total.astype(BF16).T
        grad_probs = lax.dot_general(grad_half, vv[cols, :], NT, preferred_element_type=F32)
        row_dot = jnp.sum(
            grad_half.astype(F32) * att[0, x, rows, :].astype(F32), axis=-1, keepdims=True
        )
        grad_scores = (prob[rows, cols] * (grad_probs - row_dot)).astype(BF16)
        gq_out[rows, :] = (
            jnp.dot(grad_scores, kk[cols, :], preferred_element_type=F32) * SCALE
        ).astype(BF16)

    came(y_in, y_recv)
    mine[...] = jnp.maximum(st[...], jnp.max(y_in[...], axis=0))
    for rel in range(1, NZL * NC):
        dl, dk = rel // NC, rel % NC
        back = NC * ((NZL - dl) % NZL) + dk - 1
        rcopy(
            mine, zl_in.at[back], zl_send, zl_recv, zl=mod(zl + dl, NZL), core=lax.rem(k + dk, NC)
        ).start()
    came(x_in, x_recv)
    cst[1] = jnp.maximum(cst[0], jnp.max(x_in[...], axis=0))
    for slot in (1, 2):
        o = other(slot)
        rcopy(cst.at[1], zh_in.at[slot_of(zh, o) - 1], zh_send, zh_recv, zh=o).start()
    over_x(0)
    came(ga_in, ga_recv)
    for i in range(3):
        back_rows(i)
    came(zl_in, zl_recv)
    rows_out[...] = jnp.maximum(mine[...], jnp.max(zl_in[...], axis=0))
    came(zh_in, zh_recv)
    cols_out[...] = jnp.maximum(cst[1], jnp.max(zh_in[...], axis=0))

    def left(ref, send):
        rcopy(ref, ref, send, zh_recv, core=k).wait_send()

    left(gz.at[0, 0, 0 : UNIT * 8, :], spread_send)
    wait_units(
        landing, 6, lambda c: left(gz.at[0, 0:c, 0 : UNIT * NZH * (NZL - 1), :], relay_send)
    )
    for whole, send in (
        (gz.at[:, 0:7], ring_send),
        (gz.at[:, 0:8], core_send),
        (att.at[0, 0:2], att_send),
        (att.at[:, 0:3], attx_send),
        (gx_in, gx_send),
        (ga_in, ga_send),
        (y_in, y_send),
        (zl_in, zl_send),
        (x_in, x_send),
        (zh_in, zh_send),
    ):
        left(whole, send)


def codes(gq, nw, fnew, snew, rows, cols, gq_out, nw_out, nfc_out, nfr_out, nfcol_out, nsc_out, nsr_out, nscol_out):
    gq_out[...] = gq[...]
    nw_out[...] = nw[...]
    nfcol_out[...] = cols[0]
    nscol_out[...] = cols[1]
    for c, start, size in row_chunks():
        at = pl.ds(start, size)
        nfr_out[at] = rows[0, c, 0:size]
        nsr_out[at] = rows[1, c, 0:size]
        low_first = jnp.minimum(down_rows(rows[0, c : c + 1, :])[:size], cols[0:1])
        low_second = jnp.minimum(down_rows(rows[1, c : c + 1, :])[:size], cols[1:2])
        nfc_out[at, :] = (fnew[at, :] / (low_first + code_eps)).astype(BF16)
        nsc_out[at, :] = (snew[at, :] / (low_second + code_eps)).astype(BF16)


def per_device(queries, keys, values, grad_out, weight, fc, frow, fcol, sc, srow, scol):
    shape = jax.ShapeDtypeStruct
    vmem = pl.BlockSpec(memory_space=pltpu.VMEM)
    hbm = pl.BlockSpec(memory_space=pltpu.HBM)
    dma = pltpu.SemaphoreType.DMA
    gq, nw, fnew, snew, rows, cols = pl.pallas_call(
        body,
        name="whole",
        out_shape=(
            shape((SEQ, HD), BF16),
            shape((ROWS, HD), F32),
            shape((ROWS, HD), F32),
            shape((ROWS, HD), F32),
            shape((2, 8, HD), F32),
            shape((2, HD), F32),
        ),
        in_specs=[hbm] * 11,
        out_specs=[vmem] * 6,
        scratch_shapes=[
            pltpu.VMEM((SEQ, HD), BF16),
            pltpu.VMEM((SEQ, HD), BF16),
            pltpu.VMEM((SEQ, HD), BF16),
            pltpu.VMEM((SEQ, HD), BF16),
            pltpu.VMEM((ROWS, HD), F32),
            pltpu.VMEM((ROWS, HD), BF16),
            pltpu.VMEM((ROWS, HD), BF16),
            pltpu.VMEM((ROWS,), F32),
            pltpu.VMEM((HD,), F32),
            pltpu.VMEM((ROWS,), F32),
            pltpu.VMEM((HD,), F32),
            pltpu.VMEM((HD, SEQ), BF16),
            pltpu.VMEM((NZH, 4 * NX, QROWS, SEQ), BF16),
            pltpu.VMEM((HD, ROWS), BF16),
            pltpu.VMEM((NZH, NX, SEQ, HD), BF16),
            pltpu.VMEM((SEQ, SEQ), F32),
            pltpu.VMEM((NZH, HD, SEQ), F32),
            pltpu.VMEM((NZH, NX, HD, SEQ), BF16),
            pltpu.VMEM((NZH, NX - 1, HD, SEQ), BF16),
            pltpu.VMEM((2, HD, SEQ), BF16),
            pltpu.VMEM((2, HD, SEQ), BF16),
            pltpu.VMEM((PADROWS, HD), F32),
            pltpu.VMEM((2, 8, HD), F32),
            pltpu.VMEM((NY - 1, 2, 8, HD), F32),
            pltpu.VMEM((NZL * NC - 1, 2, 8, HD), F32),
            pltpu.VMEM((2, 8, HD), F32),
            pltpu.VMEM((2, 2, HD), F32),
            pltpu.VMEM((NX - 1, 2, HD), F32),
            pltpu.VMEM((NZH - 1, 2, HD), F32),
            dma((11,)),
            dma,
            dma,
            dma((NZH,)),
            dma((NZH,)),
            dma,
            dma((2, NZH, 4, 2)),
            dma,
            dma((NZH, 5)),
            dma,
            dma((2,)),
            dma,
            dma((NZH,)),
            dma,
            dma((NZH,)),
            dma,
            dma,
            dma,
            dma,
            dma,
            dma,
            dma,
            dma,
            dma,
            dma,
        ],
        compiler_params=pltpu.CompilerParams(
            collective_id=0, has_side_effects=True, vmem_limit_bytes=48 * 1024 * 1024
        ),
    )(
        *(
            pltpu.with_memory_space_constraint(a, pltpu.HBM)
            for a in (queries, keys, values, grad_out, weight, fc, frow, fcol, sc, srow, scol)
        )
    )
    return pl.pallas_call(
        codes,
        name="codes",
        out_shape=(
            shape((SEQ, HD), BF16),
            shape((ROWS, HD), F32),
            shape((ROWS, HD), BF16),
            shape((ROWS,), F32),
            shape((HD,), F32),
            shape((ROWS, HD), BF16),
            shape((ROWS,), F32),
            shape((HD,), F32),
        ),
        compiler_params=pltpu.CompilerParams(vmem_limit_bytes=8 * 1024 * 1024),
        in_specs=[vmem] * 6,
        out_specs=[vmem] * 8,
    )(gq, nw, fnew, snew, rows, cols)


def solution(mesh):
    finer = Mesh(mesh.devices.reshape(NX, NZH, NY, NZL, NC), AXES)
    placed = (
        P(DP, TENSOR),
        P(DP, None),
        P(DP, None),
        P(DP, TENSOR),
        P(DP, TENSOR),
        P(DP, TENSOR),
        P(DP),
        P(TENSOR),
        P(DP, TENSOR),
        P(DP),
        P(TENSOR),
    )
    return jax.shard_map(
        per_device,
        mesh=finer,
        in_specs=placed,
        out_specs=(
            P(DP, TENSOR),
            P(DP, TENSOR),
            P(DP, TENSOR),
            P(DP),
            P(TENSOR),
            P(DP, TENSOR),
            P(DP),
            P(TENSOR),
        ),
        check_vma=False,
    )
```

```python
import functools

import jax
import jax.numpy as jnp
from jax import lax
from jax.experimental import pallas as pl
from jax.experimental.pallas import tpu as pltpu
from jax.sharding import Mesh
from jax.sharding import PartitionSpec as P

NX, NZH, NY, NZL, NC = 4, 3, 8, 4, 2
AXES = ("x", "zh", "y", "zl", "core")
DP = ("x", "zh")
TENSOR = ("y", "zl", "core")
MESH = pl.DeviceIdType.MESH

HD = 128
SEQ = 384
ROWS = 688
UNIT = 16
UNITS = ROWS // UNIT
ALL_UNITS = 512
HOMES = NY * NC
SLOTS = 4
SLOT = 3 * UNITS
SCALE = HD ** (-0.5)

beta_first = 0.9
beta_second = 0.95
learning = 0.01
decay_rate = 0.1
adam_eps = 1e-08
code_eps = 1e-06
correct_first = 1.0 - 0.9**10
correct_second = 1.0 - 0.95**10

F32 = jnp.float32
BF16 = jnp.bfloat16
NT = (((1,), (1,)), ((), ()))


def mod(a, n):
    return lax.rem(a + n, n)


def row_chunks():
    return [(c, 128 * c, min(128, ROWS - 128 * c)) for c in range(6)]


def lane_rows(values):
    highest = jnp.max(values, axis=1, keepdims=True)
    out = []
    for c, start, size in row_chunks():
        eye = lax.broadcasted_iota(jnp.int32, (size, 128), 0) == lax.broadcasted_iota(
            jnp.int32, (size, 128), 1
        )
        out.append(
            jnp.max(jnp.where(eye, highest[start : start + size], 0.0), axis=0, keepdims=True)
        )
    out.append(jnp.zeros((2, 128), F32))
    return jnp.concatenate(out, axis=0)


def down(vector, start, size):
    row = vector[pl.ds(start, size)].reshape(1, size)
    if size < 128:
        row = jnp.concatenate([row, jnp.zeros((1, 128 - size), F32)], axis=1)
    return down_rows(row)[:size]


def down_rows(row):
    return jnp.broadcast_to(row, (128, 128)).T


def body(
    q_hbm,
    k_hbm,
    v_hbm,
    g_hbm,
    w_hbm,
    fc_hbm,
    frow_hbm,
    fcol_hbm,
    sc_hbm,
    srow_hbm,
    scol_hbm,
    gq_out,
    nw_out,
    fnew_out,
    snew_out,
    rows_out,
    cols_out,
    q,
    kk,
    vv,
    g,
    w,
    fc,
    sc,
    frow,
    fcol,
    srow,
    scol,
    gt,
    gz,
    wt,
    att,
    prob,
    acct,
    ga_stage,
    ga_in,
    dwacc,
    dw_stage,
    dw_in,
    st,
    y_in,
    zl_in,
    mine,
    cst,
    x_in,
    zh_in,
    in_sem,
    spread_send,
    relay_send,
    far_recv,
    near_recv,
    ring_send,
    ring_recv,
    core_send,
    core_recv,
    att_send,
    att_recv,
    w_send,
    w_recv,
    ga_send,
    ga_recv,
    dw_send,
    dw_recv,
    y_send,
    y_recv,
    zl_send,
    zl_recv,
    x_send,
    x_recv,
    zh_send,
    zh_recv,
):
    x, zh, y, zl, k = (lax.axis_index(a) for a in AXES)
    t = 8 * y + 2 * zl + k
    pair = lax.div(y, 2)

    def rcopy(src, dst, send, recv, **dev):
        return pltpu.make_async_remote_copy(
            src_ref=src, dst_ref=dst, send_sem=send, recv_sem=recv, device_id=dev, device_id_type=MESH
        )

    def came(ref, recv):
        rcopy(ref, ref, core_send, recv, core=k).wait_recv()

    def sequence_of(source, plane):
        return jnp.where(source == plane, 0, source + (source < plane).astype(jnp.int32))

    def other(sequence):
        return sequence - 1 + (sequence - 1 >= zh).astype(jnp.int32)

    heads = pl.ds(pl.multiple_of(y * HD, HD), HD)
    loads = [
        pltpu.make_async_copy(src, dst, in_sem.at[i])
        for i, (src, dst) in enumerate(
            [
                (g_hbm, g),
                (q_hbm, q),
                (k_hbm.at[:, heads], kk),
                (v_hbm.at[:, heads], vv),
                (w_hbm, w),
                (fc_hbm, fc),
                (sc_hbm, sc),
                (frow_hbm, frow),
                (fcol_hbm, fcol),
                (srow_hbm, srow),
                (scol_hbm, scol),
            ]
        )
    ]
    for load in loads:
        load.start()

    me = 2 * y + k

    def rows_of(u):
        return pl.ds(pl.multiple_of(UNIT * u, UNIT), UNIT)

    def goes_to(u):
        unit = 8 * t + u
        d = lax.div(unit, UNITS)
        xd, zd = lax.div(d, NZH), lax.rem(d, NZH)
        ahead = mod(xd - x, NX)
        sequence = sequence_of(zh, zd)
        turn = 2 * (ahead - 1) + sequence - 1
        slot = jnp.where(ahead == 0, 3, jnp.where(sequence == 0, 0, 1 + lax.div(turn + 3, 3) - 1))
        index = jnp.where(
            ahead == 0,
            lax.rem(sequence + 2, 3),
            jnp.where(sequence == 0, ahead - 1, lax.rem(turn + 3, 3)),
        )
        e = UNITS * index + unit - UNITS * d
        h = jnp.minimum(lax.div(e, 8), HOMES - 1)
        home = dict(
            zh=zd,
            y=lax.div(h, 2),
            zl=lax.rem(zl + 2 * lax.rem(u, 2), NZL),
            core=lax.rem(h, 2),
        )
        here = (zd == zh) & (h == me) & (home["zl"] == zl)
        return slot, SLOT * slot + e, home, here

    def unit_of(slot, j):
        e = 8 * me + j
        index, r = lax.div(e, UNITS), lax.rem(e, UNITS)
        if slot == 0:
            xd, z = mod(x + 1 + index, NX), zh
        elif slot == 3:
            xd, z = x, jnp.where(index == 2, zh, other(index + 1))
        else:
            turn = 3 * (slot - 1) + index
            xd, z = mod(x + 1 + lax.div(turn, 2), NX), other(1 + lax.rem(turn, 2))
        unit = UNITS * (NZH * xd + zh) + r
        mine_too = (j < 8) | (me == HOMES - 1)
        return z, lax.div(unit, 8), lax.rem(unit, 8), mine_too & (unit < ALL_UNITS), mine_too

    def lands_here(slot, j):
        z, column, u, there, _ = unit_of(slot, j)
        line = lax.rem(lax.rem(lax.div(column, 2), NZL) + 2 * lax.rem(u, 2), NZL)
        return there & (line == zl), there & (line != zl), (z == zh) & (column == t)

    def count(flags):
        return sum(f.astype(jnp.int32) for f in flags)

    landing = [count(lands_here(s, j)[0] for j in range(9)) for s in range(SLOTS)]
    coming = [count(lands_here(s, j)[1] for j in range(9)) for s in range(SLOTS)]
    staying = [
        count(lands_here(s, j)[0] & lands_here(s, j)[2] for j in range(9)) for s in range(SLOTS)
    ]

    barrier = pltpu.get_barrier_semaphore()

    def greet(**dev):
        pl.semaphore_signal(barrier, inc=1, device_id=dev, device_id_type=MESH)

    def greet_home(u, carry):
        slot, place, home, here = goes_to(u)
        pl.when(jnp.logical_not(here))(functools.partial(greet, **home))
        return carry

    def greet_sources(slot, j, carry):
        z, column, u, there, _ = unit_of(slot, j)
        lands, _, same = lands_here(slot, j)

        @pl.when(lands & jnp.logical_not(same))
        def _():
            greet(zh=z, y=lax.div(column, 8), zl=lax.rem(lax.div(column, 2), NZL), core=lax.rem(column, 2))

        return carry

    lax.fori_loop(0, 8, greet_home, 0)
    for slot in range(SLOTS):
        lax.fori_loop(0, 9, functools.partial(greet_sources, slot), 0)
    for dz in (1, 2):
        greet(zh=mod(zh + dz, NZH))
    for dx in range(1, NX):
        greet(x=mod(x + dx, NX))
    for dy in range(1, NY):
        greet(y=mod(y + dy, NY))
    for rel in range(1, NZL * NC):
        greet(zl=mod(zl + rel // NC, NZL), core=lax.rem(k + rel % NC, NC))
    greeted = 8 + sum(landing) - 2 * sum(staying) + 2 + 3 + 7 + 7

    loads[0].wait()
    gt[...] = g[...].T

    for slot in range(SLOTS):

        def clear(j, carry):
            _, _, _, there, mine_too = unit_of(slot, j)

            @pl.when(mine_too & jnp.logical_not(there))
            def _():
                gz[SLOT * slot + 8 * me + j] = jnp.zeros((UNIT, SEQ), BF16)

            return carry

        lax.fori_loop(0, 9, clear, 0)

    pl.semaphore_wait(barrier, greeted)

    def spread(wanted, u, carry):
        slot, place, home, here = goes_to(u)

        @pl.when((slot == wanted) & here)
        def _():
            gz[place] = gt[rows_of(u), :]

        @pl.when((slot == wanted) & jnp.logical_not(here))
        def _():
            rcopy(gt.at[rows_of(u), :], gz.at[place], spread_send, far_recv.at[slot], **home).start()

        return carry

    for slot in range(SLOTS):
        lax.fori_loop(0, 8, functools.partial(spread, slot), 0)

    loads[4].wait()
    wt[3] = w[...].astype(BF16).T
    for dx in (1, 3, 2):
        rcopy(wt.at[3], wt.at[NX - 1 - dx], w_send, w_recv, x=mod(x + dx, NX)).start()

    for i in (1, 2, 3):
        loads[i].wait()
    for i in range(3):
        rows, cols = pl.ds(128 * i, 128), pl.ds(0, 128 * (i + 1))
        scores = (
            lax.dot_general(q[rows, :], kk[cols, :], NT, preferred_element_type=F32) * SCALE
        )
        future = lax.broadcasted_iota(jnp.int32, scores.shape, 1) > (
            lax.broadcasted_iota(jnp.int32, scores.shape, 0) + 128 * i
        )
        scores = jnp.where(future, -1e30, scores)
        exponent = jnp.exp(scores - jnp.max(scores, axis=-1, keepdims=True))
        probabilities = exponent / jnp.sum(exponent, axis=-1, keepdims=True)
        prob[rows, cols] = probabilities
        att[0, rows, :] = jnp.dot(
            probabilities.astype(BF16), vv[cols, :], preferred_element_type=F32
        ).astype(BF16)

    def send_att():
        for sequence in (1, 2):
            o = other(sequence)
            there = sequence_of(zh, o)
            rcopy(att.at[0], att.at[there], att_send, att_recv.at[there - 1], zh=o).start()

    def wait_units(n, most, wait):
        for c in range(1, most + 1):
            pl.when(n == c)(functools.partial(wait, c))

    def units_came(recv, c):
        came(gz.at[0:c], recv)

    def relay(slot):
        wait_units(
            landing[slot] - staying[slot], 9, functools.partial(units_came, far_recv.at[slot])
        )

        def give(j, carry):
            piece = gz.at[SLOT * slot + 8 * me + j]

            @pl.when(lands_here(slot, j)[0])
            def _():
                for dl in (1, 3, 2):
                    rcopy(
                        piece, piece, relay_send.at[slot], near_recv.at[slot], zl=mod(zl + dl, NZL)
                    ).start()

            return carry

        lax.fori_loop(0, 9, give, 0)

    def reach(way, slot):
        return 4 if way == slot % 2 else 3

    def from_source(way, hops):
        return mod(y - hops, NY) if way == 0 else mod(y + hops, NY)

    def parts_of(slot, source, core):
        start = SLOT * slot + 8 * (2 * source + core)
        last = (source == NY - 1) & (core == 1)
        return (
            ((start, 4, None),),
            ((start + 4, 4, jnp.logical_not(last)), (start + 4, 5, last)),
        )

    def each_size(sizes, act):
        for start, units, when in sizes:
            ref = gz.at[pl.ds(start, units)]
            if when is None:
                act(ref)
            else:
                pl.when(when)(functools.partial(act, ref))

    def forward(way, slot, hops, part):
        def go(piece):
            rcopy(
                piece,
                piece,
                ring_send,
                ring_recv.at[way, slot, hops, part],
                y=mod(y + 1, NY) if way == 0 else mod(y - 1, NY),
            ).start()

        each_size(parts_of(slot, from_source(way, hops), k)[part], go)

    def to_partner(way, slot, hops, part):
        def go(piece):
            rcopy(piece, piece, core_send, core_recv.at[way, slot, hops], core=1 - k).start()

        each_size(parts_of(slot, from_source(way, hops), k)[part], go)

    def start_ring(slot):
        wait_units(coming[slot], 9, functools.partial(units_came, near_recv.at[slot]))
        for part in (0, 1):
            for way in (0, 1):
                forward(way, slot, 0, part)
        for part in (0, 1):
            to_partner(0, slot, 0, part)

    def pass_on(slot, hops):
        for part in (0, 1):
            for way in (0, 1):
                if hops <= reach(way, slot):
                    each_size(
                        parts_of(slot, from_source(way, hops), k)[part],
                        lambda piece: came(piece, ring_recv.at[way, slot, hops - 1, part]),
                    )
                    if hops < reach(way, slot):
                        forward(way, slot, hops, part)
                    to_partner(way, slot, hops, part)

    def partner_has(slot):
        for hops in range(5):
            for way in (0, 1):
                if (hops > 0 or way == 0) and hops <= reach(way, slot):
                    last = (from_source(way, hops) == NY - 1) & (k == 0)
                    recv = core_recv.at[way, slot, hops]
                    pl.when(last)(functools.partial(came, gz.at[0:9], recv))
                    pl.when(jnp.logical_not(last))(functools.partial(came, gz.at[0:8], recv))

    def block_of(slot, index):
        return gz[pl.ds(SLOT * slot + UNITS * index, UNITS)].reshape(ROWS, SEQ)

    def member(slot, index):
        if slot == 0:
            return index, 0
        if slot == 3:
            return 3, (index + 1) % 3
        turn = 3 * (slot - 1) + index
        return turn // 2, 1 + turn % 2

    started = set()

    def weight_term(slot, index):
        rows, sequence = member(slot, index)
        term = jnp.dot(block_of(slot, index), att[sequence], preferred_element_type=F32)
        dwacc[rows] = dwacc[rows] + term if ("w", rows) in started else term
        started.add(("w", rows))

    def multiply(slot, index):
        rows, sequence = member(slot, index)
        term = jnp.dot(wt[rows], block_of(slot, index), preferred_element_type=F32)
        acct[sequence] = acct[sequence] + term if ("g", sequence) in started else term
        started.add(("g", sequence))

    def send_term(rows):
        dw_stage[rows] = dwacc[rows].astype(BF16)
        rcopy(
            dw_stage.at[rows], dw_in.at[NX - 2 - rows], dw_send, dw_recv, x=mod(x + 1 + rows, NX)
        ).start()

    def send_grad(sequence):
        ga_stage[sequence - 1] = acct[sequence].astype(BF16)
        o = other(sequence)
        rcopy(
            ga_stage.at[sequence - 1], ga_in.at[sequence_of(zh, o) - 1], ga_send, ga_recv, zh=o
        ).start()

    relay(0)
    start_ring(0)
    relay(1)
    relay(2)
    relay(3)
    pass_on(0, 1)
    start_ring(1)
    pass_on(0, 2)
    start_ring(2)
    send_att()
    pass_on(1, 1)
    pass_on(0, 3)
    start_ring(3)
    pass_on(2, 1)
    pass_on(1, 2)
    pass_on(0, 4)
    pass_on(3, 1)
    partner_has(0)
    weight_term(0, 0)
    weight_term(0, 1)
    pass_on(2, 2)
    weight_term(0, 2)
    came(wt.at[0:3], w_recv)
    multiply(0, 0)
    pass_on(1, 3)
    multiply(0, 1)
    multiply(0, 2)
    pass_on(1, 4)
    pass_on(3, 2)
    came(att.at[1], att_recv.at[0])
    came(att.at[2], att_recv.at[1])
    partner_has(1)
    weight_term(1, 0)
    weight_term(1, 1)
    send_term(0)
    pass_on(2, 3)
    weight_term(1, 2)
    multiply(1, 0)
    multiply(1, 1)
    pass_on(2, 4)
    multiply(1, 2)
    pass_on(3, 3)
    partner_has(2)
    weight_term(2, 0)
    send_term(1)
    weight_term(2, 1)
    weight_term(2, 2)
    send_term(2)
    pass_on(3, 4)
    for index in range(3):
        multiply(2, index)
    partner_has(3)
    for index in range(3):
        weight_term(3, index)

    for load in loads[5:]:
        load.wait()
    came(dw_in, dw_recv)
    for c, start, size in row_chunks():
        rows = pl.ds(start, size)
        grad = dwacc[3, rows, :]
        for i in range(NX - 1):
            grad = grad + dw_in[i, rows, :].astype(F32)
        low_first = jnp.minimum(down(frow, start, size), fcol[...].reshape(1, HD))
        low_second = jnp.minimum(down(srow, start, size), scol[...].reshape(1, HD))
        first = fc[rows, :].astype(F32) * low_first
        second = sc[rows, :].astype(F32) * low_second
        first_new = beta_first * first + (1.0 - beta_first) * grad
        second_new = beta_second * second + (1.0 - beta_second) * grad * grad
        step_size = first_new / correct_first / (jnp.sqrt(second_new / correct_second) + adam_eps)
        weight = w[rows, :]
        nw_out[rows, :] = weight - learning * (step_size + decay_rate * weight)
        fnew_out[rows, :] = first_new
        snew_out[rows, :] = second_new

    first_abs, second_abs = jnp.abs(fnew_out[...]), jnp.abs(snew_out[...])
    st[0] = lane_rows(first_abs)
    st[1] = lane_rows(second_abs)
    for dy in range(1, NY):
        rcopy(st, y_in.at[NY - dy - 1], y_send, y_recv, y=mod(y + dy, NY)).start()
    cst[0, 0:1, :] = jnp.max(first_abs, axis=0, keepdims=True)
    cst[0, 1:2, :] = jnp.max(second_abs, axis=0, keepdims=True)
    for dx in range(1, NX):
        rcopy(cst.at[0], x_in.at[NX - dx - 1], x_send, x_recv, x=mod(x + dx, NX)).start()

    multiply(3, 0)
    send_grad(1)
    multiply(3, 1)
    send_grad(2)
    multiply(3, 2)

    def back_rows(i):
        rows, cols = pl.ds(128 * i, 128), pl.ds(0, 128 * (i + 1))
        total = acct[0, :, rows]
        for s in range(2):
            total = total + ga_in[s, :, rows].astype(F32)
        grad_half = total.astype(BF16).T
        grad_probs = lax.dot_general(grad_half, vv[cols, :], NT, preferred_element_type=F32)
        row_dot = jnp.sum(
            grad_half.astype(F32) * att[0, rows, :].astype(F32), axis=-1, keepdims=True
        )
        grad_scores = (prob[rows, cols] * (grad_probs - row_dot)).astype(BF16)
        gq_out[rows, :] = (
            jnp.dot(grad_scores, kk[cols, :], preferred_element_type=F32) * SCALE
        ).astype(BF16)

    came(x_in, x_recv)
    cst[1] = jnp.maximum(cst[0], jnp.max(x_in[...], axis=0))
    for sequence in (1, 2):
        o = other(sequence)
        rcopy(cst.at[1], zh_in.at[sequence_of(zh, o) - 1], zh_send, zh_recv, zh=o).start()
    came(y_in, y_recv)
    mine[...] = jnp.maximum(st[...], jnp.max(y_in[...], axis=0))
    for rel in range(1, NZL * NC):
        dl, dk = rel // NC, rel % NC
        back = NC * ((NZL - dl) % NZL) + dk - 1
        rcopy(
            mine, zl_in.at[back], zl_send, zl_recv, zl=mod(zl + dl, NZL), core=lax.rem(k + dk, NC)
        ).start()
    came(ga_in, ga_recv)
    for i in range(3):
        back_rows(i)
    came(zl_in, zl_recv)
    rows_out[...] = jnp.maximum(mine[...], jnp.max(zl_in[...], axis=0))
    came(zh_in, zh_recv)
    cols_out[...] = jnp.maximum(cst[1], jnp.max(zh_in[...], axis=0))

    def left(ref, send):
        rcopy(ref, ref, send, zh_recv, core=k).wait_send()

    wait_units(8 - sum(staying), 8, lambda c: left(gz.at[0:c], spread_send))
    for slot in range(SLOTS):
        wait_units(landing[slot], 9, lambda c: left(gz.at[0 : 3 * c], relay_send.at[slot]))
    longer = count(
        (from_source(way, hops) == NY - 1) & (k == 1)
        for slot in range(SLOTS)
        for way in (0, 1)
        for hops in range(reach(way, slot))
    )
    for c in range(9):
        pl.when(longer == c)(functools.partial(left, gz.at[0 : 56 * SLOTS + c], ring_send))
    for c in (0, 1):
        pl.when(k == c)(functools.partial(left, gz.at[0 : 64 * SLOTS + SLOTS * c], core_send))
    for whole, send in (
        (att.at[0:2], att_send),
        (wt.at[0:3], w_send),
        (ga_in, ga_send),
        (dw_in, dw_send),
        (y_in, y_send),
        (zl_in, zl_send),
        (x_in, x_send),
        (zh_in, zh_send),
    ):
        left(whole, send)


def codes(gq, nw, fnew, snew, rows, cols, gq_out, nw_out, nfc_out, nfr_out, nfcol_out, nsc_out, nsr_out, nscol_out):
    gq_out[...] = gq[...]
    nw_out[...] = nw[...]
    nfcol_out[...] = cols[0]
    nscol_out[...] = cols[1]
    for c, start, size in row_chunks():
        at = pl.ds(start, size)
        nfr_out[at] = rows[0, c, 0:size]
        nsr_out[at] = rows[1, c, 0:size]
        low_first = jnp.minimum(down_rows(rows[0, c : c + 1, :])[:size], cols[0:1])
        low_second = jnp.minimum(down_rows(rows[1, c : c + 1, :])[:size], cols[1:2])
        nfc_out[at, :] = (fnew[at, :] / (low_first + code_eps)).astype(BF16)
        nsc_out[at, :] = (snew[at, :] / (low_second + code_eps)).astype(BF16)


def per_device(queries, keys, values, grad_out, weight, fc, frow, fcol, sc, srow, scol):
    shape = jax.ShapeDtypeStruct
    vmem = pl.BlockSpec(memory_space=pltpu.VMEM)
    hbm = pl.BlockSpec(memory_space=pltpu.HBM)
    dma = pltpu.SemaphoreType.DMA
    gq, nw, fnew, snew, rows, cols = pl.pallas_call(
        body,
        name="whole",
        out_shape=(
            shape((SEQ, HD), BF16),
            shape((ROWS, HD), F32),
            shape((ROWS, HD), F32),
            shape((ROWS, HD), F32),
            shape((2, 8, HD), F32),
            shape((2, HD), F32),
        ),
        in_specs=[hbm] * 11,
        out_specs=[vmem] * 6,
        scratch_shapes=[
            pltpu.VMEM((SEQ, HD), BF16),
            pltpu.VMEM((SEQ, HD), BF16),
            pltpu.VMEM((SEQ, HD), BF16),
            pltpu.VMEM((SEQ, HD), BF16),
            pltpu.VMEM((ROWS, HD), F32),
            pltpu.VMEM((ROWS, HD), BF16),
            pltpu.VMEM((ROWS, HD), BF16),
            pltpu.VMEM((ROWS,), F32),
            pltpu.VMEM((HD,), F32),
            pltpu.VMEM((ROWS,), F32),
            pltpu.VMEM((HD,), F32),
            pltpu.VMEM((HD, SEQ), BF16),
            pltpu.VMEM((SLOTS * SLOT, UNIT, SEQ), BF16),
            pltpu.VMEM((NX, HD, ROWS), BF16),
            pltpu.VMEM((NZH, SEQ, HD), BF16),
            pltpu.VMEM((SEQ, SEQ), F32),
            pltpu.VMEM((NZH, HD, SEQ), F32),
            pltpu.VMEM((2, HD, SEQ), BF16),
            pltpu.VMEM((2, HD, SEQ), BF16),
            pltpu.VMEM((NX, ROWS, HD), F32),
            pltpu.VMEM((NX - 1, ROWS, HD), BF16),
            pltpu.VMEM((NX - 1, ROWS, HD), BF16),
            pltpu.VMEM((2, 8, HD), F32),
            pltpu.VMEM((NY - 1, 2, 8, HD), F32),
            pltpu.VMEM((NZL * NC - 1, 2, 8, HD), F32),
            pltpu.VMEM((2, 8, HD), F32),
            pltpu.VMEM((2, 2, HD), F32),
            pltpu.VMEM((NX - 1, 2, HD), F32),
            pltpu.VMEM((NZH - 1, 2, HD), F32),
            dma((11,)),
            dma,
            dma((SLOTS,)),
            dma((SLOTS,)),
            dma((SLOTS,)),
            dma,
            dma((2, SLOTS, 4, 2)),
            dma,
            dma((2, SLOTS, 5)),
            dma,
            dma((2,)),
            dma,
            dma,
            dma,
            dma,
            dma,
            dma,
            dma,
            dma,
            dma,
            dma,
            dma,
            dma,
            dma,
            dma,
        ],
        compiler_params=pltpu.CompilerParams(
            collective_id=0, has_side_effects=True, vmem_limit_bytes=48 * 1024 * 1024
        ),
    )(
        *(
            pltpu.with_memory_space_constraint(a, pltpu.HBM)
            for a in (queries, keys, values, grad_out, weight, fc, frow, fcol, sc, srow, scol)
        )
    )
    return pl.pallas_call(
        codes,
        name="codes",
        out_shape=(
            shape((SEQ, HD), BF16),
            shape((ROWS, HD), F32),
            shape((ROWS, HD), BF16),
            shape((ROWS,), F32),
            shape((HD,), F32),
            shape((ROWS, HD), BF16),
            shape((ROWS,), F32),
            shape((HD,), F32),
        ),
        compiler_params=pltpu.CompilerParams(vmem_limit_bytes=8 * 1024 * 1024),
        in_specs=[vmem] * 6,
        out_specs=[vmem] * 8,
    )(gq, nw, fnew, snew, rows, cols)


def solution(mesh):
    finer = Mesh(mesh.devices.reshape(NX, NZH, NY, NZL, NC), AXES)
    placed = (
        P(DP, TENSOR),
        P(DP, None),
        P(DP, None),
        P(DP, TENSOR),
        P(DP, TENSOR),
        P(DP, TENSOR),
        P(DP),
        P(TENSOR),
        P(DP, TENSOR),
        P(DP),
        P(TENSOR),
    )
    return jax.shard_map(
        per_device,
        mesh=finer,
        in_specs=placed,
        out_specs=(
            P(DP, TENSOR),
            P(DP, TENSOR),
            P(DP, TENSOR),
            P(DP),
            P(TENSOR),
            P(DP, TENSOR),
            P(DP),
            P(TENSOR),
        ),
        check_vma=False,
    )
```

```python
import functools

import jax
import jax.numpy as jnp
from jax import lax
from jax.experimental import pallas as pl
from jax.experimental.pallas import tpu as pltpu
from jax.sharding import Mesh
from jax.sharding import PartitionSpec as P

NX, NZH, NY, NZL, NC = 4, 3, 8, 4, 2
AXES = ("x", "zh", "y", "zl", "core")
DP = ("x", "zh")
TENSOR = ("y", "zl", "core")
MESH = pl.DeviceIdType.MESH

HD = 128
SEQ = 384
ROWS = 688
UNIT = 16
UNITS = ROWS // UNIT
ALL_UNITS = 512
HOMES = NY * NC
SLOTS = 4
SLOT = 3 * UNITS
SCALE = HD ** (-0.5)

beta_first = 0.9
beta_second = 0.95
learning = 0.01
decay_rate = 0.1
adam_eps = 1e-08
code_eps = 1e-06
correct_first = 1.0 - 0.9**10
correct_second = 1.0 - 0.95**10

F32 = jnp.float32
BF16 = jnp.bfloat16
NT = (((1,), (1,)), ((), ()))


def mod(a, n):
    return lax.rem(a + n, n)


def row_chunks():
    return [(c, 128 * c, min(128, ROWS - 128 * c)) for c in range(6)]


def lane_rows(values):
    highest = jnp.max(values, axis=1, keepdims=True)
    out = []
    for c, start, size in row_chunks():
        eye = lax.broadcasted_iota(jnp.int32, (size, 128), 0) == lax.broadcasted_iota(
            jnp.int32, (size, 128), 1
        )
        out.append(
            jnp.max(jnp.where(eye, highest[start : start + size], 0.0), axis=0, keepdims=True)
        )
    out.append(jnp.zeros((2, 128), F32))
    return jnp.concatenate(out, axis=0)


def down(vector, start, size):
    row = vector[pl.ds(start, size)].reshape(1, size)
    if size < 128:
        row = jnp.concatenate([row, jnp.zeros((1, 128 - size), F32)], axis=1)
    return down_rows(row)[:size]


def down_rows(row):
    return jnp.broadcast_to(row, (128, 128)).T


def body(
    q_hbm,
    k_hbm,
    v_hbm,
    g_hbm,
    w_hbm,
    fc_hbm,
    frow_hbm,
    fcol_hbm,
    sc_hbm,
    srow_hbm,
    scol_hbm,
    gq_out,
    nw_out,
    fnew_out,
    snew_out,
    rows_out,
    cols_out,
    q,
    kk,
    vv,
    g,
    w,
    fc,
    sc,
    frow,
    fcol,
    srow,
    scol,
    gt,
    gz,
    wt,
    att,
    prob,
    acct,
    ga_stage,
    ga_in,
    dwacc,
    dw_stage,
    dw_in,
    st,
    y_in,
    zl_in,
    mine,
    cst,
    x_in,
    zh_in,
    in_sem,
    spread_send,
    relay_send,
    far_recv,
    near_recv,
    ring_send,
    ring_recv,
    core_send,
    core_recv,
    att_send,
    att_recv,
    w_send,
    w_recv,
    ga_send,
    ga_recv,
    dw_send,
    dw_recv,
    y_send,
    y_recv,
    zl_send,
    zl_recv,
    x_send,
    x_recv,
    zh_send,
    zh_recv,
):
    x, zh, y, zl, k = (lax.axis_index(a) for a in AXES)
    t = 8 * y + 2 * zl + k
    pair = lax.div(y, 2)

    def rcopy(src, dst, send, recv, **dev):
        return pltpu.make_async_remote_copy(
            src_ref=src, dst_ref=dst, send_sem=send, recv_sem=recv, device_id=dev, device_id_type=MESH
        )

    def came(ref, recv):
        rcopy(ref, ref, core_send, recv, core=k).wait_recv()

    def sequence_of(source, plane):
        return jnp.where(source == plane, 0, source + (source < plane).astype(jnp.int32))

    def other(sequence):
        return sequence - 1 + (sequence - 1 >= zh).astype(jnp.int32)

    heads = pl.ds(pl.multiple_of(y * HD, HD), HD)
    loads = [
        pltpu.make_async_copy(src, dst, in_sem.at[i])
        for i, (src, dst) in enumerate(
            [
                (g_hbm, g),
                (q_hbm, q),
                (k_hbm.at[:, heads], kk),
                (v_hbm.at[:, heads], vv),
                (w_hbm, w),
                (fc_hbm, fc),
                (sc_hbm, sc),
                (frow_hbm, frow),
                (fcol_hbm, fcol),
                (srow_hbm, srow),
                (scol_hbm, scol),
            ]
        )
    ]
    for load in loads:
        load.start()

    me = 2 * y + k

    def rows_of(u):
        return pl.ds(pl.multiple_of(UNIT * u, UNIT), UNIT)

    def slot_and_index(ahead, sequence):
        turn = 2 * ahead + sequence
        far = (turn >= 6).astype(jnp.int32)
        slot = jnp.where(ahead == 0, 3, jnp.where(sequence == 0, 0, 1 + far))
        index = jnp.where(
            ahead == 0,
            sequence - 1 + 3 * (sequence == 0).astype(jnp.int32),
            jnp.where(sequence == 0, ahead - 1, turn - 3 - 3 * far),
        )
        return slot, index

    first_owner = lax.div(8 * t, UNITS)
    first_row = 8 * t - UNITS * first_owner
    turnover = UNITS - first_row
    sides = []
    for owner in (first_owner, first_owner + 1):
        xd = lax.div(owner, NZH)
        zd = owner - NZH * xd
        slot, index = slot_and_index(mod(xd - x, NX), sequence_of(zh, zd))
        sides.append((zd, slot, UNITS * index))

    def goes_to(u):
        over = u >= turnover
        zd, slot, start = (jnp.where(over, b, a) for a, b in zip(*sides))
        e = start + first_row + u - jnp.where(over, UNITS, 0)
        h = jnp.minimum(lax.shift_right_logical(e, 3), HOMES - 1)
        home = dict(
            zh=zd,
            y=lax.shift_right_logical(h, 1),
            zl=zl ^ (2 * (u & 1)),
            core=h & 1,
        )
        here = (zd == zh) & (h == me) & (home["zl"] == zl)
        return slot, SLOT * slot + e, home, here

    first_index = lax.div(8 * me, UNITS)
    first_place = 8 * me - UNITS * first_index
    has_last = me == HOMES - 1
    units = []
    for slot in range(SLOTS):
        blocks = []
        for index in (first_index, first_index + 1):
            if slot == 0:
                xd, z = (x + 1 + index) & 3, zh
            elif slot == 3:
                xd, z = x, jnp.where(index == 2, zh, other(index + 1))
            else:
                turn = 3 * (slot - 1) + index
                xd, z = (x + 1 + lax.shift_right_logical(turn, 1)) & 3, other(1 + (turn & 1))
            blocks.append((z, UNITS * (NZH * xd + zh)))
        held = []
        for j in range(9):
            over = first_place + j >= UNITS
            z, start = (jnp.where(over, b, a) for a, b in zip(*blocks))
            unit = start + first_place + j - jnp.where(over, UNITS, 0)
            column = lax.shift_right_logical(unit, 3)
            line = lax.shift_right_logical(column, 1) & 3
            there = unit < ALL_UNITS
            if j == 8:
                there = there & has_last
            here = (line ^ (2 * (unit & 1))) == zl
            source = dict(zh=z, y=lax.shift_right_logical(column, 3), zl=line, core=column & 1)
            held.append((there, there & here, source, (z == zh) & (column == t)))
        units.append(held)

    def count(flags):
        return sum(f.astype(jnp.int32) for f in flags)

    landing = [count(lands for _, lands, _, _ in held) for held in units]
    coming = [count(there for there, _, _, _ in held) - n for held, n in zip(units, landing)]
    staying = [count(lands & same for _, lands, _, same in held) for held in units]

    barrier = pltpu.get_barrier_semaphore()

    def greet(**dev):
        pl.semaphore_signal(barrier, inc=1, device_id=dev, device_id_type=MESH)

    def greet_home(u, carry):
        slot, place, home, here = goes_to(u)
        pl.when(jnp.logical_not(here))(functools.partial(greet, **home))
        return carry

    lax.fori_loop(0, 8, greet_home, 0)
    for held in units:
        for _, lands, source, same in held:
            pl.when(lands & jnp.logical_not(same))(functools.partial(greet, **source))
    for dz in (1, 2):
        greet(zh=mod(zh + dz, NZH))
    for dx in range(1, NX):
        greet(x=mod(x + dx, NX))
    for dy in range(1, NY):
        greet(y=mod(y + dy, NY))
    for rel in range(1, NZL * NC):
        greet(zl=mod(zl + rel // NC, NZL), core=lax.rem(k + rel % NC, NC))
    greeted = 8 + sum(landing) - 2 * sum(staying) + 2 + 3 + 7 + 7

    loads[0].wait()
    gt[...] = g[...].T

    for slot, held in enumerate(units):
        for j, (there, _, _, _) in enumerate(held):
            missing = jnp.logical_not(there)

            @pl.when(missing & has_last if j == 8 else missing)
            def _():
                gz[SLOT * slot + 8 * me + j] = jnp.zeros((UNIT, SEQ), BF16)

    pl.semaphore_wait(barrier, greeted)

    def spread(wanted, u, carry):
        slot, place, home, here = goes_to(u)

        @pl.when((slot == wanted) & here)
        def _():
            gz[place] = gt[rows_of(u), :]

        @pl.when((slot == wanted) & jnp.logical_not(here))
        def _():
            rcopy(gt.at[rows_of(u), :], gz.at[place], spread_send, far_recv.at[slot], **home).start()

        return carry

    for slot in range(SLOTS):
        lax.fori_loop(0, 8, functools.partial(spread, slot), 0)

    loads[4].wait()
    wt[3] = w[...].astype(BF16).T
    for dx in (1, 3, 2):
        rcopy(wt.at[3], wt.at[NX - 1 - dx], w_send, w_recv, x=mod(x + dx, NX)).start()

    for i in (1, 2, 3):
        loads[i].wait()
    for i in range(3):
        rows, cols = pl.ds(128 * i, 128), pl.ds(0, 128 * (i + 1))
        scores = (
            lax.dot_general(q[rows, :], kk[cols, :], NT, preferred_element_type=F32) * SCALE
        )
        future = lax.broadcasted_iota(jnp.int32, scores.shape, 1) > (
            lax.broadcasted_iota(jnp.int32, scores.shape, 0) + 128 * i
        )
        scores = jnp.where(future, -1e30, scores)
        exponent = jnp.exp(scores - jnp.max(scores, axis=-1, keepdims=True))
        probabilities = exponent / jnp.sum(exponent, axis=-1, keepdims=True)
        prob[rows, cols] = probabilities
        att[0, rows, :] = jnp.dot(
            probabilities.astype(BF16), vv[cols, :], preferred_element_type=F32
        ).astype(BF16)

    def send_att():
        for sequence in (1, 2):
            o = other(sequence)
            there = sequence_of(zh, o)
            rcopy(att.at[0], att.at[there], att_send, att_recv.at[there - 1], zh=o).start()

    def wait_units(n, most, wait):
        for c in range(1, most + 1):
            pl.when(n == c)(functools.partial(wait, c))

    def units_came(recv, c):
        came(gz.at[0:c], recv)

    def relay(slot):
        wait_units(
            landing[slot] - staying[slot], 9, functools.partial(units_came, far_recv.at[slot])
        )

        for j, (_, lands, _, _) in enumerate(units[slot]):
            piece = gz.at[SLOT * slot + 8 * me + j]

            @pl.when(lands)
            def _():
                for dl in (1, 3, 2):
                    rcopy(
                        piece, piece, relay_send.at[slot], near_recv.at[slot], zl=mod(zl + dl, NZL)
                    ).start()

    def reach(way, slot):
        return 4 if way == slot % 2 else 3

    def from_source(way, hops):
        return mod(y - hops, NY) if way == 0 else mod(y + hops, NY)

    def parts_of(slot, source, core):
        start = SLOT * slot + 8 * (2 * source + core)
        last = (source == NY - 1) & (core == 1)
        return (
            ((start, 4, None),),
            ((start + 4, 4, jnp.logical_not(last)), (start + 4, 5, last)),
        )

    def each_size(sizes, act):
        for start, units, when in sizes:
            ref = gz.at[pl.ds(start, units)]
            if when is None:
                act(ref)
            else:
                pl.when(when)(functools.partial(act, ref))

    def forward(way, slot, hops, part):
        def go(piece):
            rcopy(
                piece,
                piece,
                ring_send,
                ring_recv.at[way, slot, hops, part],
                y=mod(y + 1, NY) if way == 0 else mod(y - 1, NY),
            ).start()

        each_size(parts_of(slot, from_source(way, hops), k)[part], go)

    def to_partner(way, slot, hops, part):
        def go(piece):
            rcopy(piece, piece, core_send, core_recv.at[way, slot, hops], core=1 - k).start()

        each_size(parts_of(slot, from_source(way, hops), k)[part], go)

    def start_ring(slot):
        wait_units(coming[slot], 9, functools.partial(units_came, near_recv.at[slot]))
        for part in (0, 1):
            for way in (0, 1):
                forward(way, slot, 0, part)
        for part in (0, 1):
            to_partner(0, slot, 0, part)

    def pass_on(slot, hops):
        for part in (0, 1):
            for way in (0, 1):
                if hops <= reach(way, slot):
                    each_size(
                        parts_of(slot, from_source(way, hops), k)[part],
                        lambda piece: came(piece, ring_recv.at[way, slot, hops - 1, part]),
                    )
                    if hops < reach(way, slot):
                        forward(way, slot, hops, part)
                    to_partner(way, slot, hops, part)

    def partner_has(slot):
        for hops in range(5):
            for way in (0, 1):
                if (hops > 0 or way == 0) and hops <= reach(way, slot):
                    last = (from_source(way, hops) == NY - 1) & (k == 0)
                    recv = core_recv.at[way, slot, hops]
                    pl.when(last)(functools.partial(came, gz.at[0:9], recv))
                    pl.when(jnp.logical_not(last))(functools.partial(came, gz.at[0:8], recv))

    def block_of(slot, index):
        return gz[pl.ds(SLOT * slot + UNITS * index, UNITS)].reshape(ROWS, SEQ)

    def member(slot, index):
        if slot == 0:
            return index, 0
        if slot == 3:
            return 3, (index + 1) % 3
        turn = 3 * (slot - 1) + index
        return turn // 2, 1 + turn % 2

    started = set()

    def weight_term(slot, index):
        rows, sequence = member(slot, index)
        term = jnp.dot(block_of(slot, index), att[sequence], preferred_element_type=F32)
        dwacc[rows] = dwacc[rows] + term if ("w", rows) in started else term
        started.add(("w", rows))

    def multiply(slot, index):
        rows, sequence = member(slot, index)
        term = jnp.dot(wt[rows], block_of(slot, index), preferred_element_type=F32)
        acct[sequence] = acct[sequence] + term if ("g", sequence) in started else term
        started.add(("g", sequence))

    def send_term(rows):
        dw_stage[rows] = dwacc[rows].astype(BF16)
        rcopy(
            dw_stage.at[rows], dw_in.at[NX - 2 - rows], dw_send, dw_recv, x=mod(x + 1 + rows, NX)
        ).start()

    def send_grad(sequence):
        ga_stage[sequence - 1] = acct[sequence].astype(BF16)
        o = other(sequence)
        rcopy(
            ga_stage.at[sequence - 1], ga_in.at[sequence_of(zh, o) - 1], ga_send, ga_recv, zh=o
        ).start()

    relay(0)
    start_ring(0)
    relay(1)
    relay(2)
    relay(3)
    pass_on(0, 1)
    start_ring(1)
    pass_on(0, 2)
    pass_on(1, 1)
    pass_on(0, 3)
    start_ring(2)
    send_att()
    pass_on(1, 2)
    pass_on(2, 1)
    pass_on(1, 3)
    pass_on(2, 2)
    start_ring(3)
    pass_on(0, 4)
    pass_on(2, 3)
    partner_has(0)
    weight_term(0, 0)
    weight_term(0, 1)
    pass_on(3, 1)
    weight_term(0, 2)
    came(wt.at[0:3], w_recv)
    multiply(0, 0)
    multiply(0, 1)
    multiply(0, 2)
    pass_on(1, 4)
    came(att.at[1], att_recv.at[0])
    came(att.at[2], att_recv.at[1])
    partner_has(1)
    weight_term(1, 0)
    weight_term(1, 1)
    send_term(0)
    pass_on(3, 2)
    weight_term(1, 2)
    pass_on(2, 4)
    partner_has(2)
    weight_term(2, 0)
    send_term(1)
    weight_term(2, 1)
    weight_term(2, 2)
    send_term(2)
    pass_on(3, 3)
    for slot in (1, 2):
        for index in range(3):
            multiply(slot, index)
    pass_on(3, 4)
    partner_has(3)
    multiply(3, 0)
    send_grad(1)
    multiply(3, 1)
    send_grad(2)
    for index in range(3):
        weight_term(3, index)

    for load in loads[5:]:
        load.wait()
    came(dw_in, dw_recv)
    for c, start, size in row_chunks():
        rows = pl.ds(start, size)
        grad = dwacc[3, rows, :]
        for i in range(NX - 1):
            grad = grad + dw_in[i, rows, :].astype(F32)
        low_first = jnp.minimum(down(frow, start, size), fcol[...].reshape(1, HD))
        low_second = jnp.minimum(down(srow, start, size), scol[...].reshape(1, HD))
        first = fc[rows, :].astype(F32) * low_first
        second = sc[rows, :].astype(F32) * low_second
        first_new = beta_first * first + (1.0 - beta_first) * grad
        second_new = beta_second * second + (1.0 - beta_second) * grad * grad
        step_size = first_new / correct_first / (jnp.sqrt(second_new / correct_second) + adam_eps)
        weight = w[rows, :]
        nw_out[rows, :] = weight - learning * (step_size + decay_rate * weight)
        fnew_out[rows, :] = first_new
        snew_out[rows, :] = second_new

    first_abs, second_abs = jnp.abs(fnew_out[...]), jnp.abs(snew_out[...])
    st[0] = lane_rows(first_abs)
    st[1] = lane_rows(second_abs)
    for dy in range(1, NY):
        rcopy(st, y_in.at[NY - dy - 1], y_send, y_recv, y=mod(y + dy, NY)).start()
    cst[0, 0:1, :] = jnp.max(first_abs, axis=0, keepdims=True)
    cst[0, 1:2, :] = jnp.max(second_abs, axis=0, keepdims=True)
    for dx in range(1, NX):
        rcopy(cst.at[0], x_in.at[NX - dx - 1], x_send, x_recv, x=mod(x + dx, NX)).start()

    multiply(3, 2)

    def back_rows(i):
        rows, cols = pl.ds(128 * i, 128), pl.ds(0, 128 * (i + 1))
        total = acct[0, :, rows]
        for s in range(2):
            total = total + ga_in[s, :, rows].astype(F32)
        grad_half = total.astype(BF16).T
        grad_probs = lax.dot_general(grad_half, vv[cols, :], NT, preferred_element_type=F32)
        row_dot = jnp.sum(
            grad_half.astype(F32) * att[0, rows, :].astype(F32), axis=-1, keepdims=True
        )
        grad_scores = (prob[rows, cols] * (grad_probs - row_dot)).astype(BF16)
        gq_out[rows, :] = (
            jnp.dot(grad_scores, kk[cols, :], preferred_element_type=F32) * SCALE
        ).astype(BF16)

    came(x_in, x_recv)
    cst[1] = jnp.maximum(cst[0], jnp.max(x_in[...], axis=0))
    for sequence in (1, 2):
        o = other(sequence)
        rcopy(cst.at[1], zh_in.at[sequence_of(zh, o) - 1], zh_send, zh_recv, zh=o).start()
    came(y_in, y_recv)
    mine[...] = jnp.maximum(st[...], jnp.max(y_in[...], axis=0))
    for rel in range(1, NZL * NC):
        dl, dk = rel // NC, rel % NC
        back = NC * ((NZL - dl) % NZL) + dk - 1
        rcopy(
            mine, zl_in.at[back], zl_send, zl_recv, zl=mod(zl + dl, NZL), core=lax.rem(k + dk, NC)
        ).start()
    came(ga_in, ga_recv)
    for i in range(3):
        back_rows(i)
    came(zl_in, zl_recv)
    rows_out[...] = jnp.maximum(mine[...], jnp.max(zl_in[...], axis=0))
    came(zh_in, zh_recv)
    cols_out[...] = jnp.maximum(cst[1], jnp.max(zh_in[...], axis=0))

    def left(ref, send):
        rcopy(ref, ref, send, zh_recv, core=k).wait_send()

    wait_units(8 - sum(staying), 8, lambda c: left(gz.at[0:c], spread_send))
    for slot in range(SLOTS):
        wait_units(landing[slot], 9, lambda c: left(gz.at[0 : 3 * c], relay_send.at[slot]))
    longer = count(
        (from_source(way, hops) == NY - 1) & (k == 1)
        for slot in range(SLOTS)
        for way in (0, 1)
        for hops in range(reach(way, slot))
    )
    for c in range(9):
        pl.when(longer == c)(functools.partial(left, gz.at[0 : 56 * SLOTS + c], ring_send))
    for c in (0, 1):
        pl.when(k == c)(functools.partial(left, gz.at[0 : 64 * SLOTS + SLOTS * c], core_send))
    for whole, send in (
        (att.at[0:2], att_send),
        (wt.at[0:3], w_send),
        (ga_in, ga_send),
        (dw_in, dw_send),
        (y_in, y_send),
        (zl_in, zl_send),
        (x_in, x_send),
        (zh_in, zh_send),
    ):
        left(whole, send)


def codes(gq, nw, fnew, snew, rows, cols, gq_out, nw_out, nfc_out, nfr_out, nfcol_out, nsc_out, nsr_out, nscol_out):
    gq_out[...] = gq[...]
    nw_out[...] = nw[...]
    nfcol_out[...] = cols[0]
    nscol_out[...] = cols[1]
    for c, start, size in row_chunks():
        at = pl.ds(start, size)
        nfr_out[at] = rows[0, c, 0:size]
        nsr_out[at] = rows[1, c, 0:size]
        low_first = jnp.minimum(down_rows(rows[0, c : c + 1, :])[:size], cols[0:1])
        low_second = jnp.minimum(down_rows(rows[1, c : c + 1, :])[:size], cols[1:2])
        nfc_out[at, :] = (fnew[at, :] / (low_first + code_eps)).astype(BF16)
        nsc_out[at, :] = (snew[at, :] / (low_second + code_eps)).astype(BF16)


def per_device(queries, keys, values, grad_out, weight, fc, frow, fcol, sc, srow, scol):
    shape = jax.ShapeDtypeStruct
    vmem = pl.BlockSpec(memory_space=pltpu.VMEM)
    hbm = pl.BlockSpec(memory_space=pltpu.HBM)
    dma = pltpu.SemaphoreType.DMA
    gq, nw, fnew, snew, rows, cols = pl.pallas_call(
        body,
        name="whole",
        out_shape=(
            shape((SEQ, HD), BF16),
            shape((ROWS, HD), F32),
            shape((ROWS, HD), F32),
            shape((ROWS, HD), F32),
            shape((2, 8, HD), F32),
            shape((2, HD), F32),
        ),
        in_specs=[hbm] * 11,
        out_specs=[vmem] * 6,
        scratch_shapes=[
            pltpu.VMEM((SEQ, HD), BF16),
            pltpu.VMEM((SEQ, HD), BF16),
            pltpu.VMEM((SEQ, HD), BF16),
            pltpu.VMEM((SEQ, HD), BF16),
            pltpu.VMEM((ROWS, HD), F32),
            pltpu.VMEM((ROWS, HD), BF16),
            pltpu.VMEM((ROWS, HD), BF16),
            pltpu.VMEM((ROWS,), F32),
            pltpu.VMEM((HD,), F32),
            pltpu.VMEM((ROWS,), F32),
            pltpu.VMEM((HD,), F32),
            pltpu.VMEM((HD, SEQ), BF16),
            pltpu.VMEM((SLOTS * SLOT, UNIT, SEQ), BF16),
            pltpu.VMEM((NX, HD, ROWS), BF16),
            pltpu.VMEM((NZH, SEQ, HD), BF16),
            pltpu.VMEM((SEQ, SEQ), F32),
            pltpu.VMEM((NZH, HD, SEQ), F32),
            pltpu.VMEM((2, HD, SEQ), BF16),
            pltpu.VMEM((2, HD, SEQ), BF16),
            pltpu.VMEM((NX, ROWS, HD), F32),
            pltpu.VMEM((NX - 1, ROWS, HD), BF16),
            pltpu.VMEM((NX - 1, ROWS, HD), BF16),
            pltpu.VMEM((2, 8, HD), F32),
            pltpu.VMEM((NY - 1, 2, 8, HD), F32),
            pltpu.VMEM((NZL * NC - 1, 2, 8, HD), F32),
            pltpu.VMEM((2, 8, HD), F32),
            pltpu.VMEM((2, 2, HD), F32),
            pltpu.VMEM((NX - 1, 2, HD), F32),
            pltpu.VMEM((NZH - 1, 2, HD), F32),
            dma((11,)),
            dma,
            dma((SLOTS,)),
            dma((SLOTS,)),
            dma((SLOTS,)),
            dma,
            dma((2, SLOTS, 4, 2)),
            dma,
            dma((2, SLOTS, 5)),
            dma,
            dma((2,)),
            dma,
            dma,
            dma,
            dma,
            dma,
            dma,
            dma,
            dma,
            dma,
            dma,
            dma,
            dma,
            dma,
            dma,
        ],
        compiler_params=pltpu.CompilerParams(
            collective_id=0, has_side_effects=True, vmem_limit_bytes=48 * 1024 * 1024
        ),
    )(
        *(
            pltpu.with_memory_space_constraint(a, pltpu.HBM)
            for a in (queries, keys, values, grad_out, weight, fc, frow, fcol, sc, srow, scol)
        )
    )
    return pl.pallas_call(
        codes,
        name="codes",
        out_shape=(
            shape((SEQ, HD), BF16),
            shape((ROWS, HD), F32),
            shape((ROWS, HD), BF16),
            shape((ROWS,), F32),
            shape((HD,), F32),
            shape((ROWS, HD), BF16),
            shape((ROWS,), F32),
            shape((HD,), F32),
        ),
        compiler_params=pltpu.CompilerParams(vmem_limit_bytes=8 * 1024 * 1024),
        in_specs=[vmem] * 6,
        out_specs=[vmem] * 8,
    )(gq, nw, fnew, snew, rows, cols)


def solution(mesh):
    finer = Mesh(mesh.devices.reshape(NX, NZH, NY, NZL, NC), AXES)
    placed = (
        P(DP, TENSOR),
        P(DP, None),
        P(DP, None),
        P(DP, TENSOR),
        P(DP, TENSOR),
        P(DP, TENSOR),
        P(DP),
        P(TENSOR),
        P(DP, TENSOR),
        P(DP),
        P(TENSOR),
    )
    return jax.shard_map(
        per_device,
        mesh=finer,
        in_specs=placed,
        out_specs=(
            P(DP, TENSOR),
            P(DP, TENSOR),
            P(DP, TENSOR),
            P(DP),
            P(TENSOR),
            P(DP, TENSOR),
            P(DP),
            P(TENSOR),
        ),
        check_vma=False,
    )
```

```python
import functools

import jax
import jax.numpy as jnp
from jax import lax
from jax.experimental import pallas as pl
from jax.experimental.pallas import tpu as pltpu
from jax.sharding import Mesh
from jax.sharding import PartitionSpec as P

NX, NZH, NY, NZL, NC = 4, 3, 8, 4, 2
AXES = ("x", "zh", "y", "zl", "core")
DP = ("x", "zh")
TENSOR = ("y", "zl", "core")
MESH = pl.DeviceIdType.MESH

HD = 128
SEQ = 384
ROWS = 688
UNIT = 16
UNITS = ROWS // UNIT
ALL_UNITS = 512
HOMES = NY * NC
SLOTS = 4
SLOT = 3 * UNITS
SPLIT = (0,)
AHEAD = (2, 1, 3)
SCALE = HD ** (-0.5)

beta_first = 0.9
beta_second = 0.95
learning = 0.01
decay_rate = 0.1
adam_eps = 1e-08
code_eps = 1e-06
correct_first = 1.0 - 0.9**10
correct_second = 1.0 - 0.95**10

F32 = jnp.float32
BF16 = jnp.bfloat16
NT = (((1,), (1,)), ((), ()))


def mod(a, n):
    return lax.rem(a + n, n)


def row_chunks():
    return [(c, 128 * c, min(128, ROWS - 128 * c)) for c in range(6)]


def lane_rows(values):
    highest = jnp.max(values, axis=1, keepdims=True)
    out = []
    for c, start, size in row_chunks():
        eye = lax.broadcasted_iota(jnp.int32, (size, 128), 0) == lax.broadcasted_iota(
            jnp.int32, (size, 128), 1
        )
        out.append(
            jnp.max(jnp.where(eye, highest[start : start + size], 0.0), axis=0, keepdims=True)
        )
    out.append(jnp.zeros((2, 128), F32))
    return jnp.concatenate(out, axis=0)


def down(vector, start, size):
    row = vector[pl.ds(start, size)].reshape(1, size)
    if size < 128:
        row = jnp.concatenate([row, jnp.zeros((1, 128 - size), F32)], axis=1)
    return down_rows(row)[:size]


def down_rows(row):
    return jnp.broadcast_to(row, (128, 128)).T


def body(
    q_hbm,
    k_hbm,
    v_hbm,
    g_hbm,
    w_hbm,
    fc_hbm,
    frow_hbm,
    fcol_hbm,
    sc_hbm,
    srow_hbm,
    scol_hbm,
    gq_out,
    nw_out,
    fnew_out,
    snew_out,
    rows_out,
    cols_out,
    q,
    kk,
    vv,
    g,
    w,
    fc,
    sc,
    frow,
    fcol,
    srow,
    scol,
    gt,
    gz,
    wt,
    att,
    prob,
    acct,
    ga_stage,
    ga_in,
    dwacc,
    dw_stage,
    dw_in,
    st,
    y_in,
    zl_in,
    mine,
    cst,
    x_in,
    zh_in,
    in_sem,
    spread_send,
    relay_send,
    far_recv,
    near_recv,
    ring_send,
    ring_recv,
    beside_send,
    beside_recv,
    shared_recv,
    core_send,
    core_recv,
    att_send,
    att_recv,
    w_send,
    w_recv,
    ga_send,
    ga_recv,
    dw_send,
    dw_recv,
    y_send,
    y_recv,
    zl_send,
    zl_recv,
    x_send,
    x_recv,
    zh_send,
    zh_recv,
):
    x, zh, y, zl, k = (lax.axis_index(a) for a in AXES)
    t = 8 * y + 2 * zl + k
    pair = lax.div(y, 2)

    def rcopy(src, dst, send, recv, **dev):
        return pltpu.make_async_remote_copy(
            src_ref=src, dst_ref=dst, send_sem=send, recv_sem=recv, device_id=dev, device_id_type=MESH
        )

    def came(ref, recv):
        rcopy(ref, ref, core_send, recv, core=k).wait_recv()

    def sequence_of(source, plane):
        return jnp.where(source == plane, 0, source + (source < plane).astype(jnp.int32))

    def other(sequence):
        return sequence - 1 + (sequence - 1 >= zh).astype(jnp.int32)

    heads = pl.ds(pl.multiple_of(y * HD, HD), HD)
    loads = [
        pltpu.make_async_copy(src, dst, in_sem.at[i])
        for i, (src, dst) in enumerate(
            [
                (g_hbm, g),
                (q_hbm, q),
                (k_hbm.at[:, heads], kk),
                (v_hbm.at[:, heads], vv),
                (w_hbm, w),
                (fc_hbm, fc),
                (sc_hbm, sc),
                (frow_hbm, frow),
                (fcol_hbm, fcol),
                (srow_hbm, srow),
                (scol_hbm, scol),
            ]
        )
    ]
    for load in loads:
        load.start()

    barrier = pltpu.get_barrier_semaphore()

    def greet(**dev):
        pl.semaphore_signal(barrier, inc=1, device_id=dev, device_id_type=MESH)

    for dz in (1, 2):
        greet(zh=mod(zh + dz, NZH))
    for dx in range(1, NX):
        greet(x=mod(x + dx, NX))
    for dy in range(1, NY):
        greet(y=mod(y + dy, NY))
    for rel in range(1, NZL * NC):
        greet(zl=mod(zl + rel // NC, NZL), core=lax.rem(k + rel % NC, NC))
    me = 2 * y + k
    side = zl & 1

    def rows_of(u):
        return pl.ds(pl.multiple_of(UNIT * u, UNIT), UNIT)

    def ahead_of(turn):
        return jnp.where(turn == 0, 2, 2 * turn - 1)

    def slot_and_index(ahead, sequence):
        turn = jnp.where(ahead == 2, 0, lax.shift_right_logical(ahead + 1, 1))
        pair = 2 * turn + sequence - 1
        far = (pair >= 3).astype(jnp.int32)
        slot = jnp.where(ahead == 0, 3, jnp.where(sequence == 0, 0, 1 + far))
        index = jnp.where(
            ahead == 0,
            sequence - 1 + 3 * (sequence == 0).astype(jnp.int32),
            jnp.where(sequence == 0, turn, pair - 3 * far),
        )
        return slot, index

    first_owner = lax.div(8 * t, UNITS)
    first_row = 8 * t - UNITS * first_owner
    turnover = UNITS - first_row
    sides = []
    for owner in (first_owner, first_owner + 1):
        xd = lax.div(owner, NZH)
        zd = owner - NZH * xd
        slot, index = slot_and_index(mod(xd - x, NX), sequence_of(zh, zd))
        sides.append((zd, slot, UNITS * index))

    def goes_to(u):
        over = u >= turnover
        zd, slot, start = (jnp.where(over, b, a) for a, b in zip(*sides))
        e = start + first_row + u - jnp.where(over, UNITS, 0)
        h = jnp.minimum(lax.shift_right_logical(e, 3), HOMES - 1)
        line = zl ^ (2 * (u & 1))
        for split in SPLIT:
            shared = (zl & 2) + (e - 8 * h >= 4).astype(jnp.int32)
            line = jnp.where(slot == split, shared, line)
        home = dict(zh=zd, y=lax.shift_right_logical(h, 1), zl=line, core=h & 1)
        here = (zd == zh) & (h == me) & (home["zl"] == zl)
        return slot, SLOT * slot + e, home, here

    first_index = lax.div(8 * me, UNITS)
    first_place = 8 * me - UNITS * first_index
    has_last = me == HOMES - 1
    units = []
    for slot in range(SLOTS):
        blocks = []
        for index in (first_index, first_index + 1):
            if slot == 0:
                xd, z = (x + ahead_of(index)) & 3, zh
            elif slot == 3:
                xd, z = x, jnp.where(index == 2, zh, other(index + 1))
            else:
                turn = 3 * (slot - 1) + index
                xd = (x + ahead_of(lax.shift_right_logical(turn, 1))) & 3
                z = other(1 + (turn & 1))
            blocks.append((z, UNITS * (NZH * xd + zh)))
        held = []
        for j in range(9):
            over = first_place + j >= UNITS
            z, start = (jnp.where(over, b, a) for a, b in zip(*blocks))
            unit = start + first_place + j - jnp.where(over, UNITS, 0)
            column = lax.shift_right_logical(unit, 3)
            line = lax.shift_right_logical(column, 1) & 3
            there = unit < ALL_UNITS
            missing = jnp.logical_not(there)
            if j == 8:
                there, missing = there & has_last, missing & has_last
            if slot in SPLIT:
                taken = side == min(j // 4, 1)
                there, missing = there & taken, missing & taken
                here = (line & 2) == (zl & 2)
            else:
                here = (line ^ (2 * (unit & 1))) == zl
            source = dict(zh=z, y=lax.shift_right_logical(column, 3), zl=line, core=column & 1)
            held.append((there, there & here, source, (z == zh) & (column == t), missing))
        units.append(held)

    def count(flags):
        return sum(f.astype(jnp.int32) for f in flags)

    landing = [count(lands for _, lands, _, _, _ in held) for held in units]
    coming = [count(there for there, _, _, _, _ in held) - n for held, n in zip(units, landing)]
    staying = [count(lands & same for _, lands, _, same, _ in held) for held in units]

    def greet_home(u, carry):
        slot, place, home, here = goes_to(u)
        pl.when(jnp.logical_not(here))(functools.partial(greet, **home))
        return carry

    lax.fori_loop(0, 8, greet_home, 0)
    for held in units:
        for _, lands, source, same, _ in held:
            pl.when(lands & jnp.logical_not(same))(functools.partial(greet, **source))
    greeted = 8 + sum(landing) - 2 * sum(staying) + 2 + 3 + 7 + 7

    loads[0].wait()
    gt[...] = g[...].T

    for slot, held in enumerate(units):
        for j, (_, _, _, _, missing) in enumerate(held):

            @pl.when(missing)
            def _():
                gz[SLOT * slot + 8 * me + j] = jnp.zeros((UNIT, SEQ), BF16)

    pl.semaphore_wait(barrier, greeted)

    def spread(wanted, u, carry):
        slot, place, home, here = goes_to(u)

        @pl.when((slot == wanted) & here)
        def _():
            gz[place] = gt[rows_of(u), :]

        @pl.when((slot == wanted) & jnp.logical_not(here))
        def _():
            rcopy(gt.at[rows_of(u), :], gz.at[place], spread_send, far_recv.at[slot], **home).start()

        return carry

    for slot in range(SLOTS):
        lax.fori_loop(0, 8, functools.partial(spread, slot), 0)

    loads[4].wait()
    wt[3] = w[...].astype(BF16).T
    for dx in (1, 3, 2):
        rcopy(wt.at[3], wt.at[AHEAD.index(NX - dx)], w_send, w_recv, x=mod(x + dx, NX)).start()

    for i in (1, 2, 3):
        loads[i].wait()
    for i in range(3):
        rows, cols = pl.ds(128 * i, 128), pl.ds(0, 128 * (i + 1))
        scores = (
            lax.dot_general(q[rows, :], kk[cols, :], NT, preferred_element_type=F32) * SCALE
        )
        future = lax.broadcasted_iota(jnp.int32, scores.shape, 1) > (
            lax.broadcasted_iota(jnp.int32, scores.shape, 0) + 128 * i
        )
        scores = jnp.where(future, -1e30, scores)
        exponent = jnp.exp(scores - jnp.max(scores, axis=-1, keepdims=True))
        probabilities = exponent / jnp.sum(exponent, axis=-1, keepdims=True)
        prob[rows, cols] = probabilities
        att[0, rows, :] = jnp.dot(
            probabilities.astype(BF16), vv[cols, :], preferred_element_type=F32
        ).astype(BF16)

    def send_att():
        for sequence in (1, 2):
            o = other(sequence)
            there = sequence_of(zh, o)
            rcopy(att.at[0], att.at[there], att_send, att_recv.at[there - 1], zh=o).start()

    def wait_units(n, most, wait):
        for c in range(1, most + 1):
            pl.when(n == c)(functools.partial(wait, c))

    def units_came(recv, c):
        came(gz.at[0:c], recv)

    def relay(slot):
        wait_units(
            landing[slot] - staying[slot], 9, functools.partial(units_came, far_recv.at[slot])
        )

        for j, (_, lands, _, _, _) in enumerate(units[slot]):
            piece = gz.at[SLOT * slot + 8 * me + j]

            @pl.when(lands)
            def _():
                for dl in (2,) if slot in SPLIT else (1, 3, 2):
                    rcopy(
                        piece, piece, relay_send.at[slot], near_recv.at[slot], zl=mod(zl + dl, NZL)
                    ).start()

    def parts(slot):
        return (0, 1) if slot == SLOTS - 1 else (0,)

    def reach(way, slot):
        return 4 if way == slot % 2 else 3

    def from_source(way, hops):
        return mod(y - hops, NY) if way == 0 else mod(y + hops, NY)

    def parts_of(slot, source, core):
        start = SLOT * slot + 8 * (2 * source + core)
        last = (source == NY - 1) & (core == 1)
        if slot in SPLIT:
            longer = last & (side == 1)
            start = start + 4 * side
            return (((start, 4, jnp.logical_not(longer)), (start, 5, longer)),)
        if len(parts(slot)) == 1:
            return (((start, 8, jnp.logical_not(last)), (start, 9, last)),)
        return (
            ((start, 4, None),),
            ((start + 4, 4, jnp.logical_not(last)), (start + 4, 5, last)),
        )

    def each_size(sizes, act):
        for start, units, when in sizes:
            ref = gz.at[pl.ds(start, units)]
            if when is None:
                act(ref)
            else:
                pl.when(when)(functools.partial(act, ref))

    def forward(way, slot, hops, part):
        def go(piece):
            rcopy(
                piece,
                piece,
                ring_send,
                ring_recv.at[way, slot, hops, part],
                y=mod(y + 1, NY) if way == 0 else mod(y - 1, NY),
            ).start()

        each_size(parts_of(slot, from_source(way, hops), k)[part], go)

    def to_partner(way, slot, hops, part):
        def go(piece):
            rcopy(piece, piece, core_send, core_recv.at[slot, hops // 4], core=1 - k).start()

        each_size(parts_of(slot, from_source(way, hops), k)[part], go)

    def to_beside(way, slot, hops):
        def go(piece):
            rcopy(piece, piece, beside_send, beside_recv.at[slot], zl=zl ^ 1).start()

        if slot in SPLIT:
            each_size(parts_of(slot, from_source(way, hops), k)[0], go)

    def start_ring(slot):
        wait_units(coming[slot], 9, functools.partial(units_came, near_recv.at[slot]))
        for part in parts(slot):
            for way in (0, 1):
                forward(way, slot, 0, part)
        to_beside(0, slot, 0)
        for part in parts(slot):
            to_partner(0, slot, 0, part)

    def pass_on(slot, hops):
        for part in parts(slot):
            for way in (0, 1):
                if hops <= reach(way, slot):
                    each_size(
                        parts_of(slot, from_source(way, hops), k)[part],
                        lambda piece: came(piece, ring_recv.at[way, slot, hops - 1, part]),
                    )
                    if hops < reach(way, slot):
                        forward(way, slot, hops, part)
                    to_beside(way, slot, hops)
                    to_partner(way, slot, hops, part)

    def beside_came(slot):
        longer = (k == 1) & (side == 0)
        pl.when(longer)(functools.partial(came, gz.at[0:33], beside_recv.at[slot]))
        pl.when(jnp.logical_not(longer))(functools.partial(came, gz.at[0:32], beside_recv.at[slot]))
        for source in range(NY):
            start = SLOT * slot + 8 * (2 * source + k) + 4 * (1 - side)

            def go(units):
                piece = gz.at[pl.ds(start, units)]
                rcopy(piece, piece, core_send, shared_recv.at[slot], core=1 - k).start()

            if source < NY - 1:
                go(4)
            else:
                pl.when(longer)(functools.partial(go, 5))
                pl.when(jnp.logical_not(longer))(functools.partial(go, 4))

    def partner_beside(slot):
        longer = (k == 0) & (side == 0)
        pl.when(longer)(functools.partial(came, gz.at[0:33], shared_recv.at[slot]))
        pl.when(jnp.logical_not(longer))(functools.partial(came, gz.at[0:32], shared_recv.at[slot]))

    def partner_near(slot):
        more = (k == 0) & (y != NY // 2 - 1)
        each = 8
        if slot in SPLIT:
            more, each = more & (side == 1), 4
        pl.when(more)(functools.partial(came, gz.at[0 : 7 * each + 1], core_recv.at[slot, 0]))
        pl.when(jnp.logical_not(more))(functools.partial(came, gz.at[0 : 7 * each], core_recv.at[slot, 0]))

    def partner_across(slot):
        more = (k == 0) & (y == NY // 2 - 1)
        each = 8
        if slot in SPLIT:
            more, each = more & (side == 1), 4
        pl.when(more)(functools.partial(came, gz.at[0 : each + 1], core_recv.at[slot, 1]))
        pl.when(jnp.logical_not(more))(functools.partial(came, gz.at[0:each], core_recv.at[slot, 1]))

    def partner_has(slot):
        partner_near(slot)
        partner_across(slot)

    def block_of(slot, index):
        return gz[pl.ds(SLOT * slot + UNITS * index, UNITS)].reshape(ROWS, SEQ)

    def member(slot, index):
        if slot == 0:
            return index, 0
        if slot == 3:
            return 3, (index + 1) % 3
        turn = 3 * (slot - 1) + index
        return turn // 2, 1 + turn % 2

    started = set()

    def weight_term(slot, index):
        rows, sequence = member(slot, index)
        term = jnp.dot(block_of(slot, index), att[sequence], preferred_element_type=F32)
        dwacc[rows] = dwacc[rows] + term if ("w", rows) in started else term
        started.add(("w", rows))

    def multiply(slot, index):
        rows, sequence = member(slot, index)
        term = jnp.dot(wt[rows], block_of(slot, index), preferred_element_type=F32)
        acct[sequence] = acct[sequence] + term if ("g", sequence) in started else term
        started.add(("g", sequence))

    early = jnp.where(lax.rem(y + NY // 2, NY) <= 2, 2, 0)
    last_blocks = (early, jnp.where(early == 2, 0, 1), jnp.where(early == 2, 1, 2))

    def last_term(turn):
        index = last_blocks[turn]
        term = jnp.dot(
            block_of(SLOTS - 1, index), att[lax.rem(index + 1, NZH)], preferred_element_type=F32
        )
        dwacc[3] = dwacc[3] + term if turn > 0 else term

    def last_multiply(turn):
        index = last_blocks[turn]
        term = jnp.dot(wt[3], block_of(SLOTS - 1, index), preferred_element_type=F32)
        sequence = lax.rem(index + 1, NZH)
        acct[sequence] = acct[sequence] + term

    def send_term(rows):
        dw_stage[rows] = dwacc[rows].astype(BF16)
        rcopy(
            dw_stage.at[rows], dw_in.at[rows], dw_send, dw_recv, x=mod(x + AHEAD[rows], NX)
        ).start()

    def send_grad(sequence):
        ga_stage[sequence - 1] = acct[sequence].astype(BF16)
        o = other(sequence)
        rcopy(
            ga_stage.at[sequence - 1], ga_in.at[sequence_of(zh, o) - 1], ga_send, ga_recv, zh=o
        ).start()

    def old_moments():
        for load in loads[5:]:
            load.wait()
        for c, start, size in row_chunks():
            rows = pl.ds(start, size)
            low_first = jnp.minimum(down(frow, start, size), fcol[...].reshape(1, HD))
            low_second = jnp.minimum(down(srow, start, size), scol[...].reshape(1, HD))
            fnew_out[rows, :] = beta_first * (fc[rows, :].astype(F32) * low_first)
            snew_out[rows, :] = beta_second * (sc[rows, :].astype(F32) * low_second)
            weight = w[rows, :]
            nw_out[rows, :] = weight - learning * (decay_rate * weight)

    relay(0)
    start_ring(0)
    relay(1)
    relay(2)
    relay(3)
    pass_on(0, 1)
    start_ring(1)
    pass_on(0, 2)
    pass_on(1, 1)
    start_ring(2)
    send_att()
    pass_on(0, 3)
    pass_on(1, 2)
    pass_on(2, 1)
    start_ring(3)
    pass_on(0, 4)
    pass_on(1, 3)
    pass_on(2, 2)
    old_moments()
    pass_on(3, 1)
    pass_on(1, 4)
    beside_came(0)
    pass_on(2, 3)
    partner_has(1)
    partner_has(0)
    partner_beside(0)
    came(wt.at[0:3], w_recv)
    multiply(0, 0)
    came(att.at[1], att_recv.at[0])
    came(att.at[2], att_recv.at[1])
    weight_term(1, 0)
    multiply(0, 2)
    pass_on(3, 2)
    weight_term(1, 1)
    weight_term(0, 0)
    send_term(0)
    weight_term(0, 2)
    pass_on(2, 4)
    multiply(1, 1)
    weight_term(1, 2)
    weight_term(0, 1)
    partner_has(2)
    pass_on(3, 3)
    weight_term(2, 0)
    send_term(1)
    weight_term(2, 1)
    weight_term(2, 2)
    send_term(2)
    multiply(2, 0)
    multiply(1, 2)
    partner_near(3)
    last_term(0)
    pass_on(3, 4)
    multiply(0, 1)
    last_multiply(0)
    multiply(2, 1)
    multiply(2, 2)
    multiply(1, 0)
    partner_across(3)
    last_multiply(1)
    last_multiply(2)
    send_grad(1)
    send_grad(2)
    last_term(1)
    last_term(2)

    came(dw_in, dw_recv)
    for c, start, size in row_chunks():
        rows = pl.ds(start, size)
        grad = dwacc[3, rows, :]
        for i in range(NX - 1):
            grad = grad + dw_in[i, rows, :].astype(F32)
        first_new = fnew_out[rows, :] + (1.0 - beta_first) * grad
        second_new = snew_out[rows, :] + (1.0 - beta_second) * grad * grad
        step_size = (
            first_new * (1.0 / correct_first) / (jnp.sqrt(second_new * (1.0 / correct_second)) + adam_eps)
        )
        nw_out[rows, :] = nw_out[rows, :] - learning * step_size
        fnew_out[rows, :] = first_new
        snew_out[rows, :] = second_new

    first_abs, second_abs = jnp.abs(fnew_out[...]), jnp.abs(snew_out[...])
    st[0] = lane_rows(first_abs)
    st[1] = lane_rows(second_abs)
    for dy in range(1, NY):
        rcopy(st, y_in.at[NY - dy - 1], y_send, y_recv, y=mod(y + dy, NY)).start()
    cst[0, 0:1, :] = jnp.max(first_abs, axis=0, keepdims=True)
    cst[0, 1:2, :] = jnp.max(second_abs, axis=0, keepdims=True)
    for dx in range(1, NX):
        rcopy(cst.at[0], x_in.at[NX - dx - 1], x_send, x_recv, x=mod(x + dx, NX)).start()

    def back_rows(i):
        rows, cols = pl.ds(128 * i, 128), pl.ds(0, 128 * (i + 1))
        total = acct[0, :, rows]
        for s in range(2):
            total = total + ga_in[s, :, rows].astype(F32)
        grad_half = total.astype(BF16).T
        grad_probs = lax.dot_general(grad_half, vv[cols, :], NT, preferred_element_type=F32)
        row_dot = jnp.sum(
            grad_half.astype(F32) * att[0, rows, :].astype(F32), axis=-1, keepdims=True
        )
        grad_scores = (prob[rows, cols] * (grad_probs - row_dot)).astype(BF16)
        gq_out[rows, :] = (
            jnp.dot(grad_scores, kk[cols, :], preferred_element_type=F32) * SCALE
        ).astype(BF16)

    came(x_in, x_recv)
    cst[1] = jnp.maximum(cst[0], jnp.max(x_in[...], axis=0))
    for sequence in (1, 2):
        o = other(sequence)
        rcopy(cst.at[1], zh_in.at[sequence_of(zh, o) - 1], zh_send, zh_recv, zh=o).start()
    came(y_in, y_recv)
    mine[...] = jnp.maximum(st[...], jnp.max(y_in[...], axis=0))
    for rel in range(1, NZL * NC):
        dl, dk = rel // NC, rel % NC
        back = NC * ((NZL - dl) % NZL) + dk - 1
        rcopy(
            mine, zl_in.at[back], zl_send, zl_recv, zl=mod(zl + dl, NZL), core=lax.rem(k + dk, NC)
        ).start()
    came(ga_in, ga_recv)
    for i in range(3):
        back_rows(i)
    came(zl_in, zl_recv)
    rows_out[...] = jnp.maximum(mine[...], jnp.max(zl_in[...], axis=0))
    came(zh_in, zh_recv)
    cols_out[...] = jnp.maximum(cst[1], jnp.max(zh_in[...], axis=0))

    def left(ref, send):
        rcopy(ref, ref, send, zh_recv, core=k).wait_send()

    wait_units(8 - sum(staying), 8, lambda c: left(gz.at[0:c], spread_send))
    for slot in range(SLOTS):
        copies = 1 if slot in SPLIT else 3
        wait_units(landing[slot], 9, lambda c: left(gz.at[0 : copies * c], relay_send.at[slot]))
    longer = count(
        (from_source(way, hops) == NY - 1) & (k == 1) & ((side == 1) | (slot not in SPLIT))
        for slot in range(SLOTS)
        for way in (0, 1)
        for hops in range(reach(way, slot))
    )
    usual = 56 * SLOTS - 28 * len(SPLIT)
    for c in range(9):
        pl.when(longer == c)(functools.partial(left, gz.at[0 : usual + c], ring_send))
    more = (k == 1) & (side == 1)
    for flag, each in ((more, 33), (jnp.logical_not(more), 32)):
        pl.when(flag)(functools.partial(left, gz.at[0 : each * len(SPLIT)], beside_send))
    for c in (0, 1):
        pl.when(k == c)(functools.partial(left, gz.at[0 : 64 * SLOTS + SLOTS * c], core_send))
    for whole, send in (
        (att.at[0:2], att_send),
        (wt.at[0:3], w_send),
        (ga_in, ga_send),
        (dw_in, dw_send),
        (y_in, y_send),
        (zl_in, zl_send),
        (x_in, x_send),
        (zh_in, zh_send),
    ):
        left(whole, send)


def codes(gq, nw, fnew, snew, rows, cols, gq_out, nw_out, nfc_out, nfr_out, nfcol_out, nsc_out, nsr_out, nscol_out):
    gq_out[...] = gq[...]
    nw_out[...] = nw[...]
    nfcol_out[...] = cols[0]
    nscol_out[...] = cols[1]
    for c, start, size in row_chunks():
        at = pl.ds(start, size)
        nfr_out[at] = rows[0, c, 0:size]
        nsr_out[at] = rows[1, c, 0:size]
        low_first = jnp.minimum(down_rows(rows[0, c : c + 1, :])[:size], cols[0:1])
        low_second = jnp.minimum(down_rows(rows[1, c : c + 1, :])[:size], cols[1:2])
        nfc_out[at, :] = (fnew[at, :] / (low_first + code_eps)).astype(BF16)
        nsc_out[at, :] = (snew[at, :] / (low_second + code_eps)).astype(BF16)


def per_device(queries, keys, values, grad_out, weight, fc, frow, fcol, sc, srow, scol):
    shape = jax.ShapeDtypeStruct
    vmem = pl.BlockSpec(memory_space=pltpu.VMEM)
    hbm = pl.BlockSpec(memory_space=pltpu.HBM)
    dma = pltpu.SemaphoreType.DMA
    gq, nw, fnew, snew, rows, cols = pl.pallas_call(
        body,
        name="whole",
        out_shape=(
            shape((SEQ, HD), BF16),
            shape((ROWS, HD), F32),
            shape((ROWS, HD), F32),
            shape((ROWS, HD), F32),
            shape((2, 8, HD), F32),
            shape((2, HD), F32),
        ),
        in_specs=[hbm] * 11,
        out_specs=[vmem] * 6,
        scratch_shapes=[
            pltpu.VMEM((SEQ, HD), BF16),
            pltpu.VMEM((SEQ, HD), BF16),
            pltpu.VMEM((SEQ, HD), BF16),
            pltpu.VMEM((SEQ, HD), BF16),
            pltpu.VMEM((ROWS, HD), F32),
            pltpu.VMEM((ROWS, HD), BF16),
            pltpu.VMEM((ROWS, HD), BF16),
            pltpu.VMEM((ROWS,), F32),
            pltpu.VMEM((HD,), F32),
            pltpu.VMEM((ROWS,), F32),
            pltpu.VMEM((HD,), F32),
            pltpu.VMEM((HD, SEQ), BF16),
            pltpu.VMEM((SLOTS * SLOT, UNIT, SEQ), BF16),
            pltpu.VMEM((NX, HD, ROWS), BF16),
            pltpu.VMEM((NZH, SEQ, HD), BF16),
            pltpu.VMEM((SEQ, SEQ), F32),
            pltpu.VMEM((NZH, HD, SEQ), F32),
            pltpu.VMEM((2, HD, SEQ), BF16),
            pltpu.VMEM((2, HD, SEQ), BF16),
            pltpu.VMEM((NX, ROWS, HD), F32),
            pltpu.VMEM((NX - 1, ROWS, HD), BF16),
            pltpu.VMEM((NX - 1, ROWS, HD), BF16),
            pltpu.VMEM((2, 8, HD), F32),
            pltpu.VMEM((NY - 1, 2, 8, HD), F32),
            pltpu.VMEM((NZL * NC - 1, 2, 8, HD), F32),
            pltpu.VMEM((2, 8, HD), F32),
            pltpu.VMEM((2, 2, HD), F32),
            pltpu.VMEM((NX - 1, 2, HD), F32),
            pltpu.VMEM((NZH - 1, 2, HD), F32),
            dma((11,)),
            dma,
            dma((SLOTS,)),
            dma((SLOTS,)),
            dma((SLOTS,)),
            dma,
            dma((2, SLOTS, 4, 2)),
            dma,
            dma((SLOTS,)),
            dma((SLOTS,)),
            dma,
            dma((SLOTS, 2)),
            dma,
            dma((2,)),
            dma,
            dma,
            dma,
            dma,
            dma,
            dma,
            dma,
            dma,
            dma,
            dma,
            dma,
            dma,
            dma,
            dma,
        ],
        compiler_params=pltpu.CompilerParams(
            collective_id=0, has_side_effects=True, vmem_limit_bytes=48 * 1024 * 1024
        ),
    )(
        *(
            pltpu.with_memory_space_constraint(a, pltpu.HBM)
            for a in (queries, keys, values, grad_out, weight, fc, frow, fcol, sc, srow, scol)
        )
    )
    return pl.pallas_call(
        codes,
        name="codes",
        out_shape=(
            shape((SEQ, HD), BF16),
            shape((ROWS, HD), F32),
            shape((ROWS, HD), BF16),
            shape((ROWS,), F32),
            shape((HD,), F32),
            shape((ROWS, HD), BF16),
            shape((ROWS,), F32),
            shape((HD,), F32),
        ),
        compiler_params=pltpu.CompilerParams(vmem_limit_bytes=8 * 1024 * 1024),
        in_specs=[vmem] * 6,
        out_specs=[vmem] * 8,
    )(gq, nw, fnew, snew, rows, cols)


def solution(mesh):
    finer = Mesh(mesh.devices.reshape(NX, NZH, NY, NZL, NC), AXES)
    placed = (
        P(DP, TENSOR),
        P(DP, None),
        P(DP, None),
        P(DP, TENSOR),
        P(DP, TENSOR),
        P(DP, TENSOR),
        P(DP),
        P(TENSOR),
        P(DP, TENSOR),
        P(DP),
        P(TENSOR),
    )
    return jax.shard_map(
        per_device,
        mesh=finer,
        in_specs=placed,
        out_specs=(
            P(DP, TENSOR),
            P(DP, TENSOR),
            P(DP, TENSOR),
            P(DP),
            P(TENSOR),
            P(DP, TENSOR),
            P(DP),
            P(TENSOR),
        ),
        check_vma=False,
    )
```

```python
import functools

import jax
import jax.numpy as jnp
from jax import lax
from jax.experimental import pallas as pl
from jax.experimental.pallas import tpu as pltpu
from jax.sharding import Mesh
from jax.sharding import PartitionSpec as P

NX, NZH, NY, NZL, NC = 4, 3, 8, 4, 2
AXES = ("x", "zh", "y", "zl", "core")
DP = ("x", "zh")
TENSOR = ("y", "zl", "core")
MESH = pl.DeviceIdType.MESH

HD = 128
SEQ = 384
ROWS = 688
UNIT = 16
UNITS = ROWS // UNIT
ALL_UNITS = 512
HOMES = NY * NC
SLOTS = 4
SLOT = 3 * UNITS
SPLIT = (0,)
AHEAD = (2, 1, 3)
SCALE = HD ** (-0.5)

beta_first = 0.9
beta_second = 0.95
learning = 0.01
decay_rate = 0.1
adam_eps = 1e-08
code_eps = 1e-06
correct_first = 1.0 - 0.9**10
correct_second = 1.0 - 0.95**10

F32 = jnp.float32
BF16 = jnp.bfloat16
NT = (((1,), (1,)), ((), ()))


def mod(a, n):
    return lax.rem(a + n, n)


def row_chunks():
    return [(c, 128 * c, min(128, ROWS - 128 * c)) for c in range(6)]


def lane_rows(values):
    highest = jnp.max(values, axis=1, keepdims=True)
    out = []
    for c, start, size in row_chunks():
        eye = lax.broadcasted_iota(jnp.int32, (size, 128), 0) == lax.broadcasted_iota(
            jnp.int32, (size, 128), 1
        )
        out.append(
            jnp.max(jnp.where(eye, highest[start : start + size], 0.0), axis=0, keepdims=True)
        )
    out.append(jnp.zeros((2, 128), F32))
    return jnp.concatenate(out, axis=0)


def down(vector, start, size):
    row = vector[pl.ds(start, size)].reshape(1, size)
    if size < 128:
        row = jnp.concatenate([row, jnp.zeros((1, 128 - size), F32)], axis=1)
    return down_rows(row)[:size]


def down_rows(row):
    return jnp.broadcast_to(row, (128, 128)).T


def body(
    q_hbm,
    k_hbm,
    v_hbm,
    g_hbm,
    w_hbm,
    fc_hbm,
    frow_hbm,
    fcol_hbm,
    sc_hbm,
    srow_hbm,
    scol_hbm,
    gq_out,
    nw_out,
    fnew_out,
    snew_out,
    rows_out,
    cols_out,
    q,
    kk,
    vv,
    g,
    w,
    fc,
    sc,
    frow,
    fcol,
    srow,
    scol,
    gt,
    gz,
    wt,
    att,
    prob,
    acct,
    ga_stage,
    ga_in,
    dwacc,
    dw_stage,
    dw_in,
    st,
    y_in,
    zl_in,
    mine,
    cst,
    x_in,
    zh_in,
    in_sem,
    spread_send,
    relay_send,
    far_recv,
    near_recv,
    ring_send,
    ring_recv,
    beside_send,
    beside_recv,
    shared_recv,
    core_send,
    core_recv,
    att_send,
    att_recv,
    w_send,
    w_recv,
    ga_send,
    ga_recv,
    dw_send,
    dw_recv,
    y_send,
    y_recv,
    zl_send,
    zl_recv,
    x_send,
    x_recv,
    zh_send,
    zh_recv,
):
    x, zh, y, zl, k = (lax.axis_index(a) for a in AXES)
    t = 8 * y + 2 * zl + k
    pair = lax.div(y, 2)

    def rcopy(src, dst, send, recv, **dev):
        return pltpu.make_async_remote_copy(
            src_ref=src, dst_ref=dst, send_sem=send, recv_sem=recv, device_id=dev, device_id_type=MESH
        )

    def came(ref, recv):
        rcopy(ref, ref, core_send, recv, core=k).wait_recv()

    def sequence_of(source, plane):
        return jnp.where(source == plane, 0, source + (source < plane).astype(jnp.int32))

    def other(sequence):
        return sequence - 1 + (sequence - 1 >= zh).astype(jnp.int32)

    barrier = pltpu.get_barrier_semaphore()

    def greet(**dev):
        pl.semaphore_signal(barrier, inc=1, device_id=dev, device_id_type=MESH)

    for dz in (1, 2):
        greet(zh=mod(zh + dz, NZH))
    for dx in range(1, NX):
        greet(x=mod(x + dx, NX))
    for dy in range(1, NY):
        greet(y=mod(y + dy, NY))
    for rel in range(1, NZL * NC):
        greet(zl=mod(zl + rel // NC, NZL), core=lax.rem(k + rel % NC, NC))
    heads = pl.ds(pl.multiple_of(y * HD, HD), HD)
    loads = [
        pltpu.make_async_copy(src, dst, in_sem.at[i])
        for i, (src, dst) in enumerate(
            [
                (g_hbm, g),
                (q_hbm, q),
                (k_hbm.at[:, heads], kk),
                (v_hbm.at[:, heads], vv),
                (w_hbm, w),
                (fc_hbm, fc),
                (sc_hbm, sc),
                (frow_hbm, frow),
                (fcol_hbm, fcol),
                (srow_hbm, srow),
                (scol_hbm, scol),
            ]
        )
    ]
    for load in loads:
        load.start()

    me = 2 * y + k
    side = zl & 1

    def rows_of(u):
        return pl.ds(pl.multiple_of(UNIT * u, UNIT), UNIT)

    def ahead_of(turn):
        return jnp.where(turn == 0, 2, 2 * turn - 1)

    def slot_and_index(ahead, sequence):
        turn = jnp.where(ahead == 2, 0, lax.shift_right_logical(ahead + 1, 1))
        pair = 2 * turn + sequence - 1
        far = (pair >= 3).astype(jnp.int32)
        slot = jnp.where(ahead == 0, 3, jnp.where(sequence == 0, 0, 1 + far))
        index = jnp.where(
            ahead == 0,
            sequence - 1 + 3 * (sequence == 0).astype(jnp.int32),
            jnp.where(sequence == 0, turn, pair - 3 * far),
        )
        return slot, index

    first_owner = lax.div(8 * t, UNITS)
    first_row = 8 * t - UNITS * first_owner
    turnover = UNITS - first_row
    sides = []
    for owner in (first_owner, first_owner + 1):
        xd = lax.div(owner, NZH)
        zd = owner - NZH * xd
        slot, index = slot_and_index(mod(xd - x, NX), sequence_of(zh, zd))
        sides.append((zd, slot, UNITS * index))

    def goes_to(u):
        over = u >= turnover
        zd, slot, start = (jnp.where(over, b, a) for a, b in zip(*sides))
        e = start + first_row + u - jnp.where(over, UNITS, 0)
        h = jnp.minimum(lax.shift_right_logical(e, 3), HOMES - 1)
        line = zl ^ (2 * (u & 1))
        for split in SPLIT:
            shared = (zl & 2) + (e - 8 * h >= 4).astype(jnp.int32)
            line = jnp.where(slot == split, shared, line)
        home = dict(zh=zd, y=lax.shift_right_logical(h, 1), zl=line, core=h & 1)
        here = (zd == zh) & (h == me) & (home["zl"] == zl)
        return slot, SLOT * slot + e, home, here

    first_index = lax.div(8 * me, UNITS)
    first_place = 8 * me - UNITS * first_index
    has_last = me == HOMES - 1
    units = []
    for slot in range(SLOTS):
        blocks = []
        for index in (first_index, first_index + 1):
            if slot == 0:
                xd, z = (x + ahead_of(index)) & 3, zh
            elif slot == 3:
                xd, z = x, jnp.where(index == 2, zh, other(index + 1))
            else:
                turn = 3 * (slot - 1) + index
                xd = (x + ahead_of(lax.shift_right_logical(turn, 1))) & 3
                z = other(1 + (turn & 1))
            blocks.append((z, UNITS * (NZH * xd + zh)))
        held = []
        for j in range(9):
            over = first_place + j >= UNITS
            z, start = (jnp.where(over, b, a) for a, b in zip(*blocks))
            unit = start + first_place + j - jnp.where(over, UNITS, 0)
            column = lax.shift_right_logical(unit, 3)
            line = lax.shift_right_logical(column, 1) & 3
            there = unit < ALL_UNITS
            missing = jnp.logical_not(there)
            if j == 8:
                there, missing = there & has_last, missing & has_last
            if slot in SPLIT:
                taken = side == min(j // 4, 1)
                there, missing = there & taken, missing & taken
                here = (line & 2) == (zl & 2)
            else:
                here = (line ^ (2 * (unit & 1))) == zl
            source = dict(zh=z, y=lax.shift_right_logical(column, 3), zl=line, core=column & 1)
            held.append((there, there & here, source, (z == zh) & (column == t), missing))
        units.append(held)

    def count(flags):
        return sum(f.astype(jnp.int32) for f in flags)

    landing = [count(lands for _, lands, _, _, _ in held) for held in units]
    coming = [count(there for there, _, _, _, _ in held) - n for held, n in zip(units, landing)]
    staying = [count(lands & same for _, lands, _, same, _ in held) for held in units]

    def greet_home(u, carry):
        slot, place, home, here = goes_to(u)
        pl.when(jnp.logical_not(here))(functools.partial(greet, **home))
        return carry

    lax.fori_loop(0, 8, greet_home, 0)
    for held in units:
        for _, lands, source, same, _ in held:
            pl.when(lands & jnp.logical_not(same))(functools.partial(greet, **source))
    greeted = 8 + sum(landing) - 2 * sum(staying) + 2 + 3 + 7 + 7

    loads[0].wait()
    gt[...] = g[...].T

    for slot, held in enumerate(units):
        for j, (_, _, _, _, missing) in enumerate(held):

            @pl.when(missing)
            def _():
                gz[SLOT * slot + 8 * me + j] = jnp.zeros((UNIT, SEQ), BF16)

    pl.semaphore_wait(barrier, greeted)

    def spread(wanted, u, carry):
        slot, place, home, here = goes_to(u)

        @pl.when((slot == wanted) & here)
        def _():
            gz[place] = gt[rows_of(u), :]

        @pl.when((slot == wanted) & jnp.logical_not(here))
        def _():
            rcopy(gt.at[rows_of(u), :], gz.at[place], spread_send, far_recv.at[slot], **home).start()

        return carry

    for slot in range(SLOTS):
        lax.fori_loop(0, 8, functools.partial(spread, slot), 0)

    loads[4].wait()
    wt[3] = w[...].astype(BF16).T
    for dx in (1, 3, 2):
        rcopy(wt.at[3], wt.at[AHEAD.index(NX - dx)], w_send, w_recv, x=mod(x + dx, NX)).start()

    for i in (1, 2, 3):
        loads[i].wait()
    for i in range(3):
        rows, cols = pl.ds(128 * i, 128), pl.ds(0, 128 * (i + 1))
        scores = (
            lax.dot_general(q[rows, :], kk[cols, :], NT, preferred_element_type=F32) * SCALE
        )
        future = lax.broadcasted_iota(jnp.int32, scores.shape, 1) > (
            lax.broadcasted_iota(jnp.int32, scores.shape, 0) + 128 * i
        )
        scores = jnp.where(future, -1e30, scores)
        exponent = jnp.exp(scores - jnp.max(scores, axis=-1, keepdims=True))
        probabilities = exponent / jnp.sum(exponent, axis=-1, keepdims=True)
        prob[rows, cols] = probabilities
        att[0, rows, :] = jnp.dot(
            probabilities.astype(BF16), vv[cols, :], preferred_element_type=F32
        ).astype(BF16)

    def send_att():
        for sequence in (1, 2):
            o = other(sequence)
            there = sequence_of(zh, o)
            rcopy(att.at[0], att.at[there], att_send, att_recv.at[there - 1], zh=o).start()

    def wait_units(n, most, wait):
        for c in range(1, most + 1):
            pl.when(n == c)(functools.partial(wait, c))

    def units_came(recv, c):
        came(gz.at[0:c], recv)

    def relay(slot):
        wait_units(
            landing[slot] - staying[slot], 9, functools.partial(units_came, far_recv.at[slot])
        )

        for j, (_, lands, _, _, _) in enumerate(units[slot]):
            piece = gz.at[SLOT * slot + 8 * me + j]

            @pl.when(lands)
            def _():
                for dl in (2,) if slot in SPLIT else (1, 3, 2):
                    rcopy(
                        piece, piece, relay_send.at[slot], near_recv.at[slot], zl=mod(zl + dl, NZL)
                    ).start()

    def parts(slot):
        return (0, 1) if slot == SLOTS - 1 else (0,)

    def reach(way, slot):
        return 4 if way == slot % 2 else 3

    def from_source(way, hops):
        return mod(y - hops, NY) if way == 0 else mod(y + hops, NY)

    def parts_of(slot, source, core):
        start = SLOT * slot + 8 * (2 * source + core)
        last = (source == NY - 1) & (core == 1)
        if slot in SPLIT:
            longer = last & (side == 1)
            start = start + 4 * side
            return (((start, 4, jnp.logical_not(longer)), (start, 5, longer)),)
        if len(parts(slot)) == 1:
            return (((start, 8, jnp.logical_not(last)), (start, 9, last)),)
        return (
            ((start, 4, None),),
            ((start + 4, 4, jnp.logical_not(last)), (start + 4, 5, last)),
        )

    def each_size(sizes, act):
        for start, units, when in sizes:
            ref = gz.at[pl.ds(start, units)]
            if when is None:
                act(ref)
            else:
                pl.when(when)(functools.partial(act, ref))

    def forward(way, slot, hops, part):
        def go(piece):
            rcopy(
                piece,
                piece,
                ring_send,
                ring_recv.at[way, slot + part, hops],
                y=mod(y + 1, NY) if way == 0 else mod(y - 1, NY),
            ).start()

        each_size(parts_of(slot, from_source(way, hops), k)[part], go)

    def to_partner(way, slot, hops, part):
        def go(piece):
            rcopy(piece, piece, core_send, core_recv.at[slot, hops // 4], core=1 - k).start()

        each_size(parts_of(slot, from_source(way, hops), k)[part], go)

    def to_beside(way, slot, hops):
        def go(piece):
            rcopy(piece, piece, beside_send, beside_recv.at[SPLIT.index(slot)], zl=zl ^ 1).start()

        if slot in SPLIT:
            each_size(parts_of(slot, from_source(way, hops), k)[0], go)

    def start_ring(slot):
        wait_units(coming[slot], 9, functools.partial(units_came, near_recv.at[slot]))
        for part in parts(slot):
            for way in (0, 1):
                forward(way, slot, 0, part)
        to_beside(0, slot, 0)
        for part in parts(slot):
            to_partner(0, slot, 0, part)

    def pass_on(slot, hops):
        for part in parts(slot):
            for way in (0, 1):
                if hops <= reach(way, slot):
                    each_size(
                        parts_of(slot, from_source(way, hops), k)[part],
                        lambda piece: came(piece, ring_recv.at[way, slot + part, hops - 1]),
                    )
                    if hops < reach(way, slot):
                        forward(way, slot, hops, part)
                    to_beside(way, slot, hops)
                    to_partner(way, slot, hops, part)

    def beside_came(slot):
        longer = (k == 1) & (side == 0)
        pl.when(longer)(functools.partial(came, gz.at[0:33], beside_recv.at[SPLIT.index(slot)]))
        pl.when(jnp.logical_not(longer))(functools.partial(came, gz.at[0:32], beside_recv.at[SPLIT.index(slot)]))
        for source in range(NY):
            start = SLOT * slot + 8 * (2 * source + k) + 4 * (1 - side)

            def go(units):
                piece = gz.at[pl.ds(start, units)]
                rcopy(piece, piece, core_send, shared_recv.at[SPLIT.index(slot)], core=1 - k).start()

            if source < NY - 1:
                go(4)
            else:
                pl.when(longer)(functools.partial(go, 5))
                pl.when(jnp.logical_not(longer))(functools.partial(go, 4))

    def partner_beside(slot):
        longer = (k == 0) & (side == 0)
        pl.when(longer)(functools.partial(came, gz.at[0:33], shared_recv.at[SPLIT.index(slot)]))
        pl.when(jnp.logical_not(longer))(functools.partial(came, gz.at[0:32], shared_recv.at[SPLIT.index(slot)]))

    def partner_near(slot):
        more = (k == 0) & (y != NY // 2 - 1)
        each = 8
        if slot in SPLIT:
            more, each = more & (side == 1), 4
        pl.when(more)(functools.partial(came, gz.at[0 : 7 * each + 1], core_recv.at[slot, 0]))
        pl.when(jnp.logical_not(more))(functools.partial(came, gz.at[0 : 7 * each], core_recv.at[slot, 0]))

    def partner_across(slot):
        more = (k == 0) & (y == NY // 2 - 1)
        each = 8
        if slot in SPLIT:
            more, each = more & (side == 1), 4
        pl.when(more)(functools.partial(came, gz.at[0 : each + 1], core_recv.at[slot, 1]))
        pl.when(jnp.logical_not(more))(functools.partial(came, gz.at[0:each], core_recv.at[slot, 1]))

    def partner_has(slot):
        partner_near(slot)
        partner_across(slot)

    def member(slot, index):
        if slot == 0:
            return index, 0
        turn = 3 * (slot - 1) + index
        return turn // 2, 1 + turn % 2

    started = {("g", 0)}

    def add_to(ref, key, term):
        ref[...] = ref[...] + term if key in started else term
        started.add(key)

    def side_by_side(slot, indices):
        blocks = [gz[pl.ds(SLOT * slot + UNITS * i, UNITS)].reshape(ROWS, SEQ) for i in indices]
        return jnp.concatenate(blocks, axis=1) if len(blocks) > 1 else blocks[0]

    def one_below_another(sequences):
        parts = [att[s] for s in sequences]
        return jnp.concatenate(parts, axis=0) if len(parts) > 1 else parts[0]

    def weight_term(slot, *indices):
        members = [member(slot, i) for i in indices]
        rows = members[0][0]
        term = jnp.dot(
            side_by_side(slot, indices),
            one_below_another([sequence for _, sequence in members]),
            preferred_element_type=F32,
        )
        add_to(dwacc.at[rows], ("w", rows), term)

    def multiply(slot, *indices):
        members = [member(slot, i) for i in indices]
        term = jnp.dot(wt[members[0][0]], side_by_side(slot, indices), preferred_element_type=F32)
        for i, (_, sequence) in enumerate(members):
            add_to(acct.at[sequence], ("g", sequence), term[:, SEQ * i : SEQ * (i + 1)])

    early = jnp.where(lax.rem(y + NY // 2, NY) <= 2, 2, 0)
    last_blocks = (early, jnp.where(early == 2, 0, 1), jnp.where(early == 2, 1, 2))

    def last_term(*turns):
        indices = [last_blocks[turn] for turn in turns]
        term = jnp.dot(
            side_by_side(SLOTS - 1, indices),
            one_below_another([lax.rem(i + 1, NZH) for i in indices]),
            preferred_element_type=F32,
        )
        add_to(dwacc.at[3], ("w", 3), term)

    def last_multiply(*turns):
        indices = [last_blocks[turn] for turn in turns]
        term = jnp.dot(wt[3], side_by_side(SLOTS - 1, indices), preferred_element_type=F32)
        for i, index in enumerate(indices):
            sequence = lax.rem(index + 1, NZH)
            acct[sequence] = acct[sequence] + term[:, SEQ * i : SEQ * (i + 1)]

    def send_term(rows):
        dw_stage[rows] = dwacc[rows].astype(BF16)
        rcopy(
            dw_stage.at[rows], dw_in.at[rows], dw_send, dw_recv, x=mod(x + AHEAD[rows], NX)
        ).start()

    def send_grads():
        for i in range(3):
            for sequence in (1, 2):
                o = other(sequence)
                ga_stage[sequence - 1, i] = acct[sequence, :, 128 * i : 128 * (i + 1)].astype(BF16)
                rcopy(
                    ga_stage.at[sequence - 1, i],
                    ga_in.at[sequence_of(zh, o) - 1, i],
                    ga_send,
                    ga_recv.at[i],
                    zh=o,
                ).start()

    def old_moments():
        acct[0] = jnp.zeros((HD, SEQ), F32)
        for load in loads[5:]:
            load.wait()
        for c, start, size in row_chunks():
            rows = pl.ds(start, size)
            low_first = jnp.minimum(down(frow, start, size), fcol[...].reshape(1, HD))
            low_second = jnp.minimum(down(srow, start, size), scol[...].reshape(1, HD))
            fnew_out[rows, :] = beta_first * (fc[rows, :].astype(F32) * low_first)
            snew_out[rows, :] = beta_second * (sc[rows, :].astype(F32) * low_second)
            weight = w[rows, :]
            nw_out[rows, :] = weight - learning * (decay_rate * weight)

    relay(0)
    start_ring(0)
    relay(1)
    relay(2)
    relay(3)
    pass_on(0, 1)
    start_ring(1)
    pass_on(0, 2)
    pass_on(1, 1)
    start_ring(2)
    send_att()
    pass_on(0, 3)
    pass_on(1, 2)
    pass_on(2, 1)
    start_ring(3)
    pass_on(0, 4)
    pass_on(1, 3)
    pass_on(2, 2)
    old_moments()
    pass_on(3, 1)
    pass_on(1, 4)
    beside_came(0)
    pass_on(2, 3)
    pass_on(3, 2)
    partner_has(1)
    came(att.at[1], att_recv.at[0])
    came(att.at[2], att_recv.at[1])
    weight_term(1, 0, 1)
    partner_has(0)
    partner_beside(0)
    weight_term(0, 0)
    send_term(0)
    pass_on(2, 4)
    weight_term(1, 2)
    weight_term(0, 2)
    pass_on(3, 3)
    weight_term(0, 1)
    partner_has(2)
    weight_term(2, 0)
    send_term(1)
    weight_term(2, 1, 2)
    send_term(2)
    came(wt.at[0:3], w_recv)
    multiply(1, 0, 1)
    multiply(1, 2)
    partner_near(3)
    last_term(0)
    pass_on(3, 4)
    multiply(2, 0)
    multiply(2, 1, 2)
    last_multiply(0)
    partner_across(3)
    last_multiply(1, 2)
    send_grads()
    last_term(1, 2)

    came(dw_in, dw_recv)
    for c, start, size in row_chunks():
        rows = pl.ds(start, size)
        grad = dwacc[3, rows, :]
        for i in range(NX - 1):
            grad = grad + dw_in[i, rows, :].astype(F32)
        first_new = fnew_out[rows, :] + (1.0 - beta_first) * grad
        second_new = snew_out[rows, :] + (1.0 - beta_second) * grad * grad
        step_size = (
            first_new * (1.0 / correct_first) / (jnp.sqrt(second_new * (1.0 / correct_second)) + adam_eps)
        )
        nw_out[rows, :] = nw_out[rows, :] - learning * step_size
        fnew_out[rows, :] = first_new
        snew_out[rows, :] = second_new

    first_abs, second_abs = jnp.abs(fnew_out[...]), jnp.abs(snew_out[...])
    st[0] = lane_rows(first_abs)
    st[1] = lane_rows(second_abs)
    for dy in range(1, NY):
        rcopy(st, y_in.at[NY - dy - 1], y_send, y_recv, y=mod(y + dy, NY)).start()
    cst[0, 0:1, :] = jnp.max(first_abs, axis=0, keepdims=True)
    cst[0, 1:2, :] = jnp.max(second_abs, axis=0, keepdims=True)
    for dx in range(1, NX):
        rcopy(cst.at[0], x_in.at[NX - dx - 1], x_send, x_recv, x=mod(x + dx, NX)).start()

    multiply(0, 0)
    multiply(0, 1)
    multiply(0, 2)

    def back_rows(i):
        rows, cols = pl.ds(128 * i, 128), pl.ds(0, 128 * (i + 1))
        came(ga_in.at[:, i], ga_recv.at[i])
        total = acct[0, :, rows]
        for s in range(2):
            total = total + ga_in[s, i].astype(F32)
        grad_half = total.astype(BF16).T
        grad_probs = lax.dot_general(grad_half, vv[cols, :], NT, preferred_element_type=F32)
        row_dot = jnp.sum(
            grad_half.astype(F32) * att[0, rows, :].astype(F32), axis=-1, keepdims=True
        )
        grad_scores = (prob[rows, cols] * (grad_probs - row_dot)).astype(BF16)
        gq_out[rows, :] = (
            jnp.dot(grad_scores, kk[cols, :], preferred_element_type=F32) * SCALE
        ).astype(BF16)

    came(x_in, x_recv)
    cst[1] = jnp.maximum(cst[0], jnp.max(x_in[...], axis=0))
    for sequence in (1, 2):
        o = other(sequence)
        rcopy(cst.at[1], zh_in.at[sequence_of(zh, o) - 1], zh_send, zh_recv, zh=o).start()
    came(y_in, y_recv)
    mine[...] = jnp.maximum(st[...], jnp.max(y_in[...], axis=0))
    for rel in range(1, NZL * NC):
        dl, dk = rel // NC, rel % NC
        back = NC * ((NZL - dl) % NZL) + dk - 1
        rcopy(
            mine, zl_in.at[back], zl_send, zl_recv, zl=mod(zl + dl, NZL), core=lax.rem(k + dk, NC)
        ).start()
    for i in range(3):
        back_rows(i)
    came(zl_in, zl_recv)
    rows_out[...] = jnp.maximum(mine[...], jnp.max(zl_in[...], axis=0))
    came(zh_in, zh_recv)
    cols_out[...] = jnp.maximum(cst[1], jnp.max(zh_in[...], axis=0))

    def left(ref, send):
        rcopy(ref, ref, send, zh_recv, core=k).wait_send()

    wait_units(8 - sum(staying), 8, lambda c: left(gz.at[0:c], spread_send))
    for slot in range(SLOTS):
        copies = 1 if slot in SPLIT else 3
        wait_units(landing[slot], 9, lambda c: left(gz.at[0 : copies * c], relay_send.at[slot]))
    longer = count(
        (from_source(way, hops) == NY - 1) & (k == 1) & ((side == 1) | (slot not in SPLIT))
        for slot in range(SLOTS)
        for way in (0, 1)
        for hops in range(reach(way, slot))
    )
    usual = 56 * SLOTS - 28 * len(SPLIT)
    for c in range(9):
        pl.when(longer == c)(functools.partial(left, gz.at[0 : usual + c], ring_send))
    more = (k == 1) & (side == 1)
    for flag, each in ((more, 33), (jnp.logical_not(more), 32)):
        pl.when(flag)(functools.partial(left, gz.at[0 : each * len(SPLIT)], beside_send))
    for c in (0, 1):
        pl.when(k == c)(functools.partial(left, gz.at[0 : 64 * SLOTS + SLOTS * c], core_send))
    for whole, send in (
        (att.at[0:2], att_send),
        (wt.at[0:3], w_send),
        (ga_in, ga_send),
        (dw_in, dw_send),
        (y_in, y_send),
        (zl_in, zl_send),
        (x_in, x_send),
        (zh_in, zh_send),
    ):
        left(whole, send)


def codes(gq, nw, fnew, snew, rows, cols, gq_out, nw_out, nfc_out, nfr_out, nfcol_out, nsc_out, nsr_out, nscol_out):
    gq_out[...] = gq[...]
    nw_out[...] = nw[...]
    nfcol_out[...] = cols[0]
    nscol_out[...] = cols[1]
    for c, start, size in row_chunks():
        at = pl.ds(start, size)
        nfr_out[at] = rows[0, c, 0:size]
        nsr_out[at] = rows[1, c, 0:size]
        low_first = jnp.minimum(down_rows(rows[0, c : c + 1, :])[:size], cols[0:1])
        low_second = jnp.minimum(down_rows(rows[1, c : c + 1, :])[:size], cols[1:2])
        nfc_out[at, :] = (fnew[at, :] / (low_first + code_eps)).astype(BF16)
        nsc_out[at, :] = (snew[at, :] / (low_second + code_eps)).astype(BF16)


def per_device(queries, keys, values, grad_out, weight, fc, frow, fcol, sc, srow, scol):
    shape = jax.ShapeDtypeStruct
    vmem = pl.BlockSpec(memory_space=pltpu.VMEM)
    hbm = pl.BlockSpec(memory_space=pltpu.HBM)
    dma = pltpu.SemaphoreType.DMA
    gq, nw, fnew, snew, rows, cols = pl.pallas_call(
        body,
        name="whole",
        out_shape=(
            shape((SEQ, HD), BF16),
            shape((ROWS, HD), F32),
            shape((ROWS, HD), F32),
            shape((ROWS, HD), F32),
            shape((2, 8, HD), F32),
            shape((2, HD), F32),
        ),
        in_specs=[hbm] * 11,
        out_specs=[vmem] * 6,
        scratch_shapes=[
            pltpu.VMEM((SEQ, HD), BF16),
            pltpu.VMEM((SEQ, HD), BF16),
            pltpu.VMEM((SEQ, HD), BF16),
            pltpu.VMEM((SEQ, HD), BF16),
            pltpu.VMEM((ROWS, HD), F32),
            pltpu.VMEM((ROWS, HD), BF16),
            pltpu.VMEM((ROWS, HD), BF16),
            pltpu.VMEM((ROWS,), F32),
            pltpu.VMEM((HD,), F32),
            pltpu.VMEM((ROWS,), F32),
            pltpu.VMEM((HD,), F32),
            pltpu.VMEM((HD, SEQ), BF16),
            pltpu.VMEM((SLOTS * SLOT, UNIT, SEQ), BF16),
            pltpu.VMEM((NX, HD, ROWS), BF16),
            pltpu.VMEM((NZH, SEQ, HD), BF16),
            pltpu.VMEM((SEQ, SEQ), F32),
            pltpu.VMEM((NZH, HD, SEQ), F32),
            pltpu.VMEM((2, 3, HD, HD), BF16),
            pltpu.VMEM((2, 3, HD, HD), BF16),
            pltpu.VMEM((NX, ROWS, HD), F32),
            pltpu.VMEM((NX - 1, ROWS, HD), BF16),
            pltpu.VMEM((NX - 1, ROWS, HD), BF16),
            pltpu.VMEM((2, 8, HD), F32),
            pltpu.VMEM((NY - 1, 2, 8, HD), F32),
            pltpu.VMEM((NZL * NC - 1, 2, 8, HD), F32),
            pltpu.VMEM((2, 8, HD), F32),
            pltpu.VMEM((2, 2, HD), F32),
            pltpu.VMEM((NX - 1, 2, HD), F32),
            pltpu.VMEM((NZH - 1, 2, HD), F32),
            dma((11,)),
            dma,
            dma((SLOTS,)),
            dma((SLOTS,)),
            dma((SLOTS,)),
            dma,
            dma((2, SLOTS + 1, 4)),
            dma,
            dma((len(SPLIT),)),
            dma((len(SPLIT),)),
            dma,
            dma((SLOTS, 2)),
            dma,
            dma((2,)),
            dma,
            dma,
            dma,
            dma((3,)),
            dma,
            dma,
            dma,
            dma,
            dma,
            dma,
            dma,
            dma,
            dma,
            dma,
        ],
        compiler_params=pltpu.CompilerParams(
            collective_id=0, has_side_effects=True, vmem_limit_bytes=48 * 1024 * 1024
        ),
    )(
        *(
            pltpu.with_memory_space_constraint(a, pltpu.HBM)
            for a in (queries, keys, values, grad_out, weight, fc, frow, fcol, sc, srow, scol)
        )
    )
    return pl.pallas_call(
        codes,
        name="codes",
        out_shape=(
            shape((SEQ, HD), BF16),
            shape((ROWS, HD), F32),
            shape((ROWS, HD), BF16),
            shape((ROWS,), F32),
            shape((HD,), F32),
            shape((ROWS, HD), BF16),
            shape((ROWS,), F32),
            shape((HD,), F32),
        ),
        compiler_params=pltpu.CompilerParams(vmem_limit_bytes=8 * 1024 * 1024),
        in_specs=[vmem] * 6,
        out_specs=[vmem] * 8,
    )(gq, nw, fnew, snew, rows, cols)


def solution(mesh):
    finer = Mesh(mesh.devices.reshape(NX, NZH, NY, NZL, NC), AXES)
    placed = (
        P(DP, TENSOR),
        P(DP, None),
        P(DP, None),
        P(DP, TENSOR),
        P(DP, TENSOR),
        P(DP, TENSOR),
        P(DP),
        P(TENSOR),
        P(DP, TENSOR),
        P(DP),
        P(TENSOR),
    )
    return jax.shard_map(
        per_device,
        mesh=finer,
        in_specs=placed,
        out_specs=(
            P(DP, TENSOR),
            P(DP, TENSOR),
            P(DP, TENSOR),
            P(DP),
            P(TENSOR),
            P(DP, TENSOR),
            P(DP),
            P(TENSOR),
        ),
        check_vma=False,
    )
```

```python
import functools

import jax
import jax.numpy as jnp
from jax import lax
from jax.experimental import pallas as pl
from jax.experimental.pallas import tpu as pltpu
from jax.sharding import Mesh
from jax.sharding import PartitionSpec as P

NX, NZH, NY, NZL, NC = 4, 3, 8, 4, 2
AXES = ("x", "zh", "y", "zl", "core")
DP = ("x", "zh")
TENSOR = ("y", "zl", "core")
MESH = pl.DeviceIdType.MESH

HD = 128
SEQ = 384
ROWS = 688
UNIT = 16
UNITS = ROWS // UNIT
ALL_UNITS = 512
HOMES = NY * NC
SLOTS = 4
SLOT = 3 * UNITS
SPLIT = (0,)
AHEAD = (2, 1, 3)
SCALE = HD ** (-0.5)

beta_first = 0.9
beta_second = 0.95
learning = 0.01
decay_rate = 0.1
adam_eps = 1e-08
code_eps = 1e-06
correct_first = 1.0 - 0.9**10
correct_second = 1.0 - 0.95**10

F32 = jnp.float32
BF16 = jnp.bfloat16
NT = (((1,), (1,)), ((), ()))


def mod(a, n):
    return lax.rem(a + n, n)


def row_chunks():
    return [(c, 128 * c, min(128, ROWS - 128 * c)) for c in range(6)]


def lane_rows(values):
    highest = jnp.max(values, axis=1, keepdims=True)
    out = []
    for c, start, size in row_chunks():
        eye = lax.broadcasted_iota(jnp.int32, (size, 128), 0) == lax.broadcasted_iota(
            jnp.int32, (size, 128), 1
        )
        out.append(
            jnp.max(jnp.where(eye, highest[start : start + size], 0.0), axis=0, keepdims=True)
        )
    out.append(jnp.zeros((2, 128), F32))
    return jnp.concatenate(out, axis=0)


def down(vector, start, size):
    row = vector[pl.ds(start, size)].reshape(1, size)
    if size < 128:
        row = jnp.concatenate([row, jnp.zeros((1, 128 - size), F32)], axis=1)
    return down_rows(row)[:size]


def down_rows(row):
    return jnp.broadcast_to(row, (128, 128)).T


def body(
    q_hbm,
    k_hbm,
    v_hbm,
    g_hbm,
    w_hbm,
    fc_hbm,
    frow_hbm,
    fcol_hbm,
    sc_hbm,
    srow_hbm,
    scol_hbm,
    gq_out,
    nw_out,
    fnew_out,
    snew_out,
    rows_out,
    cols_out,
    q,
    kk,
    vv,
    g,
    w,
    fc,
    sc,
    frow,
    fcol,
    srow,
    scol,
    gt,
    gz,
    wt,
    att,
    prob,
    acct,
    ga_stage,
    ga_in,
    dwacc,
    dw_stage,
    dw_in,
    st,
    y_in,
    zl_in,
    mine,
    cst,
    x_in,
    zh_in,
    in_sem,
    spread_send,
    relay_send,
    far_recv,
    near_recv,
    ring_send,
    ring_recv,
    beside_send,
    beside_recv,
    shared_recv,
    core_send,
    core_recv,
    att_send,
    att_recv,
    w_send,
    w_recv,
    ga_send,
    ga_recv,
    dw_send,
    dw_recv,
    y_send,
    y_recv,
    zl_send,
    zl_recv,
    x_send,
    x_recv,
    zh_send,
    zh_recv,
):
    x, zh, y, zl, k = (lax.axis_index(a) for a in AXES)
    t = 8 * y + 2 * zl + k
    pair = lax.div(y, 2)

    def rcopy(src, dst, send, recv, **dev):
        return pltpu.make_async_remote_copy(
            src_ref=src, dst_ref=dst, send_sem=send, recv_sem=recv, device_id=dev, device_id_type=MESH
        )

    def came(ref, recv):
        rcopy(ref, ref, core_send, recv, core=k).wait_recv()

    def sequence_of(source, plane):
        return jnp.where(source == plane, 0, source + (source < plane).astype(jnp.int32))

    def other(sequence):
        return sequence - 1 + (sequence - 1 >= zh).astype(jnp.int32)

    barrier = pltpu.get_barrier_semaphore()

    def greet(**dev):
        pl.semaphore_signal(barrier, inc=1, device_id=dev, device_id_type=MESH)

    for dz in (1, 2):
        greet(zh=mod(zh + dz, NZH))
    for dx in range(1, NX):
        greet(x=mod(x + dx, NX))
    for dy in range(1, NY):
        greet(y=mod(y + dy, NY))
    for rel in range(1, NZL * NC):
        greet(zl=mod(zl + rel // NC, NZL), core=lax.rem(k + rel % NC, NC))
    heads = pl.ds(pl.multiple_of(y * HD, HD), HD)
    loads = [
        pltpu.make_async_copy(src, dst, in_sem.at[i])
        for i, (src, dst) in enumerate(
            [
                (g_hbm, g),
                (q_hbm, q),
                (k_hbm.at[:, heads], kk),
                (v_hbm.at[:, heads], vv),
                (w_hbm, w),
                (fc_hbm, fc),
                (sc_hbm, sc),
                (frow_hbm, frow),
                (fcol_hbm, fcol),
                (srow_hbm, srow),
                (scol_hbm, scol),
            ]
        )
    ]
    for load in loads:
        load.start()

    me = 2 * y + k
    side = zl & 1

    def rows_of(u):
        return pl.ds(pl.multiple_of(UNIT * u, UNIT), UNIT)

    def ahead_of(turn):
        return jnp.where(turn == 0, 2, 2 * turn - 1)

    def slot_and_index(ahead, sequence):
        turn = jnp.where(ahead == 2, 0, lax.shift_right_logical(ahead + 1, 1))
        pair = 2 * turn + sequence - 1
        far = (pair >= 3).astype(jnp.int32)
        slot = jnp.where(ahead == 0, 3, jnp.where(sequence == 0, 0, 1 + far))
        index = jnp.where(
            ahead == 0,
            sequence - 1 + 3 * (sequence == 0).astype(jnp.int32),
            jnp.where(sequence == 0, turn, pair - 3 * far),
        )
        return slot, index

    first_owner = lax.div(8 * t, UNITS)
    first_row = 8 * t - UNITS * first_owner
    turnover = UNITS - first_row
    sides = []
    for owner in (first_owner, first_owner + 1):
        xd = lax.div(owner, NZH)
        zd = owner - NZH * xd
        slot, index = slot_and_index(mod(xd - x, NX), sequence_of(zh, zd))
        sides.append((zd, slot, UNITS * index))

    def goes_to(u):
        over = u >= turnover
        zd, slot, start = (jnp.where(over, b, a) for a, b in zip(*sides))
        e = start + first_row + u - jnp.where(over, UNITS, 0)
        h = jnp.minimum(lax.shift_right_logical(e, 3), HOMES - 1)
        line = zl ^ (2 * (u & 1))
        for split in SPLIT:
            shared = (zl & 2) + (e - 8 * h >= 4).astype(jnp.int32)
            line = jnp.where(slot == split, shared, line)
        home = dict(zh=zd, y=lax.shift_right_logical(h, 1), zl=line, core=h & 1)
        here = (zd == zh) & (h == me) & (home["zl"] == zl)
        return slot, SLOT * slot + e, home, here

    def greet_home(u, carry):
        slot, place, home, here = goes_to(u)
        pl.when(jnp.logical_not(here))(functools.partial(greet, **home))
        return carry

    lax.fori_loop(0, 8, greet_home, 0)

    first_index = lax.div(8 * me, UNITS)
    first_place = 8 * me - UNITS * first_index
    has_last = me == HOMES - 1
    units = []
    for slot in range(SLOTS):
        blocks = []
        for index in (first_index, first_index + 1):
            if slot == 0:
                xd, z = (x + ahead_of(index)) & 3, zh
            elif slot == 3:
                xd, z = x, jnp.where(index == 2, zh, other(index + 1))
            else:
                turn = 3 * (slot - 1) + index
                xd = (x + ahead_of(lax.shift_right_logical(turn, 1))) & 3
                z = other(1 + (turn & 1))
            blocks.append((z, UNITS * (NZH * xd + zh)))
        held = []
        for j in range(9):
            over = first_place + j >= UNITS
            z, start = (jnp.where(over, b, a) for a, b in zip(*blocks))
            unit = start + first_place + j - jnp.where(over, UNITS, 0)
            column = lax.shift_right_logical(unit, 3)
            line = lax.shift_right_logical(column, 1) & 3
            there = unit < ALL_UNITS
            missing = jnp.logical_not(there)
            if j == 8:
                there, missing = there & has_last, missing & has_last
            if slot in SPLIT:
                taken = side == min(j // 4, 1)
                there, missing = there & taken, missing & taken
                here = (line & 2) == (zl & 2)
            else:
                here = (line ^ (2 * (unit & 1))) == zl
            source = dict(zh=z, y=lax.shift_right_logical(column, 3), zl=line, core=column & 1)
            held.append((there, there & here, source, (z == zh) & (column == t), missing))
        units.append(held)

    def count(flags):
        return sum(f.astype(jnp.int32) for f in flags)

    landing = [count(lands for _, lands, _, _, _ in held) for held in units]
    coming = [count(there for there, _, _, _, _ in held) - n for held, n in zip(units, landing)]
    staying = [count(lands & same for _, lands, _, same, _ in held) for held in units]

    for held in units:
        for _, lands, source, same, _ in held:
            pl.when(lands & jnp.logical_not(same))(functools.partial(greet, **source))
    greeted = 8 + sum(landing) - 2 * sum(staying) + 2 + 3 + 7 + 7

    loads[0].wait()
    gt[...] = g[...].T

    pl.semaphore_wait(barrier, greeted)

    def spread(u, carry):
        slot, place, home, here = goes_to(u)

        @pl.when(here)
        def _():
            gz[place] = gt[rows_of(u), :]

        @pl.when(jnp.logical_not(here))
        def _():
            rcopy(gt.at[rows_of(u), :], gz.at[place], spread_send, far_recv.at[slot], **home).start()

        return carry

    lax.fori_loop(0, 8, spread, 0)

    loads[4].wait()
    wt[3] = w[...].astype(BF16).T
    for dx in (1, 3, 2):
        rcopy(wt.at[3], wt.at[AHEAD.index(NX - dx)], w_send, w_recv, x=mod(x + dx, NX)).start()

    for i in (1, 2, 3):
        loads[i].wait()
    for i in range(3):
        rows, cols = pl.ds(128 * i, 128), pl.ds(0, 128 * (i + 1))
        scores = (
            lax.dot_general(q[rows, :], kk[cols, :], NT, preferred_element_type=F32) * SCALE
        )
        future = lax.broadcasted_iota(jnp.int32, scores.shape, 1) > (
            lax.broadcasted_iota(jnp.int32, scores.shape, 0) + 128 * i
        )
        scores = jnp.where(future, -1e30, scores)
        exponent = jnp.exp(scores - jnp.max(scores, axis=-1, keepdims=True))
        probabilities = exponent / jnp.sum(exponent, axis=-1, keepdims=True)
        prob[rows, cols] = probabilities
        att[0, rows, :] = jnp.dot(
            probabilities.astype(BF16), vv[cols, :], preferred_element_type=F32
        ).astype(BF16)

    for slot, held in enumerate(units):
        for j, (_, _, _, _, missing) in enumerate(held):

            @pl.when(missing)
            def _():
                gz[SLOT * slot + 8 * me + j] = jnp.zeros((UNIT, SEQ), BF16)

    def send_att():
        for sequence in (1, 2):
            o = other(sequence)
            there = sequence_of(zh, o)
            rcopy(att.at[0], att.at[there], att_send, att_recv.at[there - 1], zh=o).start()

    def wait_units(n, most, wait):
        for c in range(1, most + 1):
            pl.when(n == c)(functools.partial(wait, c))

    def units_came(recv, c):
        came(gz.at[0:c], recv)

    def relay(slot):
        wait_units(
            landing[slot] - staying[slot], 9, functools.partial(units_came, far_recv.at[slot])
        )

        for j, (_, lands, _, _, _) in enumerate(units[slot]):
            piece = gz.at[SLOT * slot + 8 * me + j]

            @pl.when(lands)
            def _():
                for dl in (2,) if slot in SPLIT else (1, 3, 2):
                    rcopy(
                        piece, piece, relay_send.at[slot], near_recv.at[slot], zl=mod(zl + dl, NZL)
                    ).start()

    def parts(slot):
        return (0, 1) if slot == SLOTS - 1 else (0,)

    def reach(way, slot):
        return 4 if way == slot % 2 else 3

    def from_source(way, hops):
        return mod(y - hops, NY) if way == 0 else mod(y + hops, NY)

    def parts_of(slot, source, core):
        start = SLOT * slot + 8 * (2 * source + core)
        last = (source == NY - 1) & (core == 1)
        if slot in SPLIT:
            longer = last & (side == 1)
            start = start + 4 * side
            return (((start, 4, jnp.logical_not(longer)), (start, 5, longer)),)
        if len(parts(slot)) == 1:
            return (((start, 8, jnp.logical_not(last)), (start, 9, last)),)
        return (
            ((start, 4, None),),
            ((start + 4, 4, jnp.logical_not(last)), (start + 4, 5, last)),
        )

    def each_size(sizes, act):
        for start, units, when in sizes:
            ref = gz.at[pl.ds(start, units)]
            if when is None:
                act(ref)
            else:
                pl.when(when)(functools.partial(act, ref))

    def forward(way, slot, hops, part):
        def go(piece):
            rcopy(
                piece,
                piece,
                ring_send,
                ring_recv.at[way, slot + part, hops],
                y=mod(y + 1, NY) if way == 0 else mod(y - 1, NY),
            ).start()

        each_size(parts_of(slot, from_source(way, hops), k)[part], go)

    def to_partner(way, slot, hops, part):
        def go(piece):
            rcopy(piece, piece, core_send, core_recv.at[slot, hops // 4], core=1 - k).start()

        each_size(parts_of(slot, from_source(way, hops), k)[part], go)

    def to_beside(way, slot, hops):
        def go(piece):
            rcopy(piece, piece, beside_send, beside_recv.at[SPLIT.index(slot)], zl=zl ^ 1).start()

        if slot in SPLIT:
            each_size(parts_of(slot, from_source(way, hops), k)[0], go)

    def start_ring(slot):
        wait_units(coming[slot], 9, functools.partial(units_came, near_recv.at[slot]))
        for part in parts(slot):
            for way in (0, 1):
                forward(way, slot, 0, part)
        to_beside(0, slot, 0)
        for part in parts(slot):
            to_partner(0, slot, 0, part)

    def pass_on(slot, hops):
        for part in parts(slot):
            for way in (0, 1):
                if hops <= reach(way, slot):
                    each_size(
                        parts_of(slot, from_source(way, hops), k)[part],
                        lambda piece: came(piece, ring_recv.at[way, slot + part, hops - 1]),
                    )
                    if hops < reach(way, slot):
                        forward(way, slot, hops, part)
                    to_beside(way, slot, hops)
                    to_partner(way, slot, hops, part)

    def beside_came(slot):
        longer = (k == 1) & (side == 0)
        pl.when(longer)(functools.partial(came, gz.at[0:33], beside_recv.at[SPLIT.index(slot)]))
        pl.when(jnp.logical_not(longer))(functools.partial(came, gz.at[0:32], beside_recv.at[SPLIT.index(slot)]))
        for source in range(NY):
            start = SLOT * slot + 8 * (2 * source + k) + 4 * (1 - side)

            def go(units):
                piece = gz.at[pl.ds(start, units)]
                rcopy(piece, piece, core_send, shared_recv.at[SPLIT.index(slot)], core=1 - k).start()

            if source < NY - 1:
                go(4)
            else:
                pl.when(longer)(functools.partial(go, 5))
                pl.when(jnp.logical_not(longer))(functools.partial(go, 4))

    def partner_beside(slot):
        longer = (k == 0) & (side == 0)
        pl.when(longer)(functools.partial(came, gz.at[0:33], shared_recv.at[SPLIT.index(slot)]))
        pl.when(jnp.logical_not(longer))(functools.partial(came, gz.at[0:32], shared_recv.at[SPLIT.index(slot)]))

    def partner_near(slot):
        more = (k == 0) & (y != NY // 2 - 1)
        each = 8
        if slot in SPLIT:
            more, each = more & (side == 1), 4
        pl.when(more)(functools.partial(came, gz.at[0 : 7 * each + 1], core_recv.at[slot, 0]))
        pl.when(jnp.logical_not(more))(functools.partial(came, gz.at[0 : 7 * each], core_recv.at[slot, 0]))

    def partner_across(slot):
        more = (k == 0) & (y == NY // 2 - 1)
        each = 8
        if slot in SPLIT:
            more, each = more & (side == 1), 4
        pl.when(more)(functools.partial(came, gz.at[0 : each + 1], core_recv.at[slot, 1]))
        pl.when(jnp.logical_not(more))(functools.partial(came, gz.at[0:each], core_recv.at[slot, 1]))

    def partner_has(slot):
        partner_near(slot)
        partner_across(slot)

    def member(slot, index):
        if slot == 0:
            return index, 0
        turn = 3 * (slot - 1) + index
        return turn // 2, 1 + turn % 2

    started = {("g", 0)}

    def add_to(ref, key, term):
        ref[...] = ref[...] + term if key in started else term
        started.add(key)

    def side_by_side(slot, indices):
        blocks = [gz[pl.ds(SLOT * slot + UNITS * i, UNITS)].reshape(ROWS, SEQ) for i in indices]
        return jnp.concatenate(blocks, axis=1) if len(blocks) > 1 else blocks[0]

    def one_below_another(sequences):
        parts = [att[s] for s in sequences]
        return jnp.concatenate(parts, axis=0) if len(parts) > 1 else parts[0]

    def weight_term(slot, *indices):
        members = [member(slot, i) for i in indices]
        rows = members[0][0]
        term = jnp.dot(
            side_by_side(slot, indices),
            one_below_another([sequence for _, sequence in members]),
            preferred_element_type=F32,
        )
        add_to(dwacc.at[rows], ("w", rows), term)

    def multiply(slot, *indices):
        members = [member(slot, i) for i in indices]
        term = jnp.dot(wt[members[0][0]], side_by_side(slot, indices), preferred_element_type=F32)
        for i, (_, sequence) in enumerate(members):
            add_to(acct.at[sequence], ("g", sequence), term[:, SEQ * i : SEQ * (i + 1)])

    early = jnp.where(lax.rem(y + NY // 2, NY) <= 2, 2, 0)
    last_blocks = (early, jnp.where(early == 2, 0, 1), jnp.where(early == 2, 1, 2))

    def last_term(*turns):
        indices = [last_blocks[turn] for turn in turns]
        term = jnp.dot(
            side_by_side(SLOTS - 1, indices),
            one_below_another([lax.rem(i + 1, NZH) for i in indices]),
            preferred_element_type=F32,
        )
        add_to(dwacc.at[3], ("w", 3), term)

    def last_multiply(*turns):
        indices = [last_blocks[turn] for turn in turns]
        term = jnp.dot(wt[3], side_by_side(SLOTS - 1, indices), preferred_element_type=F32)
        for i, index in enumerate(indices):
            sequence = lax.rem(index + 1, NZH)
            acct[sequence] = acct[sequence] + term[:, SEQ * i : SEQ * (i + 1)]

    def send_term(rows):
        dw_stage[rows] = dwacc[rows].astype(BF16)
        rcopy(
            dw_stage.at[rows], dw_in.at[rows], dw_send, dw_recv, x=mod(x + AHEAD[rows], NX)
        ).start()

    def send_grads():
        for i in range(3):
            for sequence in (1, 2):
                o = other(sequence)
                ga_stage[sequence - 1, i] = acct[sequence, :, 128 * i : 128 * (i + 1)].astype(BF16)
                rcopy(
                    ga_stage.at[sequence - 1, i],
                    ga_in.at[sequence_of(zh, o) - 1, i],
                    ga_send,
                    ga_recv.at[i],
                    zh=o,
                ).start()

    def old_moments():
        acct[0] = jnp.zeros((HD, SEQ), F32)
        for load in loads[5:]:
            load.wait()
        for c, start, size in row_chunks():
            rows = pl.ds(start, size)
            low_first = jnp.minimum(down(frow, start, size), fcol[...].reshape(1, HD))
            low_second = jnp.minimum(down(srow, start, size), scol[...].reshape(1, HD))
            fnew_out[rows, :] = beta_first * (fc[rows, :].astype(F32) * low_first)
            snew_out[rows, :] = beta_second * (sc[rows, :].astype(F32) * low_second)
            weight = w[rows, :]
            nw_out[rows, :] = weight - learning * (decay_rate * weight)

    relay(0)
    start_ring(0)
    relay(1)
    relay(2)
    relay(3)
    pass_on(0, 1)
    start_ring(1)
    pass_on(0, 2)
    pass_on(1, 1)
    start_ring(2)
    send_att()
    pass_on(0, 3)
    pass_on(1, 2)
    pass_on(2, 1)
    start_ring(3)
    pass_on(0, 4)
    pass_on(1, 3)
    pass_on(2, 2)
    old_moments()
    pass_on(3, 1)
    pass_on(1, 4)
    beside_came(0)
    pass_on(2, 3)
    pass_on(3, 2)
    partner_has(1)
    came(att.at[1], att_recv.at[0])
    came(att.at[2], att_recv.at[1])
    weight_term(1, 0, 1)
    partner_has(0)
    partner_beside(0)
    weight_term(0, 0)
    send_term(0)
    pass_on(2, 4)
    weight_term(1, 2)
    weight_term(0, 2)
    pass_on(3, 3)
    weight_term(0, 1)
    partner_has(2)
    weight_term(2, 0)
    send_term(1)
    weight_term(2, 1, 2)
    send_term(2)
    came(wt.at[0:3], w_recv)
    multiply(1, 0, 1)
    multiply(1, 2)
    partner_near(3)
    last_term(0)
    pass_on(3, 4)
    multiply(2, 0)
    multiply(2, 1, 2)
    last_multiply(0)
    partner_across(3)
    last_multiply(1, 2)
    send_grads()
    last_term(1, 2)

    came(dw_in, dw_recv)
    for c, start, size in row_chunks():
        rows = pl.ds(start, size)
        grad = dwacc[3, rows, :]
        for i in range(NX - 1):
            grad = grad + dw_in[i, rows, :].astype(F32)
        first_new = fnew_out[rows, :] + (1.0 - beta_first) * grad
        second_new = snew_out[rows, :] + (1.0 - beta_second) * grad * grad
        step_size = (
            first_new * (1.0 / correct_first) / (jnp.sqrt(second_new * (1.0 / correct_second)) + adam_eps)
        )
        nw_out[rows, :] = nw_out[rows, :] - learning * step_size
        fnew_out[rows, :] = first_new
        snew_out[rows, :] = second_new

    first_abs, second_abs = jnp.abs(fnew_out[...]), jnp.abs(snew_out[...])
    st[0] = lane_rows(first_abs)
    st[1] = lane_rows(second_abs)
    for dy in range(1, NY):
        rcopy(st, y_in.at[NY - dy - 1], y_send, y_recv, y=mod(y + dy, NY)).start()
    cst[0, 0:1, :] = jnp.max(first_abs, axis=0, keepdims=True)
    cst[0, 1:2, :] = jnp.max(second_abs, axis=0, keepdims=True)
    for dx in range(1, NX):
        rcopy(cst.at[0], x_in.at[NX - dx - 1], x_send, x_recv, x=mod(x + dx, NX)).start()

    multiply(0, 0)
    multiply(0, 1)
    multiply(0, 2)

    def back_rows(i):
        rows, cols = pl.ds(128 * i, 128), pl.ds(0, 128 * (i + 1))
        came(ga_in.at[:, i], ga_recv.at[i])
        total = acct[0, :, rows]
        for s in range(2):
            total = total + ga_in[s, i].astype(F32)
        grad_half = total.astype(BF16).T
        grad_probs = lax.dot_general(grad_half, vv[cols, :], NT, preferred_element_type=F32)
        row_dot = jnp.sum(
            grad_half.astype(F32) * att[0, rows, :].astype(F32), axis=-1, keepdims=True
        )
        grad_scores = (prob[rows, cols] * (grad_probs - row_dot)).astype(BF16)
        gq_out[rows, :] = (
            jnp.dot(grad_scores, kk[cols, :], preferred_element_type=F32) * SCALE
        ).astype(BF16)

    def left(ref, send):
        rcopy(ref, ref, send, zh_recv, core=k).wait_send()

    wait_units(8 - sum(staying), 8, lambda c: left(gz.at[0:c], spread_send))
    for slot in range(SLOTS):
        copies = 1 if slot in SPLIT else 3
        wait_units(landing[slot], 9, lambda c: left(gz.at[0 : copies * c], relay_send.at[slot]))
    longer = count(
        (from_source(way, hops) == NY - 1) & (k == 1) & ((side == 1) | (slot not in SPLIT))
        for slot in range(SLOTS)
        for way in (0, 1)
        for hops in range(reach(way, slot))
    )
    usual = 56 * SLOTS - 28 * len(SPLIT)
    for c in range(9):
        pl.when(longer == c)(functools.partial(left, gz.at[0 : usual + c], ring_send))
    more = (k == 1) & (side == 1)
    for flag, each in ((more, 33), (jnp.logical_not(more), 32)):
        pl.when(flag)(functools.partial(left, gz.at[0 : each * len(SPLIT)], beside_send))
    for c in (0, 1):
        pl.when(k == c)(functools.partial(left, gz.at[0 : 64 * SLOTS + SLOTS * c], core_send))
    for whole, send in (
        (att.at[0:2], att_send),
        (wt.at[0:3], w_send),
        (dw_in, dw_send),
    ):
        left(whole, send)

    came(x_in, x_recv)
    cst[1] = jnp.maximum(cst[0], jnp.max(x_in[...], axis=0))
    for sequence in (1, 2):
        o = other(sequence)
        rcopy(cst.at[1], zh_in.at[sequence_of(zh, o) - 1], zh_send, zh_recv, zh=o).start()
    came(y_in, y_recv)
    mine[...] = jnp.maximum(st[...], jnp.max(y_in[...], axis=0))
    for rel in range(1, NZL * NC):
        dl, dk = rel // NC, rel % NC
        back = NC * ((NZL - dl) % NZL) + dk - 1
        rcopy(
            mine, zl_in.at[back], zl_send, zl_recv, zl=mod(zl + dl, NZL), core=lax.rem(k + dk, NC)
        ).start()
    for i in range(3):
        back_rows(i)
    came(zl_in, zl_recv)
    rows_out[...] = jnp.maximum(mine[...], jnp.max(zl_in[...], axis=0))
    came(zh_in, zh_recv)
    cols_out[...] = jnp.maximum(cst[1], jnp.max(zh_in[...], axis=0))

    for whole, send in (
        (ga_in, ga_send),
        (y_in, y_send),
        (zl_in, zl_send),
        (x_in, x_send),
        (zh_in, zh_send),
    ):
        left(whole, send)


def codes(
    gq,
    nw,
    fnew,
    snew,
    rows,
    cols,
    gq_out,
    nw_out,
    nfc_out,
    nfr_out,
    nfcol_out,
    nsc_out,
    nsr_out,
    nscol_out,
    first_code,
    second_code,
    first_rows,
    second_rows,
    first_cols,
    second_cols,
    sem,
):
    copies = []

    def out(src, dst):
        copy = pltpu.make_async_copy(src, dst, sem.at[len(copies)])
        copy.start()
        copies.append(copy)

    out(gq, gq_out)
    out(nw, nw_out)
    for moment, (new, code, code_out, maxima, maxima_out, col, col_out) in enumerate(
        (
            (fnew, first_code, nfc_out, first_rows, nfr_out, first_cols, nfcol_out),
            (snew, second_code, nsc_out, second_rows, nsr_out, second_cols, nscol_out),
        )
    ):
        col[...] = cols[moment]
        for c, start, size in row_chunks():
            at = pl.ds(start, size)
            maxima[at] = rows[moment, c, 0:size]
            low = jnp.minimum(
                down_rows(rows[moment, c : c + 1, :])[:size], cols[moment : moment + 1]
            )
            code[at, :] = (new[at, :] / (low + code_eps)).astype(BF16)
        out(code, code_out)
        out(maxima, maxima_out)
        out(col, col_out)
    for copy in copies:
        copy.wait()


def per_device(queries, keys, values, grad_out, weight, fc, frow, fcol, sc, srow, scol):
    shape = jax.ShapeDtypeStruct
    vmem = pl.BlockSpec(memory_space=pltpu.VMEM)
    hbm = pl.BlockSpec(memory_space=pltpu.HBM)
    dma = pltpu.SemaphoreType.DMA
    gq, nw, fnew, snew, rows, cols = pl.pallas_call(
        body,
        name="whole",
        out_shape=(
            shape((SEQ, HD), BF16),
            shape((ROWS, HD), F32),
            shape((ROWS, HD), F32),
            shape((ROWS, HD), F32),
            shape((2, 8, HD), F32),
            shape((2, HD), F32),
        ),
        in_specs=[hbm] * 11,
        out_specs=[vmem] * 6,
        scratch_shapes=[
            pltpu.VMEM((SEQ, HD), BF16),
            pltpu.VMEM((SEQ, HD), BF16),
            pltpu.VMEM((SEQ, HD), BF16),
            pltpu.VMEM((SEQ, HD), BF16),
            pltpu.VMEM((ROWS, HD), F32),
            pltpu.VMEM((ROWS, HD), BF16),
            pltpu.VMEM((ROWS, HD), BF16),
            pltpu.VMEM((ROWS,), F32),
            pltpu.VMEM((HD,), F32),
            pltpu.VMEM((ROWS,), F32),
            pltpu.VMEM((HD,), F32),
            pltpu.VMEM((HD, SEQ), BF16),
            pltpu.VMEM((SLOTS * SLOT, UNIT, SEQ), BF16),
            pltpu.VMEM((NX, HD, ROWS), BF16),
            pltpu.VMEM((NZH, SEQ, HD), BF16),
            pltpu.VMEM((SEQ, SEQ), F32),
            pltpu.VMEM((NZH, HD, SEQ), F32),
            pltpu.VMEM((2, 3, HD, HD), BF16),
            pltpu.VMEM((2, 3, HD, HD), BF16),
            pltpu.VMEM((NX, ROWS, HD), F32),
            pltpu.VMEM((NX - 1, ROWS, HD), BF16),
            pltpu.VMEM((NX - 1, ROWS, HD), BF16),
            pltpu.VMEM((2, 8, HD), F32),
            pltpu.VMEM((NY - 1, 2, 8, HD), F32),
            pltpu.VMEM((NZL * NC - 1, 2, 8, HD), F32),
            pltpu.VMEM((2, 8, HD), F32),
            pltpu.VMEM((2, 2, HD), F32),
            pltpu.VMEM((NX - 1, 2, HD), F32),
            pltpu.VMEM((NZH - 1, 2, HD), F32),
            dma((11,)),
            dma,
            dma((SLOTS,)),
            dma((SLOTS,)),
            dma((SLOTS,)),
            dma,
            dma((2, SLOTS + 1, 4)),
            dma,
            dma((len(SPLIT),)),
            dma((len(SPLIT),)),
            dma,
            dma((SLOTS, 2)),
            dma,
            dma((2,)),
            dma,
            dma,
            dma,
            dma((3,)),
            dma,
            dma,
            dma,
            dma,
            dma,
            dma,
            dma,
            dma,
            dma,
            dma,
        ],
        compiler_params=pltpu.CompilerParams(
            collective_id=0, has_side_effects=True, vmem_limit_bytes=48 * 1024 * 1024
        ),
    )(
        *(
            pltpu.with_memory_space_constraint(a, pltpu.HBM)
            for a in (queries, keys, values, grad_out, weight, fc, frow, fcol, sc, srow, scol)
        )
    )
    return pl.pallas_call(
        codes,
        name="codes",
        out_shape=(
            shape((SEQ, HD), BF16),
            shape((ROWS, HD), F32),
            shape((ROWS, HD), BF16),
            shape((ROWS,), F32),
            shape((HD,), F32),
            shape((ROWS, HD), BF16),
            shape((ROWS,), F32),
            shape((HD,), F32),
        ),
        compiler_params=pltpu.CompilerParams(vmem_limit_bytes=8 * 1024 * 1024),
        in_specs=[vmem] * 6,
        out_specs=[hbm] * 8,
        scratch_shapes=[
            pltpu.VMEM((ROWS, HD), BF16),
            pltpu.VMEM((ROWS, HD), BF16),
            pltpu.VMEM((ROWS,), F32),
            pltpu.VMEM((ROWS,), F32),
            pltpu.VMEM((HD,), F32),
            pltpu.VMEM((HD,), F32),
            dma((8,)),
        ],
    )(gq, nw, fnew, snew, rows, cols)


def solution(mesh):
    finer = Mesh(mesh.devices.reshape(NX, NZH, NY, NZL, NC), AXES)
    placed = (
        P(DP, TENSOR),
        P(DP, None),
        P(DP, None),
        P(DP, TENSOR),
        P(DP, TENSOR),
        P(DP, TENSOR),
        P(DP),
        P(TENSOR),
        P(DP, TENSOR),
        P(DP),
        P(TENSOR),
    )
    return jax.shard_map(
        per_device,
        mesh=finer,
        in_specs=placed,
        out_specs=(
            P(DP, TENSOR),
            P(DP, TENSOR),
            P(DP, TENSOR),
            P(DP),
            P(TENSOR),
            P(DP, TENSOR),
            P(DP),
            P(TENSOR),
        ),
        check_vma=False,
    )
```

```python
import functools

import jax
import jax.numpy as jnp
from jax import lax
from jax.experimental import pallas as pl
from jax.experimental.pallas import tpu as pltpu
from jax.sharding import Mesh
from jax.sharding import PartitionSpec as P

NX, NZH, NY, NZL, NC = 4, 3, 8, 4, 2
AXES = ("x", "zh", "y", "zl", "core")
DP = ("x", "zh")
TENSOR = ("y", "zl", "core")
MESH = pl.DeviceIdType.MESH

HD = 128
SEQ = 384
ROWS = 688
UNIT = 16
UNITS = ROWS // UNIT
ALL_UNITS = 512
HOMES = NY * NC
SLOTS = 4
SLOT = 3 * UNITS
SPLIT = (0,)
AHEAD = (2, 1, 3)
SCALE = HD ** (-0.5)

beta_first = 0.9
beta_second = 0.95
learning = 0.01
decay_rate = 0.1
adam_eps = 1e-08
code_eps = 1e-06
correct_first = 1.0 - 0.9**10
correct_second = 1.0 - 0.95**10

F32 = jnp.float32
BF16 = jnp.bfloat16
NT = (((1,), (1,)), ((), ()))


def mod(a, n):
    return lax.rem(a + n, n)


def row_chunks():
    return [(c, 128 * c, min(128, ROWS - 128 * c)) for c in range(6)]


def lane_rows(values):
    highest = jnp.max(values, axis=1, keepdims=True)
    out = []
    for c, start, size in row_chunks():
        eye = lax.broadcasted_iota(jnp.int32, (size, 128), 0) == lax.broadcasted_iota(
            jnp.int32, (size, 128), 1
        )
        out.append(
            jnp.max(jnp.where(eye, highest[start : start + size], 0.0), axis=0, keepdims=True)
        )
    out.append(jnp.zeros((2, 128), F32))
    return jnp.concatenate(out, axis=0)


def down(vector, start, size):
    row = vector[pl.ds(start, size)].reshape(1, size)
    if size < 128:
        row = jnp.concatenate([row, jnp.zeros((1, 128 - size), F32)], axis=1)
    return down_rows(row)[:size]


def down_rows(row):
    return jnp.broadcast_to(row, (128, 128)).T


def body(
    q_hbm,
    k_hbm,
    v_hbm,
    g_hbm,
    w_hbm,
    fc_hbm,
    frow_hbm,
    fcol_hbm,
    sc_hbm,
    srow_hbm,
    scol_hbm,
    gq_out,
    nw_out,
    fnew_out,
    snew_out,
    rows_out,
    cols_out,
    q,
    kk,
    vv,
    g,
    w,
    fc,
    sc,
    frow,
    fcol,
    srow,
    scol,
    gt,
    gz,
    wt,
    att,
    prob,
    acct,
    ga_stage,
    ga_in,
    dwacc,
    dw_stage,
    dw_in,
    st,
    y_in,
    zl_in,
    mine,
    cst,
    x_in,
    zh_in,
    in_sem,
    spread_send,
    relay_send,
    far_recv,
    near_recv,
    ring_send,
    ring_recv,
    beside_send,
    beside_recv,
    shared_recv,
    core_send,
    core_recv,
    att_send,
    att_recv,
    w_send,
    w_recv,
    ga_send,
    ga_recv,
    dw_send,
    dw_recv,
    y_send,
    y_recv,
    zl_send,
    zl_recv,
    x_send,
    x_recv,
    zh_send,
    zh_recv,
):
    x, zh, y, zl, k = (lax.axis_index(a) for a in AXES)
    t = 8 * y + 2 * zl + k
    pair = lax.div(y, 2)

    def rcopy(src, dst, send, recv, **dev):
        return pltpu.make_async_remote_copy(
            src_ref=src, dst_ref=dst, send_sem=send, recv_sem=recv, device_id=dev, device_id_type=MESH
        )

    def came(ref, recv):
        rcopy(ref, ref, core_send, recv, core=k).wait_recv()

    def sequence_of(source, plane):
        return jnp.where(source == plane, 0, source + (source < plane).astype(jnp.int32))

    def other(sequence):
        return sequence - 1 + (sequence - 1 >= zh).astype(jnp.int32)

    barrier = pltpu.get_barrier_semaphore()

    def greet(**dev):
        pl.semaphore_signal(barrier, inc=1, device_id=dev, device_id_type=MESH)

    for dz in (1, 2):
        greet(zh=mod(zh + dz, NZH))
    for dx in range(1, NX):
        greet(x=mod(x + dx, NX))
    for dy in range(1, NY):
        greet(y=mod(y + dy, NY))
    for rel in range(1, NZL * NC):
        greet(zl=mod(zl + rel // NC, NZL), core=lax.rem(k + rel % NC, NC))
    heads = pl.ds(pl.multiple_of(y * HD, HD), HD)
    loads = [
        pltpu.make_async_copy(src, dst, in_sem.at[i])
        for i, (src, dst) in enumerate(
            [
                (g_hbm, g),
                (q_hbm, q),
                (k_hbm.at[:, heads], kk),
                (v_hbm.at[:, heads], vv),
                (w_hbm, w),
                (fc_hbm, fc),
                (sc_hbm, sc),
                (frow_hbm, frow),
                (fcol_hbm, fcol),
                (srow_hbm, srow),
                (scol_hbm, scol),
            ]
        )
    ]
    for load in loads:
        load.start()

    me = 2 * y + k
    side = zl & 1

    def rows_of(u):
        return pl.ds(pl.multiple_of(UNIT * u, UNIT), UNIT)

    def ahead_of(turn):
        return jnp.where(turn == 0, 2, 2 * turn - 1)

    def slot_and_index(ahead, sequence):
        turn = jnp.where(ahead == 2, 0, lax.shift_right_logical(ahead + 1, 1))
        pair = 2 * turn + sequence - 1
        far = (pair >= 3).astype(jnp.int32)
        slot = jnp.where(ahead == 0, 3, jnp.where(sequence == 0, 0, 1 + far))
        index = jnp.where(
            ahead == 0,
            sequence - 1 + 3 * (sequence == 0).astype(jnp.int32),
            jnp.where(sequence == 0, turn, pair - 3 * far),
        )
        return slot, index

    first_index = lax.div(8 * me, UNITS)
    first_place = 8 * me - UNITS * first_index
    has_last = me == HOMES - 1
    units = []
    for slot in range(SLOTS):
        blocks = []
        for index in (first_index, first_index + 1):
            if slot == 0:
                xd, z = (x + ahead_of(index)) & 3, zh
            elif slot == 3:
                xd, z = x, jnp.where(index == 2, zh, other(index + 1))
            else:
                turn = 3 * (slot - 1) + index
                xd = (x + ahead_of(lax.shift_right_logical(turn, 1))) & 3
                z = other(1 + (turn & 1))
            blocks.append((z, UNITS * (NZH * xd + zh)))
        held = []
        for j in range(9):
            over = first_place + j >= UNITS
            z, start = (jnp.where(over, b, a) for a, b in zip(*blocks))
            unit = start + first_place + j - jnp.where(over, UNITS, 0)
            column = lax.shift_right_logical(unit, 3)
            line = lax.shift_right_logical(column, 1) & 3
            there = unit < ALL_UNITS
            if j == 8:
                there = there & has_last
            if slot in SPLIT:
                taken = side == min(j // 4, 1)
                there = there & taken
                here = (line & 2) == (zl & 2)
            else:
                here = (line ^ (2 * (unit & 1))) == zl
            source = dict(zh=z, y=lax.shift_right_logical(column, 3), zl=line, core=column & 1)
            held.append((there, there & here, source, (z == zh) & (column == t), unit))
        units.append(held)

    for held in units:
        for _, lands, source, same, _ in held:
            pl.when(lands & jnp.logical_not(same))(functools.partial(greet, **source))

    def count(flags):
        return sum(f.astype(jnp.int32) for f in flags)

    landing = [count(lands for _, lands, _, _, _ in held) for held in units]
    coming = [count(there for there, _, _, _, _ in held) - n for held, n in zip(units, landing)]
    staying = [count(lands & same for _, lands, _, same, _ in held) for held in units]
    greeted = 8 - sum(staying) + 2 + 3 + 7 + 7

    first_owner = lax.div(8 * t, UNITS)
    first_row = 8 * t - UNITS * first_owner
    turnover = UNITS - first_row
    sides = []
    for owner in (first_owner, first_owner + 1):
        xd = lax.div(owner, NZH)
        zd = owner - NZH * xd
        slot, index = slot_and_index(mod(xd - x, NX), sequence_of(zh, zd))
        sides.append((zd, slot, UNITS * index))

    def goes_to(u):
        over = u >= turnover
        zd, slot, start = (jnp.where(over, b, a) for a, b in zip(*sides))
        e = start + first_row + u - jnp.where(over, UNITS, 0)
        h = jnp.minimum(lax.shift_right_logical(e, 3), HOMES - 1)
        line = zl ^ (2 * (u & 1))
        for split in SPLIT:
            shared = (zl & 2) + (e - 8 * h >= 4).astype(jnp.int32)
            line = jnp.where(slot == split, shared, line)
        home = dict(zh=zd, y=lax.shift_right_logical(h, 1), zl=line, core=h & 1)
        here = (zd == zh) & (h == me) & (home["zl"] == zl)
        return slot, SLOT * slot + e, home, here

    loads[0].wait()
    gt[...] = g[...].T

    pl.semaphore_wait(barrier, greeted)

    def spread(u, carry):
        slot, place, home, here = goes_to(u)

        @pl.when(here)
        def _():
            gz[place] = gt[rows_of(u), :]

        @pl.when(jnp.logical_not(here))
        def _():
            rcopy(gt.at[rows_of(u), :], gz.at[place], spread_send, far_recv.at[slot], **home).start()

        return carry

    lax.fori_loop(0, 8, spread, 0)

    loads[4].wait()
    wt[3] = w[...].astype(BF16).T
    for dx in (1, 3, 2):
        rcopy(wt.at[3], wt.at[AHEAD.index(NX - dx)], w_send, w_recv, x=mod(x + dx, NX)).start()

    for i in (1, 2, 3):
        loads[i].wait()
    for i in range(3):
        rows, cols = pl.ds(128 * i, 128), pl.ds(0, 128 * (i + 1))
        scores = (
            lax.dot_general(q[rows, :], kk[cols, :], NT, preferred_element_type=F32) * SCALE
        )
        future = lax.broadcasted_iota(jnp.int32, scores.shape, 1) > (
            lax.broadcasted_iota(jnp.int32, scores.shape, 0) + 128 * i
        )
        scores = jnp.where(future, -1e30, scores)
        exponent = jnp.exp(scores - jnp.max(scores, axis=-1, keepdims=True))
        probabilities = exponent / jnp.sum(exponent, axis=-1, keepdims=True)
        prob[rows, cols] = probabilities
        att[0, rows, :] = jnp.dot(
            probabilities.astype(BF16), vv[cols, :], preferred_element_type=F32
        ).astype(BF16)

    for slot, held in enumerate(units):
        for j, (_, _, _, _, unit) in enumerate(held):
            missing = unit >= ALL_UNITS
            if j == 8:
                missing = missing & has_last
            if slot in SPLIT:
                missing = missing & (side == min(j // 4, 1))

            @pl.when(missing)
            def _():
                gz[SLOT * slot + 8 * me + j] = jnp.zeros((UNIT, SEQ), BF16)

    def send_att():
        for sequence in (1, 2):
            o = other(sequence)
            there = sequence_of(zh, o)
            rcopy(att.at[0], att.at[there], att_send, att_recv.at[there - 1], zh=o).start()

    def wait_units(n, most, wait):
        for c in range(1, most + 1):
            pl.when(n == c)(functools.partial(wait, c))

    def units_came(recv, c):
        came(gz.at[0:c], recv)

    def relay(slot):
        wait_units(
            landing[slot] - staying[slot], 9, functools.partial(units_came, far_recv.at[slot])
        )

        for j, (_, lands, _, _, _) in enumerate(units[slot]):
            piece = gz.at[SLOT * slot + 8 * me + j]

            @pl.when(lands)
            def _():
                for dl in (2,) if slot in SPLIT else (1, 3, 2):
                    rcopy(
                        piece, piece, relay_send.at[slot], near_recv.at[slot], zl=mod(zl + dl, NZL)
                    ).start()

    def parts(slot):
        return (0, 1) if slot == SLOTS - 1 else (0,)

    def reach(way, slot):
        return 4 if way == slot % 2 else 3

    def from_source(way, hops):
        return mod(y - hops, NY) if way == 0 else mod(y + hops, NY)

    def parts_of(slot, source, core):
        start = SLOT * slot + 8 * (2 * source + core)
        last = (source == NY - 1) & (core == 1)
        if slot in SPLIT:
            longer = last & (side == 1)
            start = start + 4 * side
            return (((start, 4, jnp.logical_not(longer)), (start, 5, longer)),)
        if len(parts(slot)) == 1:
            return (((start, 8, jnp.logical_not(last)), (start, 9, last)),)
        return (
            ((start, 4, None),),
            ((start + 4, 4, jnp.logical_not(last)), (start + 4, 5, last)),
        )

    def each_size(sizes, act):
        for start, units, when in sizes:
            ref = gz.at[pl.ds(start, units)]
            if when is None:
                act(ref)
            else:
                pl.when(when)(functools.partial(act, ref))

    def forward(way, slot, hops, part):
        def go(piece):
            rcopy(
                piece,
                piece,
                ring_send,
                ring_recv.at[way, slot + part, hops],
                y=mod(y + 1, NY) if way == 0 else mod(y - 1, NY),
            ).start()

        each_size(parts_of(slot, from_source(way, hops), k)[part], go)

    def to_partner(way, slot, hops, part):
        def go(piece):
            rcopy(piece, piece, core_send, core_recv.at[slot, hops // 4], core=1 - k).start()

        each_size(parts_of(slot, from_source(way, hops), k)[part], go)

    def to_beside(way, slot, hops):
        def go(piece):
            rcopy(piece, piece, beside_send, beside_recv.at[SPLIT.index(slot)], zl=zl ^ 1).start()

        if slot in SPLIT:
            each_size(parts_of(slot, from_source(way, hops), k)[0], go)

    def start_ring(slot):
        wait_units(coming[slot], 9, functools.partial(units_came, near_recv.at[slot]))
        for part in parts(slot):
            for way in (0, 1):
                forward(way, slot, 0, part)
        to_beside(0, slot, 0)
        for part in parts(slot):
            to_partner(0, slot, 0, part)

    def pass_on(slot, hops):
        for part in parts(slot):
            for way in (0, 1):
                if hops <= reach(way, slot):
                    each_size(
                        parts_of(slot, from_source(way, hops), k)[part],
                        lambda piece: came(piece, ring_recv.at[way, slot + part, hops - 1]),
                    )
                    if hops < reach(way, slot):
                        forward(way, slot, hops, part)
                    to_beside(way, slot, hops)
                    to_partner(way, slot, hops, part)

    def beside_came(slot):
        longer = (k == 1) & (side == 0)
        pl.when(longer)(functools.partial(came, gz.at[0:33], beside_recv.at[SPLIT.index(slot)]))
        pl.when(jnp.logical_not(longer))(functools.partial(came, gz.at[0:32], beside_recv.at[SPLIT.index(slot)]))
        for source in range(NY):
            start = SLOT * slot + 8 * (2 * source + k) + 4 * (1 - side)

            def go(units):
                piece = gz.at[pl.ds(start, units)]
                rcopy(piece, piece, core_send, shared_recv.at[SPLIT.index(slot)], core=1 - k).start()

            if source < NY - 1:
                go(4)
            else:
                pl.when(longer)(functools.partial(go, 5))
                pl.when(jnp.logical_not(longer))(functools.partial(go, 4))

    def partner_beside(slot):
        longer = (k == 0) & (side == 0)
        pl.when(longer)(functools.partial(came, gz.at[0:33], shared_recv.at[SPLIT.index(slot)]))
        pl.when(jnp.logical_not(longer))(functools.partial(came, gz.at[0:32], shared_recv.at[SPLIT.index(slot)]))

    def partner_near(slot):
        more = (k == 0) & (y != NY // 2 - 1)
        each = 8
        if slot in SPLIT:
            more, each = more & (side == 1), 4
        pl.when(more)(functools.partial(came, gz.at[0 : 7 * each + 1], core_recv.at[slot, 0]))
        pl.when(jnp.logical_not(more))(functools.partial(came, gz.at[0 : 7 * each], core_recv.at[slot, 0]))

    def partner_across(slot):
        more = (k == 0) & (y == NY // 2 - 1)
        each = 8
        if slot in SPLIT:
            more, each = more & (side == 1), 4
        pl.when(more)(functools.partial(came, gz.at[0 : each + 1], core_recv.at[slot, 1]))
        pl.when(jnp.logical_not(more))(functools.partial(came, gz.at[0:each], core_recv.at[slot, 1]))

    def partner_has(slot):
        partner_near(slot)
        partner_across(slot)

    def member(slot, index):
        if slot == 0:
            return index, 0
        turn = 3 * (slot - 1) + index
        return turn // 2, 1 + turn % 2

    started = {("g", 0)}

    def add_to(ref, key, term):
        ref[...] = ref[...] + term if key in started else term
        started.add(key)

    def side_by_side(slot, indices):
        blocks = [gz[pl.ds(SLOT * slot + UNITS * i, UNITS)].reshape(ROWS, SEQ) for i in indices]
        return jnp.concatenate(blocks, axis=1) if len(blocks) > 1 else blocks[0]

    def one_below_another(sequences):
        parts = [att[s] for s in sequences]
        return jnp.concatenate(parts, axis=0) if len(parts) > 1 else parts[0]

    def weight_term(slot, *indices):
        members = [member(slot, i) for i in indices]
        rows = members[0][0]
        term = jnp.dot(
            side_by_side(slot, indices),
            one_below_another([sequence for _, sequence in members]),
            preferred_element_type=F32,
        )
        add_to(dwacc.at[rows], ("w", rows), term)

    def multiply(slot, *indices):
        members = [member(slot, i) for i in indices]
        term = jnp.dot(wt[members[0][0]], side_by_side(slot, indices), preferred_element_type=F32)
        for i, (_, sequence) in enumerate(members):
            add_to(acct.at[sequence], ("g", sequence), term[:, SEQ * i : SEQ * (i + 1)])

    early = jnp.where(lax.rem(y + NY // 2, NY) <= 2, 2, 0)
    last_blocks = (early, jnp.where(early == 2, 0, 1), jnp.where(early == 2, 1, 2))

    def last_term(*turns):
        indices = [last_blocks[turn] for turn in turns]
        term = jnp.dot(
            side_by_side(SLOTS - 1, indices),
            one_below_another([lax.rem(i + 1, NZH) for i in indices]),
            preferred_element_type=F32,
        )
        add_to(dwacc.at[3], ("w", 3), term)

    def last_multiply(*turns):
        indices = [last_blocks[turn] for turn in turns]
        term = jnp.dot(wt[3], side_by_side(SLOTS - 1, indices), preferred_element_type=F32)
        for i, index in enumerate(indices):
            sequence = lax.rem(index + 1, NZH)
            acct[sequence] = acct[sequence] + term[:, SEQ * i : SEQ * (i + 1)]

    def send_term(rows):
        dw_stage[rows] = dwacc[rows].astype(BF16)
        rcopy(
            dw_stage.at[rows], dw_in.at[rows], dw_send, dw_recv, x=mod(x + AHEAD[rows], NX)
        ).start()

    def send_grads():
        for i in range(3):
            for sequence in (1, 2):
                o = other(sequence)
                ga_stage[sequence - 1, i] = acct[sequence, :, 128 * i : 128 * (i + 1)].astype(BF16)
                rcopy(
                    ga_stage.at[sequence - 1, i],
                    ga_in.at[sequence_of(zh, o) - 1, i],
                    ga_send,
                    ga_recv.at[i],
                    zh=o,
                ).start()

    def old_moments():
        acct[0] = jnp.zeros((HD, SEQ), F32)
        for load in loads[5:]:
            load.wait()
        for c, start, size in row_chunks():
            rows = pl.ds(start, size)
            low_first = jnp.minimum(down(frow, start, size), fcol[...].reshape(1, HD))
            low_second = jnp.minimum(down(srow, start, size), scol[...].reshape(1, HD))
            fnew_out[rows, :] = beta_first * (fc[rows, :].astype(F32) * low_first)
            snew_out[rows, :] = beta_second * (sc[rows, :].astype(F32) * low_second)
            weight = w[rows, :]
            nw_out[rows, :] = weight - learning * (decay_rate * weight)

    relay(0)
    start_ring(0)
    relay(1)
    relay(2)
    relay(3)
    pass_on(0, 1)
    start_ring(1)
    pass_on(0, 2)
    pass_on(1, 1)
    start_ring(2)
    send_att()
    pass_on(0, 3)
    pass_on(1, 2)
    pass_on(2, 1)
    start_ring(3)
    pass_on(0, 4)
    pass_on(1, 3)
    pass_on(2, 2)
    old_moments()
    pass_on(3, 1)
    pass_on(1, 4)
    beside_came(0)
    pass_on(2, 3)
    pass_on(3, 2)
    partner_has(1)
    came(att.at[1], att_recv.at[0])
    came(att.at[2], att_recv.at[1])
    weight_term(1, 0, 1)
    partner_has(0)
    partner_beside(0)
    weight_term(0, 0)
    send_term(0)
    pass_on(2, 4)
    weight_term(1, 2)
    weight_term(0, 2)
    pass_on(3, 3)
    weight_term(0, 1)
    partner_has(2)
    weight_term(2, 0)
    send_term(1)
    weight_term(2, 1, 2)
    send_term(2)
    came(wt.at[0:3], w_recv)
    multiply(1, 0, 1)
    multiply(1, 2)
    partner_near(3)
    last_term(0)
    pass_on(3, 4)
    multiply(2, 0)
    multiply(2, 1, 2)
    last_multiply(0)
    partner_across(3)
    last_multiply(1, 2)
    send_grads()
    last_term(1, 2)

    came(dw_in, dw_recv)
    for c, start, size in row_chunks():
        rows = pl.ds(start, size)
        grad = dwacc[3, rows, :]
        for i in range(NX - 1):
            grad = grad + dw_in[i, rows, :].astype(F32)
        first_new = fnew_out[rows, :] + (1.0 - beta_first) * grad
        second_new = snew_out[rows, :] + (1.0 - beta_second) * grad * grad
        step_size = (
            first_new * (1.0 / correct_first) / (jnp.sqrt(second_new * (1.0 / correct_second)) + adam_eps)
        )
        nw_out[rows, :] = nw_out[rows, :] - learning * step_size
        fnew_out[rows, :] = first_new
        snew_out[rows, :] = second_new

    first_abs, second_abs = jnp.abs(fnew_out[...]), jnp.abs(snew_out[...])
    st[0] = lane_rows(first_abs)
    st[1] = lane_rows(second_abs)
    for dy in range(1, NY):
        rcopy(st, y_in.at[NY - dy - 1], y_send, y_recv, y=mod(y + dy, NY)).start()
    cst[0, 0:1, :] = jnp.max(first_abs, axis=0, keepdims=True)
    cst[0, 1:2, :] = jnp.max(second_abs, axis=0, keepdims=True)
    for dx in range(1, NX):
        rcopy(cst.at[0], x_in.at[NX - dx - 1], x_send, x_recv, x=mod(x + dx, NX)).start()

    multiply(0, 0)
    multiply(0, 1)
    multiply(0, 2)

    def back_rows(i):
        rows, cols = pl.ds(128 * i, 128), pl.ds(0, 128 * (i + 1))
        came(ga_in.at[:, i], ga_recv.at[i])
        total = acct[0, :, rows]
        for s in range(2):
            total = total + ga_in[s, i].astype(F32)
        grad_half = total.astype(BF16).T
        grad_probs = lax.dot_general(grad_half, vv[cols, :], NT, preferred_element_type=F32)
        row_dot = jnp.sum(
            grad_half.astype(F32) * att[0, rows, :].astype(F32), axis=-1, keepdims=True
        )
        grad_scores = (prob[rows, cols] * (grad_probs - row_dot)).astype(BF16)
        gq_out[rows, :] = (
            jnp.dot(grad_scores, kk[cols, :], preferred_element_type=F32) * SCALE
        ).astype(BF16)

    def left(ref, send):
        rcopy(ref, ref, send, zh_recv, core=k).wait_send()

    wait_units(8 - sum(staying), 8, lambda c: left(gz.at[0:c], spread_send))
    for slot in range(SLOTS):
        copies = 1 if slot in SPLIT else 3
        wait_units(landing[slot], 9, lambda c: left(gz.at[0 : copies * c], relay_send.at[slot]))
    longer = count(
        (from_source(way, hops) == NY - 1) & (k == 1) & ((side == 1) | (slot not in SPLIT))
        for slot in range(SLOTS)
        for way in (0, 1)
        for hops in range(reach(way, slot))
    )
    usual = 56 * SLOTS - 28 * len(SPLIT)
    for c in range(9):
        pl.when(longer == c)(functools.partial(left, gz.at[0 : usual + c], ring_send))
    more = (k == 1) & (side == 1)
    for flag, each in ((more, 33), (jnp.logical_not(more), 32)):
        pl.when(flag)(functools.partial(left, gz.at[0 : each * len(SPLIT)], beside_send))
    for c in (0, 1):
        pl.when(k == c)(functools.partial(left, gz.at[0 : 64 * SLOTS + SLOTS * c], core_send))
    for whole, send in (
        (att.at[0:2], att_send),
        (wt.at[0:3], w_send),
        (dw_in, dw_send),
    ):
        left(whole, send)

    came(x_in, x_recv)
    cst[1] = jnp.maximum(cst[0], jnp.max(x_in[...], axis=0))
    for sequence in (1, 2):
        o = other(sequence)
        rcopy(cst.at[1], zh_in.at[sequence_of(zh, o) - 1], zh_send, zh_recv, zh=o).start()
    came(y_in, y_recv)
    mine[...] = jnp.maximum(st[...], jnp.max(y_in[...], axis=0))
    for rel in range(1, NZL * NC):
        dl, dk = rel // NC, rel % NC
        back = NC * ((NZL - dl) % NZL) + dk - 1
        rcopy(
            mine, zl_in.at[back], zl_send, zl_recv, zl=mod(zl + dl, NZL), core=lax.rem(k + dk, NC)
        ).start()
    for i in range(3):
        back_rows(i)
    came(zl_in, zl_recv)
    rows_out[...] = jnp.maximum(mine[...], jnp.max(zl_in[...], axis=0))
    came(zh_in, zh_recv)
    cols_out[...] = jnp.maximum(cst[1], jnp.max(zh_in[...], axis=0))

    for whole, send in (
        (ga_in, ga_send),
        (y_in, y_send),
        (zl_in, zl_send),
        (x_in, x_send),
        (zh_in, zh_send),
    ):
        left(whole, send)


def codes(
    gq,
    nw,
    fnew,
    snew,
    rows,
    cols,
    gq_out,
    nw_out,
    nfc_out,
    nfr_out,
    nfcol_out,
    nsc_out,
    nsr_out,
    nscol_out,
    first_code,
    second_code,
    first_rows,
    second_rows,
    first_cols,
    second_cols,
    sem,
):
    copies = []

    def out(src, dst):
        copy = pltpu.make_async_copy(src, dst, sem.at[len(copies)])
        copy.start()
        copies.append(copy)

    out(gq, gq_out)
    out(nw, nw_out)
    for moment, (new, code, code_out, maxima, maxima_out, col, col_out) in enumerate(
        (
            (fnew, first_code, nfc_out, first_rows, nfr_out, first_cols, nfcol_out),
            (snew, second_code, nsc_out, second_rows, nsr_out, second_cols, nscol_out),
        )
    ):
        col[...] = cols[moment]
        for c, start, size in row_chunks():
            at = pl.ds(start, size)
            maxima[at] = rows[moment, c, 0:size]
            low = jnp.minimum(
                down_rows(rows[moment, c : c + 1, :])[:size], cols[moment : moment + 1]
            )
            code[at, :] = (new[at, :] / (low + code_eps)).astype(BF16)
        out(code, code_out)
        out(maxima, maxima_out)
        out(col, col_out)
    for copy in copies:
        copy.wait()


def per_device(queries, keys, values, grad_out, weight, fc, frow, fcol, sc, srow, scol):
    shape = jax.ShapeDtypeStruct
    vmem = pl.BlockSpec(memory_space=pltpu.VMEM)
    hbm = pl.BlockSpec(memory_space=pltpu.HBM)
    dma = pltpu.SemaphoreType.DMA
    gq, nw, fnew, snew, rows, cols = pl.pallas_call(
        body,
        name="whole",
        out_shape=(
            shape((SEQ, HD), BF16),
            shape((ROWS, HD), F32),
            shape((ROWS, HD), F32),
            shape((ROWS, HD), F32),
            shape((2, 8, HD), F32),
            shape((2, HD), F32),
        ),
        in_specs=[hbm] * 11,
        out_specs=[vmem] * 6,
        scratch_shapes=[
            pltpu.VMEM((SEQ, HD), BF16),
            pltpu.VMEM((SEQ, HD), BF16),
            pltpu.VMEM((SEQ, HD), BF16),
            pltpu.VMEM((SEQ, HD), BF16),
            pltpu.VMEM((ROWS, HD), F32),
            pltpu.VMEM((ROWS, HD), BF16),
            pltpu.VMEM((ROWS, HD), BF16),
            pltpu.VMEM((ROWS,), F32),
            pltpu.VMEM((HD,), F32),
            pltpu.VMEM((ROWS,), F32),
            pltpu.VMEM((HD,), F32),
            pltpu.VMEM((HD, SEQ), BF16),
            pltpu.VMEM((SLOTS * SLOT, UNIT, SEQ), BF16),
            pltpu.VMEM((NX, HD, ROWS), BF16),
            pltpu.VMEM((NZH, SEQ, HD), BF16),
            pltpu.VMEM((SEQ, SEQ), F32),
            pltpu.VMEM((NZH, HD, SEQ), F32),
            pltpu.VMEM((2, 3, HD, HD), BF16),
            pltpu.VMEM((2, 3, HD, HD), BF16),
            pltpu.VMEM((NX, ROWS, HD), F32),
            pltpu.VMEM((NX - 1, ROWS, HD), BF16),
            pltpu.VMEM((NX - 1, ROWS, HD), BF16),
            pltpu.VMEM((2, 8, HD), F32),
            pltpu.VMEM((NY - 1, 2, 8, HD), F32),
            pltpu.VMEM((NZL * NC - 1, 2, 8, HD), F32),
            pltpu.VMEM((2, 8, HD), F32),
            pltpu.VMEM((2, 2, HD), F32),
            pltpu.VMEM((NX - 1, 2, HD), F32),
            pltpu.VMEM((NZH - 1, 2, HD), F32),
            dma((11,)),
            dma,
            dma((SLOTS,)),
            dma((SLOTS,)),
            dma((SLOTS,)),
            dma,
            dma((2, SLOTS + 1, 4)),
            dma,
            dma((len(SPLIT),)),
            dma((len(SPLIT),)),
            dma,
            dma((SLOTS, 2)),
            dma,
            dma((2,)),
            dma,
            dma,
            dma,
            dma((3,)),
            dma,
            dma,
            dma,
            dma,
            dma,
            dma,
            dma,
            dma,
            dma,
            dma,
        ],
        compiler_params=pltpu.CompilerParams(
            collective_id=0, has_side_effects=True, vmem_limit_bytes=48 * 1024 * 1024
        ),
    )(
        *(
            pltpu.with_memory_space_constraint(a, pltpu.HBM)
            for a in (queries, keys, values, grad_out, weight, fc, frow, fcol, sc, srow, scol)
        )
    )
    return pl.pallas_call(
        codes,
        name="codes",
        out_shape=(
            shape((SEQ, HD), BF16),
            shape((ROWS, HD), F32),
            shape((ROWS, HD), BF16),
            shape((ROWS,), F32),
            shape((HD,), F32),
            shape((ROWS, HD), BF16),
            shape((ROWS,), F32),
            shape((HD,), F32),
        ),
        compiler_params=pltpu.CompilerParams(vmem_limit_bytes=8 * 1024 * 1024),
        in_specs=[vmem] * 6,
        out_specs=[hbm] * 8,
        scratch_shapes=[
            pltpu.VMEM((ROWS, HD), BF16),
            pltpu.VMEM((ROWS, HD), BF16),
            pltpu.VMEM((ROWS,), F32),
            pltpu.VMEM((ROWS,), F32),
            pltpu.VMEM((HD,), F32),
            pltpu.VMEM((HD,), F32),
            dma((8,)),
        ],
    )(gq, nw, fnew, snew, rows, cols)


def solution(mesh):
    finer = Mesh(mesh.devices.reshape(NX, NZH, NY, NZL, NC), AXES)
    placed = (
        P(DP, TENSOR),
        P(DP, None),
        P(DP, None),
        P(DP, TENSOR),
        P(DP, TENSOR),
        P(DP, TENSOR),
        P(DP),
        P(TENSOR),
        P(DP, TENSOR),
        P(DP),
        P(TENSOR),
    )
    return jax.shard_map(
        per_device,
        mesh=finer,
        in_specs=placed,
        out_specs=(
            P(DP, TENSOR),
            P(DP, TENSOR),
            P(DP, TENSOR),
            P(DP),
            P(TENSOR),
            P(DP, TENSOR),
            P(DP),
            P(TENSOR),
        ),
        check_vma=False,
    )
```

```python
import functools

import jax
import jax.numpy as jnp
from jax import lax
from jax.experimental import pallas as pl
from jax.experimental.pallas import tpu as pltpu
from jax.sharding import Mesh
from jax.sharding import PartitionSpec as P

NX, NZH, NY, NZL, NC = 4, 3, 8, 4, 2
AXES = ("x", "zh", "y", "zl", "core")
DP = ("x", "zh")
TENSOR = ("y", "zl", "core")
MESH = pl.DeviceIdType.MESH

HD = 128
SEQ = 384
ROWS = 688
UNIT = 16
UNITS = ROWS // UNIT
ALL_UNITS = 512
HOMES = NY * NC
SLOTS = 4
SLOT = 3 * UNITS
SPLIT = (0,)
AHEAD = (2, 1, 3)
SCALE = HD ** (-0.5)

beta_first = 0.9
beta_second = 0.95
learning = 0.01
decay_rate = 0.1
adam_eps = 1e-08
code_eps = 1e-06
correct_first = 1.0 - 0.9**10
correct_second = 1.0 - 0.95**10

F32 = jnp.float32
BF16 = jnp.bfloat16
NT = (((1,), (1,)), ((), ()))


def mod(a, n):
    return lax.rem(a + n, n)


def row_chunks():
    return [(c, 128 * c, min(128, ROWS - 128 * c)) for c in range(6)]


def lane_rows(values):
    highest = jnp.max(values, axis=1, keepdims=True)
    out = []
    for c, start, size in row_chunks():
        eye = lax.broadcasted_iota(jnp.int32, (size, 128), 0) == lax.broadcasted_iota(
            jnp.int32, (size, 128), 1
        )
        out.append(
            jnp.max(jnp.where(eye, highest[start : start + size], 0.0), axis=0, keepdims=True)
        )
    out.append(jnp.zeros((2, 128), F32))
    return jnp.concatenate(out, axis=0)


def down(vector, start, size):
    row = vector[pl.ds(start, size)].reshape(1, size)
    if size < 128:
        row = jnp.concatenate([row, jnp.zeros((1, 128 - size), F32)], axis=1)
    return down_rows(row)[:size]


def down_rows(row):
    return jnp.broadcast_to(row, (128, 128)).T


def body(
    q_hbm,
    k_hbm,
    v_hbm,
    g_hbm,
    w_hbm,
    fc_hbm,
    frow_hbm,
    fcol_hbm,
    sc_hbm,
    srow_hbm,
    scol_hbm,
    gq_out,
    nw_out,
    fnew_out,
    snew_out,
    rows_out,
    cols_out,
    q,
    kk,
    vv,
    g,
    w,
    fc,
    sc,
    frow,
    fcol,
    srow,
    scol,
    gt,
    gz,
    wt,
    att,
    prob,
    acct,
    ga_stage,
    ga_in,
    dwacc,
    dw_stage,
    dw_in,
    st,
    y_in,
    zl_in,
    mine,
    cst,
    x_in,
    zh_in,
    in_sem,
    spread_send,
    relay_send,
    far_recv,
    near_recv,
    ring_send,
    ring_recv,
    beside_send,
    beside_recv,
    shared_recv,
    core_send,
    core_recv,
    att_send,
    att_recv,
    w_send,
    w_recv,
    ga_send,
    ga_recv,
    dw_send,
    dw_recv,
    y_send,
    y_recv,
    zl_send,
    zl_recv,
    x_send,
    x_recv,
    zh_send,
    zh_recv,
):
    x, zh, y, zl, k = (lax.axis_index(a) for a in AXES)
    t = 8 * y + 2 * zl + k
    pair = lax.div(y, 2)

    def rcopy(src, dst, send, recv, **dev):
        return pltpu.make_async_remote_copy(
            src_ref=src, dst_ref=dst, send_sem=send, recv_sem=recv, device_id=dev, device_id_type=MESH
        )

    def came(ref, recv):
        rcopy(ref, ref, core_send, recv, core=k).wait_recv()

    def sequence_of(source, plane):
        return jnp.where(source == plane, 0, source + (source < plane).astype(jnp.int32))

    def other(sequence):
        return sequence - 1 + (sequence - 1 >= zh).astype(jnp.int32)

    barrier = pltpu.get_barrier_semaphore()

    def greet(**dev):
        pl.semaphore_signal(barrier, inc=1, device_id=dev, device_id_type=MESH)

    for dz in (1, 2):
        greet(zh=mod(zh + dz, NZH))
    for dx in range(1, NX):
        greet(x=mod(x + dx, NX))
    for dy in range(1, NY):
        greet(y=mod(y + dy, NY))
    for rel in range(1, NZL * NC):
        greet(zl=mod(zl + rel // NC, NZL), core=lax.rem(k + rel % NC, NC))
    heads = pl.ds(pl.multiple_of(y * HD, HD), HD)
    loads = [
        pltpu.make_async_copy(src, dst, in_sem.at[i])
        for i, (src, dst) in enumerate(
            [
                (g_hbm, g),
                (q_hbm, q),
                (k_hbm.at[:, heads], kk),
                (v_hbm.at[:, heads], vv),
                (w_hbm, w),
                (fc_hbm, fc),
                (sc_hbm, sc),
                (frow_hbm, frow),
                (fcol_hbm, fcol),
                (srow_hbm, srow),
                (scol_hbm, scol),
            ]
        )
    ]
    for load in loads:
        load.start()

    turned = (
        (2 * x + NY - 1 + (zh == 2).astype(jnp.int32)) & (NY - 1),
        jnp.int32(0),
        (2 * x + 1 + (zh > 0).astype(jnp.int32)) & (NY - 1),
        jnp.int32(0),
    )

    def seat(slot, column):
        return (column + NY - turned[slot]) & (NY - 1)

    homes = [2 * seat(slot, y) + k for slot in range(SLOTS)]
    side = zl & 1

    def rows_of(u):
        return pl.ds(pl.multiple_of(UNIT * u, UNIT), UNIT)

    def ahead_of(turn):
        return jnp.where(turn == 0, 2, 2 * turn - 1)

    def slot_and_index(ahead, sequence):
        turn = jnp.where(ahead == 2, 0, lax.shift_right_logical(ahead + 1, 1))
        pair = 2 * turn + sequence - 1
        far = (pair >= 3).astype(jnp.int32)
        slot = jnp.where(ahead == 0, 3, jnp.where(sequence == 0, 0, 1 + far))
        index = jnp.where(
            ahead == 0,
            sequence - 1 + 3 * (sequence == 0).astype(jnp.int32),
            jnp.where(sequence == 0, turn, pair - 3 * far),
        )
        return slot, index

    units = []
    for slot in range(SLOTS):
        first_index = lax.div(8 * homes[slot], UNITS)
        first_place = 8 * homes[slot] - UNITS * first_index
        has_last = homes[slot] == HOMES - 1
        blocks = []
        for index in (first_index, first_index + 1):
            if slot == 0:
                xd, z = (x + ahead_of(index)) & 3, zh
            elif slot == 3:
                xd, z = x, jnp.where(index == 2, zh, other(index + 1))
            else:
                turn = 3 * (slot - 1) + index
                xd = (x + ahead_of(lax.shift_right_logical(turn, 1))) & 3
                z = other(1 + (turn & 1))
            blocks.append((z, UNITS * (NZH * xd + zh)))
        held = []
        for j in range(9):
            over = first_place + j >= UNITS
            z, start = (jnp.where(over, b, a) for a, b in zip(*blocks))
            unit = start + first_place + j - jnp.where(over, UNITS, 0)
            column = lax.shift_right_logical(unit, 3)
            line = lax.shift_right_logical(column, 1) & 3
            there = unit < ALL_UNITS
            if j == 8:
                there = there & has_last
            if slot in SPLIT:
                taken = side == min(j // 4, 1)
                there = there & taken
                here = (line & 2) == (zl & 2)
            else:
                here = (line ^ (2 * (unit & 1))) == zl
            source = dict(zh=z, y=lax.shift_right_logical(column, 3), zl=line, core=column & 1)
            held.append((there, there & here, source, (z == zh) & (column == t), unit))
        units.append(held)

    for held in units:
        for _, lands, source, same, _ in held:
            pl.when(lands & jnp.logical_not(same))(functools.partial(greet, **source))

    def count(flags):
        return sum(f.astype(jnp.int32) for f in flags)

    landing = [count(lands for _, lands, _, _, _ in held) for held in units]
    coming = [count(there for there, _, _, _, _ in held) - n for held, n in zip(units, landing)]
    staying = [count(lands & same for _, lands, _, same, _ in held) for held in units]
    greeted = 8 - sum(staying) + 2 + 3 + 7 + 7

    first_owner = lax.div(8 * t, UNITS)
    first_row = 8 * t - UNITS * first_owner
    turnover = UNITS - first_row
    sides = []

    def turn_of(slot, zd):
        first = 2 * x + NY - 1 + (zd == 2).astype(jnp.int32)
        third = 2 * x + 1 + (zd > 0).astype(jnp.int32)
        return jnp.where(slot == 0, first, jnp.where(slot == 2, third, 0))

    for owner in (first_owner, first_owner + 1):
        xd = lax.div(owner, NZH)
        zd = owner - NZH * xd
        slot, index = slot_and_index(mod(xd - x, NX), sequence_of(zh, zd))
        sides.append((zd, slot, UNITS * index, turn_of(slot, zd)))

    def goes_to(u):
        over = u >= turnover
        zd, slot, start, turn = (jnp.where(over, b, a) for a, b in zip(*sides))
        e = start + first_row + u - jnp.where(over, UNITS, 0)
        h = jnp.minimum(lax.shift_right_logical(e, 3), HOMES - 1)
        line = zl ^ (2 * (u & 1))
        for split in SPLIT:
            shared = (zl & 2) + (e - 8 * h >= 4).astype(jnp.int32)
            line = jnp.where(slot == split, shared, line)
        home = dict(zh=zd, y=(lax.shift_right_logical(h, 1) + turn) & (NY - 1), zl=line, core=h & 1)
        here = (zd == zh) & (home["y"] == y) & (home["core"] == k) & (home["zl"] == zl)
        return slot, SLOT * slot + e, home, here

    loads[0].wait()
    gt[...] = g[...].T

    pl.semaphore_wait(barrier, greeted)

    def spread(u, carry):
        slot, place, home, here = goes_to(u)

        @pl.when(here)
        def _():
            gz[place] = gt[rows_of(u), :]

        @pl.when(jnp.logical_not(here))
        def _():
            rcopy(gt.at[rows_of(u), :], gz.at[place], spread_send, far_recv.at[slot], **home).start()

        return carry

    lax.fori_loop(0, 8, spread, 0)

    loads[4].wait()
    wt[3] = w[...].astype(BF16).T
    for dx in (1, 3, 2):
        rcopy(wt.at[3], wt.at[AHEAD.index(NX - dx)], w_send, w_recv, x=mod(x + dx, NX)).start()

    for i in (1, 2, 3):
        loads[i].wait()
    for i in range(3):
        rows, cols = pl.ds(128 * i, 128), pl.ds(0, 128 * (i + 1))
        scores = (
            lax.dot_general(q[rows, :], kk[cols, :], NT, preferred_element_type=F32) * SCALE
        )
        future = lax.broadcasted_iota(jnp.int32, scores.shape, 1) > (
            lax.broadcasted_iota(jnp.int32, scores.shape, 0) + 128 * i
        )
        scores = jnp.where(future, -1e30, scores)
        exponent = jnp.exp(scores - jnp.max(scores, axis=-1, keepdims=True))
        probabilities = exponent / jnp.sum(exponent, axis=-1, keepdims=True)
        prob[rows, cols] = probabilities
        att[0, rows, :] = jnp.dot(
            probabilities.astype(BF16), vv[cols, :], preferred_element_type=F32
        ).astype(BF16)

    for slot, held in enumerate(units):
        for j, (_, _, _, _, unit) in enumerate(held):
            missing = unit >= ALL_UNITS
            if j == 8:
                missing = missing & (homes[slot] == HOMES - 1)
            if slot in SPLIT:
                missing = missing & (side == min(j // 4, 1))

            @pl.when(missing)
            def _():
                gz[SLOT * slot + 8 * homes[slot] + j] = jnp.zeros((UNIT, SEQ), BF16)

    def send_att():
        for sequence in (1, 2):
            o = other(sequence)
            there = sequence_of(zh, o)
            rcopy(att.at[0], att.at[there], att_send, att_recv.at[there - 1], zh=o).start()

    def wait_units(n, most, wait):
        for c in range(1, most + 1):
            pl.when(n == c)(functools.partial(wait, c))

    def units_came(recv, c):
        came(gz.at[0:c], recv)

    def relay(slot):
        wait_units(
            landing[slot] - staying[slot], 9, functools.partial(units_came, far_recv.at[slot])
        )

        for j, (_, lands, _, _, _) in enumerate(units[slot]):
            piece = gz.at[SLOT * slot + 8 * homes[slot] + j]

            @pl.when(lands)
            def _():
                for dl in (2,) if slot in SPLIT else (1, 3, 2):
                    rcopy(
                        piece, piece, relay_send.at[slot], near_recv.at[slot], zl=mod(zl + dl, NZL)
                    ).start()

    def parts(slot):
        return (0, 1) if slot == SLOTS - 1 else (0,)

    def reach(way, slot):
        return 4 if way == slot % 2 else 3

    def from_source(way, hops):
        return mod(y - hops, NY) if way == 0 else mod(y + hops, NY)

    def parts_of(slot, source, core):
        start = SLOT * slot + 8 * (2 * seat(slot, source) + core)
        last = (seat(slot, source) == NY - 1) & (core == 1)
        if slot in SPLIT:
            longer = last & (side == 1)
            start = start + 4 * side
            return (((start, 4, jnp.logical_not(longer)), (start, 5, longer)),)
        if len(parts(slot)) == 1:
            return (((start, 8, jnp.logical_not(last)), (start, 9, last)),)
        return (
            ((start, 4, None),),
            ((start + 4, 4, jnp.logical_not(last)), (start + 4, 5, last)),
        )

    def each_size(sizes, act):
        for start, units, when in sizes:
            ref = gz.at[pl.ds(start, units)]
            if when is None:
                act(ref)
            else:
                pl.when(when)(functools.partial(act, ref))

    def forward(way, slot, hops, part):
        def go(piece):
            rcopy(
                piece,
                piece,
                ring_send,
                ring_recv.at[way, slot + part, hops],
                y=mod(y + 1, NY) if way == 0 else mod(y - 1, NY),
            ).start()

        each_size(parts_of(slot, from_source(way, hops), k)[part], go)

    def to_partner(way, slot, hops, part):
        def go(piece):
            rcopy(piece, piece, core_send, core_recv.at[slot, hops // 4], core=1 - k).start()

        each_size(parts_of(slot, from_source(way, hops), k)[part], go)

    def to_beside(way, slot, hops):
        def go(piece):
            rcopy(piece, piece, beside_send, beside_recv.at[SPLIT.index(slot)], zl=zl ^ 1).start()

        if slot in SPLIT:
            each_size(parts_of(slot, from_source(way, hops), k)[0], go)

    def start_ring(slot):
        wait_units(coming[slot], 9, functools.partial(units_came, near_recv.at[slot]))
        for part in parts(slot):
            for way in (0, 1):
                forward(way, slot, 0, part)
        to_beside(0, slot, 0)
        for part in parts(slot):
            to_partner(0, slot, 0, part)

    def pass_on(slot, hops):
        for part in parts(slot):
            for way in (0, 1):
                if hops <= reach(way, slot):
                    each_size(
                        parts_of(slot, from_source(way, hops), k)[part],
                        lambda piece: came(piece, ring_recv.at[way, slot + part, hops - 1]),
                    )
                    if hops < reach(way, slot):
                        forward(way, slot, hops, part)
                    to_beside(way, slot, hops)
                    to_partner(way, slot, hops, part)

    def beside_came(slot):
        longer = (k == 1) & (side == 0)
        pl.when(longer)(functools.partial(came, gz.at[0:33], beside_recv.at[SPLIT.index(slot)]))
        pl.when(jnp.logical_not(longer))(functools.partial(came, gz.at[0:32], beside_recv.at[SPLIT.index(slot)]))
        for source in range(NY):
            start = SLOT * slot + 8 * (2 * source + k) + 4 * (1 - side)

            def go(units):
                piece = gz.at[pl.ds(start, units)]
                rcopy(piece, piece, core_send, shared_recv.at[SPLIT.index(slot)], core=1 - k).start()

            if source < NY - 1:
                go(4)
            else:
                pl.when(longer)(functools.partial(go, 5))
                pl.when(jnp.logical_not(longer))(functools.partial(go, 4))

    def partner_beside(slot):
        longer = (k == 0) & (side == 0)
        pl.when(longer)(functools.partial(came, gz.at[0:33], shared_recv.at[SPLIT.index(slot)]))
        pl.when(jnp.logical_not(longer))(functools.partial(came, gz.at[0:32], shared_recv.at[SPLIT.index(slot)]))

    def partner_near(slot):
        more = (k == 0) & (seat(slot, y) != NY // 2 - 1)
        each = 8
        if slot in SPLIT:
            more, each = more & (side == 1), 4
        pl.when(more)(functools.partial(came, gz.at[0 : 7 * each + 1], core_recv.at[slot, 0]))
        pl.when(jnp.logical_not(more))(functools.partial(came, gz.at[0 : 7 * each], core_recv.at[slot, 0]))

    def partner_across(slot):
        more = (k == 0) & (seat(slot, y) == NY // 2 - 1)
        each = 8
        if slot in SPLIT:
            more, each = more & (side == 1), 4
        pl.when(more)(functools.partial(came, gz.at[0 : each + 1], core_recv.at[slot, 1]))
        pl.when(jnp.logical_not(more))(functools.partial(came, gz.at[0:each], core_recv.at[slot, 1]))

    def partner_has(slot):
        partner_near(slot)
        partner_across(slot)

    def member(slot, index):
        if slot == 0:
            return index, 0
        turn = 3 * (slot - 1) + index
        return turn // 2, 1 + turn % 2

    started = {("g", 0)}

    def add_to(ref, key, term):
        ref[...] = ref[...] + term if key in started else term
        started.add(key)

    def side_by_side(slot, indices):
        blocks = [gz[pl.ds(SLOT * slot + UNITS * i, UNITS)].reshape(ROWS, SEQ) for i in indices]
        return jnp.concatenate(blocks, axis=1) if len(blocks) > 1 else blocks[0]

    def one_below_another(sequences):
        parts = [att[s] for s in sequences]
        return jnp.concatenate(parts, axis=0) if len(parts) > 1 else parts[0]

    def weight_term(slot, *indices):
        members = [member(slot, i) for i in indices]
        rows = members[0][0]
        term = jnp.dot(
            side_by_side(slot, indices),
            one_below_another([sequence for _, sequence in members]),
            preferred_element_type=F32,
        )
        add_to(dwacc.at[rows], ("w", rows), term)

    def multiply(slot, *indices):
        members = [member(slot, i) for i in indices]
        term = jnp.dot(wt[members[0][0]], side_by_side(slot, indices), preferred_element_type=F32)
        for i, (_, sequence) in enumerate(members):
            add_to(acct.at[sequence], ("g", sequence), term[:, SEQ * i : SEQ * (i + 1)])

    early = jnp.where(lax.rem(y + NY // 2, NY) <= 2, 2, 0)
    last_blocks = (early, jnp.where(early == 2, 0, 1), jnp.where(early == 2, 1, 2))

    def last_term(*turns):
        indices = [last_blocks[turn] for turn in turns]
        term = jnp.dot(
            side_by_side(SLOTS - 1, indices),
            one_below_another([lax.rem(i + 1, NZH) for i in indices]),
            preferred_element_type=F32,
        )
        add_to(dwacc.at[3], ("w", 3), term)

    def last_multiply(*turns):
        indices = [last_blocks[turn] for turn in turns]
        term = jnp.dot(wt[3], side_by_side(SLOTS - 1, indices), preferred_element_type=F32)
        for i, index in enumerate(indices):
            sequence = lax.rem(index + 1, NZH)
            acct[sequence] = acct[sequence] + term[:, SEQ * i : SEQ * (i + 1)]

    def send_term(rows):
        dw_stage[rows] = dwacc[rows].astype(BF16)
        rcopy(
            dw_stage.at[rows], dw_in.at[rows], dw_send, dw_recv, x=mod(x + AHEAD[rows], NX)
        ).start()

    def send_grads():
        for i in range(3):
            for sequence in (1, 2):
                o = other(sequence)
                ga_stage[sequence - 1, i] = acct[sequence, :, 128 * i : 128 * (i + 1)].astype(BF16)
                rcopy(
                    ga_stage.at[sequence - 1, i],
                    ga_in.at[sequence_of(zh, o) - 1, i],
                    ga_send,
                    ga_recv.at[i],
                    zh=o,
                ).start()

    def old_moments():
        acct[0] = jnp.zeros((HD, SEQ), F32)
        for load in loads[5:]:
            load.wait()
        for c, start, size in row_chunks():
            rows = pl.ds(start, size)
            low_first = jnp.minimum(down(frow, start, size), fcol[...].reshape(1, HD))
            low_second = jnp.minimum(down(srow, start, size), scol[...].reshape(1, HD))
            fnew_out[rows, :] = beta_first * (fc[rows, :].astype(F32) * low_first)
            snew_out[rows, :] = beta_second * (sc[rows, :].astype(F32) * low_second)
            weight = w[rows, :]
            nw_out[rows, :] = weight - learning * (decay_rate * weight)

    relay(0)
    start_ring(0)
    relay(1)
    relay(2)
    relay(3)
    pass_on(0, 1)
    start_ring(1)
    pass_on(0, 2)
    pass_on(1, 1)
    start_ring(2)
    send_att()
    pass_on(0, 3)
    pass_on(1, 2)
    pass_on(2, 1)
    start_ring(3)
    pass_on(0, 4)
    pass_on(1, 3)
    pass_on(2, 2)
    old_moments()
    pass_on(3, 1)
    pass_on(1, 4)
    beside_came(0)
    pass_on(2, 3)
    pass_on(3, 2)
    partner_has(1)
    came(att.at[1], att_recv.at[0])
    came(att.at[2], att_recv.at[1])
    weight_term(1, 0, 1)
    partner_has(0)
    partner_beside(0)
    weight_term(0, 0)
    send_term(0)
    pass_on(2, 4)
    weight_term(1, 2)
    weight_term(0, 2)
    pass_on(3, 3)
    weight_term(0, 1)
    partner_has(2)
    weight_term(2, 0)
    send_term(1)
    weight_term(2, 1, 2)
    send_term(2)
    came(wt.at[0:3], w_recv)
    multiply(1, 0, 1)
    multiply(1, 2)
    partner_near(3)
    last_term(0)
    pass_on(3, 4)
    multiply(2, 0)
    multiply(2, 1, 2)
    last_multiply(0)
    partner_across(3)
    last_multiply(1, 2)
    send_grads()
    last_term(1, 2)

    came(dw_in, dw_recv)
    for c, start, size in row_chunks():
        rows = pl.ds(start, size)
        grad = dwacc[3, rows, :]
        for i in range(NX - 1):
            grad = grad + dw_in[i, rows, :].astype(F32)
        first_new = fnew_out[rows, :] + (1.0 - beta_first) * grad
        second_new = snew_out[rows, :] + (1.0 - beta_second) * grad * grad
        step_size = (
            first_new * (1.0 / correct_first) / (jnp.sqrt(second_new * (1.0 / correct_second)) + adam_eps)
        )
        nw_out[rows, :] = nw_out[rows, :] - learning * step_size
        fnew_out[rows, :] = first_new
        snew_out[rows, :] = second_new

    first_abs, second_abs = jnp.abs(fnew_out[...]), jnp.abs(snew_out[...])
    st[0] = lane_rows(first_abs)
    st[1] = lane_rows(second_abs)
    for dy in range(1, NY):
        rcopy(st, y_in.at[NY - dy - 1], y_send, y_recv, y=mod(y + dy, NY)).start()
    cst[0, 0:1, :] = jnp.max(first_abs, axis=0, keepdims=True)
    cst[0, 1:2, :] = jnp.max(second_abs, axis=0, keepdims=True)
    for dx in range(1, NX):
        rcopy(cst.at[0], x_in.at[NX - dx - 1], x_send, x_recv, x=mod(x + dx, NX)).start()

    multiply(0, 0)
    multiply(0, 1)
    multiply(0, 2)

    def back_rows(i):
        rows, cols = pl.ds(128 * i, 128), pl.ds(0, 128 * (i + 1))
        came(ga_in.at[:, i], ga_recv.at[i])
        total = acct[0, :, rows]
        for s in range(2):
            total = total + ga_in[s, i].astype(F32)
        grad_half = total.astype(BF16).T
        grad_probs = lax.dot_general(grad_half, vv[cols, :], NT, preferred_element_type=F32)
        row_dot = jnp.sum(
            grad_half.astype(F32) * att[0, rows, :].astype(F32), axis=-1, keepdims=True
        )
        grad_scores = (prob[rows, cols] * (grad_probs - row_dot)).astype(BF16)
        gq_out[rows, :] = (
            jnp.dot(grad_scores, kk[cols, :], preferred_element_type=F32) * SCALE
        ).astype(BF16)

    def left(ref, send):
        rcopy(ref, ref, send, zh_recv, core=k).wait_send()

    wait_units(8 - sum(staying), 8, lambda c: left(gz.at[0:c], spread_send))
    for slot in range(SLOTS):
        copies = 1 if slot in SPLIT else 3
        wait_units(landing[slot], 9, lambda c: left(gz.at[0 : copies * c], relay_send.at[slot]))
    longer = count(
        (seat(slot, from_source(way, hops)) == NY - 1) & (k == 1) & ((side == 1) | (slot not in SPLIT))
        for slot in range(SLOTS)
        for way in (0, 1)
        for hops in range(reach(way, slot))
    )
    usual = 56 * SLOTS - 28 * len(SPLIT)
    for c in range(9):
        pl.when(longer == c)(functools.partial(left, gz.at[0 : usual + c], ring_send))
    more = (k == 1) & (side == 1)
    for flag, each in ((more, 33), (jnp.logical_not(more), 32)):
        pl.when(flag)(functools.partial(left, gz.at[0 : each * len(SPLIT)], beside_send))
    for c in (0, 1):
        pl.when(k == c)(functools.partial(left, gz.at[0 : 64 * SLOTS + SLOTS * c], core_send))
    for whole, send in (
        (att.at[0:2], att_send),
        (wt.at[0:3], w_send),
        (dw_in, dw_send),
    ):
        left(whole, send)

    came(x_in, x_recv)
    cst[1] = jnp.maximum(cst[0], jnp.max(x_in[...], axis=0))
    for sequence in (1, 2):
        o = other(sequence)
        rcopy(cst.at[1], zh_in.at[sequence_of(zh, o) - 1], zh_send, zh_recv, zh=o).start()
    came(y_in, y_recv)
    mine[...] = jnp.maximum(st[...], jnp.max(y_in[...], axis=0))
    for rel in range(1, NZL * NC):
        dl, dk = rel // NC, rel % NC
        back = NC * ((NZL - dl) % NZL) + dk - 1
        rcopy(
            mine, zl_in.at[back], zl_send, zl_recv, zl=mod(zl + dl, NZL), core=lax.rem(k + dk, NC)
        ).start()
    for i in range(3):
        back_rows(i)
    came(zl_in, zl_recv)
    rows_out[...] = jnp.maximum(mine[...], jnp.max(zl_in[...], axis=0))
    came(zh_in, zh_recv)
    cols_out[...] = jnp.maximum(cst[1], jnp.max(zh_in[...], axis=0))

    for whole, send in (
        (ga_in, ga_send),
        (y_in, y_send),
        (zl_in, zl_send),
        (x_in, x_send),
        (zh_in, zh_send),
    ):
        left(whole, send)


def codes(
    gq,
    nw,
    fnew,
    snew,
    rows,
    cols,
    gq_out,
    nw_out,
    nfc_out,
    nfr_out,
    nfcol_out,
    nsc_out,
    nsr_out,
    nscol_out,
    first_code,
    second_code,
    first_rows,
    second_rows,
    first_cols,
    second_cols,
    sem,
):
    copies = []

    def out(src, dst):
        copy = pltpu.make_async_copy(src, dst, sem.at[len(copies)])
        copy.start()
        copies.append(copy)

    out(gq, gq_out)
    out(nw, nw_out)
    for moment, (new, code, code_out, maxima, maxima_out, col, col_out) in enumerate(
        (
            (fnew, first_code, nfc_out, first_rows, nfr_out, first_cols, nfcol_out),
            (snew, second_code, nsc_out, second_rows, nsr_out, second_cols, nscol_out),
        )
    ):
        col[...] = cols[moment]
        for c, start, size in row_chunks():
            at = pl.ds(start, size)
            maxima[at] = rows[moment, c, 0:size]
            low = jnp.minimum(
                down_rows(rows[moment, c : c + 1, :])[:size], cols[moment : moment + 1]
            )
            code[at, :] = (new[at, :] / (low + code_eps)).astype(BF16)
        out(code, code_out)
        out(maxima, maxima_out)
        out(col, col_out)
    for copy in copies:
        copy.wait()


def per_device(queries, keys, values, grad_out, weight, fc, frow, fcol, sc, srow, scol):
    shape = jax.ShapeDtypeStruct
    vmem = pl.BlockSpec(memory_space=pltpu.VMEM)
    hbm = pl.BlockSpec(memory_space=pltpu.HBM)
    dma = pltpu.SemaphoreType.DMA
    gq, nw, fnew, snew, rows, cols = pl.pallas_call(
        body,
        name="whole",
        out_shape=(
            shape((SEQ, HD), BF16),
            shape((ROWS, HD), F32),
            shape((ROWS, HD), F32),
            shape((ROWS, HD), F32),
            shape((2, 8, HD), F32),
            shape((2, HD), F32),
        ),
        in_specs=[hbm] * 11,
        out_specs=[vmem] * 6,
        scratch_shapes=[
            pltpu.VMEM((SEQ, HD), BF16),
            pltpu.VMEM((SEQ, HD), BF16),
            pltpu.VMEM((SEQ, HD), BF16),
            pltpu.VMEM((SEQ, HD), BF16),
            pltpu.VMEM((ROWS, HD), F32),
            pltpu.VMEM((ROWS, HD), BF16),
            pltpu.VMEM((ROWS, HD), BF16),
            pltpu.VMEM((ROWS,), F32),
            pltpu.VMEM((HD,), F32),
            pltpu.VMEM((ROWS,), F32),
            pltpu.VMEM((HD,), F32),
            pltpu.VMEM((HD, SEQ), BF16),
            pltpu.VMEM((SLOTS * SLOT, UNIT, SEQ), BF16),
            pltpu.VMEM((NX, HD, ROWS), BF16),
            pltpu.VMEM((NZH, SEQ, HD), BF16),
            pltpu.VMEM((SEQ, SEQ), F32),
            pltpu.VMEM((NZH, HD, SEQ), F32),
            pltpu.VMEM((2, 3, HD, HD), BF16),
            pltpu.VMEM((2, 3, HD, HD), BF16),
            pltpu.VMEM((NX, ROWS, HD), F32),
            pltpu.VMEM((NX - 1, ROWS, HD), BF16),
            pltpu.VMEM((NX - 1, ROWS, HD), BF16),
            pltpu.VMEM((2, 8, HD), F32),
            pltpu.VMEM((NY - 1, 2, 8, HD), F32),
            pltpu.VMEM((NZL * NC - 1, 2, 8, HD), F32),
            pltpu.VMEM((2, 8, HD), F32),
            pltpu.VMEM((2, 2, HD), F32),
            pltpu.VMEM((NX - 1, 2, HD), F32),
            pltpu.VMEM((NZH - 1, 2, HD), F32),
            dma((11,)),
            dma,
            dma((SLOTS,)),
            dma((SLOTS,)),
            dma((SLOTS,)),
            dma,
            dma((2, SLOTS + 1, 4)),
            dma,
            dma((len(SPLIT),)),
            dma((len(SPLIT),)),
            dma,
            dma((SLOTS, 2)),
            dma,
            dma((2,)),
            dma,
            dma,
            dma,
            dma((3,)),
            dma,
            dma,
            dma,
            dma,
            dma,
            dma,
            dma,
            dma,
            dma,
            dma,
        ],
        compiler_params=pltpu.CompilerParams(
            collective_id=0, has_side_effects=True, vmem_limit_bytes=48 * 1024 * 1024
        ),
    )(
        *(
            pltpu.with_memory_space_constraint(a, pltpu.HBM)
            for a in (queries, keys, values, grad_out, weight, fc, frow, fcol, sc, srow, scol)
        )
    )
    return pl.pallas_call(
        codes,
        name="codes",
        out_shape=(
            shape((SEQ, HD), BF16),
            shape((ROWS, HD), F32),
            shape((ROWS, HD), BF16),
            shape((ROWS,), F32),
            shape((HD,), F32),
            shape((ROWS, HD), BF16),
            shape((ROWS,), F32),
            shape((HD,), F32),
        ),
        compiler_params=pltpu.CompilerParams(vmem_limit_bytes=8 * 1024 * 1024),
        in_specs=[vmem] * 6,
        out_specs=[hbm] * 8,
        scratch_shapes=[
            pltpu.VMEM((ROWS, HD), BF16),
            pltpu.VMEM((ROWS, HD), BF16),
            pltpu.VMEM((ROWS,), F32),
            pltpu.VMEM((ROWS,), F32),
            pltpu.VMEM((HD,), F32),
            pltpu.VMEM((HD,), F32),
            dma((8,)),
        ],
    )(gq, nw, fnew, snew, rows, cols)


def solution(mesh):
    finer = Mesh(mesh.devices.reshape(NX, NZH, NY, NZL, NC), AXES)
    placed = (
        P(DP, TENSOR),
        P(DP, None),
        P(DP, None),
        P(DP, TENSOR),
        P(DP, TENSOR),
        P(DP, TENSOR),
        P(DP),
        P(TENSOR),
        P(DP, TENSOR),
        P(DP),
        P(TENSOR),
    )
    return jax.shard_map(
        per_device,
        mesh=finer,
        in_specs=placed,
        out_specs=(
            P(DP, TENSOR),
            P(DP, TENSOR),
            P(DP, TENSOR),
            P(DP),
            P(TENSOR),
            P(DP, TENSOR),
            P(DP),
            P(TENSOR),
        ),
        check_vma=False,
    )
```

```python
import functools

import jax
import jax.numpy as jnp
from jax import lax
from jax.experimental import pallas as pl
from jax.experimental.pallas import tpu as pltpu
from jax.sharding import Mesh
from jax.sharding import PartitionSpec as P

NX, NZH, NY, NZL, NC = 4, 3, 8, 4, 2
AXES = ("x", "zh", "y", "zl", "core")
DP = ("x", "zh")
TENSOR = ("y", "zl", "core")
MESH = pl.DeviceIdType.MESH

HD = 128
SEQ = 384
ROWS = 688
UNIT = 16
UNITS = ROWS // UNIT
ALL_UNITS = 512
HOMES = NY * NC
SLOTS = 4
SLOT = 3 * UNITS
SPLIT = (0,)
AHEAD = (2, 1, 3)
SCALE = HD ** (-0.5)

beta_first = 0.9
beta_second = 0.95
learning = 0.01
decay_rate = 0.1
adam_eps = 1e-08
code_eps = 1e-06
correct_first = 1.0 - 0.9**10
correct_second = 1.0 - 0.95**10

F32 = jnp.float32
BF16 = jnp.bfloat16
NT = (((1,), (1,)), ((), ()))


def mod(a, n):
    return lax.rem(a + n, n)


def row_chunks():
    return [(c, 128 * c, min(128, ROWS - 128 * c)) for c in range(6)]


def lane_rows(values):
    highest = jnp.max(values, axis=1, keepdims=True)
    out = []
    for c, start, size in row_chunks():
        eye = lax.broadcasted_iota(jnp.int32, (size, 128), 0) == lax.broadcasted_iota(
            jnp.int32, (size, 128), 1
        )
        out.append(
            jnp.max(jnp.where(eye, highest[start : start + size], 0.0), axis=0, keepdims=True)
        )
    out.append(jnp.zeros((2, 128), F32))
    return jnp.concatenate(out, axis=0)


def down(vector, start, size):
    row = vector[pl.ds(start, size)].reshape(1, size)
    if size < 128:
        row = jnp.concatenate([row, jnp.zeros((1, 128 - size), F32)], axis=1)
    return down_rows(row)[:size]


def down_rows(row):
    return jnp.broadcast_to(row, (128, 128)).T


def body(
    q_hbm,
    k_hbm,
    v_hbm,
    g_hbm,
    w_hbm,
    fc_hbm,
    frow_hbm,
    fcol_hbm,
    sc_hbm,
    srow_hbm,
    scol_hbm,
    gq_out,
    nw_out,
    fnew_out,
    snew_out,
    rows_out,
    cols_out,
    q,
    kk,
    vv,
    g,
    w,
    fc,
    sc,
    frow,
    fcol,
    srow,
    scol,
    gt,
    gz,
    wt,
    att,
    prob,
    acct,
    ga_stage,
    ga_in,
    dwacc,
    dw_stage,
    dw_in,
    st,
    y_in,
    zl_in,
    mine,
    cst,
    x_in,
    zh_in,
    in_sem,
    spread_send,
    relay_send,
    far_recv,
    near_recv,
    ring_send,
    ring_recv,
    beside_send,
    beside_recv,
    shared_recv,
    core_send,
    core_recv,
    att_send,
    att_recv,
    w_send,
    w_recv,
    ga_send,
    ga_recv,
    dw_send,
    dw_recv,
    y_send,
    y_recv,
    zl_send,
    zl_recv,
    x_send,
    x_recv,
    zh_send,
    zh_recv,
):
    x, zh, y, zl, k = (lax.axis_index(a) for a in AXES)
    t = 8 * y + 2 * zl + k
    pair = lax.div(y, 2)

    def rcopy(src, dst, send, recv, **dev):
        return pltpu.make_async_remote_copy(
            src_ref=src, dst_ref=dst, send_sem=send, recv_sem=recv, device_id=dev, device_id_type=MESH
        )

    def came(ref, recv):
        rcopy(ref, ref, core_send, recv, core=k).wait_recv()

    def sequence_of(source, plane):
        return jnp.where(source == plane, 0, source + (source < plane).astype(jnp.int32))

    def other(sequence):
        return sequence - 1 + (sequence - 1 >= zh).astype(jnp.int32)

    barrier = pltpu.get_barrier_semaphore()

    def greet(**dev):
        pl.semaphore_signal(barrier, inc=1, device_id=dev, device_id_type=MESH)

    for dz in (1, 2):
        greet(zh=mod(zh + dz, NZH))
    for dx in range(1, NX):
        greet(x=mod(x + dx, NX))
    for dy in range(1, NY):
        greet(y=mod(y + dy, NY))
    for rel in range(1, NZL * NC):
        greet(zl=mod(zl + rel // NC, NZL), core=lax.rem(k + rel % NC, NC))
    heads = pl.ds(pl.multiple_of(y * HD, HD), HD)
    loads = [
        pltpu.make_async_copy(src, dst, in_sem.at[i])
        for i, (src, dst) in enumerate(
            [
                (g_hbm, g),
                (q_hbm, q),
                (k_hbm.at[:, heads], kk),
                (v_hbm.at[:, heads], vv),
                (w_hbm, w),
                (fc_hbm, fc),
                (sc_hbm, sc),
                (frow_hbm, frow),
                (fcol_hbm, fcol),
                (srow_hbm, srow),
                (scol_hbm, scol),
            ]
        )
    ]
    for load in loads:
        load.start()

    turned = (
        (2 * x + NY - 1 + (zh == 2).astype(jnp.int32)) & (NY - 1),
        jnp.int32(0),
        (2 * x + 1 + (zh > 0).astype(jnp.int32)) & (NY - 1),
        jnp.int32(0),
    )

    def seat(slot, column):
        return (column + NY - turned[slot]) & (NY - 1)

    homes = [2 * seat(slot, y) + k for slot in range(SLOTS)]
    side = zl & 1

    def rows_of(u):
        return pl.ds(pl.multiple_of(UNIT * u, UNIT), UNIT)

    def ahead_of(turn):
        return jnp.where(turn == 0, 2, 2 * turn - 1)

    def slot_and_index(ahead, sequence):
        turn = jnp.where(ahead == 2, 0, lax.shift_right_logical(ahead + 1, 1))
        pair = 2 * turn + sequence - 1
        far = (pair >= 3).astype(jnp.int32)
        slot = jnp.where(ahead == 0, 3, jnp.where(sequence == 0, 0, 1 + far))
        index = jnp.where(
            ahead == 0,
            sequence - 1 + 3 * (sequence == 0).astype(jnp.int32),
            jnp.where(sequence == 0, turn, pair - 3 * far),
        )
        return slot, index

    units = []
    for slot in range(SLOTS):
        first_index = lax.div(8 * homes[slot], UNITS)
        first_place = 8 * homes[slot] - UNITS * first_index
        has_last = homes[slot] == HOMES - 1
        blocks = []
        for index in (first_index, first_index + 1):
            if slot == 0:
                xd, z = (x + ahead_of(index)) & 3, zh
            elif slot == 3:
                xd, z = x, jnp.where(index == 2, zh, other(index + 1))
            else:
                turn = 3 * (slot - 1) + index
                xd = (x + ahead_of(lax.shift_right_logical(turn, 1))) & 3
                z = other(1 + (turn & 1))
            blocks.append((z, UNITS * (NZH * xd + zh)))
        held = []
        for j in range(9):
            over = first_place + j >= UNITS
            z, start = (jnp.where(over, b, a) for a, b in zip(*blocks))
            unit = start + first_place + j - jnp.where(over, UNITS, 0)
            column = lax.shift_right_logical(unit, 3)
            line = lax.shift_right_logical(column, 1) & 3
            there = unit < ALL_UNITS
            if j == 8:
                there = there & has_last
            if slot in SPLIT:
                taken = side == min(j // 4, 1)
                there = there & taken
                here = (line & 2) == (zl & 2)
            else:
                here = (line ^ (2 * (unit & 1))) == zl
            source = dict(zh=z, y=lax.shift_right_logical(column, 3), zl=line, core=column & 1)
            held.append((there, there & here, source, (z == zh) & (column == t), unit))
        units.append(held)

    for held in units:
        for _, lands, source, same, _ in held:
            pl.when(lands & jnp.logical_not(same))(functools.partial(greet, **source))

    def count(flags):
        return sum(f.astype(jnp.int32) for f in flags)

    landing = [count(lands for _, lands, _, _, _ in held) for held in units]
    coming = [count(there for there, _, _, _, _ in held) - n for held, n in zip(units, landing)]
    staying = [count(lands & same for _, lands, _, same, _ in held) for held in units]
    greeted = 8 - sum(staying) + 2 + 3 + 7 + 7

    first_owner = lax.div(8 * t, UNITS)
    first_row = 8 * t - UNITS * first_owner
    turnover = UNITS - first_row
    sides = []

    def turn_of(slot, zd):
        first = 2 * x + NY - 1 + (zd == 2).astype(jnp.int32)
        third = 2 * x + 1 + (zd > 0).astype(jnp.int32)
        return jnp.where(slot == 0, first, jnp.where(slot == 2, third, 0))

    for owner in (first_owner, first_owner + 1):
        xd = lax.div(owner, NZH)
        zd = owner - NZH * xd
        slot, index = slot_and_index(mod(xd - x, NX), sequence_of(zh, zd))
        sides.append((zd, slot, UNITS * index, turn_of(slot, zd)))

    def goes_to(u):
        over = u >= turnover
        zd, slot, start, turn = (jnp.where(over, b, a) for a, b in zip(*sides))
        e = start + first_row + u - jnp.where(over, UNITS, 0)
        h = jnp.minimum(lax.shift_right_logical(e, 3), HOMES - 1)
        line = zl ^ (2 * (u & 1))
        for split in SPLIT:
            shared = (zl & 2) + (e - 8 * h >= 4).astype(jnp.int32)
            line = jnp.where(slot == split, shared, line)
        home = dict(zh=zd, y=(lax.shift_right_logical(h, 1) + turn) & (NY - 1), zl=line, core=h & 1)
        here = (zd == zh) & (home["y"] == y) & (home["core"] == k) & (home["zl"] == zl)
        return slot, SLOT * slot + e, home, here

    loads[0].wait()
    gt[...] = g[...].T

    pl.semaphore_wait(barrier, greeted)

    def spread(u, carry):
        slot, place, home, here = goes_to(u)

        @pl.when(here)
        def _():
            gz[place] = gt[rows_of(u), :]

        @pl.when(jnp.logical_not(here))
        def _():
            rcopy(gt.at[rows_of(u), :], gz.at[place], spread_send, far_recv.at[slot], **home).start()

        return carry

    lax.fori_loop(0, 8, spread, 0)

    loads[4].wait()
    wt[3] = w[...].astype(BF16).T
    for dx in (1, 3, 2):
        rcopy(wt.at[3], wt.at[AHEAD.index(NX - dx)], w_send, w_recv, x=mod(x + dx, NX)).start()

    for i in (1, 2, 3):
        loads[i].wait()
    for i in range(3):
        rows, cols = pl.ds(128 * i, 128), pl.ds(0, 128 * (i + 1))
        scores = (
            lax.dot_general(q[rows, :], kk[cols, :], NT, preferred_element_type=F32) * SCALE
        )
        future = lax.broadcasted_iota(jnp.int32, scores.shape, 1) > (
            lax.broadcasted_iota(jnp.int32, scores.shape, 0) + 128 * i
        )
        scores = jnp.where(future, -1e30, scores)
        exponent = jnp.exp(scores - jnp.max(scores, axis=-1, keepdims=True))
        probabilities = exponent / jnp.sum(exponent, axis=-1, keepdims=True)
        prob[rows, cols] = probabilities
        att[0, rows, :] = jnp.dot(
            probabilities.astype(BF16), vv[cols, :], preferred_element_type=F32
        ).astype(BF16)

    for slot, held in enumerate(units):
        for j, (_, _, _, _, unit) in enumerate(held):
            missing = unit >= ALL_UNITS
            if j == 8:
                missing = missing & (homes[slot] == HOMES - 1)
            if slot in SPLIT:
                missing = missing & (side == min(j // 4, 1))

            @pl.when(missing)
            def _():
                gz[SLOT * slot + 8 * homes[slot] + j] = jnp.zeros((UNIT, SEQ), BF16)

    def send_att():
        for sequence in (1, 2):
            o = other(sequence)
            there = sequence_of(zh, o)
            rcopy(att.at[0], att.at[there], att_send, att_recv.at[there - 1], zh=o).start()

    def wait_units(n, most, wait):
        for c in range(1, most + 1):
            pl.when(n == c)(functools.partial(wait, c))

    def units_came(recv, c):
        came(gz.at[0:c], recv)

    def relay(slot):
        wait_units(
            landing[slot] - staying[slot], 9, functools.partial(units_came, far_recv.at[slot])
        )

        for j, (_, lands, _, _, _) in enumerate(units[slot]):
            piece = gz.at[SLOT * slot + 8 * homes[slot] + j]

            @pl.when(lands)
            def _():
                for dl in (2,) if slot in SPLIT else (1, 2, 3):
                    rcopy(
                        piece, piece, relay_send.at[slot], near_recv.at[slot], zl=mod(zl + dl, NZL)
                    ).start()

    def parts(slot):
        return (0, 1) if slot == SLOTS - 1 else (0,)

    def reach(way, slot):
        return 4 if way == slot % 2 else 3

    def from_source(way, hops):
        return mod(y - hops, NY) if way == 0 else mod(y + hops, NY)

    def parts_of(slot, source, core):
        start = SLOT * slot + 8 * (2 * seat(slot, source) + core)
        last = (seat(slot, source) == NY - 1) & (core == 1)
        if slot in SPLIT:
            longer = last & (side == 1)
            start = start + 4 * side
            return (((start, 4, jnp.logical_not(longer)), (start, 5, longer)),)
        if len(parts(slot)) == 1:
            return (((start, 8, jnp.logical_not(last)), (start, 9, last)),)
        return (
            ((start, 4, None),),
            ((start + 4, 4, jnp.logical_not(last)), (start + 4, 5, last)),
        )

    def each_size(sizes, act):
        for start, units, when in sizes:
            ref = gz.at[pl.ds(start, units)]
            if when is None:
                act(ref)
            else:
                pl.when(when)(functools.partial(act, ref))

    def forward(way, slot, hops, part):
        def go(piece):
            rcopy(
                piece,
                piece,
                ring_send,
                ring_recv.at[way, slot + part, hops],
                y=mod(y + 1, NY) if way == 0 else mod(y - 1, NY),
            ).start()

        each_size(parts_of(slot, from_source(way, hops), k)[part], go)

    def to_partner(way, slot, hops, part):
        def go(piece):
            rcopy(piece, piece, core_send, core_recv.at[slot, hops // 4], core=1 - k).start()

        each_size(parts_of(slot, from_source(way, hops), k)[part], go)

    def to_beside(way, slot, hops):
        def go(piece):
            rcopy(piece, piece, beside_send, beside_recv.at[SPLIT.index(slot)], zl=zl ^ 1).start()

        if slot in SPLIT:
            each_size(parts_of(slot, from_source(way, hops), k)[0], go)

    def start_ring(slot):
        wait_units(coming[slot], 9, functools.partial(units_came, near_recv.at[slot]))
        for part in parts(slot):
            for way in (0, 1):
                forward(way, slot, 0, part)
        to_beside(0, slot, 0)
        for part in parts(slot):
            to_partner(0, slot, 0, part)

    def pass_on(slot, hops):
        for part in parts(slot):
            for way in (0, 1):
                if hops <= reach(way, slot):
                    each_size(
                        parts_of(slot, from_source(way, hops), k)[part],
                        lambda piece: came(piece, ring_recv.at[way, slot + part, hops - 1]),
                    )
                    if hops < reach(way, slot):
                        forward(way, slot, hops, part)
                    to_beside(way, slot, hops)
                    to_partner(way, slot, hops, part)

    def beside_came(slot):
        longer = (k == 1) & (side == 0)
        pl.when(longer)(functools.partial(came, gz.at[0:33], beside_recv.at[SPLIT.index(slot)]))
        pl.when(jnp.logical_not(longer))(functools.partial(came, gz.at[0:32], beside_recv.at[SPLIT.index(slot)]))
        for source in range(NY):
            start = SLOT * slot + 8 * (2 * source + k) + 4 * (1 - side)

            def go(units):
                piece = gz.at[pl.ds(start, units)]
                rcopy(piece, piece, core_send, shared_recv.at[SPLIT.index(slot)], core=1 - k).start()

            if source < NY - 1:
                go(4)
            else:
                pl.when(longer)(functools.partial(go, 5))
                pl.when(jnp.logical_not(longer))(functools.partial(go, 4))

    def partner_beside(slot):
        longer = (k == 0) & (side == 0)
        pl.when(longer)(functools.partial(came, gz.at[0:33], shared_recv.at[SPLIT.index(slot)]))
        pl.when(jnp.logical_not(longer))(functools.partial(came, gz.at[0:32], shared_recv.at[SPLIT.index(slot)]))

    def partner_near(slot):
        more = (k == 0) & (seat(slot, y) != NY // 2 - 1)
        each = 8
        if slot in SPLIT:
            more, each = more & (side == 1), 4
        pl.when(more)(functools.partial(came, gz.at[0 : 7 * each + 1], core_recv.at[slot, 0]))
        pl.when(jnp.logical_not(more))(functools.partial(came, gz.at[0 : 7 * each], core_recv.at[slot, 0]))

    def partner_across(slot):
        more = (k == 0) & (seat(slot, y) == NY // 2 - 1)
        each = 8
        if slot in SPLIT:
            more, each = more & (side == 1), 4
        pl.when(more)(functools.partial(came, gz.at[0 : each + 1], core_recv.at[slot, 1]))
        pl.when(jnp.logical_not(more))(functools.partial(came, gz.at[0:each], core_recv.at[slot, 1]))

    def partner_has(slot):
        partner_near(slot)
        partner_across(slot)

    def member(slot, index):
        if slot == 0:
            return index, 0
        turn = 3 * (slot - 1) + index
        return turn // 2, 1 + turn % 2

    started = {("g", 0)}

    def add_to(ref, key, term):
        ref[...] = ref[...] + term if key in started else term
        started.add(key)

    def side_by_side(slot, indices):
        blocks = [gz[pl.ds(SLOT * slot + UNITS * i, UNITS)].reshape(ROWS, SEQ) for i in indices]
        return jnp.concatenate(blocks, axis=1) if len(blocks) > 1 else blocks[0]

    def one_below_another(sequences):
        parts = [att[s] for s in sequences]
        return jnp.concatenate(parts, axis=0) if len(parts) > 1 else parts[0]

    def weight_term(slot, *indices):
        members = [member(slot, i) for i in indices]
        rows = members[0][0]
        term = jnp.dot(
            side_by_side(slot, indices),
            one_below_another([sequence for _, sequence in members]),
            preferred_element_type=F32,
        )
        add_to(dwacc.at[rows], ("w", rows), term)

    def multiply(slot, *indices):
        members = [member(slot, i) for i in indices]
        term = jnp.dot(wt[members[0][0]], side_by_side(slot, indices), preferred_element_type=F32)
        for i, (_, sequence) in enumerate(members):
            add_to(acct.at[sequence], ("g", sequence), term[:, SEQ * i : SEQ * (i + 1)])

    early = jnp.where(lax.rem(y + NY // 2, NY) <= 2, 2, 0)
    last_blocks = (early, jnp.where(early == 2, 0, 1), jnp.where(early == 2, 1, 2))

    def last_term(*turns):
        indices = [last_blocks[turn] for turn in turns]
        term = jnp.dot(
            side_by_side(SLOTS - 1, indices),
            one_below_another([lax.rem(i + 1, NZH) for i in indices]),
            preferred_element_type=F32,
        )
        add_to(dwacc.at[3], ("w", 3), term)

    def last_multiply(*turns):
        indices = [last_blocks[turn] for turn in turns]
        term = jnp.dot(wt[3], side_by_side(SLOTS - 1, indices), preferred_element_type=F32)
        for i, index in enumerate(indices):
            sequence = lax.rem(index + 1, NZH)
            acct[sequence] = acct[sequence] + term[:, SEQ * i : SEQ * (i + 1)]

    def send_term(rows):
        dw_stage[rows] = dwacc[rows].astype(BF16)
        rcopy(
            dw_stage.at[rows], dw_in.at[rows], dw_send, dw_recv, x=mod(x + AHEAD[rows], NX)
        ).start()

    def send_grad(sequence, i):
        o = other(sequence)
        ga_stage[sequence - 1, i] = acct[sequence, :, 128 * i : 128 * (i + 1)].astype(BF16)
        rcopy(
            ga_stage.at[sequence - 1, i],
            ga_in.at[sequence_of(zh, o) - 1, i],
            ga_send,
            ga_recv.at[i],
            zh=o,
        ).start()

    def send_grads(*sequences):
        for i in range(3):
            for sequence in sequences:
                send_grad(sequence, i)

    def old_moments():
        acct[0] = jnp.zeros((HD, SEQ), F32)
        for load in loads[5:]:
            load.wait()
        for c, start, size in row_chunks():
            rows = pl.ds(start, size)
            low_first = jnp.minimum(down(frow, start, size), fcol[...].reshape(1, HD))
            low_second = jnp.minimum(down(srow, start, size), scol[...].reshape(1, HD))
            fnew_out[rows, :] = beta_first * (fc[rows, :].astype(F32) * low_first)
            snew_out[rows, :] = beta_second * (sc[rows, :].astype(F32) * low_second)
            weight = w[rows, :]
            nw_out[rows, :] = weight - learning * (decay_rate * weight)

    relay(0)
    start_ring(0)
    relay(1)
    relay(2)
    relay(3)
    pass_on(0, 1)
    start_ring(1)
    pass_on(0, 2)
    pass_on(1, 1)
    start_ring(2)
    send_att()
    pass_on(0, 3)
    pass_on(1, 2)
    pass_on(2, 1)
    start_ring(3)
    pass_on(0, 4)
    pass_on(1, 3)
    pass_on(2, 2)
    old_moments()
    pass_on(3, 1)
    pass_on(1, 4)
    beside_came(0)
    pass_on(2, 3)
    pass_on(3, 2)
    partner_has(1)
    came(att.at[1], att_recv.at[0])
    came(att.at[2], att_recv.at[1])
    weight_term(1, 0, 1)
    partner_has(0)
    partner_beside(0)
    weight_term(0, 0)
    send_term(0)
    pass_on(2, 4)
    weight_term(1, 2)
    weight_term(0, 2)
    pass_on(3, 3)
    weight_term(0, 1)
    partner_has(2)
    weight_term(2, 0)
    send_term(1)
    weight_term(2, 1, 2)
    send_term(2)
    came(wt.at[0:3], w_recv)
    multiply(1, 0, 1)
    multiply(1, 2)
    partner_near(3)
    last_term(0)
    pass_on(3, 4)
    multiply(2, 0)
    multiply(2, 1, 2)
    last_multiply(0)
    pl.when(early == 0)(functools.partial(send_grads, 1))
    partner_across(3)
    last_multiply(1)
    pl.when(early == 0)(functools.partial(send_grads, 2))
    pl.when(early == 2)(functools.partial(send_grads, 1))
    last_multiply(2)
    pl.when(early == 2)(functools.partial(send_grads, 2))
    last_term(1, 2)

    came(dw_in, dw_recv)
    for c, start, size in row_chunks():
        rows = pl.ds(start, size)
        grad = dwacc[3, rows, :]
        for i in range(NX - 1):
            grad = grad + dw_in[i, rows, :].astype(F32)
        first_new = fnew_out[rows, :] + (1.0 - beta_first) * grad
        second_new = snew_out[rows, :] + (1.0 - beta_second) * grad * grad
        step_size = (
            first_new * (1.0 / correct_first) / (jnp.sqrt(second_new * (1.0 / correct_second)) + adam_eps)
        )
        nw_out[rows, :] = nw_out[rows, :] - learning * step_size
        fnew_out[rows, :] = first_new
        snew_out[rows, :] = second_new

    first_abs, second_abs = jnp.abs(fnew_out[...]), jnp.abs(snew_out[...])
    st[0] = lane_rows(first_abs)
    st[1] = lane_rows(second_abs)
    for dy in range(1, NY):
        rcopy(st, y_in.at[NY - dy - 1], y_send, y_recv, y=mod(y + dy, NY)).start()
    cst[0, 0:1, :] = jnp.max(first_abs, axis=0, keepdims=True)
    cst[0, 1:2, :] = jnp.max(second_abs, axis=0, keepdims=True)
    for dx in range(1, NX):
        rcopy(cst.at[0], x_in.at[NX - dx - 1], x_send, x_recv, x=mod(x + dx, NX)).start()

    multiply(0, 0)
    multiply(0, 1)
    multiply(0, 2)

    def back_rows(i):
        rows, cols = pl.ds(128 * i, 128), pl.ds(0, 128 * (i + 1))
        came(ga_in.at[:, i], ga_recv.at[i])
        total = acct[0, :, rows]
        for s in range(2):
            total = total + ga_in[s, i].astype(F32)
        grad_half = total.astype(BF16).T
        grad_probs = lax.dot_general(grad_half, vv[cols, :], NT, preferred_element_type=F32)
        row_dot = jnp.sum(
            grad_half.astype(F32) * att[0, rows, :].astype(F32), axis=-1, keepdims=True
        )
        grad_scores = (prob[rows, cols] * (grad_probs - row_dot)).astype(BF16)
        gq_out[rows, :] = (
            jnp.dot(grad_scores, kk[cols, :], preferred_element_type=F32) * SCALE
        ).astype(BF16)

    def left(ref, send):
        rcopy(ref, ref, send, zh_recv, core=k).wait_send()

    wait_units(8 - sum(staying), 8, lambda c: left(gz.at[0:c], spread_send))
    for slot in range(SLOTS):
        copies = 1 if slot in SPLIT else 3
        wait_units(landing[slot], 9, lambda c: left(gz.at[0 : copies * c], relay_send.at[slot]))
    longer = count(
        (seat(slot, from_source(way, hops)) == NY - 1) & (k == 1) & ((side == 1) | (slot not in SPLIT))
        for slot in range(SLOTS)
        for way in (0, 1)
        for hops in range(reach(way, slot))
    )
    usual = 56 * SLOTS - 28 * len(SPLIT)
    for c in range(9):
        pl.when(longer == c)(functools.partial(left, gz.at[0 : usual + c], ring_send))
    more = (k == 1) & (side == 1)
    for flag, each in ((more, 33), (jnp.logical_not(more), 32)):
        pl.when(flag)(functools.partial(left, gz.at[0 : each * len(SPLIT)], beside_send))
    for c in (0, 1):
        pl.when(k == c)(functools.partial(left, gz.at[0 : 64 * SLOTS + SLOTS * c], core_send))
    for whole, send in (
        (att.at[0:2], att_send),
        (wt.at[0:3], w_send),
        (dw_in, dw_send),
    ):
        left(whole, send)

    came(x_in, x_recv)
    cst[1] = jnp.maximum(cst[0], jnp.max(x_in[...], axis=0))
    for sequence in (1, 2):
        o = other(sequence)
        rcopy(cst.at[1], zh_in.at[sequence_of(zh, o) - 1], zh_send, zh_recv, zh=o).start()
    came(y_in, y_recv)
    mine[...] = jnp.maximum(st[...], jnp.max(y_in[...], axis=0))
    for rel in range(1, NZL * NC):
        dl, dk = rel // NC, rel % NC
        back = NC * ((NZL - dl) % NZL) + dk - 1
        rcopy(
            mine, zl_in.at[back], zl_send, zl_recv, zl=mod(zl + dl, NZL), core=lax.rem(k + dk, NC)
        ).start()
    for i in range(3):
        back_rows(i)
    came(zl_in, zl_recv)
    rows_out[...] = jnp.maximum(mine[...], jnp.max(zl_in[...], axis=0))
    came(zh_in, zh_recv)
    cols_out[...] = jnp.maximum(cst[1], jnp.max(zh_in[...], axis=0))

    for whole, send in (
        (ga_in, ga_send),
        (y_in, y_send),
        (zl_in, zl_send),
        (x_in, x_send),
        (zh_in, zh_send),
    ):
        left(whole, send)


def codes(
    gq,
    nw,
    fnew,
    snew,
    rows,
    cols,
    gq_out,
    nw_out,
    nfc_out,
    nfr_out,
    nfcol_out,
    nsc_out,
    nsr_out,
    nscol_out,
    first_code,
    second_code,
    first_rows,
    second_rows,
    first_cols,
    second_cols,
    sem,
):
    copies = []

    def out(src, dst):
        copy = pltpu.make_async_copy(src, dst, sem.at[len(copies)])
        copy.start()
        copies.append(copy)

    out(gq, gq_out)
    out(nw, nw_out)
    for moment, (new, code, code_out, maxima, maxima_out, col, col_out) in enumerate(
        (
            (fnew, first_code, nfc_out, first_rows, nfr_out, first_cols, nfcol_out),
            (snew, second_code, nsc_out, second_rows, nsr_out, second_cols, nscol_out),
        )
    ):
        col[...] = cols[moment]
        for c, start, size in row_chunks():
            at = pl.ds(start, size)
            maxima[at] = rows[moment, c, 0:size]
            low = jnp.minimum(
                down_rows(rows[moment, c : c + 1, :])[:size], cols[moment : moment + 1]
            )
            code[at, :] = (new[at, :] / (low + code_eps)).astype(BF16)
        out(code, code_out)
        out(maxima, maxima_out)
        out(col, col_out)
    for copy in copies:
        copy.wait()


def per_device(queries, keys, values, grad_out, weight, fc, frow, fcol, sc, srow, scol):
    shape = jax.ShapeDtypeStruct
    vmem = pl.BlockSpec(memory_space=pltpu.VMEM)
    hbm = pl.BlockSpec(memory_space=pltpu.HBM)
    dma = pltpu.SemaphoreType.DMA
    gq, nw, fnew, snew, rows, cols = pl.pallas_call(
        body,
        name="whole",
        out_shape=(
            shape((SEQ, HD), BF16),
            shape((ROWS, HD), F32),
            shape((ROWS, HD), F32),
            shape((ROWS, HD), F32),
            shape((2, 8, HD), F32),
            shape((2, HD), F32),
        ),
        in_specs=[hbm] * 11,
        out_specs=[vmem] * 6,
        scratch_shapes=[
            pltpu.VMEM((SEQ, HD), BF16),
            pltpu.VMEM((SEQ, HD), BF16),
            pltpu.VMEM((SEQ, HD), BF16),
            pltpu.VMEM((SEQ, HD), BF16),
            pltpu.VMEM((ROWS, HD), F32),
            pltpu.VMEM((ROWS, HD), BF16),
            pltpu.VMEM((ROWS, HD), BF16),
            pltpu.VMEM((ROWS,), F32),
            pltpu.VMEM((HD,), F32),
            pltpu.VMEM((ROWS,), F32),
            pltpu.VMEM((HD,), F32),
            pltpu.VMEM((HD, SEQ), BF16),
            pltpu.VMEM((SLOTS * SLOT, UNIT, SEQ), BF16),
            pltpu.VMEM((NX, HD, ROWS), BF16),
            pltpu.VMEM((NZH, SEQ, HD), BF16),
            pltpu.VMEM((SEQ, SEQ), F32),
            pltpu.VMEM((NZH, HD, SEQ), F32),
            pltpu.VMEM((2, 3, HD, HD), BF16),
            pltpu.VMEM((2, 3, HD, HD), BF16),
            pltpu.VMEM((NX, ROWS, HD), F32),
            pltpu.VMEM((NX - 1, ROWS, HD), BF16),
            pltpu.VMEM((NX - 1, ROWS, HD), BF16),
            pltpu.VMEM((2, 8, HD), F32),
            pltpu.VMEM((NY - 1, 2, 8, HD), F32),
            pltpu.VMEM((NZL * NC - 1, 2, 8, HD), F32),
            pltpu.VMEM((2, 8, HD), F32),
            pltpu.VMEM((2, 2, HD), F32),
            pltpu.VMEM((NX - 1, 2, HD), F32),
            pltpu.VMEM((NZH - 1, 2, HD), F32),
            dma((11,)),
            dma,
            dma((SLOTS,)),
            dma((SLOTS,)),
            dma((SLOTS,)),
            dma,
            dma((2, SLOTS + 1, 4)),
            dma,
            dma((len(SPLIT),)),
            dma((len(SPLIT),)),
            dma,
            dma((SLOTS, 2)),
            dma,
            dma((2,)),
            dma,
            dma,
            dma,
            dma((3,)),
            dma,
            dma,
            dma,
            dma,
            dma,
            dma,
            dma,
            dma,
            dma,
            dma,
        ],
        compiler_params=pltpu.CompilerParams(
            collective_id=0, has_side_effects=True, vmem_limit_bytes=48 * 1024 * 1024
        ),
    )(
        *(
            pltpu.with_memory_space_constraint(a, pltpu.HBM)
            for a in (queries, keys, values, grad_out, weight, fc, frow, fcol, sc, srow, scol)
        )
    )
    return pl.pallas_call(
        codes,
        name="codes",
        out_shape=(
            shape((SEQ, HD), BF16),
            shape((ROWS, HD), F32),
            shape((ROWS, HD), BF16),
            shape((ROWS,), F32),
            shape((HD,), F32),
            shape((ROWS, HD), BF16),
            shape((ROWS,), F32),
            shape((HD,), F32),
        ),
        compiler_params=pltpu.CompilerParams(vmem_limit_bytes=8 * 1024 * 1024),
        in_specs=[vmem] * 6,
        out_specs=[hbm] * 8,
        scratch_shapes=[
            pltpu.VMEM((ROWS, HD), BF16),
            pltpu.VMEM((ROWS, HD), BF16),
            pltpu.VMEM((ROWS,), F32),
            pltpu.VMEM((ROWS,), F32),
            pltpu.VMEM((HD,), F32),
            pltpu.VMEM((HD,), F32),
            dma((8,)),
        ],
    )(gq, nw, fnew, snew, rows, cols)


def solution(mesh):
    finer = Mesh(mesh.devices.reshape(NX, NZH, NY, NZL, NC), AXES)
    placed = (
        P(DP, TENSOR),
        P(DP, None),
        P(DP, None),
        P(DP, TENSOR),
        P(DP, TENSOR),
        P(DP, TENSOR),
        P(DP),
        P(TENSOR),
        P(DP, TENSOR),
        P(DP),
        P(TENSOR),
    )
    return jax.shard_map(
        per_device,
        mesh=finer,
        in_specs=placed,
        out_specs=(
            P(DP, TENSOR),
            P(DP, TENSOR),
            P(DP, TENSOR),
            P(DP),
            P(TENSOR),
            P(DP, TENSOR),
            P(DP),
            P(TENSOR),
        ),
        check_vma=False,
    )
```

```python
import functools

import jax
import jax.numpy as jnp
from jax import lax
from jax.experimental import pallas as pl
from jax.experimental.pallas import tpu as pltpu
from jax.sharding import Mesh
from jax.sharding import PartitionSpec as P

NX, NZH, NY, NZL, NC = 4, 3, 8, 4, 2
AXES = ("x", "zh", "y", "zl", "core")
DP = ("x", "zh")
TENSOR = ("y", "zl", "core")
MESH = pl.DeviceIdType.MESH

HD = 128
SEQ = 384
ROWS = 688
UNIT = 16
UNITS = ROWS // UNIT
ALL_UNITS = 512
HOMES = NY * NC
SLOTS = 4
SLOT = 3 * UNITS
SPLIT = (0,)
AHEAD = (2, 1, 3)
SCALE = HD ** (-0.5)

beta_first = 0.9
beta_second = 0.95
learning = 0.01
decay_rate = 0.1
adam_eps = 1e-08
code_eps = 1e-06
correct_first = 1.0 - 0.9**10
correct_second = 1.0 - 0.95**10

F32 = jnp.float32
BF16 = jnp.bfloat16
NT = (((1,), (1,)), ((), ()))


def mod(a, n):
    return lax.rem(a + n, n)


def row_chunks():
    return [(c, 128 * c, min(128, ROWS - 128 * c)) for c in range(6)]


def lane_rows(values):
    highest = jnp.max(values, axis=1, keepdims=True)
    out = []
    for c, start, size in row_chunks():
        eye = lax.broadcasted_iota(jnp.int32, (size, 128), 0) == lax.broadcasted_iota(
            jnp.int32, (size, 128), 1
        )
        out.append(
            jnp.max(jnp.where(eye, highest[start : start + size], 0.0), axis=0, keepdims=True)
        )
    out.append(jnp.zeros((2, 128), F32))
    return jnp.concatenate(out, axis=0)


def down(vector, start, size):
    row = vector[pl.ds(start, size)].reshape(1, size)
    if size < 128:
        row = jnp.concatenate([row, jnp.zeros((1, 128 - size), F32)], axis=1)
    return down_rows(row)[:size]


def down_rows(row):
    return jnp.broadcast_to(row, (128, 128)).T


def body(
    q_hbm,
    k_hbm,
    v_hbm,
    g_hbm,
    w_hbm,
    fc_hbm,
    frow_hbm,
    fcol_hbm,
    sc_hbm,
    srow_hbm,
    scol_hbm,
    gq_out,
    nw_out,
    fnew_out,
    snew_out,
    rows_out,
    cols_out,
    q,
    kk,
    vv,
    g,
    w,
    fc,
    sc,
    frow,
    fcol,
    srow,
    scol,
    gt,
    gz,
    wt,
    att,
    prob,
    acct,
    ga_stage,
    ga_in,
    dwacc,
    dw_stage,
    dw_in,
    st,
    y_in,
    zl_in,
    mine,
    cst,
    x_in,
    zh_in,
    in_sem,
    spread_send,
    relay_send,
    far_recv,
    near_recv,
    ring_send,
    ring_recv,
    beside_send,
    beside_recv,
    shared_recv,
    core_send,
    core_recv,
    att_send,
    att_recv,
    w_send,
    w_recv,
    ga_send,
    ga_recv,
    dw_send,
    dw_recv,
    y_send,
    y_recv,
    zl_send,
    zl_recv,
    x_send,
    x_recv,
    zh_send,
    zh_recv,
):
    x, zh, y, zl, k = (lax.axis_index(a) for a in AXES)
    t = 8 * y + 2 * zl + k
    pair = lax.div(y, 2)

    def rcopy(src, dst, send, recv, **dev):
        return pltpu.make_async_remote_copy(
            src_ref=src, dst_ref=dst, send_sem=send, recv_sem=recv, device_id=dev, device_id_type=MESH
        )

    def came(ref, recv):
        rcopy(ref, ref, core_send, recv, core=k).wait_recv()

    def sequence_of(source, plane):
        return jnp.where(source == plane, 0, source + (source < plane).astype(jnp.int32))

    def other(sequence):
        return sequence - 1 + (sequence - 1 >= zh).astype(jnp.int32)

    barrier = pltpu.get_barrier_semaphore()

    def greet(**dev):
        pl.semaphore_signal(barrier, inc=1, device_id=dev, device_id_type=MESH)

    for dz in (1, 2):
        greet(zh=mod(zh + dz, NZH))
    for dx in range(1, NX):
        greet(x=mod(x + dx, NX))
    for dy in range(1, NY):
        greet(y=mod(y + dy, NY))
    for rel in range(1, NZL * NC):
        greet(zl=mod(zl + rel // NC, NZL), core=lax.rem(k + rel % NC, NC))
    heads = pl.ds(pl.multiple_of(y * HD, HD), HD)
    loads = [
        pltpu.make_async_copy(src, dst, in_sem.at[i])
        for i, (src, dst) in enumerate(
            [
                (g_hbm, g),
                (q_hbm, q),
                (k_hbm.at[:, heads], kk),
                (v_hbm.at[:, heads], vv),
                (w_hbm, w),
                (fc_hbm, fc),
                (sc_hbm, sc),
                (frow_hbm, frow),
                (fcol_hbm, fcol),
                (srow_hbm, srow),
                (scol_hbm, scol),
            ]
        )
    ]
    for load in loads:
        load.start()

    turned = (
        (2 * x + NY - 1 + (zh == 2).astype(jnp.int32)) & (NY - 1),
        jnp.int32(0),
        (2 * x + 1 + (zh > 0).astype(jnp.int32)) & (NY - 1),
        jnp.int32(0),
    )

    def seat(slot, column):
        return (column + NY - turned[slot]) & (NY - 1)

    homes = [2 * seat(slot, y) + k for slot in range(SLOTS)]
    side = zl & 1

    def rows_of(u):
        return pl.ds(pl.multiple_of(UNIT * u, UNIT), UNIT)

    def ahead_of(turn):
        return jnp.where(turn == 0, 2, 2 * turn - 1)

    def slot_and_index(ahead, sequence):
        turn = jnp.where(ahead == 2, 0, lax.shift_right_logical(ahead + 1, 1))
        pair = 2 * turn + sequence - 1
        far = (pair >= 3).astype(jnp.int32)
        slot = jnp.where(ahead == 0, 3, jnp.where(sequence == 0, 0, 1 + far))
        index = jnp.where(
            ahead == 0,
            sequence - 1 + 3 * (sequence == 0).astype(jnp.int32),
            jnp.where(sequence == 0, turn, pair - 3 * far),
        )
        return slot, index

    units = []
    for slot in range(SLOTS):
        first_index = lax.div(8 * homes[slot], UNITS)
        first_place = 8 * homes[slot] - UNITS * first_index
        has_last = homes[slot] == HOMES - 1
        blocks = []
        for index in (first_index, first_index + 1):
            if slot == 0:
                xd, z = (x + ahead_of(index)) & 3, zh
            elif slot == 3:
                xd, z = x, jnp.where(index == 2, zh, other(index + 1))
            else:
                turn = 3 * (slot - 1) + index
                xd = (x + ahead_of(lax.shift_right_logical(turn, 1))) & 3
                z = other(1 + (turn & 1))
            blocks.append((z, UNITS * (NZH * xd + zh)))
        held = []
        for j in range(9):
            over = first_place + j >= UNITS
            z, start = (jnp.where(over, b, a) for a, b in zip(*blocks))
            unit = start + first_place + j - jnp.where(over, UNITS, 0)
            column = lax.shift_right_logical(unit, 3)
            line = lax.shift_right_logical(column, 1) & 3
            there = unit < ALL_UNITS
            if j == 8:
                there = there & has_last
            if slot in SPLIT:
                taken = side == min(j // 4, 1)
                there = there & taken
                here = (line & 2) == (zl & 2)
            else:
                here = (line ^ (2 * (unit & 1))) == zl
            source = dict(zh=z, y=lax.shift_right_logical(column, 3), zl=line, core=column & 1)
            held.append((there, there & here, source, (z == zh) & (column == t), unit))
        units.append(held)

    for held in units:
        for _, lands, source, same, _ in held:
            pl.when(lands & jnp.logical_not(same))(functools.partial(greet, **source))

    def count(flags):
        return sum(f.astype(jnp.int32) for f in flags)

    landing = [count(lands for _, lands, _, _, _ in held) for held in units]
    coming = [count(there for there, _, _, _, _ in held) - n for held, n in zip(units, landing)]
    staying = [count(lands & same for _, lands, _, same, _ in held) for held in units]
    greeted = 8 - sum(staying) + 2 + 3 + 7 + 7

    first_owner = lax.div(8 * t, UNITS)
    first_row = 8 * t - UNITS * first_owner
    turnover = UNITS - first_row
    sides = []

    def turn_of(slot, zd):
        first = 2 * x + NY - 1 + (zd == 2).astype(jnp.int32)
        third = 2 * x + 1 + (zd > 0).astype(jnp.int32)
        return jnp.where(slot == 0, first, jnp.where(slot == 2, third, 0))

    for owner in (first_owner, first_owner + 1):
        xd = lax.div(owner, NZH)
        zd = owner - NZH * xd
        slot, index = slot_and_index(mod(xd - x, NX), sequence_of(zh, zd))
        sides.append((zd, slot, UNITS * index, turn_of(slot, zd)))

    def goes_to(u):
        over = u >= turnover
        zd, slot, start, turn = (jnp.where(over, b, a) for a, b in zip(*sides))
        e = start + first_row + u - jnp.where(over, UNITS, 0)
        h = jnp.minimum(lax.shift_right_logical(e, 3), HOMES - 1)
        line = zl ^ (2 * (u & 1))
        for split in SPLIT:
            shared = (zl & 2) + (e - 8 * h >= 4).astype(jnp.int32)
            line = jnp.where(slot == split, shared, line)
        home = dict(zh=zd, y=(lax.shift_right_logical(h, 1) + turn) & (NY - 1), zl=line, core=h & 1)
        here = (zd == zh) & (home["y"] == y) & (home["core"] == k) & (home["zl"] == zl)
        return slot, SLOT * slot + e, home, here

    loads[0].wait()
    gt[...] = g[...].T

    pl.semaphore_wait(barrier, greeted)

    def spread(u, carry):
        slot, place, home, here = goes_to(u)

        @pl.when(here)
        def _():
            gz[place] = gt[rows_of(u), :]

        @pl.when(jnp.logical_not(here))
        def _():
            rcopy(gt.at[rows_of(u), :], gz.at[place], spread_send, far_recv.at[slot], **home).start()

        return carry

    lax.fori_loop(0, 8, spread, 0)

    loads[4].wait()
    wt[3] = w[...].astype(BF16).T
    for dx in (1, 3, 2):
        rcopy(wt.at[3], wt.at[AHEAD.index(NX - dx)], w_send, w_recv, x=mod(x + dx, NX)).start()

    for i in (1, 2, 3):
        loads[i].wait()
    for i in range(3):
        rows, cols = pl.ds(128 * i, 128), pl.ds(0, 128 * (i + 1))
        scores = (
            lax.dot_general(q[rows, :], kk[cols, :], NT, preferred_element_type=F32) * SCALE
        )
        future = lax.broadcasted_iota(jnp.int32, scores.shape, 1) > (
            lax.broadcasted_iota(jnp.int32, scores.shape, 0) + 128 * i
        )
        scores = jnp.where(future, -1e30, scores)
        exponent = jnp.exp(scores - jnp.max(scores, axis=-1, keepdims=True))
        probabilities = exponent / jnp.sum(exponent, axis=-1, keepdims=True)
        prob[rows, cols] = probabilities
        att[0, rows, :] = jnp.dot(
            probabilities.astype(BF16), vv[cols, :], preferred_element_type=F32
        ).astype(BF16)

    for slot, held in enumerate(units):
        for j, (_, _, _, _, unit) in enumerate(held):
            missing = unit >= ALL_UNITS
            if j == 8:
                missing = missing & (homes[slot] == HOMES - 1)
            if slot in SPLIT:
                missing = missing & (side == min(j // 4, 1))

            @pl.when(missing)
            def _():
                gz[SLOT * slot + 8 * homes[slot] + j] = jnp.zeros((UNIT, SEQ), BF16)

    def send_att():
        for sequence in (1, 2):
            o = other(sequence)
            there = sequence_of(zh, o)
            rcopy(att.at[0], att.at[there], att_send, att_recv.at[there - 1], zh=o).start()

    def wait_units(n, most, wait):
        for c in range(1, most + 1):
            pl.when(n == c)(functools.partial(wait, c))

    def units_came(recv, c):
        came(gz.at[0:c], recv)

    def relay(slot):
        wait_units(
            landing[slot] - staying[slot], 9, functools.partial(units_came, far_recv.at[slot])
        )

        for j, (_, lands, _, _, _) in enumerate(units[slot]):
            piece = gz.at[SLOT * slot + 8 * homes[slot] + j]

            @pl.when(lands)
            def _():
                for dl in (2,) if slot in SPLIT else (1, 2, 3):
                    rcopy(
                        piece, piece, relay_send.at[slot], near_recv.at[slot], zl=mod(zl + dl, NZL)
                    ).start()

    def parts(slot):
        return (0, 1) if slot == SLOTS - 1 else (0,)

    def reach(way, slot):
        return 4 if way == slot % 2 else 3

    def from_source(way, hops):
        return mod(y - hops, NY) if way == 0 else mod(y + hops, NY)

    def parts_of(slot, source, core):
        start = SLOT * slot + 8 * (2 * seat(slot, source) + core)
        last = (seat(slot, source) == NY - 1) & (core == 1)
        if slot in SPLIT:
            longer = last & (side == 1)
            start = start + 4 * side
            return (((start, 4, jnp.logical_not(longer)), (start, 5, longer)),)
        if len(parts(slot)) == 1:
            return (((start, 8, jnp.logical_not(last)), (start, 9, last)),)
        return (
            ((start, 4, None),),
            ((start + 4, 4, jnp.logical_not(last)), (start + 4, 5, last)),
        )

    def each_size(sizes, act):
        for start, units, when in sizes:
            ref = gz.at[pl.ds(start, units)]
            if when is None:
                act(ref)
            else:
                pl.when(when)(functools.partial(act, ref))

    def forward(way, slot, hops, part):
        def go(piece):
            rcopy(
                piece,
                piece,
                ring_send,
                ring_recv.at[way, slot + part, hops],
                y=mod(y + 1, NY) if way == 0 else mod(y - 1, NY),
            ).start()

        each_size(parts_of(slot, from_source(way, hops), k)[part], go)

    def to_partner(way, slot, hops, part):
        def go(piece):
            rcopy(piece, piece, core_send, core_recv.at[slot, hops // 4], core=1 - k).start()

        each_size(parts_of(slot, from_source(way, hops), k)[part], go)

    def to_beside(way, slot, hops):
        def go(piece):
            rcopy(piece, piece, beside_send, beside_recv.at[SPLIT.index(slot)], zl=zl ^ 1).start()

        if slot in SPLIT:
            each_size(parts_of(slot, from_source(way, hops), k)[0], go)

    def start_ring(slot):
        wait_units(coming[slot], 9, functools.partial(units_came, near_recv.at[slot]))
        for part in parts(slot):
            for way in (0, 1):
                forward(way, slot, 0, part)
        to_beside(0, slot, 0)
        for part in parts(slot):
            to_partner(0, slot, 0, part)

    def pass_on(slot, hops):
        for part in parts(slot):
            for way in (0, 1):
                if hops <= reach(way, slot):
                    each_size(
                        parts_of(slot, from_source(way, hops), k)[part],
                        lambda piece: came(piece, ring_recv.at[way, slot + part, hops - 1]),
                    )
                    if hops < reach(way, slot):
                        forward(way, slot, hops, part)
                    to_beside(way, slot, hops)
                    to_partner(way, slot, hops, part)

    def beside_came(slot):
        longer = (k == 1) & (side == 0)
        pl.when(longer)(functools.partial(came, gz.at[0:33], beside_recv.at[SPLIT.index(slot)]))
        pl.when(jnp.logical_not(longer))(functools.partial(came, gz.at[0:32], beside_recv.at[SPLIT.index(slot)]))
        for source in range(NY):
            start = SLOT * slot + 8 * (2 * source + k) + 4 * (1 - side)

            def go(units):
                piece = gz.at[pl.ds(start, units)]
                rcopy(piece, piece, core_send, shared_recv.at[SPLIT.index(slot)], core=1 - k).start()

            if source < NY - 1:
                go(4)
            else:
                pl.when(longer)(functools.partial(go, 5))
                pl.when(jnp.logical_not(longer))(functools.partial(go, 4))

    def partner_beside(slot):
        longer = (k == 0) & (side == 0)
        pl.when(longer)(functools.partial(came, gz.at[0:33], shared_recv.at[SPLIT.index(slot)]))
        pl.when(jnp.logical_not(longer))(functools.partial(came, gz.at[0:32], shared_recv.at[SPLIT.index(slot)]))

    def partner_near(slot):
        more = (k == 0) & (seat(slot, y) != NY // 2 - 1)
        each = 8
        if slot in SPLIT:
            more, each = more & (side == 1), 4
        pl.when(more)(functools.partial(came, gz.at[0 : 7 * each + 1], core_recv.at[slot, 0]))
        pl.when(jnp.logical_not(more))(functools.partial(came, gz.at[0 : 7 * each], core_recv.at[slot, 0]))

    def partner_across(slot):
        more = (k == 0) & (seat(slot, y) == NY // 2 - 1)
        each = 8
        if slot in SPLIT:
            more, each = more & (side == 1), 4
        pl.when(more)(functools.partial(came, gz.at[0 : each + 1], core_recv.at[slot, 1]))
        pl.when(jnp.logical_not(more))(functools.partial(came, gz.at[0:each], core_recv.at[slot, 1]))

    def partner_has(slot):
        partner_near(slot)
        partner_across(slot)

    def member(slot, index):
        if slot == 0:
            return index, 0
        turn = 3 * (slot - 1) + index
        return turn // 2, 1 + turn % 2

    started = {("g", 0)}

    def add_to(ref, key, term):
        ref[...] = ref[...] + term if key in started else term
        started.add(key)

    def side_by_side(slot, indices):
        blocks = [gz[pl.ds(SLOT * slot + UNITS * i, UNITS)].reshape(ROWS, SEQ) for i in indices]
        return jnp.concatenate(blocks, axis=1) if len(blocks) > 1 else blocks[0]

    def one_below_another(sequences):
        parts = [att[s] for s in sequences]
        return jnp.concatenate(parts, axis=0) if len(parts) > 1 else parts[0]

    def weight_term(slot, *indices):
        members = [member(slot, i) for i in indices]
        rows = members[0][0]
        term = jnp.dot(
            side_by_side(slot, indices),
            one_below_another([sequence for _, sequence in members]),
            preferred_element_type=F32,
        )
        add_to(dwacc.at[rows], ("w", rows), term)

    def multiply(slot, *indices):
        members = [member(slot, i) for i in indices]
        term = jnp.dot(wt[members[0][0]], side_by_side(slot, indices), preferred_element_type=F32)
        for i, (_, sequence) in enumerate(members):
            add_to(acct.at[sequence], ("g", sequence), term[:, SEQ * i : SEQ * (i + 1)])

    early = jnp.where(lax.rem(y + NY // 2, NY) <= 2, 2, 0)
    last_blocks = (early, jnp.where(early == 2, 0, 1), jnp.where(early == 2, 1, 2))

    def last_term(*turns):
        indices = [last_blocks[turn] for turn in turns]
        term = jnp.dot(
            side_by_side(SLOTS - 1, indices),
            one_below_another([lax.rem(i + 1, NZH) for i in indices]),
            preferred_element_type=F32,
        )
        add_to(dwacc.at[3], ("w", 3), term)

    def last_multiply(*turns):
        indices = [last_blocks[turn] for turn in turns]
        term = jnp.dot(wt[3], side_by_side(SLOTS - 1, indices), preferred_element_type=F32)
        for i, index in enumerate(indices):
            sequence = lax.rem(index + 1, NZH)
            acct[sequence] = acct[sequence] + term[:, SEQ * i : SEQ * (i + 1)]

    def send_term(rows):
        for start, size in ((0, 352), (352, ROWS - 352)):
            part = pl.ds(start, size)
            dw_stage[rows, part, :] = dwacc[rows, part, :].astype(BF16)
            rcopy(
                dw_stage.at[rows, part],
                dw_in.at[rows, part],
                dw_send,
                dw_recv,
                x=mod(x + AHEAD[rows], NX),
            ).start()

    def send_grad(sequence, i):
        o = other(sequence)
        ga_stage[sequence - 1, i] = acct[sequence, :, 128 * i : 128 * (i + 1)].astype(BF16)
        rcopy(
            ga_stage.at[sequence - 1, i],
            ga_in.at[sequence_of(zh, o) - 1, i],
            ga_send,
            ga_recv.at[i],
            zh=o,
        ).start()

    def send_grads(*sequences):
        for i in range(3):
            for sequence in sequences:
                send_grad(sequence, i)

    def old_moments():
        acct[0] = jnp.zeros((HD, SEQ), F32)
        for load in loads[5:]:
            load.wait()
        for c, start, size in row_chunks():
            rows = pl.ds(start, size)
            low_first = jnp.minimum(down(frow, start, size), fcol[...].reshape(1, HD))
            low_second = jnp.minimum(down(srow, start, size), scol[...].reshape(1, HD))
            fnew_out[rows, :] = beta_first * (fc[rows, :].astype(F32) * low_first)
            snew_out[rows, :] = beta_second * (sc[rows, :].astype(F32) * low_second)
            weight = w[rows, :]
            nw_out[rows, :] = weight - learning * (decay_rate * weight)

    relay(0)
    start_ring(0)
    relay(1)
    relay(2)
    relay(3)
    pass_on(0, 1)
    start_ring(1)
    pass_on(0, 2)
    pass_on(1, 1)
    start_ring(2)
    send_att()
    pass_on(0, 3)
    pass_on(1, 2)
    pass_on(2, 1)
    start_ring(3)
    pass_on(0, 4)
    pass_on(1, 3)
    pass_on(2, 2)
    old_moments()
    pass_on(3, 1)
    pass_on(1, 4)
    beside_came(0)
    pass_on(2, 3)
    pass_on(3, 2)
    partner_has(1)
    came(att.at[1], att_recv.at[0])
    came(att.at[2], att_recv.at[1])
    weight_term(1, 0, 1)
    partner_has(0)
    partner_beside(0)
    weight_term(0, 0)
    send_term(0)
    pass_on(2, 4)
    weight_term(1, 2)
    weight_term(0, 2)
    pass_on(3, 3)
    weight_term(0, 1)
    partner_has(2)
    weight_term(2, 0)
    send_term(1)
    weight_term(2, 1, 2)
    send_term(2)
    came(wt.at[0:3], w_recv)
    multiply(1, 0, 1)
    multiply(1, 2)
    partner_near(3)
    last_term(0)
    pass_on(3, 4)
    multiply(2, 0)
    multiply(2, 1, 2)
    last_multiply(0)
    pl.when(early == 0)(functools.partial(send_grads, 1))
    partner_across(3)
    last_multiply(1)
    pl.when(early == 0)(functools.partial(send_grads, 2))
    pl.when(early == 2)(functools.partial(send_grads, 1))
    last_multiply(2)
    pl.when(early == 2)(functools.partial(send_grads, 2))
    last_term(1, 2)

    came(dw_in, dw_recv)
    for c, start, size in row_chunks():
        rows = pl.ds(start, size)
        grad = dwacc[3, rows, :]
        for i in range(NX - 1):
            grad = grad + dw_in[i, rows, :].astype(F32)
        first_new = fnew_out[rows, :] + (1.0 - beta_first) * grad
        second_new = snew_out[rows, :] + (1.0 - beta_second) * grad * grad
        step_size = (
            first_new * (1.0 / correct_first) / (jnp.sqrt(second_new * (1.0 / correct_second)) + adam_eps)
        )
        nw_out[rows, :] = nw_out[rows, :] - learning * step_size
        fnew_out[rows, :] = first_new
        snew_out[rows, :] = second_new

    first_abs, second_abs = jnp.abs(fnew_out[...]), jnp.abs(snew_out[...])
    st[0] = lane_rows(first_abs)
    st[1] = lane_rows(second_abs)
    for dy in range(1, NY):
        rcopy(st, y_in.at[NY - dy - 1], y_send, y_recv, y=mod(y + dy, NY)).start()
    cst[0, 0:1, :] = jnp.max(first_abs, axis=0, keepdims=True)
    cst[0, 1:2, :] = jnp.max(second_abs, axis=0, keepdims=True)
    for dx in range(1, NX):
        rcopy(cst.at[0], x_in.at[NX - dx - 1], x_send, x_recv, x=mod(x + dx, NX)).start()

    multiply(0, 0)
    multiply(0, 1)
    multiply(0, 2)

    def back_rows(i):
        rows, cols = pl.ds(128 * i, 128), pl.ds(0, 128 * (i + 1))
        came(ga_in.at[:, i], ga_recv.at[i])
        total = acct[0, :, rows]
        for s in range(2):
            total = total + ga_in[s, i].astype(F32)
        grad_half = total.astype(BF16).T
        grad_probs = lax.dot_general(grad_half, vv[cols, :], NT, preferred_element_type=F32)
        row_dot = jnp.sum(
            grad_half.astype(F32) * att[0, rows, :].astype(F32), axis=-1, keepdims=True
        )
        grad_scores = (prob[rows, cols] * (grad_probs - row_dot)).astype(BF16)
        gq_out[rows, :] = (
            jnp.dot(grad_scores, kk[cols, :], preferred_element_type=F32) * SCALE
        ).astype(BF16)

    def left(ref, send):
        rcopy(ref, ref, send, zh_recv, core=k).wait_send()

    wait_units(8 - sum(staying), 8, lambda c: left(gz.at[0:c], spread_send))
    for slot in range(SLOTS):
        copies = 1 if slot in SPLIT else 3
        wait_units(landing[slot], 9, lambda c: left(gz.at[0 : copies * c], relay_send.at[slot]))
    longer = count(
        (seat(slot, from_source(way, hops)) == NY - 1) & (k == 1) & ((side == 1) | (slot not in SPLIT))
        for slot in range(SLOTS)
        for way in (0, 1)
        for hops in range(reach(way, slot))
    )
    usual = 56 * SLOTS - 28 * len(SPLIT)
    for c in range(9):
        pl.when(longer == c)(functools.partial(left, gz.at[0 : usual + c], ring_send))
    more = (k == 1) & (side == 1)
    for flag, each in ((more, 33), (jnp.logical_not(more), 32)):
        pl.when(flag)(functools.partial(left, gz.at[0 : each * len(SPLIT)], beside_send))
    for c in (0, 1):
        pl.when(k == c)(functools.partial(left, gz.at[0 : 64 * SLOTS + SLOTS * c], core_send))
    for whole, send in (
        (att.at[0:2], att_send),
        (wt.at[0:3], w_send),
        (dw_in, dw_send),
    ):
        left(whole, send)

    came(x_in, x_recv)
    cst[1] = jnp.maximum(cst[0], jnp.max(x_in[...], axis=0))
    for sequence in (1, 2):
        o = other(sequence)
        rcopy(cst.at[1], zh_in.at[sequence_of(zh, o) - 1], zh_send, zh_recv, zh=o).start()
    came(y_in, y_recv)
    mine[...] = jnp.maximum(st[...], jnp.max(y_in[...], axis=0))
    for rel in range(1, NZL * NC):
        dl, dk = rel // NC, rel % NC
        back = NC * ((NZL - dl) % NZL) + dk - 1
        rcopy(
            mine, zl_in.at[back], zl_send, zl_recv, zl=mod(zl + dl, NZL), core=lax.rem(k + dk, NC)
        ).start()
    for i in range(3):
        back_rows(i)
    came(zl_in, zl_recv)
    rows_out[...] = jnp.maximum(mine[...], jnp.max(zl_in[...], axis=0))
    came(zh_in, zh_recv)
    cols_out[...] = jnp.maximum(cst[1], jnp.max(zh_in[...], axis=0))

    for whole, send in (
        (ga_in, ga_send),
        (y_in, y_send),
        (zl_in, zl_send),
        (x_in, x_send),
        (zh_in, zh_send),
    ):
        left(whole, send)


def codes(
    gq,
    nw,
    fnew,
    snew,
    rows,
    cols,
    gq_out,
    nw_out,
    nfc_out,
    nfr_out,
    nfcol_out,
    nsc_out,
    nsr_out,
    nscol_out,
    first_code,
    second_code,
    first_rows,
    second_rows,
    first_cols,
    second_cols,
    sem,
):
    copies = []

    def out(src, dst):
        copy = pltpu.make_async_copy(src, dst, sem.at[len(copies)])
        copy.start()
        copies.append(copy)

    out(gq, gq_out)
    out(nw, nw_out)
    for moment, (new, code, code_out, maxima, maxima_out, col, col_out) in enumerate(
        (
            (fnew, first_code, nfc_out, first_rows, nfr_out, first_cols, nfcol_out),
            (snew, second_code, nsc_out, second_rows, nsr_out, second_cols, nscol_out),
        )
    ):
        col[...] = cols[moment]
        for c, start, size in row_chunks():
            at = pl.ds(start, size)
            maxima[at] = rows[moment, c, 0:size]
            low = jnp.minimum(
                down_rows(rows[moment, c : c + 1, :])[:size], cols[moment : moment + 1]
            )
            code[at, :] = (new[at, :] / (low + code_eps)).astype(BF16)
        out(code, code_out)
        out(maxima, maxima_out)
        out(col, col_out)
    for copy in copies:
        copy.wait()


def per_device(queries, keys, values, grad_out, weight, fc, frow, fcol, sc, srow, scol):
    shape = jax.ShapeDtypeStruct
    vmem = pl.BlockSpec(memory_space=pltpu.VMEM)
    hbm = pl.BlockSpec(memory_space=pltpu.HBM)
    dma = pltpu.SemaphoreType.DMA
    gq, nw, fnew, snew, rows, cols = pl.pallas_call(
        body,
        name="whole",
        out_shape=(
            shape((SEQ, HD), BF16),
            shape((ROWS, HD), F32),
            shape((ROWS, HD), F32),
            shape((ROWS, HD), F32),
            shape((2, 8, HD), F32),
            shape((2, HD), F32),
        ),
        in_specs=[hbm] * 11,
        out_specs=[vmem] * 6,
        scratch_shapes=[
            pltpu.VMEM((SEQ, HD), BF16),
            pltpu.VMEM((SEQ, HD), BF16),
            pltpu.VMEM((SEQ, HD), BF16),
            pltpu.VMEM((SEQ, HD), BF16),
            pltpu.VMEM((ROWS, HD), F32),
            pltpu.VMEM((ROWS, HD), BF16),
            pltpu.VMEM((ROWS, HD), BF16),
            pltpu.VMEM((ROWS,), F32),
            pltpu.VMEM((HD,), F32),
            pltpu.VMEM((ROWS,), F32),
            pltpu.VMEM((HD,), F32),
            pltpu.VMEM((HD, SEQ), BF16),
            pltpu.VMEM((SLOTS * SLOT, UNIT, SEQ), BF16),
            pltpu.VMEM((NX, HD, ROWS), BF16),
            pltpu.VMEM((NZH, SEQ, HD), BF16),
            pltpu.VMEM((SEQ, SEQ), F32),
            pltpu.VMEM((NZH, HD, SEQ), F32),
            pltpu.VMEM((2, 3, HD, HD), BF16),
            pltpu.VMEM((2, 3, HD, HD), BF16),
            pltpu.VMEM((NX, ROWS, HD), F32),
            pltpu.VMEM((NX - 1, ROWS, HD), BF16),
            pltpu.VMEM((NX - 1, ROWS, HD), BF16),
            pltpu.VMEM((2, 8, HD), F32),
            pltpu.VMEM((NY - 1, 2, 8, HD), F32),
            pltpu.VMEM((NZL * NC - 1, 2, 8, HD), F32),
            pltpu.VMEM((2, 8, HD), F32),
            pltpu.VMEM((2, 2, HD), F32),
            pltpu.VMEM((NX - 1, 2, HD), F32),
            pltpu.VMEM((NZH - 1, 2, HD), F32),
            dma((11,)),
            dma,
            dma((SLOTS,)),
            dma((SLOTS,)),
            dma((SLOTS,)),
            dma,
            dma((2, SLOTS + 1, 4)),
            dma,
            dma((len(SPLIT),)),
            dma((len(SPLIT),)),
            dma,
            dma((SLOTS, 2)),
            dma,
            dma((2,)),
            dma,
            dma,
            dma,
            dma((3,)),
            dma,
            dma,
            dma,
            dma,
            dma,
            dma,
            dma,
            dma,
            dma,
            dma,
        ],
        compiler_params=pltpu.CompilerParams(
            collective_id=0, has_side_effects=True, vmem_limit_bytes=48 * 1024 * 1024
        ),
    )(
        *(
            pltpu.with_memory_space_constraint(a, pltpu.HBM)
            for a in (queries, keys, values, grad_out, weight, fc, frow, fcol, sc, srow, scol)
        )
    )
    return pl.pallas_call(
        codes,
        name="codes",
        out_shape=(
            shape((SEQ, HD), BF16),
            shape((ROWS, HD), F32),
            shape((ROWS, HD), BF16),
            shape((ROWS,), F32),
            shape((HD,), F32),
            shape((ROWS, HD), BF16),
            shape((ROWS,), F32),
            shape((HD,), F32),
        ),
        compiler_params=pltpu.CompilerParams(vmem_limit_bytes=8 * 1024 * 1024),
        in_specs=[vmem] * 6,
        out_specs=[hbm] * 8,
        scratch_shapes=[
            pltpu.VMEM((ROWS, HD), BF16),
            pltpu.VMEM((ROWS, HD), BF16),
            pltpu.VMEM((ROWS,), F32),
            pltpu.VMEM((ROWS,), F32),
            pltpu.VMEM((HD,), F32),
            pltpu.VMEM((HD,), F32),
            dma((8,)),
        ],
    )(gq, nw, fnew, snew, rows, cols)


def solution(mesh):
    finer = Mesh(mesh.devices.reshape(NX, NZH, NY, NZL, NC), AXES)
    placed = (
        P(DP, TENSOR),
        P(DP, None),
        P(DP, None),
        P(DP, TENSOR),
        P(DP, TENSOR),
        P(DP, TENSOR),
        P(DP),
        P(TENSOR),
        P(DP, TENSOR),
        P(DP),
        P(TENSOR),
    )
    return jax.shard_map(
        per_device,
        mesh=finer,
        in_specs=placed,
        out_specs=(
            P(DP, TENSOR),
            P(DP, TENSOR),
            P(DP, TENSOR),
            P(DP),
            P(TENSOR),
            P(DP, TENSOR),
            P(DP),
            P(TENSOR),
        ),
        check_vma=False,
    )
```

```python
import functools

import jax
import jax.numpy as jnp
from jax import lax
from jax.experimental import pallas as pl
from jax.experimental.pallas import tpu as pltpu
from jax.sharding import Mesh
from jax.sharding import PartitionSpec as P

NX, NZH, NY, NZL, NC = 4, 3, 8, 4, 2
AXES = ("x", "zh", "y", "zl", "core")
DP = ("x", "zh")
TENSOR = ("y", "zl", "core")
MESH = pl.DeviceIdType.MESH

HD = 128
SEQ = 384
ROWS = 688
UNIT = 16
UNITS = ROWS // UNIT
ALL_UNITS = 512
HOMES = NY * NC
SLOTS = 4
SLOT = 3 * UNITS
SPLIT = (0,)
AHEAD = (2, 1, 3)
SCALE = HD ** (-0.5)

beta_first = 0.9
beta_second = 0.95
learning = 0.01
decay_rate = 0.1
adam_eps = 1e-08
code_eps = 1e-06
correct_first = 1.0 - 0.9**10
correct_second = 1.0 - 0.95**10

F32 = jnp.float32
BF16 = jnp.bfloat16
NT = (((1,), (1,)), ((), ()))


def mod(a, n):
    return lax.rem(a + n, n)


def row_chunks():
    return [(c, 128 * c, min(128, ROWS - 128 * c)) for c in range(6)]


def lane_rows(values):
    highest = jnp.max(values, axis=1, keepdims=True)
    out = []
    for c, start, size in row_chunks():
        eye = lax.broadcasted_iota(jnp.int32, (size, 128), 0) == lax.broadcasted_iota(
            jnp.int32, (size, 128), 1
        )
        out.append(
            jnp.max(jnp.where(eye, highest[start : start + size], 0.0), axis=0, keepdims=True)
        )
    out.append(jnp.zeros((2, 128), F32))
    return jnp.concatenate(out, axis=0)


def down(vector, start, size):
    row = vector[pl.ds(start, size)].reshape(1, size)
    if size < 128:
        row = jnp.concatenate([row, jnp.zeros((1, 128 - size), F32)], axis=1)
    return down_rows(row)[:size]


def down_rows(row):
    return jnp.broadcast_to(row, (128, 128)).T


def body(
    q_hbm,
    k_hbm,
    v_hbm,
    g_hbm,
    w_hbm,
    fc_hbm,
    frow_hbm,
    fcol_hbm,
    sc_hbm,
    srow_hbm,
    scol_hbm,
    gq_out,
    nw_out,
    fnew_out,
    snew_out,
    rows_out,
    cols_out,
    q,
    kk,
    vv,
    g,
    w,
    fc,
    sc,
    frow,
    fcol,
    srow,
    scol,
    gt,
    gz,
    wt,
    att,
    prob,
    acct,
    ga_stage,
    ga_in,
    dwacc,
    dw_stage,
    dw_in,
    st,
    y_in,
    zl_in,
    mine,
    cst,
    x_in,
    zh_in,
    in_sem,
    spread_send,
    relay_send,
    far_recv,
    near_recv,
    ring_send,
    ring_recv,
    beside_send,
    beside_recv,
    shared_recv,
    core_send,
    core_recv,
    att_send,
    att_recv,
    w_send,
    w_recv,
    ga_send,
    ga_recv,
    dw_send,
    dw_recv,
    y_send,
    y_recv,
    zl_send,
    zl_recv,
    x_send,
    x_recv,
    zh_send,
    zh_recv,
):
    x, zh, y, zl, k = (lax.axis_index(a) for a in AXES)
    t = 8 * y + 2 * zl + k
    pair = lax.div(y, 2)

    def rcopy(src, dst, send, recv, **dev):
        return pltpu.make_async_remote_copy(
            src_ref=src, dst_ref=dst, send_sem=send, recv_sem=recv, device_id=dev, device_id_type=MESH
        )

    def came(ref, recv):
        rcopy(ref, ref, core_send, recv, core=k).wait_recv()

    def sequence_of(source, plane):
        return jnp.where(source == plane, 0, source + (source < plane).astype(jnp.int32))

    def other(sequence):
        return sequence - 1 + (sequence - 1 >= zh).astype(jnp.int32)

    barrier = pltpu.get_barrier_semaphore()

    def greet(**dev):
        pl.semaphore_signal(barrier, inc=1, device_id=dev, device_id_type=MESH)

    for dz in (1, 2):
        greet(zh=mod(zh + dz, NZH))
    for dx in range(1, NX):
        greet(x=mod(x + dx, NX))
    for dy in range(1, NY):
        greet(y=mod(y + dy, NY))
    for rel in range(1, NZL * NC):
        greet(zl=mod(zl + rel // NC, NZL), core=lax.rem(k + rel % NC, NC))
    heads = pl.ds(pl.multiple_of(y * HD, HD), HD)
    loads = [
        pltpu.make_async_copy(src, dst, in_sem.at[i])
        for i, (src, dst) in enumerate(
            [
                (g_hbm, g),
                (q_hbm, q),
                (k_hbm.at[:, heads], kk),
                (v_hbm.at[:, heads], vv),
                (w_hbm, w),
                (fc_hbm, fc),
                (sc_hbm, sc),
                (frow_hbm, frow),
                (fcol_hbm, fcol),
                (srow_hbm, srow),
                (scol_hbm, scol),
            ]
        )
    ]
    for load in loads:
        load.start()

    turned = (
        (2 * x + NY - 1 + (zh == 2).astype(jnp.int32)) & (NY - 1),
        jnp.int32(0),
        (2 * x + 1 + (zh > 0).astype(jnp.int32)) & (NY - 1),
        jnp.int32(0),
    )

    def seat(slot, column):
        return (column + NY - turned[slot]) & (NY - 1)

    homes = [2 * seat(slot, y) + k for slot in range(SLOTS)]
    side = zl & 1

    def rows_of(u):
        return pl.ds(pl.multiple_of(UNIT * u, UNIT), UNIT)

    def ahead_of(turn):
        return jnp.where(turn == 0, 2, 2 * turn - 1)

    def slot_and_index(ahead, sequence):
        turn = jnp.where(ahead == 2, 0, lax.shift_right_logical(ahead + 1, 1))
        pair = 2 * turn + sequence - 1
        far = (pair >= 3).astype(jnp.int32)
        slot = jnp.where(ahead == 0, 3, jnp.where(sequence == 0, 0, 1 + far))
        index = jnp.where(
            ahead == 0,
            sequence - 1 + 3 * (sequence == 0).astype(jnp.int32),
            jnp.where(sequence == 0, turn, pair - 3 * far),
        )
        return slot, index

    units = []
    for slot in range(SLOTS):
        first_index = lax.div(8 * homes[slot], UNITS)
        first_place = 8 * homes[slot] - UNITS * first_index
        has_last = homes[slot] == HOMES - 1
        blocks = []
        for index in (first_index, first_index + 1):
            if slot == 0:
                xd, z = (x + ahead_of(index)) & 3, zh
            elif slot == 3:
                xd, z = x, jnp.where(index == 2, zh, other(index + 1))
            else:
                turn = 3 * (slot - 1) + index
                xd = (x + ahead_of(lax.shift_right_logical(turn, 1))) & 3
                z = other(1 + (turn & 1))
            blocks.append((z, UNITS * (NZH * xd + zh)))
        held = []
        for j in range(9):
            over = first_place + j >= UNITS
            z, start = (jnp.where(over, b, a) for a, b in zip(*blocks))
            unit = start + first_place + j - jnp.where(over, UNITS, 0)
            column = lax.shift_right_logical(unit, 3)
            line = lax.shift_right_logical(column, 1) & 3
            there = unit < ALL_UNITS
            if j == 8:
                there = there & has_last
            if slot in SPLIT:
                taken = side == min(j // 4, 1)
                there = there & taken
                here = (line & 2) == (zl & 2)
            else:
                here = (line ^ (2 * (unit & 1))) == zl
            source = dict(zh=z, y=lax.shift_right_logical(column, 3), zl=line, core=column & 1)
            held.append((there, there & here, source, (z == zh) & (column == t), unit))
        units.append(held)

    for held in units:
        for _, lands, source, same, _ in held:
            pl.when(lands & jnp.logical_not(same))(functools.partial(greet, **source))

    def count(flags):
        return sum(f.astype(jnp.int32) for f in flags)

    landing = [count(lands for _, lands, _, _, _ in held) for held in units]
    coming = [count(there for there, _, _, _, _ in held) - n for held, n in zip(units, landing)]
    staying = [count(lands & same for _, lands, _, same, _ in held) for held in units]
    greeted = 8 - sum(staying) + 2 + 3 + 7 + 7

    first_owner = lax.div(8 * t, UNITS)
    first_row = 8 * t - UNITS * first_owner
    turnover = UNITS - first_row
    sides = []

    def turn_of(slot, zd):
        first = 2 * x + NY - 1 + (zd == 2).astype(jnp.int32)
        third = 2 * x + 1 + (zd > 0).astype(jnp.int32)
        return jnp.where(slot == 0, first, jnp.where(slot == 2, third, 0))

    for owner in (first_owner, first_owner + 1):
        xd = lax.div(owner, NZH)
        zd = owner - NZH * xd
        slot, index = slot_and_index(mod(xd - x, NX), sequence_of(zh, zd))
        sides.append((zd, slot, UNITS * index, turn_of(slot, zd)))

    def goes_to(u):
        over = u >= turnover
        zd, slot, start, turn = (jnp.where(over, b, a) for a, b in zip(*sides))
        e = start + first_row + u - jnp.where(over, UNITS, 0)
        h = jnp.minimum(lax.shift_right_logical(e, 3), HOMES - 1)
        line = zl ^ (2 * (u & 1))
        for split in SPLIT:
            shared = (zl & 2) + (e - 8 * h >= 4).astype(jnp.int32)
            line = jnp.where(slot == split, shared, line)
        home = dict(zh=zd, y=(lax.shift_right_logical(h, 1) + turn) & (NY - 1), zl=line, core=h & 1)
        here = (zd == zh) & (home["y"] == y) & (home["core"] == k) & (home["zl"] == zl)
        return slot, SLOT * slot + e, home, here

    loads[0].wait()
    gt[...] = g[...].T

    pl.semaphore_wait(barrier, greeted)

    def spread(u, carry):
        slot, place, home, here = goes_to(u)

        @pl.when(here)
        def _():
            gz[place] = gt[rows_of(u), :]

        @pl.when(jnp.logical_not(here))
        def _():
            rcopy(gt.at[rows_of(u), :], gz.at[place], spread_send, far_recv.at[slot], **home).start()

        return carry

    lax.fori_loop(0, 8, spread, 0)

    loads[4].wait()
    wt[3] = w[...].astype(BF16).T
    for dx in (1, 3, 2):
        rcopy(wt.at[3], wt.at[AHEAD.index(NX - dx)], w_send, w_recv, x=mod(x + dx, NX)).start()

    for i in (1, 2, 3):
        loads[i].wait()
    for i in range(3):
        rows, cols = pl.ds(128 * i, 128), pl.ds(0, 128 * (i + 1))
        scores = (
            lax.dot_general(q[rows, :], kk[cols, :], NT, preferred_element_type=F32) * SCALE
        )
        future = lax.broadcasted_iota(jnp.int32, scores.shape, 1) > (
            lax.broadcasted_iota(jnp.int32, scores.shape, 0) + 128 * i
        )
        scores = jnp.where(future, -1e30, scores)
        exponent = jnp.exp(scores - jnp.max(scores, axis=-1, keepdims=True))
        probabilities = exponent / jnp.sum(exponent, axis=-1, keepdims=True)
        prob[rows, cols] = probabilities
        att[0, rows, :] = jnp.dot(
            probabilities.astype(BF16), vv[cols, :], preferred_element_type=F32
        ).astype(BF16)

    for slot, held in enumerate(units):
        for j, (_, _, _, _, unit) in enumerate(held):
            missing = unit >= ALL_UNITS
            if j == 8:
                missing = missing & (homes[slot] == HOMES - 1)
            if slot in SPLIT:
                missing = missing & (side == min(j // 4, 1))

            @pl.when(missing)
            def _():
                gz[SLOT * slot + 8 * homes[slot] + j] = jnp.zeros((UNIT, SEQ), BF16)

    def send_att():
        for sequence in (1, 2):
            o = other(sequence)
            there = sequence_of(zh, o)
            rcopy(att.at[0], att.at[there], att_send, att_recv.at[there - 1], zh=o).start()

    def wait_units(n, most, wait):
        for c in range(1, most + 1):
            pl.when(n == c)(functools.partial(wait, c))

    def units_came(recv, c):
        came(gz.at[0:c], recv)

    def relay(slot):
        wait_units(
            landing[slot] - staying[slot], 9, functools.partial(units_came, far_recv.at[slot])
        )

        for j, (_, lands, _, _, _) in enumerate(units[slot]):
            piece = gz.at[SLOT * slot + 8 * homes[slot] + j]

            @pl.when(lands)
            def _():
                for dl in (2,) if slot in SPLIT else (1, 2, 3):
                    rcopy(
                        piece, piece, relay_send.at[slot], near_recv.at[slot], zl=mod(zl + dl, NZL)
                    ).start()

    def parts(slot):
        return (0, 1) if slot == SLOTS - 1 else (0,)

    def reach(way, slot):
        return 4 if way == slot % 2 else 3

    def from_source(way, hops):
        return mod(y - hops, NY) if way == 0 else mod(y + hops, NY)

    def parts_of(slot, source, core):
        start = SLOT * slot + 8 * (2 * seat(slot, source) + core)
        last = (seat(slot, source) == NY - 1) & (core == 1)
        if slot in SPLIT:
            longer = last & (side == 1)
            start = start + 4 * side
            return (((start, 4, jnp.logical_not(longer)), (start, 5, longer)),)
        if len(parts(slot)) == 1:
            return (((start, 8, jnp.logical_not(last)), (start, 9, last)),)
        return (
            ((start, 4, None),),
            ((start + 4, 4, jnp.logical_not(last)), (start + 4, 5, last)),
        )

    def each_size(sizes, act):
        for start, units, when in sizes:
            ref = gz.at[pl.ds(start, units)]
            if when is None:
                act(ref)
            else:
                pl.when(when)(functools.partial(act, ref))

    def forward(way, slot, hops, part):
        def go(piece):
            rcopy(
                piece,
                piece,
                ring_send,
                ring_recv.at[way, slot + part, hops],
                y=mod(y + 1, NY) if way == 0 else mod(y - 1, NY),
            ).start()

        each_size(parts_of(slot, from_source(way, hops), k)[part], go)

    def to_partner(way, slot, hops, part):
        def go(piece):
            rcopy(piece, piece, core_send, core_recv.at[slot, hops // 4], core=1 - k).start()

        each_size(parts_of(slot, from_source(way, hops), k)[part], go)

    def to_beside(way, slot, hops):
        def go(piece):
            rcopy(piece, piece, beside_send, beside_recv.at[SPLIT.index(slot)], zl=zl ^ 1).start()

        if slot in SPLIT:
            each_size(parts_of(slot, from_source(way, hops), k)[0], go)

    def start_ring(slot):
        wait_units(coming[slot], 9, functools.partial(units_came, near_recv.at[slot]))
        for part in parts(slot):
            for way in (0, 1):
                forward(way, slot, 0, part)
        to_beside(0, slot, 0)
        for part in parts(slot):
            to_partner(0, slot, 0, part)

    def pass_on(slot, hops):
        for part in parts(slot):
            for way in (0, 1):
                if hops <= reach(way, slot):
                    each_size(
                        parts_of(slot, from_source(way, hops), k)[part],
                        lambda piece: came(piece, ring_recv.at[way, slot + part, hops - 1]),
                    )
                    if hops < reach(way, slot):
                        forward(way, slot, hops, part)
                    to_beside(way, slot, hops)
                    to_partner(way, slot, hops, part)

    def beside_came(slot):
        longer = (k == 1) & (side == 0)
        pl.when(longer)(functools.partial(came, gz.at[0:33], beside_recv.at[SPLIT.index(slot)]))
        pl.when(jnp.logical_not(longer))(functools.partial(came, gz.at[0:32], beside_recv.at[SPLIT.index(slot)]))
        for source in range(NY):
            start = SLOT * slot + 8 * (2 * source + k) + 4 * (1 - side)

            def go(units):
                piece = gz.at[pl.ds(start, units)]
                rcopy(piece, piece, core_send, shared_recv.at[SPLIT.index(slot)], core=1 - k).start()

            if source < NY - 1:
                go(4)
            else:
                pl.when(longer)(functools.partial(go, 5))
                pl.when(jnp.logical_not(longer))(functools.partial(go, 4))

    def partner_beside(slot):
        longer = (k == 0) & (side == 0)
        pl.when(longer)(functools.partial(came, gz.at[0:33], shared_recv.at[SPLIT.index(slot)]))
        pl.when(jnp.logical_not(longer))(functools.partial(came, gz.at[0:32], shared_recv.at[SPLIT.index(slot)]))

    def partner_near(slot):
        more = (k == 0) & (seat(slot, y) != NY // 2 - 1)
        each = 8
        if slot in SPLIT:
            more, each = more & (side == 1), 4
        pl.when(more)(functools.partial(came, gz.at[0 : 7 * each + 1], core_recv.at[slot, 0]))
        pl.when(jnp.logical_not(more))(functools.partial(came, gz.at[0 : 7 * each], core_recv.at[slot, 0]))

    def partner_across(slot):
        more = (k == 0) & (seat(slot, y) == NY // 2 - 1)
        each = 8
        if slot in SPLIT:
            more, each = more & (side == 1), 4
        pl.when(more)(functools.partial(came, gz.at[0 : each + 1], core_recv.at[slot, 1]))
        pl.when(jnp.logical_not(more))(functools.partial(came, gz.at[0:each], core_recv.at[slot, 1]))

    def partner_has(slot):
        partner_near(slot)
        partner_across(slot)

    def member(slot, index):
        if slot == 0:
            return index, 0
        turn = 3 * (slot - 1) + index
        return turn // 2, 1 + turn % 2

    started = {("g", 0)}

    def add_to(ref, key, term):
        ref[...] = ref[...] + term if key in started else term
        started.add(key)

    def side_by_side(slot, indices):
        blocks = [gz[pl.ds(SLOT * slot + UNITS * i, UNITS)].reshape(ROWS, SEQ) for i in indices]
        return jnp.concatenate(blocks, axis=1) if len(blocks) > 1 else blocks[0]

    def one_below_another(sequences):
        parts = [att[s] for s in sequences]
        return jnp.concatenate(parts, axis=0) if len(parts) > 1 else parts[0]

    def weight_term(slot, *indices):
        members = [member(slot, i) for i in indices]
        rows = members[0][0]
        term = jnp.dot(
            side_by_side(slot, indices),
            one_below_another([sequence for _, sequence in members]),
            preferred_element_type=F32,
        )
        add_to(dwacc.at[rows], ("w", rows), term)

    def multiply(slot, *indices):
        members = [member(slot, i) for i in indices]
        term = jnp.dot(wt[members[0][0]], side_by_side(slot, indices), preferred_element_type=F32)
        for i, (_, sequence) in enumerate(members):
            add_to(acct.at[sequence], ("g", sequence), term[:, SEQ * i : SEQ * (i + 1)])

    early = jnp.where(lax.rem(y + NY // 2, NY) <= 2, 2, 0)
    last_blocks = (early, jnp.where(early == 2, 0, 1), jnp.where(early == 2, 1, 2))

    def last_term(*turns):
        indices = [last_blocks[turn] for turn in turns]
        term = jnp.dot(
            side_by_side(SLOTS - 1, indices),
            one_below_another([lax.rem(i + 1, NZH) for i in indices]),
            preferred_element_type=F32,
        )
        add_to(dwacc.at[3], ("w", 3), term)

    def last_multiply(*turns):
        indices = [last_blocks[turn] for turn in turns]
        term = jnp.dot(wt[3], side_by_side(SLOTS - 1, indices), preferred_element_type=F32)
        for i, index in enumerate(indices):
            sequence = lax.rem(index + 1, NZH)
            acct[sequence] = acct[sequence] + term[:, SEQ * i : SEQ * (i + 1)]

    def send_term(rows):
        for start, size in ((0, 352), (352, ROWS - 352)):
            part = pl.ds(start, size)
            dw_stage[rows, part, :] = dwacc[rows, part, :].astype(BF16)
            rcopy(
                dw_stage.at[rows, part],
                dw_in.at[rows, part],
                dw_send,
                dw_recv,
                x=mod(x + AHEAD[rows], NX),
            ).start()

    def send_grad(sequence, i):
        o = other(sequence)
        ga_stage[sequence - 1, i] = acct[sequence, :, 128 * i : 128 * (i + 1)].astype(BF16)
        rcopy(
            ga_stage.at[sequence - 1, i],
            ga_in.at[sequence_of(zh, o) - 1, i],
            ga_send,
            ga_recv.at[i],
            zh=o,
        ).start()

    def send_grads(*sequences):
        for i in range(3):
            for sequence in sequences:
                send_grad(sequence, i)

    def old_moments():
        acct[0] = jnp.zeros((HD, SEQ), F32)
        for load in loads[5:]:
            load.wait()
        for c, start, size in row_chunks():
            rows = pl.ds(start, size)
            low_first = jnp.minimum(down(frow, start, size), fcol[...].reshape(1, HD))
            low_second = jnp.minimum(down(srow, start, size), scol[...].reshape(1, HD))
            fnew_out[rows, :] = beta_first * (fc[rows, :].astype(F32) * low_first)
            snew_out[rows, :] = beta_second * (sc[rows, :].astype(F32) * low_second)
            weight = w[rows, :]
            nw_out[rows, :] = weight - learning * (decay_rate * weight)

    relay(0)
    start_ring(0)
    relay(1)
    relay(2)
    relay(3)
    pass_on(0, 1)
    start_ring(1)
    pass_on(0, 2)
    pass_on(1, 1)
    start_ring(2)
    send_att()
    pass_on(0, 3)
    pass_on(1, 2)
    pass_on(2, 1)
    start_ring(3)
    pass_on(0, 4)
    pass_on(1, 3)
    pass_on(2, 2)
    old_moments()
    pass_on(3, 1)
    pass_on(1, 4)
    beside_came(0)
    pass_on(2, 3)
    pass_on(3, 2)
    partner_has(1)
    came(att.at[1], att_recv.at[0])
    came(att.at[2], att_recv.at[1])
    weight_term(1, 0, 1)
    partner_has(0)
    partner_beside(0)
    weight_term(0, 0)
    send_term(0)
    pass_on(2, 4)
    weight_term(1, 2)
    weight_term(0, 2)
    pass_on(3, 3)
    weight_term(0, 1)
    partner_has(2)
    weight_term(2, 0)
    send_term(1)
    weight_term(2, 1, 2)
    send_term(2)
    came(wt.at[0:3], w_recv)
    multiply(1, 0, 1)
    multiply(1, 2)
    partner_near(3)
    pass_on(3, 4)
    multiply(2, 0)
    multiply(2, 1, 2)
    last_multiply(0)
    pl.when(early == 0)(functools.partial(send_grads, 1))
    last_term(0)
    partner_across(3)
    last_multiply(1)
    pl.when(early == 0)(functools.partial(send_grads, 2))
    pl.when(early == 2)(functools.partial(send_grads, 1))
    last_multiply(2)
    pl.when(early == 2)(functools.partial(send_grads, 2))
    last_term(1, 2)

    came(dw_in, dw_recv)
    for c, start, size in row_chunks():
        rows = pl.ds(start, size)
        grad = dwacc[3, rows, :]
        for i in range(NX - 1):
            grad = grad + dw_in[i, rows, :].astype(F32)
        first_new = fnew_out[rows, :] + (1.0 - beta_first) * grad
        second_new = snew_out[rows, :] + (1.0 - beta_second) * grad * grad
        step_size = (
            first_new * (1.0 / correct_first) / (jnp.sqrt(second_new * (1.0 / correct_second)) + adam_eps)
        )
        nw_out[rows, :] = nw_out[rows, :] - learning * step_size
        fnew_out[rows, :] = first_new
        snew_out[rows, :] = second_new

    first_abs, second_abs = jnp.abs(fnew_out[...]), jnp.abs(snew_out[...])
    st[0] = lane_rows(first_abs)
    st[1] = lane_rows(second_abs)
    for dy in range(1, NY):
        rcopy(st, y_in.at[NY - dy - 1], y_send, y_recv, y=mod(y + dy, NY)).start()
    cst[0, 0:1, :] = jnp.max(first_abs, axis=0, keepdims=True)
    cst[0, 1:2, :] = jnp.max(second_abs, axis=0, keepdims=True)
    for dx in range(1, NX):
        rcopy(cst.at[0], x_in.at[NX - dx - 1], x_send, x_recv, x=mod(x + dx, NX)).start()

    multiply(0, 0)
    multiply(0, 1)
    multiply(0, 2)

    def back_rows(i):
        rows, cols = pl.ds(128 * i, 128), pl.ds(0, 128 * (i + 1))
        came(ga_in.at[:, i], ga_recv.at[i])
        total = acct[0, :, rows]
        for s in range(2):
            total = total + ga_in[s, i].astype(F32)
        grad_half = total.astype(BF16).T
        grad_probs = lax.dot_general(grad_half, vv[cols, :], NT, preferred_element_type=F32)
        row_dot = jnp.sum(
            grad_half.astype(F32) * att[0, rows, :].astype(F32), axis=-1, keepdims=True
        )
        grad_scores = (prob[rows, cols] * (grad_probs - row_dot)).astype(BF16)
        gq_out[rows, :] = (
            jnp.dot(grad_scores, kk[cols, :], preferred_element_type=F32) * SCALE
        ).astype(BF16)

    def left(ref, send):
        rcopy(ref, ref, send, zh_recv, core=k).wait_send()

    wait_units(8 - sum(staying), 8, lambda c: left(gz.at[0:c], spread_send))
    for slot in range(SLOTS):
        copies = 1 if slot in SPLIT else 3
        wait_units(landing[slot], 9, lambda c: left(gz.at[0 : copies * c], relay_send.at[slot]))
    longer = count(
        (seat(slot, from_source(way, hops)) == NY - 1) & (k == 1) & ((side == 1) | (slot not in SPLIT))
        for slot in range(SLOTS)
        for way in (0, 1)
        for hops in range(reach(way, slot))
    )
    usual = 56 * SLOTS - 28 * len(SPLIT)
    for c in range(9):
        pl.when(longer == c)(functools.partial(left, gz.at[0 : usual + c], ring_send))
    more = (k == 1) & (side == 1)
    for flag, each in ((more, 33), (jnp.logical_not(more), 32)):
        pl.when(flag)(functools.partial(left, gz.at[0 : each * len(SPLIT)], beside_send))
    for c in (0, 1):
        pl.when(k == c)(functools.partial(left, gz.at[0 : 64 * SLOTS + SLOTS * c], core_send))
    for whole, send in (
        (att.at[0:2], att_send),
        (wt.at[0:3], w_send),
        (dw_in, dw_send),
    ):
        left(whole, send)

    came(x_in, x_recv)
    cst[1] = jnp.maximum(cst[0], jnp.max(x_in[...], axis=0))
    for sequence in (1, 2):
        o = other(sequence)
        rcopy(cst.at[1], zh_in.at[sequence_of(zh, o) - 1], zh_send, zh_recv, zh=o).start()
    came(y_in, y_recv)
    mine[...] = jnp.maximum(st[...], jnp.max(y_in[...], axis=0))
    for rel in range(1, NZL * NC):
        dl, dk = rel // NC, rel % NC
        back = NC * ((NZL - dl) % NZL) + dk - 1
        rcopy(
            mine, zl_in.at[back], zl_send, zl_recv, zl=mod(zl + dl, NZL), core=lax.rem(k + dk, NC)
        ).start()
    for i in range(3):
        back_rows(i)
    came(zl_in, zl_recv)
    rows_out[...] = jnp.maximum(mine[...], jnp.max(zl_in[...], axis=0))
    came(zh_in, zh_recv)
    cols_out[...] = jnp.maximum(cst[1], jnp.max(zh_in[...], axis=0))

    for whole, send in (
        (ga_in, ga_send),
        (y_in, y_send),
        (zl_in, zl_send),
        (x_in, x_send),
        (zh_in, zh_send),
    ):
        left(whole, send)


def codes(
    gq,
    nw,
    fnew,
    snew,
    rows,
    cols,
    gq_out,
    nw_out,
    nfc_out,
    nfr_out,
    nfcol_out,
    nsc_out,
    nsr_out,
    nscol_out,
    first_code,
    second_code,
    first_rows,
    second_rows,
    first_cols,
    second_cols,
    sem,
):
    copies = []

    def out(src, dst):
        copy = pltpu.make_async_copy(src, dst, sem.at[len(copies)])
        copy.start()
        copies.append(copy)

    out(gq, gq_out)
    out(nw, nw_out)
    for moment, (new, code, code_out, maxima, maxima_out, col, col_out) in enumerate(
        (
            (fnew, first_code, nfc_out, first_rows, nfr_out, first_cols, nfcol_out),
            (snew, second_code, nsc_out, second_rows, nsr_out, second_cols, nscol_out),
        )
    ):
        col[...] = cols[moment]
        for c, start, size in row_chunks():
            at = pl.ds(start, size)
            maxima[at] = rows[moment, c, 0:size]
            low = jnp.minimum(
                down_rows(rows[moment, c : c + 1, :])[:size], cols[moment : moment + 1]
            )
            code[at, :] = (new[at, :] / (low + code_eps)).astype(BF16)
        out(code, code_out)
        out(maxima, maxima_out)
        out(col, col_out)
    for copy in copies:
        copy.wait()


def per_device(queries, keys, values, grad_out, weight, fc, frow, fcol, sc, srow, scol):
    shape = jax.ShapeDtypeStruct
    vmem = pl.BlockSpec(memory_space=pltpu.VMEM)
    hbm = pl.BlockSpec(memory_space=pltpu.HBM)
    dma = pltpu.SemaphoreType.DMA
    gq, nw, fnew, snew, rows, cols = pl.pallas_call(
        body,
        name="whole",
        out_shape=(
            shape((SEQ, HD), BF16),
            shape((ROWS, HD), F32),
            shape((ROWS, HD), F32),
            shape((ROWS, HD), F32),
            shape((2, 8, HD), F32),
            shape((2, HD), F32),
        ),
        in_specs=[hbm] * 11,
        out_specs=[vmem] * 6,
        scratch_shapes=[
            pltpu.VMEM((SEQ, HD), BF16),
            pltpu.VMEM((SEQ, HD), BF16),
            pltpu.VMEM((SEQ, HD), BF16),
            pltpu.VMEM((SEQ, HD), BF16),
            pltpu.VMEM((ROWS, HD), F32),
            pltpu.VMEM((ROWS, HD), BF16),
            pltpu.VMEM((ROWS, HD), BF16),
            pltpu.VMEM((ROWS,), F32),
            pltpu.VMEM((HD,), F32),
            pltpu.VMEM((ROWS,), F32),
            pltpu.VMEM((HD,), F32),
            pltpu.VMEM((HD, SEQ), BF16),
            pltpu.VMEM((SLOTS * SLOT, UNIT, SEQ), BF16),
            pltpu.VMEM((NX, HD, ROWS), BF16),
            pltpu.VMEM((NZH, SEQ, HD), BF16),
            pltpu.VMEM((SEQ, SEQ), F32),
            pltpu.VMEM((NZH, HD, SEQ), F32),
            pltpu.VMEM((2, 3, HD, HD), BF16),
            pltpu.VMEM((2, 3, HD, HD), BF16),
            pltpu.VMEM((NX, ROWS, HD), F32),
            pltpu.VMEM((NX - 1, ROWS, HD), BF16),
            pltpu.VMEM((NX - 1, ROWS, HD), BF16),
            pltpu.VMEM((2, 8, HD), F32),
            pltpu.VMEM((NY - 1, 2, 8, HD), F32),
            pltpu.VMEM((NZL * NC - 1, 2, 8, HD), F32),
            pltpu.VMEM((2, 8, HD), F32),
            pltpu.VMEM((2, 2, HD), F32),
            pltpu.VMEM((NX - 1, 2, HD), F32),
            pltpu.VMEM((NZH - 1, 2, HD), F32),
            dma((11,)),
            dma,
            dma((SLOTS,)),
            dma((SLOTS,)),
            dma((SLOTS,)),
            dma,
            dma((2, SLOTS + 1, 4)),
            dma,
            dma((len(SPLIT),)),
            dma((len(SPLIT),)),
            dma,
            dma((SLOTS, 2)),
            dma,
            dma((2,)),
            dma,
            dma,
            dma,
            dma((3,)),
            dma,
            dma,
            dma,
            dma,
            dma,
            dma,
            dma,
            dma,
            dma,
            dma,
        ],
        compiler_params=pltpu.CompilerParams(
            collective_id=0, has_side_effects=True, vmem_limit_bytes=48 * 1024 * 1024
        ),
    )(
        *(
            pltpu.with_memory_space_constraint(a, pltpu.HBM)
            for a in (queries, keys, values, grad_out, weight, fc, frow, fcol, sc, srow, scol)
        )
    )
    return pl.pallas_call(
        codes,
        name="codes",
        out_shape=(
            shape((SEQ, HD), BF16),
            shape((ROWS, HD), F32),
            shape((ROWS, HD), BF16),
            shape((ROWS,), F32),
            shape((HD,), F32),
            shape((ROWS, HD), BF16),
            shape((ROWS,), F32),
            shape((HD,), F32),
        ),
        compiler_params=pltpu.CompilerParams(vmem_limit_bytes=8 * 1024 * 1024),
        in_specs=[vmem] * 6,
        out_specs=[hbm] * 8,
        scratch_shapes=[
            pltpu.VMEM((ROWS, HD), BF16),
            pltpu.VMEM((ROWS, HD), BF16),
            pltpu.VMEM((ROWS,), F32),
            pltpu.VMEM((ROWS,), F32),
            pltpu.VMEM((HD,), F32),
            pltpu.VMEM((HD,), F32),
            dma((8,)),
        ],
    )(gq, nw, fnew, snew, rows, cols)


def solution(mesh):
    finer = Mesh(mesh.devices.reshape(NX, NZH, NY, NZL, NC), AXES)
    placed = (
        P(DP, TENSOR),
        P(DP, None),
        P(DP, None),
        P(DP, TENSOR),
        P(DP, TENSOR),
        P(DP, TENSOR),
        P(DP),
        P(TENSOR),
        P(DP, TENSOR),
        P(DP),
        P(TENSOR),
    )
    return jax.shard_map(
        per_device,
        mesh=finer,
        in_specs=placed,
        out_specs=(
            P(DP, TENSOR),
            P(DP, TENSOR),
            P(DP, TENSOR),
            P(DP),
            P(TENSOR),
            P(DP, TENSOR),
            P(DP),
            P(TENSOR),
        ),
        check_vma=False,
    )
```

```python
import functools

import jax
import jax.numpy as jnp
from jax import lax
from jax.experimental import pallas as pl
from jax.experimental.pallas import tpu as pltpu
from jax.sharding import Mesh
from jax.sharding import PartitionSpec as P

NX, NZH, NY, NZL, NC = 4, 3, 8, 4, 2
AXES = ("x", "zh", "y", "zl", "core")
DP = ("x", "zh")
TENSOR = ("y", "zl", "core")
MESH = pl.DeviceIdType.MESH

HD = 128
SEQ = 384
ROWS = 688
UNIT = 16
UNITS = ROWS // UNIT
ALL_UNITS = 512
HOMES = NY * NC
SLOTS = 4
SLOT = 3 * UNITS
SPLIT = (0,)
AHEAD = (2, 1, 3)
SCALE = HD ** (-0.5)

beta_first = 0.9
beta_second = 0.95
learning = 0.01
decay_rate = 0.1
adam_eps = 1e-08
code_eps = 1e-06
correct_first = 1.0 - 0.9**10
correct_second = 1.0 - 0.95**10

F32 = jnp.float32
BF16 = jnp.bfloat16
NT = (((1,), (1,)), ((), ()))


def mod(a, n):
    return lax.rem(a + n, n)


def row_chunks():
    return [(c, 128 * c, min(128, ROWS - 128 * c)) for c in range(6)]


def lane_rows(values):
    highest = jnp.max(values, axis=1, keepdims=True)
    out = []
    for c, start, size in row_chunks():
        eye = lax.broadcasted_iota(jnp.int32, (size, 128), 0) == lax.broadcasted_iota(
            jnp.int32, (size, 128), 1
        )
        out.append(
            jnp.max(jnp.where(eye, highest[start : start + size], 0.0), axis=0, keepdims=True)
        )
    out.append(jnp.zeros((2, 128), F32))
    return jnp.concatenate(out, axis=0)


def down(vector, start, size):
    row = vector[pl.ds(start, size)].reshape(1, size)
    if size < 128:
        row = jnp.concatenate([row, jnp.zeros((1, 128 - size), F32)], axis=1)
    return down_rows(row)[:size]


def down_rows(row):
    return jnp.broadcast_to(row, (128, 128)).T


def body(
    q_hbm,
    k_hbm,
    v_hbm,
    g_hbm,
    w_hbm,
    fc_hbm,
    frow_hbm,
    fcol_hbm,
    sc_hbm,
    srow_hbm,
    scol_hbm,
    gq_out,
    nw_out,
    fnew_out,
    snew_out,
    rows_out,
    cols_out,
    q,
    kk,
    vv,
    g,
    w,
    fc,
    sc,
    frow,
    fcol,
    srow,
    scol,
    gt,
    gz,
    wt,
    att,
    prob,
    acct,
    ga_stage,
    ga_in,
    dwacc,
    dw_stage,
    dw_in,
    st,
    y_in,
    zl_in,
    mine,
    cst,
    x_in,
    zh_in,
    in_sem,
    spread_send,
    relay_send,
    far_recv,
    near_recv,
    ring_send,
    ring_recv,
    beside_send,
    beside_recv,
    shared_recv,
    core_send,
    core_recv,
    att_send,
    att_recv,
    w_send,
    w_recv,
    ga_send,
    ga_recv,
    dw_send,
    dw_recv,
    y_send,
    y_recv,
    zl_send,
    zl_recv,
    x_send,
    x_recv,
    zh_send,
    zh_recv,
):
    x, zh, y, zl, k = (lax.axis_index(a) for a in AXES)
    t = 8 * y + 2 * zl + k
    pair = lax.div(y, 2)

    def rcopy(src, dst, send, recv, **dev):
        return pltpu.make_async_remote_copy(
            src_ref=src, dst_ref=dst, send_sem=send, recv_sem=recv, device_id=dev, device_id_type=MESH
        )

    def came(ref, recv):
        rcopy(ref, ref, core_send, recv, core=k).wait_recv()

    def sequence_of(source, plane):
        return jnp.where(source == plane, 0, source + (source < plane).astype(jnp.int32))

    def other(sequence):
        return sequence - 1 + (sequence - 1 >= zh).astype(jnp.int32)

    barrier = pltpu.get_barrier_semaphore()

    def greet(**dev):
        pl.semaphore_signal(barrier, inc=1, device_id=dev, device_id_type=MESH)

    for dz in (1, 2):
        greet(zh=mod(zh + dz, NZH))
    for dx in range(1, NX):
        greet(x=mod(x + dx, NX))
    for dy in range(1, NY):
        greet(y=mod(y + dy, NY))
    for rel in range(1, NZL * NC):
        greet(zl=mod(zl + rel // NC, NZL), core=lax.rem(k + rel % NC, NC))
    heads = pl.ds(pl.multiple_of(y * HD, HD), HD)
    loads = [
        pltpu.make_async_copy(src, dst, in_sem.at[i])
        for i, (src, dst) in enumerate(
            [
                (g_hbm, g),
                (q_hbm, q),
                (k_hbm.at[:, heads], kk),
                (v_hbm.at[:, heads], vv),
                (w_hbm, w),
                (fc_hbm, fc),
                (sc_hbm, sc),
                (frow_hbm, frow),
                (fcol_hbm, fcol),
                (srow_hbm, srow),
                (scol_hbm, scol),
            ]
        )
    ]
    for load in loads:
        load.start()

    turned = (
        (2 * x + NY - 1 + (zh == 2).astype(jnp.int32)) & (NY - 1),
        jnp.int32(0),
        (2 * x + 1 + (zh > 0).astype(jnp.int32)) & (NY - 1),
        jnp.int32(0),
    )

    def seat(slot, column):
        return (column + NY - turned[slot]) & (NY - 1)

    homes = [2 * seat(slot, y) + k for slot in range(SLOTS)]
    side = zl & 1

    def rows_of(u):
        return pl.ds(pl.multiple_of(UNIT * u, UNIT), UNIT)

    def ahead_of(turn):
        return jnp.where(turn == 0, 2, 2 * turn - 1)

    def slot_and_index(ahead, sequence):
        turn = jnp.where(ahead == 2, 0, lax.shift_right_logical(ahead + 1, 1))
        pair = 2 * turn + sequence - 1
        far = (pair >= 3).astype(jnp.int32)
        slot = jnp.where(ahead == 0, 3, jnp.where(sequence == 0, 0, 1 + far))
        index = jnp.where(
            ahead == 0,
            sequence - 1 + 3 * (sequence == 0).astype(jnp.int32),
            jnp.where(sequence == 0, turn, pair - 3 * far),
        )
        return slot, index

    units = []
    for slot in range(SLOTS):
        first_index = lax.div(8 * homes[slot], UNITS)
        first_place = 8 * homes[slot] - UNITS * first_index
        has_last = homes[slot] == HOMES - 1
        blocks = []
        for index in (first_index, first_index + 1):
            if slot == 0:
                xd, z = (x + ahead_of(index)) & 3, zh
            elif slot == 3:
                xd, z = x, jnp.where(index == 2, zh, other(index + 1))
            else:
                turn = 3 * (slot - 1) + index
                xd = (x + ahead_of(lax.shift_right_logical(turn, 1))) & 3
                z = other(1 + (turn & 1))
            blocks.append((z, UNITS * (NZH * xd + zh)))
        held = []
        for j in range(9):
            over = first_place + j >= UNITS
            z, start = (jnp.where(over, b, a) for a, b in zip(*blocks))
            unit = start + first_place + j - jnp.where(over, UNITS, 0)
            column = lax.shift_right_logical(unit, 3)
            line = lax.shift_right_logical(column, 1) & 3
            there = unit < ALL_UNITS
            if j == 8:
                there = there & has_last
            if slot in SPLIT:
                taken = side == min(j // 4, 1)
                there = there & taken
                here = (line & 2) == (zl & 2)
            else:
                here = (line ^ (2 * (unit & 1))) == zl
            source = dict(zh=z, y=lax.shift_right_logical(column, 3), zl=line, core=column & 1)
            held.append((there, there & here, source, (z == zh) & (column == t), unit))
        units.append(held)

    for held in units:
        for _, lands, source, same, _ in held:
            pl.when(lands & jnp.logical_not(same))(functools.partial(greet, **source))

    def count(flags):
        return sum(f.astype(jnp.int32) for f in flags)

    landing = [count(lands for _, lands, _, _, _ in held) for held in units]
    coming = [count(there for there, _, _, _, _ in held) - n for held, n in zip(units, landing)]
    staying = [count(lands & same for _, lands, _, same, _ in held) for held in units]
    greeted = 8 - sum(staying) + 2 + 3 + 7 + 7

    first_owner = lax.div(8 * t, UNITS)
    first_row = 8 * t - UNITS * first_owner
    turnover = UNITS - first_row
    sides = []

    def turn_of(slot, zd):
        first = 2 * x + NY - 1 + (zd == 2).astype(jnp.int32)
        third = 2 * x + 1 + (zd > 0).astype(jnp.int32)
        return jnp.where(slot == 0, first, jnp.where(slot == 2, third, 0))

    for owner in (first_owner, first_owner + 1):
        xd = lax.div(owner, NZH)
        zd = owner - NZH * xd
        slot, index = slot_and_index(mod(xd - x, NX), sequence_of(zh, zd))
        sides.append((zd, slot, UNITS * index, turn_of(slot, zd)))

    def goes_to(u):
        over = u >= turnover
        zd, slot, start, turn = (jnp.where(over, b, a) for a, b in zip(*sides))
        e = start + first_row + u - jnp.where(over, UNITS, 0)
        h = jnp.minimum(lax.shift_right_logical(e, 3), HOMES - 1)
        line = zl ^ (2 * (u & 1))
        for split in SPLIT:
            shared = (zl & 2) + (e - 8 * h >= 4).astype(jnp.int32)
            line = jnp.where(slot == split, shared, line)
        home = dict(zh=zd, y=(lax.shift_right_logical(h, 1) + turn) & (NY - 1), zl=line, core=h & 1)
        here = (zd == zh) & (home["y"] == y) & (home["core"] == k) & (home["zl"] == zl)
        return slot, SLOT * slot + e, home, here

    loads[0].wait()
    gt[...] = g[...].T

    pl.semaphore_wait(barrier, greeted)

    def spread(u, carry):
        slot, place, home, here = goes_to(u)

        @pl.when(here)
        def _():
            gz[place] = gt[rows_of(u), :]

        @pl.when(jnp.logical_not(here))
        def _():
            rcopy(gt.at[rows_of(u), :], gz.at[place], spread_send, far_recv.at[slot], **home).start()

        return carry

    lax.fori_loop(0, 8, spread, 0)

    def send_weights():
        loads[4].wait()
        wt[3] = w[...].astype(BF16).T
        for dx in (1, 3, 2):
            rcopy(wt.at[3], wt.at[AHEAD.index(NX - dx)], w_send, w_recv, x=mod(x + dx, NX)).start()

    def attend():
        for i in (1, 2, 3):
            loads[i].wait()
        for i in range(3):
            rows, cols = pl.ds(128 * i, 128), pl.ds(0, 128 * (i + 1))
            scores = (
                lax.dot_general(q[rows, :], kk[cols, :], NT, preferred_element_type=F32) * SCALE
            )
            future = lax.broadcasted_iota(jnp.int32, scores.shape, 1) > (
                lax.broadcasted_iota(jnp.int32, scores.shape, 0) + 128 * i
            )
            scores = jnp.where(future, -1e30, scores)
            exponent = jnp.exp(scores - jnp.max(scores, axis=-1, keepdims=True))
            probabilities = exponent / jnp.sum(exponent, axis=-1, keepdims=True)
            prob[rows, cols] = probabilities
            att[0, rows, :] = jnp.dot(
                probabilities.astype(BF16), vv[cols, :], preferred_element_type=F32
            ).astype(BF16)

    def fill():
        for slot, held in enumerate(units):
            for j, (_, _, _, _, unit) in enumerate(held):
                missing = unit >= ALL_UNITS
                if j == 8:
                    missing = missing & (homes[slot] == HOMES - 1)
                if slot in SPLIT:
                    missing = missing & (side == min(j // 4, 1))

                @pl.when(missing)
                def _():
                    gz[SLOT * slot + 8 * homes[slot] + j] = jnp.zeros((UNIT, SEQ), BF16)

    def send_att():
        for sequence in (1, 2):
            o = other(sequence)
            there = sequence_of(zh, o)
            rcopy(att.at[0], att.at[there], att_send, att_recv.at[there - 1], zh=o).start()

    def wait_units(n, most, wait):
        for c in range(1, most + 1):
            pl.when(n == c)(functools.partial(wait, c))

    def units_came(recv, c):
        came(gz.at[0:c], recv)

    def relay(slot):
        wait_units(
            landing[slot] - staying[slot], 9, functools.partial(units_came, far_recv.at[slot])
        )

        for j, (_, lands, _, _, _) in enumerate(units[slot]):
            piece = gz.at[SLOT * slot + 8 * homes[slot] + j]

            @pl.when(lands)
            def _():
                for dl in (2,) if slot in SPLIT else (1, 2, 3):
                    rcopy(
                        piece, piece, relay_send.at[slot], near_recv.at[slot], zl=mod(zl + dl, NZL)
                    ).start()

    def parts(slot):
        return (0, 1) if slot == SLOTS - 1 else (0,)

    def reach(way, slot):
        return 4 if way == slot % 2 else 3

    def from_source(way, hops):
        return mod(y - hops, NY) if way == 0 else mod(y + hops, NY)

    def parts_of(slot, source, core):
        start = SLOT * slot + 8 * (2 * seat(slot, source) + core)
        last = (seat(slot, source) == NY - 1) & (core == 1)
        if slot in SPLIT:
            longer = last & (side == 1)
            start = start + 4 * side
            return (((start, 4, jnp.logical_not(longer)), (start, 5, longer)),)
        if len(parts(slot)) == 1:
            return (((start, 8, jnp.logical_not(last)), (start, 9, last)),)
        return (
            ((start, 4, None),),
            ((start + 4, 4, jnp.logical_not(last)), (start + 4, 5, last)),
        )

    def each_size(sizes, act):
        for start, units, when in sizes:
            ref = gz.at[pl.ds(start, units)]
            if when is None:
                act(ref)
            else:
                pl.when(when)(functools.partial(act, ref))

    def forward(way, slot, hops, part):
        def go(piece):
            rcopy(
                piece,
                piece,
                ring_send,
                ring_recv.at[way, slot + part, hops],
                y=mod(y + 1, NY) if way == 0 else mod(y - 1, NY),
            ).start()

        each_size(parts_of(slot, from_source(way, hops), k)[part], go)

    def to_partner(way, slot, hops, part):
        def go(piece):
            rcopy(piece, piece, core_send, core_recv.at[slot, hops // 4], core=1 - k).start()

        each_size(parts_of(slot, from_source(way, hops), k)[part], go)

    def to_beside(way, slot, hops):
        def go(piece):
            rcopy(piece, piece, beside_send, beside_recv.at[SPLIT.index(slot)], zl=zl ^ 1).start()

        if slot in SPLIT:
            each_size(parts_of(slot, from_source(way, hops), k)[0], go)

    def start_ring(slot):
        wait_units(coming[slot], 9, functools.partial(units_came, near_recv.at[slot]))
        for part in parts(slot):
            for way in (0, 1):
                forward(way, slot, 0, part)
        to_beside(0, slot, 0)
        for part in parts(slot):
            to_partner(0, slot, 0, part)

    def pass_on(slot, hops):
        for part in parts(slot):
            for way in (0, 1):
                if hops <= reach(way, slot):
                    each_size(
                        parts_of(slot, from_source(way, hops), k)[part],
                        lambda piece: came(piece, ring_recv.at[way, slot + part, hops - 1]),
                    )
                    if hops < reach(way, slot):
                        forward(way, slot, hops, part)
                    to_beside(way, slot, hops)
                    to_partner(way, slot, hops, part)

    def beside_came(slot):
        longer = (k == 1) & (side == 0)
        pl.when(longer)(functools.partial(came, gz.at[0:33], beside_recv.at[SPLIT.index(slot)]))
        pl.when(jnp.logical_not(longer))(functools.partial(came, gz.at[0:32], beside_recv.at[SPLIT.index(slot)]))
        for source in range(NY):
            start = SLOT * slot + 8 * (2 * source + k) + 4 * (1 - side)

            def go(units):
                piece = gz.at[pl.ds(start, units)]
                rcopy(piece, piece, core_send, shared_recv.at[SPLIT.index(slot)], core=1 - k).start()

            if source < NY - 1:
                go(4)
            else:
                pl.when(longer)(functools.partial(go, 5))
                pl.when(jnp.logical_not(longer))(functools.partial(go, 4))

    def partner_beside(slot):
        longer = (k == 0) & (side == 0)
        pl.when(longer)(functools.partial(came, gz.at[0:33], shared_recv.at[SPLIT.index(slot)]))
        pl.when(jnp.logical_not(longer))(functools.partial(came, gz.at[0:32], shared_recv.at[SPLIT.index(slot)]))

    def partner_near(slot):
        more = (k == 0) & (seat(slot, y) != NY // 2 - 1)
        each = 8
        if slot in SPLIT:
            more, each = more & (side == 1), 4
        pl.when(more)(functools.partial(came, gz.at[0 : 7 * each + 1], core_recv.at[slot, 0]))
        pl.when(jnp.logical_not(more))(functools.partial(came, gz.at[0 : 7 * each], core_recv.at[slot, 0]))

    def partner_across(slot):
        more = (k == 0) & (seat(slot, y) == NY // 2 - 1)
        each = 8
        if slot in SPLIT:
            more, each = more & (side == 1), 4
        pl.when(more)(functools.partial(came, gz.at[0 : each + 1], core_recv.at[slot, 1]))
        pl.when(jnp.logical_not(more))(functools.partial(came, gz.at[0:each], core_recv.at[slot, 1]))

    def partner_has(slot):
        partner_near(slot)
        partner_across(slot)

    def member(slot, index):
        if slot == 0:
            return index, 0
        turn = 3 * (slot - 1) + index
        return turn // 2, 1 + turn % 2

    started = {("g", 0)}

    def add_to(ref, key, term):
        ref[...] = ref[...] + term if key in started else term
        started.add(key)

    def side_by_side(slot, indices):
        blocks = [gz[pl.ds(SLOT * slot + UNITS * i, UNITS)].reshape(ROWS, SEQ) for i in indices]
        return jnp.concatenate(blocks, axis=1) if len(blocks) > 1 else blocks[0]

    def one_below_another(sequences):
        parts = [att[s] for s in sequences]
        return jnp.concatenate(parts, axis=0) if len(parts) > 1 else parts[0]

    def weight_term(slot, *indices):
        members = [member(slot, i) for i in indices]
        rows = members[0][0]
        term = jnp.dot(
            side_by_side(slot, indices),
            one_below_another([sequence for _, sequence in members]),
            preferred_element_type=F32,
        )
        add_to(dwacc.at[rows], ("w", rows), term)

    def multiply(slot, *indices):
        members = [member(slot, i) for i in indices]
        term = jnp.dot(wt[members[0][0]], side_by_side(slot, indices), preferred_element_type=F32)
        for i, (_, sequence) in enumerate(members):
            add_to(acct.at[sequence], ("g", sequence), term[:, SEQ * i : SEQ * (i + 1)])

    early = jnp.where(lax.rem(y + NY // 2, NY) <= 2, 2, 0)
    last_blocks = (early, jnp.where(early == 2, 0, 1), jnp.where(early == 2, 1, 2))

    def last_term(*turns):
        indices = [last_blocks[turn] for turn in turns]
        term = jnp.dot(
            side_by_side(SLOTS - 1, indices),
            one_below_another([lax.rem(i + 1, NZH) for i in indices]),
            preferred_element_type=F32,
        )
        add_to(dwacc.at[3], ("w", 3), term)

    def last_multiply(*turns):
        indices = [last_blocks[turn] for turn in turns]
        term = jnp.dot(wt[3], side_by_side(SLOTS - 1, indices), preferred_element_type=F32)
        for i, index in enumerate(indices):
            sequence = lax.rem(index + 1, NZH)
            acct[sequence] = acct[sequence] + term[:, SEQ * i : SEQ * (i + 1)]

    def send_term(rows):
        for start, size in ((0, 352), (352, ROWS - 352)):
            part = pl.ds(start, size)
            dw_stage[rows, part, :] = dwacc[rows, part, :].astype(BF16)
            rcopy(
                dw_stage.at[rows, part],
                dw_in.at[rows, part],
                dw_send,
                dw_recv,
                x=mod(x + AHEAD[rows], NX),
            ).start()

    def send_grad(sequence, i):
        o = other(sequence)
        ga_stage[sequence - 1, i] = acct[sequence, :, 128 * i : 128 * (i + 1)].astype(BF16)
        rcopy(
            ga_stage.at[sequence - 1, i],
            ga_in.at[sequence_of(zh, o) - 1, i],
            ga_send,
            ga_recv.at[i],
            zh=o,
        ).start()

    def send_grads(*sequences):
        for i in range(3):
            for sequence in sequences:
                send_grad(sequence, i)

    def old_moments():
        acct[0] = jnp.zeros((HD, SEQ), F32)
        for load in loads[5:]:
            load.wait()
        for c, start, size in row_chunks():
            rows = pl.ds(start, size)
            low_first = jnp.minimum(down(frow, start, size), fcol[...].reshape(1, HD))
            low_second = jnp.minimum(down(srow, start, size), scol[...].reshape(1, HD))
            fnew_out[rows, :] = beta_first * (fc[rows, :].astype(F32) * low_first)
            snew_out[rows, :] = beta_second * (sc[rows, :].astype(F32) * low_second)
            weight = w[rows, :]
            nw_out[rows, :] = weight - learning * (decay_rate * weight)

    send_weights()
    fill()
    relay(0)
    start_ring(0)
    attend()
    relay(1)
    relay(2)
    relay(3)
    pass_on(0, 1)
    start_ring(1)
    pass_on(0, 2)
    pass_on(1, 1)
    start_ring(2)
    send_att()
    pass_on(0, 3)
    pass_on(1, 2)
    pass_on(2, 1)
    start_ring(3)
    pass_on(0, 4)
    pass_on(1, 3)
    pass_on(2, 2)
    old_moments()
    pass_on(3, 1)
    pass_on(1, 4)
    beside_came(0)
    pass_on(2, 3)
    pass_on(3, 2)
    partner_has(1)
    came(att.at[1], att_recv.at[0])
    came(att.at[2], att_recv.at[1])
    weight_term(1, 0, 1)
    partner_has(0)
    partner_beside(0)
    weight_term(0, 0)
    send_term(0)
    pass_on(2, 4)
    weight_term(1, 2)
    weight_term(0, 2)
    pass_on(3, 3)
    weight_term(0, 1)
    partner_has(2)
    weight_term(2, 0)
    send_term(1)
    weight_term(2, 1, 2)
    send_term(2)
    came(wt.at[0:3], w_recv)
    multiply(1, 0, 1)
    multiply(1, 2)
    partner_near(3)
    pass_on(3, 4)
    multiply(2, 0)
    multiply(2, 1, 2)
    last_multiply(0)
    pl.when(early == 0)(functools.partial(send_grads, 1))
    last_term(0)
    partner_across(3)
    last_multiply(1)
    pl.when(early == 0)(functools.partial(send_grads, 2))
    pl.when(early == 2)(functools.partial(send_grads, 1))
    last_multiply(2)
    pl.when(early == 2)(functools.partial(send_grads, 2))
    last_term(1, 2)

    came(dw_in, dw_recv)
    for c, start, size in row_chunks():
        rows = pl.ds(start, size)
        grad = dwacc[3, rows, :]
        for i in range(NX - 1):
            grad = grad + dw_in[i, rows, :].astype(F32)
        first_new = fnew_out[rows, :] + (1.0 - beta_first) * grad
        second_new = snew_out[rows, :] + (1.0 - beta_second) * grad * grad
        step_size = (
            first_new * (1.0 / correct_first) / (jnp.sqrt(second_new * (1.0 / correct_second)) + adam_eps)
        )
        nw_out[rows, :] = nw_out[rows, :] - learning * step_size
        fnew_out[rows, :] = first_new
        snew_out[rows, :] = second_new

    first_abs, second_abs = jnp.abs(fnew_out[...]), jnp.abs(snew_out[...])
    st[0] = lane_rows(first_abs)
    st[1] = lane_rows(second_abs)
    for dy in range(1, NY):
        rcopy(st, y_in.at[NY - dy - 1], y_send, y_recv, y=mod(y + dy, NY)).start()
    cst[0, 0:1, :] = jnp.max(first_abs, axis=0, keepdims=True)
    cst[0, 1:2, :] = jnp.max(second_abs, axis=0, keepdims=True)
    for dx in range(1, NX):
        rcopy(cst.at[0], x_in.at[NX - dx - 1], x_send, x_recv, x=mod(x + dx, NX)).start()

    multiply(0, 0)
    multiply(0, 1)
    multiply(0, 2)

    def back_rows(i):
        rows, cols = pl.ds(128 * i, 128), pl.ds(0, 128 * (i + 1))
        came(ga_in.at[:, i], ga_recv.at[i])
        total = acct[0, :, rows]
        for s in range(2):
            total = total + ga_in[s, i].astype(F32)
        grad_half = total.astype(BF16).T
        grad_probs = lax.dot_general(grad_half, vv[cols, :], NT, preferred_element_type=F32)
        row_dot = jnp.sum(
            grad_half.astype(F32) * att[0, rows, :].astype(F32), axis=-1, keepdims=True
        )
        grad_scores = (prob[rows, cols] * (grad_probs - row_dot)).astype(BF16)
        gq_out[rows, :] = (
            jnp.dot(grad_scores, kk[cols, :], preferred_element_type=F32) * SCALE
        ).astype(BF16)

    def left(ref, send):
        rcopy(ref, ref, send, zh_recv, core=k).wait_send()

    wait_units(8 - sum(staying), 8, lambda c: left(gz.at[0:c], spread_send))
    for slot in range(SLOTS):
        copies = 1 if slot in SPLIT else 3
        wait_units(landing[slot], 9, lambda c: left(gz.at[0 : copies * c], relay_send.at[slot]))
    longer = count(
        (seat(slot, from_source(way, hops)) == NY - 1) & (k == 1) & ((side == 1) | (slot not in SPLIT))
        for slot in range(SLOTS)
        for way in (0, 1)
        for hops in range(reach(way, slot))
    )
    usual = 56 * SLOTS - 28 * len(SPLIT)
    for c in range(9):
        pl.when(longer == c)(functools.partial(left, gz.at[0 : usual + c], ring_send))
    more = (k == 1) & (side == 1)
    for flag, each in ((more, 33), (jnp.logical_not(more), 32)):
        pl.when(flag)(functools.partial(left, gz.at[0 : each * len(SPLIT)], beside_send))
    for c in (0, 1):
        pl.when(k == c)(functools.partial(left, gz.at[0 : 64 * SLOTS + SLOTS * c], core_send))
    for whole, send in (
        (att.at[0:2], att_send),
        (wt.at[0:3], w_send),
        (dw_in, dw_send),
    ):
        left(whole, send)

    came(x_in, x_recv)
    cst[1] = jnp.maximum(cst[0], jnp.max(x_in[...], axis=0))
    for sequence in (1, 2):
        o = other(sequence)
        rcopy(cst.at[1], zh_in.at[sequence_of(zh, o) - 1], zh_send, zh_recv, zh=o).start()
    came(y_in, y_recv)
    mine[...] = jnp.maximum(st[...], jnp.max(y_in[...], axis=0))
    for rel in range(1, NZL * NC):
        dl, dk = rel // NC, rel % NC
        back = NC * ((NZL - dl) % NZL) + dk - 1
        rcopy(
            mine, zl_in.at[back], zl_send, zl_recv, zl=mod(zl + dl, NZL), core=lax.rem(k + dk, NC)
        ).start()
    for i in range(3):
        back_rows(i)
    came(zl_in, zl_recv)
    rows_out[...] = jnp.maximum(mine[...], jnp.max(zl_in[...], axis=0))
    came(zh_in, zh_recv)
    cols_out[...] = jnp.maximum(cst[1], jnp.max(zh_in[...], axis=0))

    for whole, send in (
        (ga_in, ga_send),
        (y_in, y_send),
        (zl_in, zl_send),
        (x_in, x_send),
        (zh_in, zh_send),
    ):
        left(whole, send)


def codes(
    gq,
    nw,
    fnew,
    snew,
    rows,
    cols,
    gq_out,
    nw_out,
    nfc_out,
    nfr_out,
    nfcol_out,
    nsc_out,
    nsr_out,
    nscol_out,
    first_code,
    second_code,
    first_rows,
    second_rows,
    first_cols,
    second_cols,
    sem,
):
    copies = []

    def out(src, dst):
        copy = pltpu.make_async_copy(src, dst, sem.at[len(copies)])
        copy.start()
        copies.append(copy)

    out(gq, gq_out)
    out(nw, nw_out)
    for moment, (new, code, code_out, maxima, maxima_out, col, col_out) in enumerate(
        (
            (fnew, first_code, nfc_out, first_rows, nfr_out, first_cols, nfcol_out),
            (snew, second_code, nsc_out, second_rows, nsr_out, second_cols, nscol_out),
        )
    ):
        col[...] = cols[moment]
        for c, start, size in row_chunks():
            at = pl.ds(start, size)
            maxima[at] = rows[moment, c, 0:size]
            low = jnp.minimum(
                down_rows(rows[moment, c : c + 1, :])[:size], cols[moment : moment + 1]
            )
            code[at, :] = (new[at, :] / (low + code_eps)).astype(BF16)
        out(code, code_out)
        out(maxima, maxima_out)
        out(col, col_out)
    for copy in copies:
        copy.wait()


def per_device(queries, keys, values, grad_out, weight, fc, frow, fcol, sc, srow, scol):
    shape = jax.ShapeDtypeStruct
    vmem = pl.BlockSpec(memory_space=pltpu.VMEM)
    hbm = pl.BlockSpec(memory_space=pltpu.HBM)
    dma = pltpu.SemaphoreType.DMA
    gq, nw, fnew, snew, rows, cols = pl.pallas_call(
        body,
        name="whole",
        out_shape=(
            shape((SEQ, HD), BF16),
            shape((ROWS, HD), F32),
            shape((ROWS, HD), F32),
            shape((ROWS, HD), F32),
            shape((2, 8, HD), F32),
            shape((2, HD), F32),
        ),
        in_specs=[hbm] * 11,
        out_specs=[vmem] * 6,
        scratch_shapes=[
            pltpu.VMEM((SEQ, HD), BF16),
            pltpu.VMEM((SEQ, HD), BF16),
            pltpu.VMEM((SEQ, HD), BF16),
            pltpu.VMEM((SEQ, HD), BF16),
            pltpu.VMEM((ROWS, HD), F32),
            pltpu.VMEM((ROWS, HD), BF16),
            pltpu.VMEM((ROWS, HD), BF16),
            pltpu.VMEM((ROWS,), F32),
            pltpu.VMEM((HD,), F32),
            pltpu.VMEM((ROWS,), F32),
            pltpu.VMEM((HD,), F32),
            pltpu.VMEM((HD, SEQ), BF16),
            pltpu.VMEM((SLOTS * SLOT, UNIT, SEQ), BF16),
            pltpu.VMEM((NX, HD, ROWS), BF16),
            pltpu.VMEM((NZH, SEQ, HD), BF16),
            pltpu.VMEM((SEQ, SEQ), F32),
            pltpu.VMEM((NZH, HD, SEQ), F32),
            pltpu.VMEM((2, 3, HD, HD), BF16),
            pltpu.VMEM((2, 3, HD, HD), BF16),
            pltpu.VMEM((NX, ROWS, HD), F32),
            pltpu.VMEM((NX - 1, ROWS, HD), BF16),
            pltpu.VMEM((NX - 1, ROWS, HD), BF16),
            pltpu.VMEM((2, 8, HD), F32),
            pltpu.VMEM((NY - 1, 2, 8, HD), F32),
            pltpu.VMEM((NZL * NC - 1, 2, 8, HD), F32),
            pltpu.VMEM((2, 8, HD), F32),
            pltpu.VMEM((2, 2, HD), F32),
            pltpu.VMEM((NX - 1, 2, HD), F32),
            pltpu.VMEM((NZH - 1, 2, HD), F32),
            dma((11,)),
            dma,
            dma((SLOTS,)),
            dma((SLOTS,)),
            dma((SLOTS,)),
            dma,
            dma((2, SLOTS + 1, 4)),
            dma,
            dma((len(SPLIT),)),
            dma((len(SPLIT),)),
            dma,
            dma((SLOTS, 2)),
            dma,
            dma((2,)),
            dma,
            dma,
            dma,
            dma((3,)),
            dma,
            dma,
            dma,
            dma,
            dma,
            dma,
            dma,
            dma,
            dma,
            dma,
        ],
        compiler_params=pltpu.CompilerParams(
            collective_id=0, has_side_effects=True, vmem_limit_bytes=48 * 1024 * 1024
        ),
    )(
        *(
            pltpu.with_memory_space_constraint(a, pltpu.HBM)
            for a in (queries, keys, values, grad_out, weight, fc, frow, fcol, sc, srow, scol)
        )
    )
    return pl.pallas_call(
        codes,
        name="codes",
        out_shape=(
            shape((SEQ, HD), BF16),
            shape((ROWS, HD), F32),
            shape((ROWS, HD), BF16),
            shape((ROWS,), F32),
            shape((HD,), F32),
            shape((ROWS, HD), BF16),
            shape((ROWS,), F32),
            shape((HD,), F32),
        ),
        compiler_params=pltpu.CompilerParams(vmem_limit_bytes=8 * 1024 * 1024),
        in_specs=[vmem] * 6,
        out_specs=[hbm] * 8,
        scratch_shapes=[
            pltpu.VMEM((ROWS, HD), BF16),
            pltpu.VMEM((ROWS, HD), BF16),
            pltpu.VMEM((ROWS,), F32),
            pltpu.VMEM((ROWS,), F32),
            pltpu.VMEM((HD,), F32),
            pltpu.VMEM((HD,), F32),
            dma((8,)),
        ],
    )(gq, nw, fnew, snew, rows, cols)


def solution(mesh):
    finer = Mesh(mesh.devices.reshape(NX, NZH, NY, NZL, NC), AXES)
    placed = (
        P(DP, TENSOR),
        P(DP, None),
        P(DP, None),
        P(DP, TENSOR),
        P(DP, TENSOR),
        P(DP, TENSOR),
        P(DP),
        P(TENSOR),
        P(DP, TENSOR),
        P(DP),
        P(TENSOR),
    )
    return jax.shard_map(
        per_device,
        mesh=finer,
        in_specs=placed,
        out_specs=(
            P(DP, TENSOR),
            P(DP, TENSOR),
            P(DP, TENSOR),
            P(DP),
            P(TENSOR),
            P(DP, TENSOR),
            P(DP),
            P(TENSOR),
        ),
        check_vma=False,
    )
```
